128 devices in a mesh: fsdp: 8 (over z_hi, y), tp: 16 (over z_lo, x, core).
Axes of the slice: x: 4, y: 4, z: 4 (z_hi: 2, z_lo: 2; z = z_hi * 2 + z_lo), core: 2. Of those that a mesh axis runs over, the one named last changes fastest.
Arguments:
- tokens: bfloat16 [2048, 8192], P('fsdp', 'tp'), may hold values from -6 to 6
- out_grad: bfloat16 [2048, 8192], P('fsdp', 'tp'), may hold values from -6 to 6
- gate_weight: bfloat16 [8192, 2048], P('fsdp', 'tp'), may hold values from -0.0625 to 0.0625
- up_weight: bfloat16 [8192, 2048], P('fsdp', 'tp'), may hold values from -0.0625 to 0.0625
- down_weight: bfloat16 [2048, 8192], P('tp', 'fsdp'), may hold values from -0.125 to 0.125
Outputs:
- input_grad: bfloat16 [2048, 8192], P('fsdp', 'tp')
- gate_grad: float32 [8192, 2048], P('fsdp', 'tp')
- up_grad: float32 [8192, 2048], P('fsdp', 'tp')
- down_grad: float32 [2048, 8192], P('tp', 'fsdp')
The draws below stay inside these ranges and needn't reach their ends.
All inputs are finite; a program needn't handle non-finite values.
Results may differ from the reference program's by a relative error of at most 0.0023.
Values may be sent and summed in bfloat16 or wider, within the bound.
A program may use at most 128 MiB of HBM per device.

```python
import math
import jax
import jax.numpy as jnp

D = 8192
FF_WIN = 2048
TOKENS = 2048


def spiked(values, stream_key, source, target, blocks, factor):
    def block_of(dim):
        return (jnp.arange(values.shape[dim]) // (values.shape[dim] // blocks)).reshape((-1,) + (1,) * (values.ndim - 1 - dim))

    one_side = jax.random.permutation(stream_key, blocks)[block_of(target)]
    other_side = (block_of(target) + blocks // 2) % blocks
    return jnp.where((block_of(source) == one_side) | (block_of(source) == other_side), factor * values, values)


def level_of(key, dims, shards, low, largest):
    factor_of = 1.0
    for dim, shards_of in shards:
        heights = jax.random.uniform(jax.random.fold_in(jax.random.fold_in(key, 6), dim), (shards_of,), jnp.float32, low / len(shards), largest / len(shards))
        factor_of = factor_of * jnp.repeat(jnp.exp(heights), dims[dim] // shards_of).reshape((-1,) + (1,) * (len(dims) - 1 - dim))
    return factor_of


def gaussian(key, extent, deviation, bound, pieces=(), dtype=jnp.bfloat16):
    array = jax.random.normal(key, extent, jnp.float32) * deviation
    if len(pieces) > 0:
        array = level_of(key, extent, pieces, -0.22, 0.18) * array
    return jnp.clip(array, min=-bound, max=bound).astype(dtype)


def bell_draw_with(rng, shape, width, most, split, heavy, kind=jnp.bfloat16):
    result = width * jax.random.normal(rng, shape, jnp.float32)
    if split:
        result = result * level_of(rng, shape, split, -0.22, 0.18)
    return jnp.clip(spiked(result, jax.random.fold_in(rng, 3), *heavy), -most, most).astype(kind)


def setup_inputs(seed: int = 0) -> dict:
    seeds = jax.random.split(jax.random.key(seed), 6)
    return {
        "tokens": bell_draw_with(seeds[0], (TOKENS, D), 1.0, 6.0, ((0, 8), (1, 16)), (0, 1, 16, 2.0)),
        "out_grad": bell_draw_with(seeds[1], (TOKENS, D), 1.0, 6.0, ((0, 8), (1, 16)), (0, 1, 16, 2.0)),
        "gate_weight": gaussian(seeds[2], (D, FF_WIN), D ** -0.5, 0.0625, ((0, 8), (1, 16))),
        "up_weight": gaussian(seeds[3], (D, FF_WIN), D ** -0.5, 0.0625, ((0, 8), (1, 16))),
        "down_weight": gaussian(seeds[4], (FF_WIN, D), FF_WIN ** -0.5, 0.125, ((0, 16), (1, 8))),
    }


def reference(tokens, out_grad, gate_weight, up_weight, down_weight):
    gate = jnp.dot(tokens, gate_weight, preferred_element_type=jnp.float32)
    up = jnp.dot(tokens, up_weight, preferred_element_type=jnp.float32)
    squashed = jax.nn.sigmoid(gate)
    activated = gate * squashed
    slope = squashed * (1.0 + gate * (1.0 - squashed))
    hidden = (activated * up).astype(jnp.bfloat16)
    hidden_grad = jnp.dot(out_grad, down_weight.T, preferred_element_type=jnp.float32)
    gate_delta = (hidden_grad * up * slope).astype(jnp.bfloat16)
    up_delta = (hidden_grad * activated).astype(jnp.bfloat16)
    input_grad = jnp.dot(gate_delta, gate_weight.T, preferred_element_type=jnp.float32)
    input_grad = input_grad + jnp.dot(up_delta, up_weight.T, preferred_element_type=jnp.float32)
    factor = 1.0 / math.sqrt(TOKENS)
    gate_grad = jnp.dot(tokens.T, gate_delta, preferred_element_type=jnp.float32) * factor
    up_grad = jnp.dot(tokens.T, up_delta, preferred_element_type=jnp.float32) * factor
    down_grad = jnp.dot(hidden.T, out_grad, preferred_element_type=jnp.float32) * factor
    return (input_grad.astype(jnp.bfloat16), gate_grad, up_grad, down_grad)
```

```python
import functools
import math

import jax
import jax.numpy as jnp
from jax import lax
from jax.sharding import PartitionSpec as P
from jax.experimental import pallas as pl
from jax.experimental.pallas import tpu as pltpu

MESH = pl.DeviceIdType.MESH
F32 = jnp.float32
BF16 = jnp.bfloat16
VMEM_LIMIT = 60 * 1024 * 1024
ROWS = ((0,), (0,))
COLS = ((1,), (1,))


def kernel(
    factor,
    tokens,
    grads,
    gate_weight,
    up_weight,
    down_weight,
    result,
    gate_out,
    up_out,
    down_out,
    xg,
    wf,
    df,
    sa,
    zra,
    zla,
    sb,
    zrb,
    zlb,
    acts,
    hidden,
    dg,
    tw,
    dpart,
    gpart,
    dtwo,
    gtwo,
    done,
    gone,
    dmid,
    gmid,
    dland,
    gland,
    gown,
    total,
    rounded,
    z_send,
    z_recv,
    x_send,
    x_recv,
    p_send,
    p_recv,
    y_send,
    y_recv,
    a_send,
    a_recv,
    b_send,
    b_recv,
    t_send,
    t_recv,
    l_send,
    l_recv,
    dx_send,
    dx_recv,
    dp_send,
    dp_recv,
    two_send,
    two_recv,
    one_send,
    one_recv,
    r_send,
    r_recv,
):
    f, t = lax.axis_index("fsdp"), lax.axis_index("tp")
    h, y = lax.div(f, 4), lax.rem(f, 4)
    l, x, k = lax.div(t, 8), lax.rem(lax.div(t, 2), 4), lax.rem(t, 2)
    z = 2 * h + l
    outer = h == l
    inner = h != l
    rows, shard = tokens.shape
    deep, width = gate_weight.shape
    part = rows // 2
    wide = 2 * width

    def at(xx, yy, hh, ll, kk):
        return (hh * 4 + yy, ll * 8 + xx * 2 + kk)

    def at_z(zz):
        return at(x, y, lax.div(zz, 2), lax.rem(zz, 2), k)

    xs = (lax.rem(x + 3, 4), lax.rem(x + 1, 4), lax.rem(x + 2, 4))
    ys = (lax.rem(y + 3, 4), lax.rem(y + 1, 4), lax.rem(y + 2, 4))
    right, left = at(xs[1], y, h, l, k), at(xs[0], y, h, l, k)
    north, south = at(x, ys[1], h, l, k), at(x, ys[0], h, l, k)
    mate = at(x, y, h, l, 1 - k)
    flip = at(x, y, h, 1 - l, k)
    across = at(x, y, 1 - h, 1 - l, k)
    step = 1 - 2 * k
    ahead = at_z(lax.rem(z + step + 4, 4))

    def remote(src, dst, send, recv, device):
        return pltpu.make_async_remote_copy(
            src_ref=src,
            dst_ref=dst,
            send_sem=send,
            recv_sem=recv,
            device_id=device,
            device_id_type=MESH,
        )

    barrier = pltpu.get_barrier_semaphore()
    for j in range(1, 16):
        pl.semaphore_signal(
            barrier, inc=1, device_id=(f, lax.rem(t + j, 16)), device_id_type=MESH
        )
    for peer in (north, south, at(x, y, 1 - h, l, k), across):
        pl.semaphore_signal(barrier, inc=1, device_id=peer, device_id_type=MESH)
    pl.semaphore_wait(barrier, 19)

    ups = (gate_weight, up_weight, down_weight)

    def w_own(w, q):
        size = ups[w].shape[0] // 2
        return ups[w].at[pl.ds(q * size, size)]

    def w_spot(o, w, q):
        if w == 2:
            return df.at[o, pl.ds(q * (width // 2), width // 2)]
        return wf.at[o, w, pl.ds(q * (deep // 2), deep // 2)]

    def w_out(way, w, q):
        return remote(
            w_own(w, q),
            w_spot(y, w, q),
            y_send.at[way, w, q],
            y_recv.at[way, w, q],
            (north, south)[way],
        )

    def w_on(w, q):
        here = w_spot(ys[q], w, q)
        return remote(here, here, y_send.at[2, w, q], y_recv.at[2, w, q], (north, south)[q])

    def w_in(d, w, q):
        here = w_spot(ys[d], w, q)
        return remote(here, here, y_send.at[2, w, q], y_recv.at[d, w, q], north)

    def w_start(w):
        for way, q in ((0, 0), (1, 1), (0, 1), (1, 0)):
            w_out(way, w, q).start()

    def w_forward(w):
        for q in range(2):
            w_in(q, w, q).wait_recv()
            w_on(w, q).start()

    def w_rest(w):
        for q in range(2):
            w_in(1 - q, w, q).wait_recv()
            w_in(2, w, q).wait_recv()

    own = (tokens, grads)
    slot = (h, 1 - h)

    def x_own(m, q):
        return own[m].at[pl.ds(q * part, part)]

    def x_spot(p, o, j, m, q):
        return xg.at[p * 4 + o, m, slot[j], pl.ds(q * part, part)]

    def z_out(m, q, device, j):
        spot = xg.at[k * 4 + x, m, h, pl.ds(q * part, part)]
        return remote(x_own(m, q), spot, z_send.at[0, m, q], z_recv.at[j, m, q], device)

    def z_on(m, q):
        here = x_spot(k, x, 1, m, q)
        return remote(here, here, z_send.at[1, m, q], z_recv.at[1, m, q], flip)

    def z_in(j, m, q):
        here = x_spot(k, x, j, m, q)
        return remote(here, here, z_send.at[0, m, q], z_recv.at[j, m, q], flip)

    def x_out(way, src, j, m, q):
        return remote(
            src,
            x_spot(k, x, j, m, q),
            x_send.at[way, j, m, q],
            x_recv.at[way, j, m, q],
            (right, left)[way],
        )

    def x_on(j, m, q):
        here = x_spot(k, xs[q], j, m, q)
        return remote(
            here, here, x_send.at[2, j, m, q], x_recv.at[2, j, m, q], (right, left)[q]
        )

    def x_in(d, j, m, q):
        here = x_spot(k, xs[d], j, m, q)
        return remote(here, here, x_send.at[2, j, m, q], x_recv.at[d, j, m, q], right)

    places = (*xs, x)

    def p_out(d, src, j, m, q):
        return remote(
            src,
            x_spot(k, places[d], j, m, q),
            p_send.at[d, j, m, q],
            p_recv.at[d, j, m, q],
            mate,
        )

    def p_in(d, j, m, q):
        here = x_spot(1 - k, places[d], j, m, q)
        return remote(here, here, p_send.at[d, j, m, q], p_recv.at[d, j, m, q], mate)

    def spread(src, j, m, q):
        for way in (0, 1) if q == 0 else (1, 0):
            x_out(way, src, j, m, q).start()
        p_out(3, src, j, m, q).start()

    def passed(d, j, m, q):
        x_in(d, j, m, q).wait_recv()
        if d == q:
            x_on(j, m, q).start()
        p_out(d, x_spot(k, places[d], j, m, q), j, m, q).start()

    def z_forward(m, q):
        @pl.when(inner)
        def _():
            z_in(1, m, q).wait_recv()
            z_on(m, q).start()

    def z_spread(m, q, own_too):
        @pl.when(inner)
        def _():
            z_in(0, m, q).wait_recv()
            spread(x_spot(k, x, 0, m, q), 0, m, q)

        @pl.when(outer)
        def _():
            if own_too:
                spread(x_own(m, q), 0, m, q)
            z_in(1, m, q).wait_recv()

        spread(x_spot(k, x, 1, m, q), 1, m, q)

    @pl.when(outer)
    def _():
        for m in range(2):
            for q in range(2):
                z_out(m, q, flip, 0).start()
            if m == 0:
                for q in range(2):
                    spread(x_own(0, q), 0, 0, q)

    @pl.when(inner)
    def _():
        for m in range(2):
            for q in range(2):
                z_out(m, q, across, 1).start()

    w_start(0)
    w_start(1)

    @pl.when(outer)
    def _():
        for m in range(2):
            xg[k * 4 + x, m, h] = own[m][...]

    wf[y, 0] = gate_weight[...]
    wf[y, 1] = up_weight[...]
    df[y] = down_weight[...]

    for q in range(2):
        z_forward(0, q)
        z_spread(0, q, False)
    for j in range(2):
        passed(0, j, 0, 0)
        passed(1, j, 0, 0)
    z_forward(1, 0)
    w_forward(0)
    for j in range(2):
        passed(1, j, 0, 1)
        passed(0, j, 0, 1)
    z_forward(1, 1)
    w_forward(1)
    w_start(2)
    for q in range(2):
        z_spread(1, q, True)
    for q in range(2):
        for j in range(2):
            passed(2, j, 0, q)
    w_rest(0)
    w_rest(1)
    for d in (3, 0, 1, 2):
        for j in range(2):
            for q in range(2):
                p_in(d, j, 0, q).wait_recv()

    tall = 2 * rows

    def block(m, o):
        return jnp.concatenate(
            [xg[p * 4 + o, m].reshape(tall, shard) for p in range(2)], axis=1
        )

    sa[...] = jnp.zeros_like(sa)

    @pl.loop(0, 4)
    def _(o):
        weights = jnp.concatenate([wf[o, 0], wf[o, 1]], axis=1)
        sa[...] += jnp.dot(block(0, o), weights, preferred_element_type=F32)

    def swap(src, mid, dst, send, recv):
        def first(c):
            at_c = pl.ds(c * rows, rows)
            return remote(src.at[at_c], mid.at[at_c], send.at[0, c], recv.at[0, c], ahead)

        def second(c):
            at_c = pl.ds(c * rows, rows)
            return remote(mid.at[at_c], dst.at[at_c], send.at[1, c], recv.at[1, c], ahead)

        return first, second

    a_first, a_second = swap(sa, zra, zla, a_send, a_recv)
    b_first, b_second = swap(sb, zrb, zlb, b_send, b_recv)

    for j in range(2):
        passed(0, j, 1, 0)
        passed(1, j, 1, 0)
        if j == 0:
            for c in range(2):
                a_first(c).start()
    w_forward(2)
    for j in range(2):
        passed(1, j, 1, 1)
        passed(0, j, 1, 1)
        a_first(j).wait_recv()
        a_second(j).start()

    def t_spot(u):
        return pl.ds(lax.rem(u, 2) * shard + lax.div(u, 8) * wide, wide)

    def t_out(j):
        u = lax.rem(t + j, 16)
        return remote(
            wf.at[lax.rem(lax.div(u, 2), 4), :, t_spot(u)],
            tw.at[t],
            t_send.at[j],
            t_recv.at[j],
            (f, u),
        )

    def t_in(j):
        u = lax.rem(t + 16 - j, 16)
        return remote(tw.at[u], tw.at[u], t_send.at[j], t_recv.at[j], (f, u))

    @pl.loop(1, 16)
    def _(j):
        t_out(j).start()

    tw[t] = wf[x, :, t_spot(t)]

    for c in range(2):
        a_second(c).wait_recv()
    sums = sa[...] + zla[...]
    gate, up = sums[:, :width], sums[:, width:]
    squashed = jax.nn.sigmoid(gate)
    activated = gate * squashed
    slope = squashed * (1.0 + gate * (1.0 - squashed))
    acts[:, :width] = up * slope
    acts[:, width:] = activated
    hidden[...] = (activated * up).astype(BF16)

    for q in range(2):
        for j in range(2):
            passed(2, j, 1, q)
    w_rest(2)
    for d in (3, 0, 1, 2):
        for j in range(2):
            for q in range(2):
                p_in(d, j, 1, q).wait_recv()

    sb[...] = jnp.zeros_like(sb)

    @pl.loop(0, 4)
    def _(o):
        sb[...] += lax.dot_general(
            block(1, o), df[o], (COLS, ((), ())), preferred_element_type=F32
        )

    def down_part(o):
        return lax.dot_general(
            hidden[...], block(1, o), (ROWS, ((), ())), preferred_element_type=F32
        )

    def gate_part(o):
        return lax.dot_general(
            block(0, o), dg[t], (ROWS, ((), ())), preferred_element_type=F32
        )

    twos, mids, parts, ones, lands = (
        (dtwo, gtwo),
        (dmid, gmid),
        (dpart, gpart),
        (done, gone),
        (dland, gland),
    )

    def halves(i, q):
        size = twos[i].shape[0] // 2
        return pl.ds(q * size, size)

    def two_out(i, q):
        return remote(
            twos[i].at[halves(i, q)],
            mids[i].at[q],
            two_send.at[i, q],
            two_recv.at[i, q],
            (north, south)[q],
        )

    def one_out(i, way, q):
        return remote(
            ones[i].at[way, halves(i, q)],
            lands[i].at[way, halves(i, q)],
            one_send.at[i, way, q],
            one_recv.at[i, way, q],
            (north, south)[way],
        )

    def one_parts(i, fn):
        for way in range(2):
            q = way
            term = fn(ys[1 - way])
            size = term.shape[0] // 2
            parts[i][way] = term[q * size : (q + 1) * size]
            ones[i][way, halves(i, 1 - q)] = term[(1 - q) * size : (2 - q) * size].astype(BF16)

    def one_merge(i):
        for way in range(2):
            two_out(i, way).wait_recv()
            ones[i][way, halves(i, way)] = (
                parts[i][way] + mids[i][way].astype(F32)
            ).astype(BF16)

    def finals(i):
        for way in range(2):
            for q in range(2):
                one_out(i, way, q).wait_recv()
        return lands[i][0].astype(F32) + lands[i][1].astype(F32)

    dtwo[...] = down_part(ys[2]).astype(BF16)
    for c in range(2):
        b_first(c).start()
    one_parts(0, down_part)
    for q in range(2):
        two_out(0, q).start()
    for way in range(2):
        one_out(0, way, 1 - way).start()
    for c in range(2):
        b_first(c).wait_recv()
        b_second(c).start()
    down_out[...] = down_part(y)
    one_merge(0)

    for c in range(2):
        b_second(c).wait_recv()
    for way in range(2):
        one_out(0, way, way).start()

    hidden_grad = sb[...] + zlb[...]
    dg[t, :, :width] = (hidden_grad * acts[:, :width]).astype(BF16)
    dg[t, :, width:] = (hidden_grad * acts[:, width:]).astype(BF16)
    gtwo[...] = gate_part(ys[2]).astype(BF16)

    sides = (l, 1 - l)

    def d_spot(c, o, j, q):
        return dg.at[sides[j] * 8 + o * 2 + c, pl.ds(q * rows, rows)]

    def l_out(q):
        here = d_spot(k, x, 0, q)
        return remote(here, here, l_send.at[q], l_recv.at[q], flip)

    def l_in(q):
        here = d_spot(k, x, 1, q)
        return remote(here, here, l_send.at[q], l_recv.at[q], flip)

    def dx_out(way, j, q):
        here = d_spot(k, x, j, q)
        return remote(
            here, here, dx_send.at[way, j, q], dx_recv.at[way, j, q], (right, left)[way]
        )

    def dx_on(j, q):
        here = d_spot(k, xs[q], j, q)
        return remote(here, here, dx_send.at[2, j, q], dx_recv.at[2, j, q], (right, left)[q])

    def dx_in(d, j, q):
        here = d_spot(k, xs[d], j, q)
        return remote(here, here, dx_send.at[2, j, q], dx_recv.at[d, j, q], right)

    def dp_out(d, j, q):
        here = d_spot(k, places[d], j, q)
        return remote(here, here, dp_send.at[d, j, q], dp_recv.at[d, j, q], mate)

    def dp_in(d, j, q):
        here = d_spot(1 - k, places[d], j, q)
        return remote(here, here, dp_send.at[d, j, q], dp_recv.at[d, j, q], mate)

    def d_spread(j, q):
        for way in (0, 1) if q == 0 else (1, 0):
            dx_out(way, j, q).start()
        dp_out(3, j, q).start()

    def d_passed(d, j, q):
        dx_in(d, j, q).wait_recv()
        if d == q:
            dx_on(j, q).start()
        dp_out(d, j, q).start()

    for q in range(2):
        l_out(q).start()
        d_spread(0, q)
    one_parts(1, gate_part)
    for q in range(2):
        two_out(1, q).start()
    for way in range(2):
        one_out(1, way, 1 - way).start()
    gown[...] = gate_part(y)
    for q in range(2):
        l_in(q).wait_recv()
        d_spread(1, q)
    down_out[...] = factor * (down_out[...] + finals(0))
    one_merge(1)
    for q in range(2):
        d_passed(q, 0, q)
    for way in range(2):
        one_out(1, way, way).start()
    for q in range(2):
        d_passed(q, 1, q)
    for j in range(2):
        for q in range(2):
            d_passed(1 - q, j, q)

    @pl.loop(1, 16)
    def _(j):
        t_in(j).wait_recv()

    total[...] = jnp.zeros_like(total)

    def gather(o, j):
        base = sides[j] * 8 + o * 2
        left_side = jnp.concatenate([dg[base], dg[base + 1]], axis=1)
        right_side = jnp.concatenate(
            [tw[base, 0], tw[base, 1], tw[base + 1, 0], tw[base + 1, 1]], axis=1
        )
        total[...] += lax.dot_general(
            left_side, right_side, (COLS, ((), ())), preferred_element_type=F32
        )

    for d in (3, 0, 1, 2):
        for j in range(2):
            for q in range(2):
                if d == 2:
                    d_passed(2, j, q)
            for q in range(2):
                dp_in(d, j, q).wait_recv()
            gather(places[d], j)
    rounded[...] = total[...].astype(BF16)

    def r_out(s):
        return remote(
            rounded.at[pl.ds(s * rows, rows)],
            result.at[:, pl.ds(pl.multiple_of(l * wide, wide), wide)],
            r_send.at[s],
            r_recv.at[l],
            at(x, y, s, h, k),
        )

    def r_in(e):
        spot = result.at[:, pl.ds(e * wide, wide)]
        return remote(spot, spot, r_send.at[0], r_recv.at[e], flip)

    both = factor * (gown[...] + finals(1))
    for s in range(2):

        @pl.when((s == h) & outer)
        def _(s=s):
            result[:, s * wide : (s + 1) * wide] = rounded[s * rows : (s + 1) * rows, :]

        @pl.when(jnp.logical_not((s == h) & outer))
        def _(s=s):
            r_out(s).start()

    gate_out[...] = both[:, :width]
    up_out[...] = both[:, width:]

    for m in range(2):
        for q in range(2):
            z_in(0, m, q).wait_send()

            @pl.when(inner)
            def _(m=m, q=q):
                z_on(m, q).wait_send()

            for j in range(2):
                for way in range(2):
                    x_out(way, x_own(m, q), j, m, q).wait_send()
                x_on(j, m, q).wait_send()
                for d in range(4):
                    p_out(d, x_own(m, q), j, m, q).wait_send()
    for w in range(3):
        for q in range(2):
            for way in range(2):
                w_out(way, w, q).wait_send()
            w_on(w, q).wait_send()
    for c in range(2):
        for copy in (a_first(c), a_second(c), b_first(c), b_second(c), l_out(c)):
            copy.wait_send()
        for i in range(2):
            two_out(i, c).wait_send()
            for q in range(2):
                one_out(i, c, q).wait_send()
        for j in range(2):
            for way in range(2):
                dx_out(way, j, c).wait_send()
            dx_on(j, c).wait_send()
            for d in range(4):
                dp_out(d, j, c).wait_send()

    @pl.loop(1, 16)
    def _(j):
        t_out(j).wait_send()

    for s in range(2):

        @pl.when(jnp.logical_not((s == h) & outer))
        def _(s=s):
            r_out(s).wait_send()

        @pl.when(jnp.logical_not((s == l) & outer))
        def _(s=s):
            r_in(s).wait_recv()


VMEM = pl.BlockSpec(memory_space=pltpu.VMEM)
DMA = pltpu.SemaphoreType.DMA


def body(tokens, out_grad, gate_weight, up_weight, down_weight):
    nf, nt = lax.axis_size("fsdp"), lax.axis_size("tp")
    rows, shard = tokens.shape
    deep, width = gate_weight.shape
    assert nf == 8 and nt == 16 and deep == 2 * shard
    factor = 1.0 / math.sqrt(rows * nf)
    tall = 2 * rows
    wide = 2 * width

    return tuple(
        pl.pallas_call(
            functools.partial(kernel, factor),
            out_shape=(
                jax.ShapeDtypeStruct((rows, shard), BF16),
                jax.ShapeDtypeStruct((deep, width), F32),
                jax.ShapeDtypeStruct((deep, width), F32),
                jax.ShapeDtypeStruct((width, deep), F32),
            ),
            in_specs=[VMEM] * 5,
            out_specs=(VMEM,) * 4,
            scratch_shapes=[
                pltpu.VMEM((8, 2, 2, rows, shard), BF16),
                pltpu.VMEM((4, 2, deep, width), BF16),
                pltpu.VMEM((4, width, deep), BF16),
                pltpu.VMEM((tall, wide), F32),
                pltpu.VMEM((tall, wide), F32),
                pltpu.VMEM((tall, wide), F32),
                pltpu.VMEM((tall, width), F32),
                pltpu.VMEM((tall, width), F32),
                pltpu.VMEM((tall, width), F32),
                pltpu.VMEM((tall, wide), F32),
                pltpu.VMEM((tall, width), BF16),
                pltpu.VMEM((nt, tall, wide), BF16),
                pltpu.VMEM((nt, 2, wide, width), BF16),
                pltpu.VMEM((2, width // 2, deep), F32),
                pltpu.VMEM((2, deep // 2, wide), F32),
                pltpu.VMEM((width, deep), BF16),
                pltpu.VMEM((deep, wide), BF16),
                pltpu.VMEM((2, width, deep), BF16),
                pltpu.VMEM((2, deep, wide), BF16),
                pltpu.VMEM((2, width // 2, deep), BF16),
                pltpu.VMEM((2, deep // 2, wide), BF16),
                pltpu.VMEM((2, width, deep), BF16),
                pltpu.VMEM((2, deep, wide), BF16),
                pltpu.VMEM((deep, wide), F32),
                pltpu.VMEM((tall, wide), F32),
                pltpu.VMEM((tall, wide), BF16),
                DMA((2, 2, 2)),
                DMA((2, 2, 2)),
                DMA((3, 2, 2, 2)),
                DMA((3, 2, 2, 2)),
                DMA((4, 2, 2, 2)),
                DMA((4, 2, 2, 2)),
                DMA((3, 3, 2)),
                DMA((3, 3, 2)),
                DMA((2, 2)),
                DMA((2, 2)),
                DMA((2, 2)),
                DMA((2, 2)),
                DMA((16,)),
                DMA((16,)),
                DMA((2,)),
                DMA((2,)),
                DMA((3, 2, 2)),
                DMA((3, 2, 2)),
                DMA((4, 2, 2)),
                DMA((4, 2, 2)),
                DMA((2, 2)),
                DMA((2, 2)),
                DMA((2, 2, 2)),
                DMA((2, 2, 2)),
                DMA((2,)),
                DMA((2,)),
            ],
            compiler_params=pltpu.CompilerParams(
                collective_id=0, has_side_effects=True, vmem_limit_bytes=VMEM_LIMIT
            ),
            name="block",
        )(tokens, out_grad, gate_weight, up_weight, down_weight)
    )


def solution(mesh):
    return jax.shard_map(
        body,
        mesh=mesh,
        in_specs=(
            P("fsdp", "tp"),
            P("fsdp", "tp"),
            P("fsdp", "tp"),
            P("fsdp", "tp"),
            P("tp", "fsdp"),
        ),
        out_specs=(P("fsdp", "tp"), P("fsdp", "tp"), P("fsdp", "tp"), P("tp", "fsdp")),
        check_vma=False,
    )
```

```python
import functools
import math

import jax
import jax.numpy as jnp
from jax import lax
from jax.sharding import PartitionSpec as P
from jax.experimental import pallas as pl
from jax.experimental.pallas import tpu as pltpu

MESH = pl.DeviceIdType.MESH
F32 = jnp.float32
BF16 = jnp.bfloat16
VMEM_LIMIT = 60 * 1024 * 1024
ROWS = ((0,), (0,))
COLS = ((1,), (1,))


def kernel(
    factor,
    tokens,
    grads,
    gate_weight,
    up_weight,
    down_weight,
    result,
    gate_out,
    up_out,
    down_out,
    xg,
    wf,
    df,
    sa,
    zla,
    sb,
    zlb,
    acts,
    hidden,
    dg,
    tw,
    dpart,
    gpart,
    dtwo,
    gtwo,
    done,
    gone,
    dmid,
    gmid,
    dland,
    gland,
    gown,
    total,
    near,
    rounded,
    z_send,
    z_recv,
    x_send,
    x_recv,
    p_send,
    p_recv,
    y_send,
    y_recv,
    a_send,
    a_recv,
    b_send,
    b_recv,
    t_send,
    t_recv,
    f_send,
    f_recv,
    dx_send,
    dx_recv,
    dp_send,
    dp_recv,
    two_send,
    two_recv,
    one_send,
    one_recv,
    r_send,
    r_recv,
):
    f, t = lax.axis_index("fsdp"), lax.axis_index("tp")
    h, y = lax.div(f, 4), lax.rem(f, 4)
    l, x, k = lax.div(t, 8), lax.rem(lax.div(t, 2), 4), lax.rem(t, 2)
    outer = h == l
    inner = h != l
    rows, shard = tokens.shape
    deep, width = gate_weight.shape
    part = rows // 2
    wide = 2 * width

    def at(xx, yy, hh, ll, kk):
        return (hh * 4 + yy, ll * 8 + xx * 2 + kk)

    xs = (lax.rem(x + 3, 4), lax.rem(x + 1, 4), lax.rem(x + 2, 4))
    ys = (lax.rem(y + 3, 4), lax.rem(y + 1, 4), lax.rem(y + 2, 4))
    right, left = at(xs[1], y, h, l, k), at(xs[0], y, h, l, k)
    north, south = at(x, ys[1], h, l, k), at(x, ys[0], h, l, k)
    mate = at(x, y, h, l, 1 - k)
    flip = at(x, y, h, 1 - l, k)
    across = at(x, y, 1 - h, 1 - l, k)
    opposite = at(x, y, 1 - h, l, k)
    me = 2 * x + k

    def remote(src, dst, send, recv, device):
        return pltpu.make_async_remote_copy(
            src_ref=src,
            dst_ref=dst,
            send_sem=send,
            recv_sem=recv,
            device_id=device,
            device_id_type=MESH,
        )

    barrier = pltpu.get_barrier_semaphore()
    for j in range(1, 16):
        pl.semaphore_signal(
            barrier, inc=1, device_id=(f, lax.rem(t + j, 16)), device_id_type=MESH
        )
    for peer in (north, south, opposite, across):
        pl.semaphore_signal(barrier, inc=1, device_id=peer, device_id_type=MESH)
    pl.semaphore_wait(barrier, 19)

    ups = (gate_weight, up_weight, down_weight)

    def w_own(w, q):
        size = ups[w].shape[0] // 2
        return ups[w].at[pl.ds(q * size, size)]

    def w_spot(o, w, q):
        if w == 2:
            return df.at[o, pl.ds(q * (width // 2), width // 2)]
        return wf.at[o, w, pl.ds(q * (deep // 2), deep // 2)]

    def w_out(way, w, q):
        return remote(
            w_own(w, q),
            w_spot(y, w, q),
            y_send.at[way, w, q],
            y_recv.at[way, w, q],
            (north, south)[way],
        )

    def w_on(w, q):
        here = w_spot(ys[q], w, q)
        return remote(here, here, y_send.at[2, w, q], y_recv.at[2, w, q], (north, south)[q])

    def w_in(d, w, q):
        here = w_spot(ys[d], w, q)
        return remote(here, here, y_send.at[2, w, q], y_recv.at[d, w, q], north)

    def w_start(w):
        for way, q in ((0, 0), (1, 1), (0, 1), (1, 0)):
            w_out(way, w, q).start()

    def w_forward(w):
        for q in range(2):
            w_in(q, w, q).wait_recv()
            w_on(w, q).start()

    def w_rest(w):
        for q in range(2):
            w_in(1 - q, w, q).wait_recv()
            w_in(2, w, q).wait_recv()

    own = (tokens, grads)
    slot = (h, 1 - h)

    def x_own(m, q):
        return own[m].at[pl.ds(q * part, part)]

    def x_spot(p, o, j, m, q):
        return xg.at[p * 4 + o, m, slot[j], pl.ds(q * part, part)]

    def z_out(m, q, device, j):
        spot = xg.at[k * 4 + x, m, h, pl.ds(q * part, part)]
        return remote(x_own(m, q), spot, z_send.at[0, m, q], z_recv.at[j, m, q], device)

    def z_on(m, q):
        here = x_spot(k, x, 1, m, q)
        return remote(here, here, z_send.at[1, m, q], z_recv.at[1, m, q], flip)

    def z_in(j, m, q):
        here = x_spot(k, x, j, m, q)
        return remote(here, here, z_send.at[0, m, q], z_recv.at[j, m, q], flip)

    def x_out(way, src, j, m, q):
        return remote(
            src,
            x_spot(k, x, j, m, q),
            x_send.at[way, j, m, q],
            x_recv.at[way, j, m, q],
            (right, left)[way],
        )

    def x_on(j, m, q):
        here = x_spot(k, xs[q], j, m, q)
        return remote(
            here, here, x_send.at[2, j, m, q], x_recv.at[2, j, m, q], (right, left)[q]
        )

    def x_in(d, j, m, q):
        here = x_spot(k, xs[d], j, m, q)
        return remote(here, here, x_send.at[2, j, m, q], x_recv.at[d, j, m, q], right)

    places = (*xs, x)

    def p_out(d, src, j, m, q):
        return remote(
            src,
            x_spot(k, places[d], j, m, q),
            p_send.at[d, j, m, q],
            p_recv.at[d, j, m, q],
            mate,
        )

    def p_in(d, j, m, q):
        here = x_spot(1 - k, places[d], j, m, q)
        return remote(here, here, p_send.at[d, j, m, q], p_recv.at[d, j, m, q], mate)

    def spread(src, j, m, q):
        for way in (0, 1) if q == 0 else (1, 0):
            x_out(way, src, j, m, q).start()
        p_out(3, src, j, m, q).start()

    def passed(d, j, m, q):
        x_in(d, j, m, q).wait_recv()
        if d == q:
            x_on(j, m, q).start()
        p_out(d, x_spot(k, places[d], j, m, q), j, m, q).start()

    def z_forward(m, q):
        @pl.when(inner)
        def _():
            z_in(1, m, q).wait_recv()
            z_on(m, q).start()

    def z_spread(m, q, own_too):
        @pl.when(inner)
        def _():
            z_in(0, m, q).wait_recv()
            spread(x_spot(k, x, 0, m, q), 0, m, q)

        @pl.when(outer)
        def _():
            if own_too:
                spread(x_own(m, q), 0, m, q)
            z_in(1, m, q).wait_recv()

        spread(x_spot(k, x, 1, m, q), 1, m, q)

    @pl.when(outer)
    def _():
        for m in range(2):
            for q in range(2):
                z_out(m, q, flip, 0).start()
            if m == 0:
                for q in range(2):
                    spread(x_own(0, q), 0, 0, q)

    @pl.when(inner)
    def _():
        for m in range(2):
            for q in range(2):
                z_out(m, q, across, 1).start()

    w_start(0)
    w_start(1)

    @pl.when(outer)
    def _():
        for m in range(2):
            xg[k * 4 + x, m, h] = own[m][...]

    wf[y, 0] = gate_weight[...]
    wf[y, 1] = up_weight[...]
    df[y] = down_weight[...]

    for q in range(2):
        z_forward(0, q)
        z_spread(0, q, False)
    for j in range(2):
        passed(0, j, 0, 0)
        passed(1, j, 0, 0)
    z_forward(1, 0)
    w_forward(0)
    for j in range(2):
        passed(1, j, 0, 1)
        passed(0, j, 0, 1)
    z_forward(1, 1)
    w_forward(1)
    w_start(2)
    for q in range(2):
        z_spread(1, q, True)
    tall = 2 * rows

    def block(m, o):
        return jnp.concatenate(
            [xg[p * 4 + o, m].reshape(tall, shard) for p in range(2)], axis=1
        )

    def pair_in(d, m):
        for q in range(2):
            for j in range(2):
                p_in(d, j, m, q).wait_recv()

    def gate_up(d):
        o = places[d]
        weights = jnp.concatenate([wf[o, 0], wf[o, 1]], axis=1)
        term = jnp.dot(block(0, o), weights, preferred_element_type=F32)
        sa[...] = term if d == 3 else sa[...] + term

    w_rest(0)
    w_rest(1)
    for d in (3, 0, 1):
        pair_in(d, 0)
        gate_up(d)
    for q in range(2):
        for j in range(2):
            passed(2, j, 0, q)
    pair_in(2, 0)
    gate_up(2)
    def swap(src, dst, send, recv):
        def copy(c):
            at_c = pl.ds(c * rows, rows)
            return remote(src.at[at_c], dst.at[at_c], send.at[c], recv.at[c], opposite)

        return copy

    a_swap = swap(sa, zla, a_send, a_recv)
    b_swap = swap(sb, zlb, b_send, b_recv)

    for j in range(2):
        passed(0, j, 1, 0)
        passed(1, j, 1, 0)
        if j == 0:
            for c in range(2):
                a_swap(c).start()
    w_forward(2)
    for j in range(2):
        passed(1, j, 1, 1)
        passed(0, j, 1, 1)

    def t_rows(u):
        return pl.ds(lax.rem(u, 2) * shard, shard)

    def t_out(j):
        u = lax.rem(me + j, 8)
        return remote(
            wf.at[lax.div(u, 2), :, t_rows(u)],
            tw.at[me],
            t_send.at[j],
            t_recv.at[j],
            (f, l * 8 + u),
        )

    def t_in(j):
        u = lax.rem(me + 8 - j, 8)
        return remote(tw.at[u], tw.at[u], t_send.at[j], t_recv.at[j], (f, l * 8 + u))

    @pl.loop(1, 8)
    def _(j):
        t_out(j).start()

    tw[me] = wf[x, :, t_rows(me)]

    for c in range(2):
        a_swap(c).wait_recv()
    sums = sa[...] + zla[...]
    gate, up = sums[:, :width], sums[:, width:]
    squashed = jax.nn.sigmoid(gate)
    activated = gate * squashed
    slope = squashed * (1.0 + gate * (1.0 - squashed))
    acts[:, :width] = up * slope
    acts[:, width:] = activated
    hidden[...] = (activated * up).astype(BF16)

    def grad_in(d):
        o = places[d]
        term = lax.dot_general(
            block(1, o), df[o], (COLS, ((), ())), preferred_element_type=F32
        )
        sb[...] = term if d == 3 else sb[...] + term

    w_rest(2)
    for d in (3, 0, 1):
        pair_in(d, 1)
        grad_in(d)
    for q in range(2):
        for j in range(2):
            passed(2, j, 1, q)
    pair_in(2, 1)
    grad_in(2)
    def down_part(o):
        return lax.dot_general(
            hidden[...], block(1, o), (ROWS, ((), ())), preferred_element_type=F32
        )

    def gate_part(o):
        return lax.dot_general(
            block(0, o), dg[me], (ROWS, ((), ())), preferred_element_type=F32
        )

    twos, mids, parts, ones, lands = (
        (dtwo, gtwo),
        (dmid, gmid),
        (dpart, gpart),
        (done, gone),
        (dland, gland),
    )

    def halves(i, q):
        size = twos[i].shape[0] // 2
        return pl.ds(q * size, size)

    def two_out(i, q):
        return remote(
            twos[i].at[halves(i, q)],
            mids[i].at[q],
            two_send.at[i, q],
            two_recv.at[i, q],
            (north, south)[q],
        )

    def one_out(i, way, q):
        return remote(
            ones[i].at[way, halves(i, q)],
            lands[i].at[way, halves(i, q)],
            one_send.at[i, way, q],
            one_recv.at[i, way, q],
            (north, south)[way],
        )

    def one_parts(i, fn):
        for way in range(2):
            q = way
            term = fn(ys[1 - way])
            size = term.shape[0] // 2
            parts[i][way] = term[q * size : (q + 1) * size]
            ones[i][way, halves(i, 1 - q)] = term[(1 - q) * size : (2 - q) * size].astype(BF16)

    def one_merge(i):
        for way in range(2):
            two_out(i, way).wait_recv()
            ones[i][way, halves(i, way)] = (
                parts[i][way] + mids[i][way].astype(F32)
            ).astype(BF16)

    def finals(i):
        for way in range(2):
            for q in range(2):
                one_out(i, way, q).wait_recv()
        return lands[i][0].astype(F32) + lands[i][1].astype(F32)

    dtwo[...] = down_part(ys[2]).astype(BF16)
    for c in range(2):
        b_swap(c).start()
    one_parts(0, down_part)
    for q in range(2):
        two_out(0, q).start()
    for way in range(2):
        one_out(0, way, 1 - way).start()
    down_out[...] = down_part(y)
    one_merge(0)

    for c in range(2):
        b_swap(c).wait_recv()
    for way in range(2):
        one_out(0, way, way).start()

    hidden_grad = sb[...] + zlb[...]
    dg[me, :, :width] = (hidden_grad * acts[:, :width]).astype(BF16)
    dg[me, :, width:] = (hidden_grad * acts[:, width:]).astype(BF16)
    gtwo[...] = gate_part(ys[2]).astype(BF16)

    def d_spot(c, o, q):
        return dg.at[o * 2 + c, pl.ds(q * rows, rows)]

    def dx_out(way, q):
        here = d_spot(k, x, q)
        return remote(here, here, dx_send.at[way, q], dx_recv.at[way, q], (right, left)[way])

    def dx_on(q):
        here = d_spot(k, xs[q], q)
        return remote(here, here, dx_send.at[2, q], dx_recv.at[2, q], (right, left)[q])

    def dx_in(d, q):
        here = d_spot(k, xs[d], q)
        return remote(here, here, dx_send.at[2, q], dx_recv.at[d, q], right)

    def dp_out(d, q):
        here = d_spot(k, places[d], q)
        return remote(here, here, dp_send.at[d, q], dp_recv.at[d, q], mate)

    def dp_in(d, q):
        here = d_spot(1 - k, places[d], q)
        return remote(here, here, dp_send.at[d, q], dp_recv.at[d, q], mate)

    def d_passed(d, q):
        dx_in(d, q).wait_recv()
        if d == q:
            dx_on(q).start()
        dp_out(d, q).start()

    for q in range(2):
        for way in (0, 1) if q == 0 else (1, 0):
            dx_out(way, q).start()
    for q in range(2):
        dp_out(3, q).start()
    one_parts(1, gate_part)
    for q in range(2):
        two_out(1, q).start()
    for way in range(2):
        one_out(1, way, 1 - way).start()
    gown[...] = gate_part(y)
    for q in range(2):
        d_passed(q, q)
    for q in range(2):
        d_passed(1 - q, q)
    down_out[...] = factor * (down_out[...] + finals(0))
    one_merge(1)
    for way in range(2):
        one_out(1, way, way).start()
    @pl.loop(1, 8)
    def _(j):
        t_in(j).wait_recv()

    def gather(d, at_s):
        base = places[d] * 2
        left_side = jnp.concatenate([dg[base, at_s], dg[base + 1, at_s]], axis=1)
        right_side = jnp.concatenate(
            [tw[base, 0], tw[base, 1], tw[base + 1, 0], tw[base + 1, 1]], axis=1
        )
        term = lax.dot_general(
            left_side, right_side, (COLS, ((), ())), preferred_element_type=F32
        )
        total[at_s] = term if d == 3 else total[at_s] + term

    for d in (3, 0, 1):
        for q in range(2):
            dp_in(d, q).wait_recv()
        gather(d, pl.ds(0, tall))
    for q in range(2):
        d_passed(2, q)
    for q in range(2):
        dp_in(2, q).wait_recv()
    mine, other = pl.ds(l * rows, rows), pl.ds((1 - l) * rows, rows)
    gather(2, other)
    gather(2, mine)

    def f_out(c):
        return remote(
            total.at[pl.ds((1 - l) * rows + c * part, part)],
            near.at[pl.ds(c * part, part)],
            f_send.at[c],
            f_recv.at[c],
            flip,
        )

    for c in range(2):
        f_out(c).start()
    both = factor * (gown[...] + finals(1))
    gate_out[...] = both[:, :width]
    up_out[...] = both[:, width:]

    def r_out(c):
        at_c = pl.ds(c * part, part)
        return remote(rounded.at[at_c], result.at[at_c], r_send.at[c], r_recv.at[c], across)

    for c in range(2):
        f_out(c).wait_recv()
        rounded[c * part : (c + 1) * part] = (
            total[pl.ds(l * rows + c * part, part)] + near[c * part : (c + 1) * part]
        ).astype(BF16)
    @pl.when(inner)
    def _():
        for c in range(2):
            r_out(c).start()

    @pl.when(outer)
    def _():
        result[...] = rounded[...]

    for m in range(2):
        for q in range(2):
            z_in(0, m, q).wait_send()

            @pl.when(inner)
            def _(m=m, q=q):
                z_on(m, q).wait_send()

            for j in range(2):
                for way in range(2):
                    x_out(way, x_own(m, q), j, m, q).wait_send()
                x_on(j, m, q).wait_send()
                for d in range(4):
                    p_out(d, x_own(m, q), j, m, q).wait_send()
    for w in range(3):
        for q in range(2):
            for way in range(2):
                w_out(way, w, q).wait_send()
            w_on(w, q).wait_send()
    for c in range(2):
        for copy in (a_swap(c), b_swap(c), f_out(c)):
            copy.wait_send()
        for i in range(2):
            two_out(i, c).wait_send()
            for q in range(2):
                one_out(i, c, q).wait_send()
        for way in range(2):
            dx_out(way, c).wait_send()
        dx_on(c).wait_send()
        for d in range(4):
            dp_out(d, c).wait_send()

    @pl.loop(1, 8)
    def _(j):
        t_out(j).wait_send()

    @pl.when(inner)
    def _():
        for c in range(2):
            r_out(c).wait()


VMEM = pl.BlockSpec(memory_space=pltpu.VMEM)
DMA = pltpu.SemaphoreType.DMA


def body(tokens, out_grad, gate_weight, up_weight, down_weight):
    nf, nt = lax.axis_size("fsdp"), lax.axis_size("tp")
    rows, shard = tokens.shape
    deep, width = gate_weight.shape
    assert nf == 8 and nt == 16 and deep == 2 * shard
    factor = 1.0 / math.sqrt(rows * nf)
    tall = 2 * rows
    wide = 2 * width

    return tuple(
        pl.pallas_call(
            functools.partial(kernel, factor),
            out_shape=(
                jax.ShapeDtypeStruct((rows, shard), BF16),
                jax.ShapeDtypeStruct((deep, width), F32),
                jax.ShapeDtypeStruct((deep, width), F32),
                jax.ShapeDtypeStruct((width, deep), F32),
            ),
            in_specs=[VMEM] * 5,
            out_specs=(VMEM,) * 4,
            scratch_shapes=[
                pltpu.VMEM((8, 2, 2, rows, shard), BF16),
                pltpu.VMEM((4, 2, deep, width), BF16),
                pltpu.VMEM((4, width, deep), BF16),
                pltpu.VMEM((tall, wide), F32),
                pltpu.VMEM((tall, wide), F32),
                pltpu.VMEM((tall, width), F32),
                pltpu.VMEM((tall, width), F32),
                pltpu.VMEM((tall, wide), F32),
                pltpu.VMEM((tall, width), BF16),
                pltpu.VMEM((8, tall, wide), BF16),
                pltpu.VMEM((8, 2, shard, width), BF16),
                pltpu.VMEM((2, width // 2, deep), F32),
                pltpu.VMEM((2, deep // 2, wide), F32),
                pltpu.VMEM((width, deep), BF16),
                pltpu.VMEM((deep, wide), BF16),
                pltpu.VMEM((2, width, deep), BF16),
                pltpu.VMEM((2, deep, wide), BF16),
                pltpu.VMEM((2, width // 2, deep), BF16),
                pltpu.VMEM((2, deep // 2, wide), BF16),
                pltpu.VMEM((2, width, deep), BF16),
                pltpu.VMEM((2, deep, wide), BF16),
                pltpu.VMEM((deep, wide), F32),
                pltpu.VMEM((tall, shard), F32),
                pltpu.VMEM((rows, shard), F32),
                pltpu.VMEM((rows, shard), BF16),
                DMA((2, 2, 2)),
                DMA((2, 2, 2)),
                DMA((3, 2, 2, 2)),
                DMA((3, 2, 2, 2)),
                DMA((4, 2, 2, 2)),
                DMA((4, 2, 2, 2)),
                DMA((3, 3, 2)),
                DMA((3, 3, 2)),
                DMA((2,)),
                DMA((2,)),
                DMA((2,)),
                DMA((2,)),
                DMA((8,)),
                DMA((8,)),
                DMA((2,)),
                DMA((2,)),
                DMA((3, 2)),
                DMA((3, 2)),
                DMA((4, 2)),
                DMA((4, 2)),
                DMA((2, 2)),
                DMA((2, 2)),
                DMA((2, 2, 2)),
                DMA((2, 2, 2)),
                DMA((2,)),
                DMA((2,)),
            ],
            compiler_params=pltpu.CompilerParams(
                collective_id=0, has_side_effects=True, vmem_limit_bytes=VMEM_LIMIT
            ),
            name="block",
        )(tokens, out_grad, gate_weight, up_weight, down_weight)
    )


def solution(mesh):
    return jax.shard_map(
        body,
        mesh=mesh,
        in_specs=(
            P("fsdp", "tp"),
            P("fsdp", "tp"),
            P("fsdp", "tp"),
            P("fsdp", "tp"),
            P("tp", "fsdp"),
        ),
        out_specs=(P("fsdp", "tp"), P("fsdp", "tp"), P("fsdp", "tp"), P("tp", "fsdp")),
        check_vma=False,
    )
```

```python
import functools
import math

import jax
import jax.numpy as jnp
from jax import lax
from jax.sharding import PartitionSpec as P
from jax.experimental import pallas as pl
from jax.experimental.pallas import tpu as pltpu

MESH = pl.DeviceIdType.MESH
F32 = jnp.float32
BF16 = jnp.bfloat16
VMEM_LIMIT = 40 * 1024 * 1024
ROWS = ((0,), (0,))
COLS = ((1,), (1,))


def kernel(
    factor,
    tokens,
    grads,
    gate_weight,
    up_weight,
    down_weight,
    result,
    gate_out,
    up_out,
    down_out,
    xg,
    wf,
    df,
    sa,
    zla,
    sb,
    zlb,
    acts,
    hidden,
    dg,
    tw,
    dpart,
    gpart,
    dtwo,
    gtwo,
    done,
    gone,
    dmid,
    gmid,
    dland,
    gland,
    gown,
    total,
    near,
    rounded,
    z_send,
    z_recv,
    x_send,
    x_recv,
    p_send,
    p_recv,
    y_send,
    y_recv,
    a_send,
    a_recv,
    b_send,
    b_recv,
    t_send,
    t_recv,
    u_send,
    u_recv,
    f_send,
    f_recv,
    dx_send,
    dx_recv,
    dp_send,
    dp_recv,
    two_send,
    two_recv,
    one_send,
    one_recv,
    r_send,
    r_recv,
):
    f, t = lax.axis_index("fsdp"), lax.axis_index("tp")
    h, y = lax.div(f, 4), lax.rem(f, 4)
    l, x, k = lax.div(t, 8), lax.rem(lax.div(t, 2), 4), lax.rem(t, 2)
    outer = h == l
    inner = h != l
    rows, shard = tokens.shape
    deep, width = gate_weight.shape
    part = rows // 2
    wide = 2 * width

    def at(xx, yy, hh, ll, kk):
        return (hh * 4 + yy, ll * 8 + xx * 2 + kk)

    xs = (lax.rem(x + 3, 4), lax.rem(x + 1, 4), lax.rem(x + 2, 4))
    ys = (lax.rem(y + 3, 4), lax.rem(y + 1, 4), lax.rem(y + 2, 4))
    right, left = at(xs[1], y, h, l, k), at(xs[0], y, h, l, k)
    north, south = at(x, ys[1], h, l, k), at(x, ys[0], h, l, k)
    mate = at(x, y, h, l, 1 - k)
    flip = at(x, y, h, 1 - l, k)
    across = at(x, y, 1 - h, 1 - l, k)
    opposite = at(x, y, 1 - h, l, k)
    me = 2 * x + k

    def remote(src, dst, send, recv, device):
        return pltpu.make_async_remote_copy(
            src_ref=src,
            dst_ref=dst,
            send_sem=send,
            recv_sem=recv,
            device_id=device,
            device_id_type=MESH,
        )

    barrier = pltpu.get_barrier_semaphore()
    for j in range(1, 16):
        pl.semaphore_signal(
            barrier, inc=1, device_id=(f, lax.rem(t + j, 16)), device_id_type=MESH
        )
    for peer in (north, south, opposite, across):
        pl.semaphore_signal(barrier, inc=1, device_id=peer, device_id_type=MESH)
    pl.semaphore_wait(barrier, 19)

    ups = (gate_weight, up_weight, down_weight)

    def w_own(w, q):
        size = ups[w].shape[0] // 2
        return ups[w].at[pl.ds(q * size, size)]

    def w_spot(o, w, q):
        if w == 2:
            return df.at[o, pl.ds(q * (width // 2), width // 2)]
        return wf.at[o, w, pl.ds(q * (deep // 2), deep // 2)]

    def w_out(way, w, q):
        return remote(
            w_own(w, q),
            w_spot(y, w, q),
            y_send.at[way, w, q],
            y_recv.at[way, w, q],
            (north, south)[way],
        )

    def w_on(w, q):
        here = w_spot(ys[q], w, q)
        return remote(here, here, y_send.at[2, w, q], y_recv.at[2, w, q], (north, south)[q])

    def w_in(d, w, q):
        here = w_spot(ys[d], w, q)
        return remote(here, here, y_send.at[2, w, q], y_recv.at[d, w, q], north)

    def w_start(w):
        for way, q in ((0, 0), (1, 1), (0, 1), (1, 0)):
            w_out(way, w, q).start()

    def w_forward(w):
        for q in range(2):
            w_in(q, w, q).wait_recv()
            w_on(w, q).start()

    def w_rest(w):
        for q in range(2):
            w_in(1 - q, w, q).wait_recv()
            w_in(2, w, q).wait_recv()

    own = (tokens, grads)
    slot = (h, 1 - h)

    def x_own(m, q):
        return own[m].at[pl.ds(q * part, part)]

    def x_spot(p, o, j, m, q):
        return xg.at[p * 4 + o, m, slot[j], pl.ds(q * part, part)]

    def z_out(m, q, device, j):
        spot = xg.at[k * 4 + x, m, h, pl.ds(q * part, part)]
        return remote(x_own(m, q), spot, z_send.at[0, m, q], z_recv.at[j, m, q], device)

    def z_on(m, q):
        here = x_spot(k, x, 1, m, q)
        return remote(here, here, z_send.at[1, m, q], z_recv.at[1, m, q], flip)

    def z_in(j, m, q):
        here = x_spot(k, x, j, m, q)
        return remote(here, here, z_send.at[0, m, q], z_recv.at[j, m, q], flip)

    def x_out(way, src, j, m, q):
        return remote(
            src,
            x_spot(k, x, j, m, q),
            x_send.at[way, j, m, q],
            x_recv.at[way, j, m, q],
            (right, left)[way],
        )

    def x_on(j, m, q):
        here = x_spot(k, xs[q], j, m, q)
        return remote(
            here, here, x_send.at[2, j, m, q], x_recv.at[2, j, m, q], (right, left)[q]
        )

    def x_in(d, j, m, q):
        here = x_spot(k, xs[d], j, m, q)
        return remote(here, here, x_send.at[2, j, m, q], x_recv.at[d, j, m, q], right)

    places = (*xs, x)

    def p_out(d, src, j, m, q):
        return remote(
            src,
            x_spot(k, places[d], j, m, q),
            p_send.at[d, j, m, q],
            p_recv.at[d, j, m, q],
            mate,
        )

    def p_in(d, j, m, q):
        here = x_spot(1 - k, places[d], j, m, q)
        return remote(here, here, p_send.at[d, j, m, q], p_recv.at[d, j, m, q], mate)

    def spread(src, j, m, q):
        for way in (0, 1) if q == 0 else (1, 0):
            x_out(way, src, j, m, q).start()
        p_out(3, src, j, m, q).start()

    def passed(d, j, m, q):
        x_in(d, j, m, q).wait_recv()
        if d == q:
            x_on(j, m, q).start()
        p_out(d, x_spot(k, places[d], j, m, q), j, m, q).start()

    def z_forward(m, q):
        @pl.when(inner)
        def _():
            z_in(1, m, q).wait_recv()
            z_on(m, q).start()

    def z_spread(m, q, own_too):
        @pl.when(inner)
        def _():
            z_in(0, m, q).wait_recv()
            spread(x_spot(k, x, 0, m, q), 0, m, q)

        @pl.when(outer)
        def _():
            if own_too:
                spread(x_own(m, q), 0, m, q)
            z_in(1, m, q).wait_recv()

        spread(x_spot(k, x, 1, m, q), 1, m, q)

    @pl.when(outer)
    def _():
        for m in range(2):
            for q in range(2):
                z_out(m, q, flip, 0).start()
            if m == 0:
                for q in range(2):
                    spread(x_own(0, q), 0, 0, q)

    @pl.when(inner)
    def _():
        for m in range(2):
            for q in range(2):
                z_out(m, q, across, 1).start()

    w_start(0)
    w_start(1)

    @pl.when(outer)
    def _():
        for m in range(2):
            xg[k * 4 + x, m, h] = own[m][...]

    wf[y, 0] = gate_weight[...]
    wf[y, 1] = up_weight[...]
    df[y] = down_weight[...]

    for q in range(2):
        z_forward(0, q)
        z_spread(0, q, False)
    for j in range(2):
        passed(0, j, 0, 0)
        passed(1, j, 0, 0)
    z_forward(1, 0)
    w_forward(0)
    for j in range(2):
        passed(1, j, 0, 1)
        passed(0, j, 0, 1)
    z_forward(1, 1)
    w_forward(1)
    w_start(2)
    for q in range(2):
        z_spread(1, q, True)
    tall = 2 * rows

    def block(m, o):
        return jnp.concatenate(
            [xg[p * 4 + o, m].reshape(tall, shard) for p in range(2)], axis=1
        )

    def pair_in(d, m):
        for q in range(2):
            for j in range(2):
                p_in(d, j, m, q).wait_recv()

    def gate_up(d):
        o = places[d]
        weights = jnp.concatenate([wf[o, 0], wf[o, 1]], axis=1)
        term = jnp.dot(block(0, o), weights, preferred_element_type=F32)
        sa[...] = term if d == 3 else sa[...] + term

    w_rest(0)
    w_rest(1)
    quarter = shard // 4

    def t_rows(u):
        return pl.ds(lax.rem(u, 2) * shard + y * quarter, quarter)

    def t_out(j):
        u = lax.rem(me + j, 8)
        return remote(
            wf.at[lax.div(u, 2), :, t_rows(u)],
            tw.at[me, :, pl.ds(y * quarter, quarter)],
            t_send.at[j],
            t_recv.at[j],
            (f, l * 8 + u),
        )

    def t_in(j):
        u = lax.rem(me + 8 - j, 8)
        spot = tw.at[u, :, pl.ds(y * quarter, quarter)]
        return remote(spot, spot, t_send.at[j], t_recv.at[j], (f, l * 8 + u))

    def u_spot(o, q):
        return tw.at[pl.ds(q * 4, 4), :, pl.ds(o * quarter, quarter)]

    def u_out(way, q):
        here = u_spot(y, q)
        return remote(here, here, u_send.at[way, q], u_recv.at[way, q], (north, south)[way])

    def u_on(q):
        here = u_spot(ys[q], q)
        return remote(here, here, u_send.at[2, q], u_recv.at[2, q], (north, south)[q])

    def u_in(d, q):
        here = u_spot(ys[d], q)
        return remote(here, here, u_send.at[2, q], u_recv.at[d, q], north)

    @pl.loop(1, 8)
    def _(j):
        t_out(j).start()

    tw[me, :, pl.ds(y * quarter, quarter)] = wf[x, :, t_rows(me)]
    for d in (3, 0, 1):
        pair_in(d, 0)
        gate_up(d)
    for q in range(2):
        for j in range(2):
            passed(2, j, 0, q)
    pair_in(2, 0)
    gate_up(2)
    def swap(src, dst, send, recv):
        def copy(c):
            at_c = pl.ds(c * rows, rows)
            return remote(src.at[at_c], dst.at[at_c], send.at[c], recv.at[c], opposite)

        return copy

    a_swap = swap(sa, zla, a_send, a_recv)
    b_swap = swap(sb, zlb, b_send, b_recv)

    for j in range(2):
        passed(0, j, 1, 0)
        passed(1, j, 1, 0)
        if j == 0:
            for c in range(2):
                a_swap(c).start()
    w_forward(2)
    for j in range(2):
        passed(1, j, 1, 1)
        passed(0, j, 1, 1)

    @pl.loop(1, 8)
    def _(j):
        t_in(j).wait_recv()

    for way, q in ((0, 0), (1, 1), (0, 1), (1, 0)):
        u_out(way, q).start()
    for c in range(2):
        a_swap(c).wait_recv()
    sums = sa[...] + zla[...]
    gate, up = sums[:, :width], sums[:, width:]
    squashed = jax.nn.sigmoid(gate)
    activated = gate * squashed
    slope = squashed * (1.0 + gate * (1.0 - squashed))
    acts[:, :width] = up * slope
    acts[:, width:] = activated
    hidden[...] = (activated * up).astype(BF16)

    def grad_in(d):
        o = places[d]
        term = lax.dot_general(
            block(1, o), df[o], (COLS, ((), ())), preferred_element_type=F32
        )
        sb[...] = term if d == 3 else sb[...] + term

    w_rest(2)
    for d in (3, 0, 1):
        pair_in(d, 1)
        grad_in(d)
    for q in range(2):
        for j in range(2):
            passed(2, j, 1, q)
    pair_in(2, 1)
    grad_in(2)
    def down_part(o):
        return lax.dot_general(
            hidden[...], block(1, o), (ROWS, ((), ())), preferred_element_type=F32
        )

    def gate_part(o):
        return lax.dot_general(
            block(0, o), dg[me], (ROWS, ((), ())), preferred_element_type=F32
        )

    twos, mids, parts, ones, lands = (
        (dtwo, gtwo),
        (dmid, gmid),
        (dpart, gpart),
        (done, gone),
        (dland, gland),
    )

    def halves(i, q):
        size = twos[i].shape[0] // 2
        return pl.ds(q * size, size)

    def two_out(i, q):
        return remote(
            twos[i].at[halves(i, q)],
            mids[i].at[q],
            two_send.at[i, q],
            two_recv.at[i, q],
            (north, south)[q],
        )

    def one_out(i, way, q):
        return remote(
            ones[i].at[way, halves(i, q)],
            lands[i].at[way, halves(i, q)],
            one_send.at[i, way, q],
            one_recv.at[i, way, q],
            (north, south)[way],
        )

    def one_parts(i, fn):
        for way in range(2):
            q = way
            term = fn(ys[1 - way])
            size = term.shape[0] // 2
            parts[i][way] = term[q * size : (q + 1) * size]
            ones[i][way, halves(i, 1 - q)] = term[(1 - q) * size : (2 - q) * size].astype(BF16)

    def one_merge(i):
        for way in range(2):
            two_out(i, way).wait_recv()
            ones[i][way, halves(i, way)] = (
                parts[i][way] + mids[i][way].astype(F32)
            ).astype(BF16)

    def finals(i):
        for way in range(2):
            for q in range(2):
                one_out(i, way, q).wait_recv()
        return lands[i][0].astype(F32) + lands[i][1].astype(F32)

    dtwo[...] = down_part(ys[2]).astype(BF16)
    for c in range(2):
        b_swap(c).start()
    one_parts(0, down_part)
    for q in range(2):
        two_out(0, q).start()
    for way in range(2):
        one_out(0, way, 1 - way).start()
    for q in range(2):
        u_in(q, q).wait_recv()
        u_on(q).start()
    down_out[...] = down_part(y)
    one_merge(0)

    for c in range(2):
        b_swap(c).wait_recv()
    for way in range(2):
        one_out(0, way, way).start()

    hidden_grad = sb[...] + zlb[...]
    dg[me, :, :width] = (hidden_grad * acts[:, :width]).astype(BF16)
    dg[me, :, width:] = (hidden_grad * acts[:, width:]).astype(BF16)
    gtwo[...] = gate_part(ys[2]).astype(BF16)

    turn = (1 - l, l)

    def d_spot(c, o, e, q):
        return dg.at[o * 2 + c, pl.ds(turn[e] * rows + q * part, part)]

    def dx_out(way, e, q):
        here = d_spot(k, x, e, q)
        return remote(
            here, here, dx_send.at[way, e, q], dx_recv.at[way, e, q], (right, left)[way]
        )

    def dx_on(e, q):
        here = d_spot(k, xs[q], e, q)
        return remote(here, here, dx_send.at[2, e, q], dx_recv.at[2, e, q], (right, left)[q])

    def dx_in(d, e, q):
        here = d_spot(k, xs[d], e, q)
        return remote(here, here, dx_send.at[2, e, q], dx_recv.at[d, e, q], right)

    def dp_out(d, e, q):
        here = d_spot(k, places[d], e, q)
        return remote(here, here, dp_send.at[d, e, q], dp_recv.at[d, e, q], mate)

    def dp_in(d, e, q):
        here = d_spot(1 - k, places[d], e, q)
        return remote(here, here, dp_send.at[d, e, q], dp_recv.at[d, e, q], mate)

    def d_start(e):
        for q in range(2):
            for way in (0, 1) if q == 0 else (1, 0):
                dx_out(way, e, q).start()
            dp_out(3, e, q).start()

    def d_passed(d, e, q):
        dx_in(d, e, q).wait_recv()
        if d == q:
            dx_on(e, q).start()
        dp_out(d, e, q).start()

    def d_near(e):
        for q in range(2):
            d_passed(q, e, q)
        for q in range(2):
            d_passed(1 - q, e, q)

    def gather(d, e):
        base = places[d] * 2
        at_s = pl.ds(turn[e] * rows, rows)
        left_side = jnp.concatenate([dg[base, at_s], dg[base + 1, at_s]], axis=1)
        right_side = jnp.concatenate(
            [tw[base, 0], tw[base, 1], tw[base + 1, 0], tw[base + 1, 1]], axis=1
        )
        term = lax.dot_general(
            left_side, right_side, (COLS, ((), ())), preferred_element_type=F32
        )
        total[e] = term if d == 3 else total[e] + term

    def gathers(e, ds):
        for d in ds:
            for q in range(2):
                dp_in(d, e, q).wait_recv()
            gather(d, e)

    piece = rows // 4

    def f_out(c):
        at_c = pl.ds(c * piece, piece)
        return remote(total.at[0, at_c], near.at[at_c], f_send.at[c], f_recv.at[c], flip)

    def r_out(c):
        at_c = pl.ds(c * piece, piece)
        return remote(rounded.at[at_c], result.at[at_c], r_send.at[c], r_recv.at[c], across)

    d_start(0)
    one_parts(1, gate_part)
    for q in range(2):
        two_out(1, q).start()
    for way in range(2):
        one_out(1, way, 1 - way).start()
    gown[...] = gate_part(y)
    d_near(0)
    d_start(1)
    for q in range(2):
        u_in(1 - q, q).wait_recv()
        u_in(2, q).wait_recv()
    gathers(0, (3, 0, 1))
    for q in range(2):
        d_passed(2, 0, q)
    gathers(0, (2,))
    d_near(1)
    for c in range(4):
        f_out(c).start()
    one_merge(1)
    gathers(1, (3,))
    for way in range(2):
        one_out(1, way, way).start()
    gathers(1, (0, 1))
    for q in range(2):
        d_passed(2, 1, q)
    gathers(1, (2,))
    down_out[...] = factor * (down_out[...] + finals(0))
    for c in range(4):
        f_out(c).wait_recv()
        at_c = pl.ds(c * piece, piece)
        rounded[at_c] = (total[1, at_c] + near[at_c]).astype(BF16)

        if c:

            @pl.when(inner)
            def _(c=c):
                r_out(c - 1).start()

    both = factor * (gown[...] + finals(1))
    gate_out[...] = both[:, :width]
    up_out[...] = both[:, width:]
    @pl.when(inner)
    def _():
        r_out(3).start()

    @pl.when(outer)
    def _():
        result[...] = rounded[...]

    for m in range(2):
        for q in range(2):
            z_in(0, m, q).wait_send()

            @pl.when(inner)
            def _(m=m, q=q):
                z_on(m, q).wait_send()

            for j in range(2):
                for way in range(2):
                    x_out(way, x_own(m, q), j, m, q).wait_send()
                x_on(j, m, q).wait_send()
                for d in range(4):
                    p_out(d, x_own(m, q), j, m, q).wait_send()
    for w in range(3):
        for q in range(2):
            for way in range(2):
                w_out(way, w, q).wait_send()
            w_on(w, q).wait_send()
    for c in range(2):
        for copy in (a_swap(c), b_swap(c), f_out(c), f_out(2 + c)):
            copy.wait_send()
        for i in range(2):
            two_out(i, c).wait_send()
            for q in range(2):
                one_out(i, c, q).wait_send()
        for way in range(2):
            u_out(way, c).wait_send()
        u_on(c).wait_send()
        for e in range(2):
            for way in range(2):
                dx_out(way, e, c).wait_send()
            dx_on(e, c).wait_send()
            for d in range(4):
                dp_out(d, e, c).wait_send()

    @pl.loop(1, 8)
    def _(j):
        t_out(j).wait_send()

    @pl.when(inner)
    def _():
        for c in range(4):
            r_out(c).wait()


VMEM = pl.BlockSpec(memory_space=pltpu.VMEM)
DMA = pltpu.SemaphoreType.DMA


def body(tokens, out_grad, gate_weight, up_weight, down_weight):
    nf, nt = lax.axis_size("fsdp"), lax.axis_size("tp")
    rows, shard = tokens.shape
    deep, width = gate_weight.shape
    assert nf == 8 and nt == 16 and deep == 2 * shard
    factor = 1.0 / math.sqrt(rows * nf)
    tall = 2 * rows
    wide = 2 * width

    return tuple(
        pl.pallas_call(
            functools.partial(kernel, factor),
            out_shape=(
                jax.ShapeDtypeStruct((rows, shard), BF16),
                jax.ShapeDtypeStruct((deep, width), F32),
                jax.ShapeDtypeStruct((deep, width), F32),
                jax.ShapeDtypeStruct((width, deep), F32),
            ),
            in_specs=[VMEM] * 5,
            out_specs=(VMEM,) * 4,
            scratch_shapes=[
                pltpu.VMEM((8, 2, 2, rows, shard), BF16),
                pltpu.VMEM((4, 2, deep, width), BF16),
                pltpu.VMEM((4, width, deep), BF16),
                pltpu.VMEM((tall, wide), F32),
                pltpu.VMEM((tall, wide), F32),
                pltpu.VMEM((tall, width), F32),
                pltpu.VMEM((tall, width), F32),
                pltpu.VMEM((tall, wide), F32),
                pltpu.VMEM((tall, width), BF16),
                pltpu.VMEM((8, tall, wide), BF16),
                pltpu.VMEM((8, 2, shard, width), BF16),
                pltpu.VMEM((2, width // 2, deep), F32),
                pltpu.VMEM((2, deep // 2, wide), F32),
                pltpu.VMEM((width, deep), BF16),
                pltpu.VMEM((deep, wide), BF16),
                pltpu.VMEM((2, width, deep), BF16),
                pltpu.VMEM((2, deep, wide), BF16),
                pltpu.VMEM((2, width // 2, deep), BF16),
                pltpu.VMEM((2, deep // 2, wide), BF16),
                pltpu.VMEM((2, width, deep), BF16),
                pltpu.VMEM((2, deep, wide), BF16),
                pltpu.VMEM((deep, wide), F32),
                pltpu.VMEM((2, rows, shard), F32),
                pltpu.VMEM((rows, shard), F32),
                pltpu.VMEM((rows, shard), BF16),
                DMA((2, 2, 2)),
                DMA((2, 2, 2)),
                DMA((3, 2, 2, 2)),
                DMA((3, 2, 2, 2)),
                DMA((4, 2, 2, 2)),
                DMA((4, 2, 2, 2)),
                DMA((3, 3, 2)),
                DMA((3, 3, 2)),
                DMA((2,)),
                DMA((2,)),
                DMA((2,)),
                DMA((2,)),
                DMA((8,)),
                DMA((8,)),
                DMA((3, 2)),
                DMA((3, 2)),
                DMA((4,)),
                DMA((4,)),
                DMA((3, 2, 2)),
                DMA((3, 2, 2)),
                DMA((4, 2, 2)),
                DMA((4, 2, 2)),
                DMA((2, 2)),
                DMA((2, 2)),
                DMA((2, 2, 2)),
                DMA((2, 2, 2)),
                DMA((4,)),
                DMA((4,)),
            ],
            compiler_params=pltpu.CompilerParams(
                collective_id=0, has_side_effects=True, vmem_limit_bytes=VMEM_LIMIT
            ),
            name="block",
        )(tokens, out_grad, gate_weight, up_weight, down_weight)
    )


def solution(mesh):
    return jax.shard_map(
        body,
        mesh=mesh,
        in_specs=(
            P("fsdp", "tp"),
            P("fsdp", "tp"),
            P("fsdp", "tp"),
            P("fsdp", "tp"),
            P("tp", "fsdp"),
        ),
        out_specs=(P("fsdp", "tp"), P("fsdp", "tp"), P("fsdp", "tp"), P("tp", "fsdp")),
        check_vma=False,
    )
```

```python
import functools
import math

import jax
import jax.numpy as jnp
from jax import lax
from jax.sharding import PartitionSpec as P
from jax.experimental import pallas as pl
from jax.experimental.pallas import tpu as pltpu

MESH = pl.DeviceIdType.MESH
F32 = jnp.float32
BF16 = jnp.bfloat16
VMEM_LIMIT = 60 * 1024 * 1024
ROWS = ((0,), (0,))
COLS = ((1,), (1,))


def kernel(
    factor,
    tokens,
    grads,
    gate_weight,
    up_weight,
    down_weight,
    result,
    gate_out,
    up_out,
    down_out,
    gate_own,
    up_own,
    down_own,
    held,
    xg,
    wf,
    df,
    sa,
    zla,
    sb,
    zlb,
    acts,
    hidden,
    dg,
    tw,
    dpart,
    gpart,
    dtwo,
    gtwo,
    done,
    gone,
    dmid,
    gmid,
    dland,
    gland,
    gown,
    total,
    near,
    rounded,
    load,
    keep,
    z_send,
    z_recv,
    x_send,
    x_recv,
    p_send,
    p_recv,
    y_send,
    y_recv,
    a_send,
    a_recv,
    b_send,
    b_recv,
    t_send,
    t_recv,
    u_send,
    u_recv,
    f_send,
    f_recv,
    dx_send,
    dx_recv,
    dp_send,
    dp_recv,
    two_send,
    two_recv,
    one_send,
    one_recv,
    r_send,
    r_recv,
):
    f, t = lax.axis_index("fsdp"), lax.axis_index("tp")
    h, y = lax.div(f, 4), lax.rem(f, 4)
    l, x, k = lax.div(t, 8), lax.rem(lax.div(t, 2), 4), lax.rem(t, 2)
    outer = h == l
    inner = h != l
    rows, shard = tokens.shape
    deep, width = gate_weight.shape
    part = rows // 2
    wide = 2 * width

    def at(xx, yy, hh, ll, kk):
        return (hh * 4 + yy, ll * 8 + xx * 2 + kk)

    xs = (lax.rem(x + 3, 4), lax.rem(x + 1, 4), lax.rem(x + 2, 4))
    ys = (lax.rem(y + 3, 4), lax.rem(y + 1, 4), lax.rem(y + 2, 4))
    right, left = at(xs[1], y, h, l, k), at(xs[0], y, h, l, k)
    north, south = at(x, ys[1], h, l, k), at(x, ys[0], h, l, k)
    mate = at(x, y, h, l, 1 - k)
    flip = at(x, y, h, 1 - l, k)
    across = at(x, y, 1 - h, 1 - l, k)
    opposite = at(x, y, 1 - h, l, k)
    me = 2 * x + k

    def remote(src, dst, send, recv, device):
        return pltpu.make_async_remote_copy(
            src_ref=src,
            dst_ref=dst,
            send_sem=send,
            recv_sem=recv,
            device_id=device,
            device_id_type=MESH,
        )

    copies = [
        pltpu.make_async_copy(ref, spot, load.at[i])
        for i, (ref, spot) in enumerate(
            (
                (tokens, held.at[0]),
                (gate_weight, wf.at[y, 0]),
                (up_weight, wf.at[y, 1]),
                (grads, held.at[1]),
                (down_weight, df.at[y]),
            )
        )
    ]
    kept = [
        pltpu.make_async_copy(ref, xg.at[k * 4 + x, m, h], load.at[5 + m])
        for m, ref in enumerate((tokens, grads))
    ]
    for copy in copies:
        copy.start()

    @pl.when(outer)
    def _():
        for copy in kept:
            copy.start()

    barrier = pltpu.get_barrier_semaphore()
    for j in range(1, 16):
        pl.semaphore_signal(
            barrier, inc=1, device_id=(f, lax.rem(t + j, 16)), device_id_type=MESH
        )
    for peer in (north, south, opposite, across):
        pl.semaphore_signal(barrier, inc=1, device_id=peer, device_id_type=MESH)
    pl.semaphore_wait(barrier, 19)

    for copy in copies:
        copy.wait()

    @pl.when(outer)
    def _():
        for copy in kept:
            copy.wait()

    def w_spot(o, w, q):
        if w == 2:
            return df.at[o, pl.ds(q * (width // 2), width // 2)]
        return wf.at[o, w, pl.ds(q * (deep // 2), deep // 2)]

    def w_out(way, w, q):
        return remote(
            w_spot(y, w, q),
            w_spot(y, w, q),
            y_send.at[way, w, q],
            y_recv.at[way, w, q],
            (north, south)[way],
        )

    def w_on(w, q):
        here = w_spot(ys[q], w, q)
        return remote(here, here, y_send.at[2, w, q], y_recv.at[2, w, q], (north, south)[q])

    def w_in(d, w, q):
        here = w_spot(ys[d], w, q)
        return remote(here, here, y_send.at[2, w, q], y_recv.at[d, w, q], north)

    def w_start(w):
        for way, q in ((0, 0), (1, 1), (0, 1), (1, 0)):
            w_out(way, w, q).start()

    def w_forward(w):
        for q in range(2):
            w_in(q, w, q).wait_recv()
            w_on(w, q).start()

    def w_rest(w):
        for q in range(2):
            w_in(1 - q, w, q).wait_recv()
            w_in(2, w, q).wait_recv()

    slot = (h, 1 - h)

    def x_own(m, q):
        return held.at[m, pl.ds(q * part, part)]

    def x_spot(p, o, j, m, q):
        return xg.at[p * 4 + o, m, slot[j], pl.ds(q * part, part)]

    def z_out(m, q, device, j):
        spot = xg.at[k * 4 + x, m, h, pl.ds(q * part, part)]
        return remote(x_own(m, q), spot, z_send.at[0, m, q], z_recv.at[j, m, q], device)

    def z_on(m, q):
        here = x_spot(k, x, 1, m, q)
        return remote(here, here, z_send.at[1, m, q], z_recv.at[1, m, q], flip)

    def z_in(j, m, q):
        here = x_spot(k, x, j, m, q)
        return remote(here, here, z_send.at[0, m, q], z_recv.at[j, m, q], flip)

    def x_out(way, src, j, m, q):
        return remote(
            src,
            x_spot(k, x, j, m, q),
            x_send.at[way, j, m, q],
            x_recv.at[way, j, m, q],
            (right, left)[way],
        )

    def x_on(j, m, q):
        here = x_spot(k, xs[q], j, m, q)
        return remote(
            here, here, x_send.at[2, j, m, q], x_recv.at[2, j, m, q], (right, left)[q]
        )

    def x_in(d, j, m, q):
        here = x_spot(k, xs[d], j, m, q)
        return remote(here, here, x_send.at[2, j, m, q], x_recv.at[d, j, m, q], right)

    places = (*xs, x)

    def p_out(d, src, j, m, q):
        return remote(
            src,
            x_spot(k, places[d], j, m, q),
            p_send.at[d, j, m, q],
            p_recv.at[d, j, m, q],
            mate,
        )

    def p_in(d, j, m, q):
        here = x_spot(1 - k, places[d], j, m, q)
        return remote(here, here, p_send.at[d, j, m, q], p_recv.at[d, j, m, q], mate)

    def spread(src, j, m, q):
        for way in (0, 1) if q == 0 else (1, 0):
            x_out(way, src, j, m, q).start()
        p_out(3, src, j, m, q).start()

    def passed(d, j, m, q):
        x_in(d, j, m, q).wait_recv()
        if d == q:
            x_on(j, m, q).start()
        p_out(d, x_spot(k, places[d], j, m, q), j, m, q).start()

    def z_forward(m, q):
        @pl.when(inner)
        def _():
            z_in(1, m, q).wait_recv()
            z_on(m, q).start()

    def z_spread(m, q, own_too):
        @pl.when(inner)
        def _():
            z_in(0, m, q).wait_recv()
            spread(x_spot(k, x, 0, m, q), 0, m, q)

        @pl.when(outer)
        def _():
            if own_too:
                spread(x_own(m, q), 0, m, q)
            z_in(1, m, q).wait_recv()

        spread(x_spot(k, x, 1, m, q), 1, m, q)

    @pl.when(outer)
    def _():
        for m in range(2):
            for q in range(2):
                z_out(m, q, flip, 0).start()
            if m == 0:
                for q in range(2):
                    spread(x_own(0, q), 0, 0, q)

    @pl.when(inner)
    def _():
        for m in range(2):
            for q in range(2):
                z_out(m, q, across, 1).start()

    w_start(0)
    w_start(1)

    for q in range(2):
        z_forward(0, q)
        z_spread(0, q, False)
    w_forward(0)
    for j in range(2):
        passed(0, j, 0, 0)
        passed(1, j, 0, 0)
    z_forward(1, 0)
    w_forward(1)
    w_start(2)
    for j in range(2):
        passed(1, j, 0, 1)
        passed(0, j, 0, 1)
    z_forward(1, 1)
    w_rest(0)
    w_rest(1)
    quarter = shard // 4

    def t_rows(u):
        return pl.ds(lax.rem(u, 2) * shard + y * quarter, quarter)

    def t_out(j):
        u = lax.rem(me + j, 8)
        return remote(
            wf.at[lax.div(u, 2), :, t_rows(u)],
            tw.at[me, :, pl.ds(y * quarter, quarter)],
            t_send.at[j],
            t_recv.at[j],
            (f, l * 8 + u),
        )

    def t_in(j):
        u = lax.rem(me + 8 - j, 8)
        spot = tw.at[u, :, pl.ds(y * quarter, quarter)]
        return remote(spot, spot, t_send.at[j], t_recv.at[j], (f, l * 8 + u))

    def u_spot(o, q):
        return tw.at[pl.ds(q * 4, 4), :, pl.ds(o * quarter, quarter)]

    def u_out(way, q):
        here = u_spot(y, q)
        return remote(here, here, u_send.at[way, q], u_recv.at[way, q], (north, south)[way])

    def u_on(q):
        here = u_spot(ys[q], q)
        return remote(here, here, u_send.at[2, q], u_recv.at[2, q], (north, south)[q])

    def u_in(d, q):
        here = u_spot(ys[d], q)
        return remote(here, here, u_send.at[2, q], u_recv.at[d, q], north)

    @pl.loop(1, 8)
    def _(j):
        t_out(j).start()

    tw[me, :, pl.ds(y * quarter, quarter)] = wf[x, :, t_rows(me)]
    for q in range(2):
        z_spread(1, q, True)
    tall = 2 * rows

    def block(m, o):
        return jnp.concatenate(
            [xg[p * 4 + o, m].reshape(tall, shard) for p in range(2)], axis=1
        )

    def pair_in(d, m):
        for q in range(2):
            for j in range(2):
                p_in(d, j, m, q).wait_recv()

    def gate_up(d):
        o = places[d]
        weights = jnp.concatenate([wf[o, 0], wf[o, 1]], axis=1)
        term = jnp.dot(block(0, o), weights, preferred_element_type=F32)
        sa[...] = term if d == 3 else sa[...] + term

    for d in (3, 0, 1):
        pair_in(d, 0)
        gate_up(d)
    for q in range(2):
        for j in range(2):
            passed(2, j, 0, q)
    pair_in(2, 0)
    gate_up(2)
    def swap(src, dst, send, recv):
        def copy(c):
            at_c = pl.ds(c * rows, rows)
            return remote(src.at[at_c], dst.at[at_c], send.at[c], recv.at[c], opposite)

        return copy

    a_swap = swap(sa, zla, a_send, a_recv)
    b_swap = swap(sb, zlb, b_send, b_recv)

    for j in range(2):
        passed(0, j, 1, 0)
        passed(1, j, 1, 0)
        if j == 0:
            for c in range(2):
                a_swap(c).start()
    w_forward(2)
    for j in range(2):
        passed(1, j, 1, 1)
        passed(0, j, 1, 1)

    @pl.loop(1, 8)
    def _(j):
        t_in(j).wait_recv()

    for way, q in ((0, 0), (1, 1), (0, 1), (1, 0)):
        u_out(way, q).start()
    for c in range(2):
        a_swap(c).wait_recv()
    sums = sa[...] + zla[...]
    gate, up = sums[:, :width], sums[:, width:]
    squashed = jax.nn.sigmoid(gate)
    activated = gate * squashed
    slope = squashed * (1.0 + gate * (1.0 - squashed))
    acts[:, :width] = up * slope
    acts[:, width:] = activated
    hidden[...] = (activated * up).astype(BF16)

    def grad_in(d):
        o = places[d]
        term = lax.dot_general(
            block(1, o), df[o], (COLS, ((), ())), preferred_element_type=F32
        )
        sb[...] = term if d == 3 else sb[...] + term

    w_rest(2)
    for d in (3, 0, 1):
        pair_in(d, 1)
        grad_in(d)
    for q in range(2):
        for j in range(2):
            passed(2, j, 1, q)
    pair_in(2, 1)
    grad_in(2)
    def down_part(o):
        return lax.dot_general(
            hidden[...], block(1, o), (ROWS, ((), ())), preferred_element_type=F32
        )

    def gate_part(o):
        return lax.dot_general(
            block(0, o), dg[me], (ROWS, ((), ())), preferred_element_type=F32
        )

    twos, mids, parts, ones, lands = (
        (dtwo, gtwo),
        (dmid, gmid),
        (dpart, gpart),
        (done, gone),
        (dland, gland),
    )

    def halves(i, q):
        size = twos[i].shape[0] // 2
        return pl.ds(q * size, size)

    def two_out(i, q):
        return remote(
            twos[i].at[halves(i, q)],
            mids[i].at[q],
            two_send.at[i, q],
            two_recv.at[i, q],
            (north, south)[q],
        )

    def one_out(i, way, q):
        return remote(
            ones[i].at[way, halves(i, q)],
            lands[i].at[way, halves(i, q)],
            one_send.at[i, way, q],
            one_recv.at[i, way, q],
            (north, south)[way],
        )

    def one_parts(i, fn):
        for way in range(2):
            q = way
            term = fn(ys[1 - way])
            size = term.shape[0] // 2
            parts[i][way] = term[q * size : (q + 1) * size]
            ones[i][way, halves(i, 1 - q)] = term[(1 - q) * size : (2 - q) * size].astype(BF16)

    def one_merge(i):
        for way in range(2):
            two_out(i, way).wait_recv()
            ones[i][way, halves(i, way)] = (
                parts[i][way] + mids[i][way].astype(F32)
            ).astype(BF16)

    def finals(i):
        for way in range(2):
            for q in range(2):
                one_out(i, way, q).wait_recv()
        return lands[i][0].astype(F32) + lands[i][1].astype(F32)

    dtwo[...] = down_part(ys[2]).astype(BF16)
    for c in range(2):
        b_swap(c).start()
    one_parts(0, down_part)
    for q in range(2):
        two_out(0, q).start()
    for way in range(2):
        one_out(0, way, 1 - way).start()
    for q in range(2):
        u_in(q, q).wait_recv()
        u_on(q).start()
    down_own[...] = down_part(y)

    for c in range(2):
        b_swap(c).wait_recv()

    hidden_grad = sb[...] + zlb[...]
    dg[me, :, :width] = (hidden_grad * acts[:, :width]).astype(BF16)
    dg[me, :, width:] = (hidden_grad * acts[:, width:]).astype(BF16)
    gtwo[...] = gate_part(ys[2]).astype(BF16)

    turn = (1 - l, l)

    def d_spot(c, o, e, q):
        return dg.at[o * 2 + c, pl.ds(turn[e] * rows + q * part, part)]

    def dx_out(way, e, q):
        here = d_spot(k, x, e, q)
        return remote(
            here, here, dx_send.at[way, e, q], dx_recv.at[way, e, q], (right, left)[way]
        )

    def dx_on(e, q):
        here = d_spot(k, xs[q], e, q)
        return remote(here, here, dx_send.at[2, e, q], dx_recv.at[2, e, q], (right, left)[q])

    def dx_in(d, e, q):
        here = d_spot(k, xs[d], e, q)
        return remote(here, here, dx_send.at[2, e, q], dx_recv.at[d, e, q], right)

    def dp_out(d, e, q):
        here = d_spot(k, places[d], e, q)
        return remote(here, here, dp_send.at[d, e, q], dp_recv.at[d, e, q], mate)

    def dp_in(d, e, q):
        here = d_spot(1 - k, places[d], e, q)
        return remote(here, here, dp_send.at[d, e, q], dp_recv.at[d, e, q], mate)

    def d_start(e):
        for q in range(2):
            for way in (0, 1) if q == 0 else (1, 0):
                dx_out(way, e, q).start()
            dp_out(3, e, q).start()

    def d_passed(d, e, q):
        dx_in(d, e, q).wait_recv()
        if d == q:
            dx_on(e, q).start()
        dp_out(d, e, q).start()

    def d_near(e):
        for q in range(2):
            d_passed(q, e, q)
        for q in range(2):
            d_passed(1 - q, e, q)

    def gather(d, e):
        base = places[d] * 2
        at_s = pl.ds(turn[e] * rows, rows)
        left_side = jnp.concatenate([dg[base, at_s], dg[base + 1, at_s]], axis=1)
        right_side = jnp.concatenate(
            [tw[base, 0], tw[base, 1], tw[base + 1, 0], tw[base + 1, 1]], axis=1
        )
        term = lax.dot_general(
            left_side, right_side, (COLS, ((), ())), preferred_element_type=F32
        )
        total[e] = term if d == 3 else total[e] + term

    def gathers(e, ds):
        for d in ds:
            for q in range(2):
                dp_in(d, e, q).wait_recv()
            gather(d, e)

    piece = rows // 4

    def f_out(c):
        at_c = pl.ds(c * piece, piece)
        return remote(total.at[0, at_c], near.at[at_c], f_send.at[c], f_recv.at[c], flip)

    def r_out(c):
        at_c = pl.ds(c * piece, piece)
        return remote(rounded.at[at_c], result.at[at_c], r_send.at[c], r_recv.at[c], across)

    d_start(0)
    one_parts(1, gate_part)
    for q in range(2):
        two_out(1, q).start()
    for way in range(2):
        one_out(1, way, 1 - way).start()
    gown[...] = gate_part(y)
    d_near(0)
    d_start(1)
    one_merge(0)
    for q in range(2):
        u_in(1 - q, q).wait_recv()
        u_in(2, q).wait_recv()
    for way in range(2):
        one_out(0, way, way).start()
    gathers(0, (3, 0, 1))
    for q in range(2):
        d_passed(2, 0, q)
    gathers(0, (2,))
    d_near(1)
    for c in range(4):
        f_out(c).start()
    one_merge(1)
    gathers(1, (3,))
    for way in range(2):
        one_out(1, way, way).start()
    gathers(1, (0, 1))
    for q in range(2):
        d_passed(2, 1, q)
    gathers(1, (2,))
    down_own[...] = factor * (down_own[...] + finals(0))
    keeps = [
        pltpu.make_async_copy(src, dst, keep.at[i])
        for i, (src, dst) in enumerate(
            ((down_own, down_out), (gate_own, gate_out), (up_own, up_out), (rounded, result))
        )
    ]
    keeps[0].start()
    for c in range(4):
        f_out(c).wait_recv()
        at_c = pl.ds(c * piece, piece)
        rounded[at_c] = (total[1, at_c] + near[at_c]).astype(BF16)

        if c:

            @pl.when(inner)
            def _(c=c):
                r_out(c - 1).start()

    both = factor * (gown[...] + finals(1))
    gate_own[...] = both[:, :width]
    up_own[...] = both[:, width:]
    @pl.when(inner)
    def _():
        r_out(3).start()

    @pl.when(outer)
    def _():
        keeps[3].start()

    for copy in keeps[1:3]:
        copy.start()

    for m in range(2):
        for q in range(2):
            z_in(0, m, q).wait_send()

            @pl.when(inner)
            def _(m=m, q=q):
                z_on(m, q).wait_send()

            for j in range(2):
                for way in range(2):
                    x_out(way, x_own(m, q), j, m, q).wait_send()
                x_on(j, m, q).wait_send()
                for d in range(4):
                    p_out(d, x_own(m, q), j, m, q).wait_send()
    for w in range(3):
        for q in range(2):
            for way in range(2):
                w_out(way, w, q).wait_send()
            w_on(w, q).wait_send()
    for c in range(2):
        for copy in (a_swap(c), b_swap(c), f_out(c), f_out(2 + c)):
            copy.wait_send()
        for i in range(2):
            two_out(i, c).wait_send()
            for q in range(2):
                one_out(i, c, q).wait_send()
        for way in range(2):
            u_out(way, c).wait_send()
        u_on(c).wait_send()
        for e in range(2):
            for way in range(2):
                dx_out(way, e, c).wait_send()
            dx_on(e, c).wait_send()
            for d in range(4):
                dp_out(d, e, c).wait_send()

    @pl.loop(1, 8)
    def _(j):
        t_out(j).wait_send()

    @pl.when(inner)
    def _():
        for c in range(4):
            r_out(c).wait()

    @pl.when(outer)
    def _():
        keeps[3].wait()

    for copy in keeps[:3]:
        copy.wait()


def store_kernel(*refs):
    found, kept, held, sem = refs[:4], refs[4:8], refs[8:12], refs[12]
    loads = [pltpu.make_async_copy(found[i], held[i], sem.at[0, i]) for i in range(4)]
    stores = [pltpu.make_async_copy(held[i], kept[i], sem.at[1, i]) for i in range(4)]
    for copy in loads:
        copy.start()
    for i in range(4):
        loads[i].wait()
        stores[i].start()
    for copy in stores:
        copy.wait()


HBM = pl.BlockSpec(memory_space=pltpu.HBM)
DMA = pltpu.SemaphoreType.DMA


def body(tokens, out_grad, gate_weight, up_weight, down_weight):
    nf, nt = lax.axis_size("fsdp"), lax.axis_size("tp")
    rows, shard = tokens.shape
    deep, width = gate_weight.shape
    assert nf == 8 and nt == 16 and deep == 2 * shard
    factor = 1.0 / math.sqrt(rows * nf)
    tall = 2 * rows
    wide = 2 * width

    shapes = (
        jax.ShapeDtypeStruct((rows, shard), BF16),
        jax.ShapeDtypeStruct((deep, width), F32),
        jax.ShapeDtypeStruct((deep, width), F32),
        jax.ShapeDtypeStruct((width, deep), F32),
    )
    found = tuple(
        pl.pallas_call(
            functools.partial(kernel, factor),
            out_shape=shapes,
            in_specs=[HBM] * 5,
            out_specs=(HBM,) * 4,
            scratch_shapes=[
                pltpu.VMEM((deep, width), F32),
                pltpu.VMEM((deep, width), F32),
                pltpu.VMEM((width, deep), F32),
                pltpu.VMEM((2, rows, shard), BF16),
                pltpu.VMEM((8, 2, 2, rows, shard), BF16),
                pltpu.VMEM((4, 2, deep, width), BF16),
                pltpu.VMEM((4, width, deep), BF16),
                pltpu.VMEM((tall, wide), F32),
                pltpu.VMEM((tall, wide), F32),
                pltpu.VMEM((tall, width), F32),
                pltpu.VMEM((tall, width), F32),
                pltpu.VMEM((tall, wide), F32),
                pltpu.VMEM((tall, width), BF16),
                pltpu.VMEM((8, tall, wide), BF16),
                pltpu.VMEM((8, 2, shard, width), BF16),
                pltpu.VMEM((2, width // 2, deep), F32),
                pltpu.VMEM((2, deep // 2, wide), F32),
                pltpu.VMEM((width, deep), BF16),
                pltpu.VMEM((deep, wide), BF16),
                pltpu.VMEM((2, width, deep), BF16),
                pltpu.VMEM((2, deep, wide), BF16),
                pltpu.VMEM((2, width // 2, deep), BF16),
                pltpu.VMEM((2, deep // 2, wide), BF16),
                pltpu.VMEM((2, width, deep), BF16),
                pltpu.VMEM((2, deep, wide), BF16),
                pltpu.VMEM((deep, wide), F32),
                pltpu.VMEM((2, rows, shard), F32),
                pltpu.VMEM((rows, shard), F32),
                pltpu.VMEM((rows, shard), BF16),
                DMA((7,)),
                DMA((4,)),
                DMA((2, 2, 2)),
                DMA((2, 2, 2)),
                DMA((3, 2, 2, 2)),
                DMA((3, 2, 2, 2)),
                DMA((4, 2, 2, 2)),
                DMA((4, 2, 2, 2)),
                DMA((3, 3, 2)),
                DMA((3, 3, 2)),
                DMA((2,)),
                DMA((2,)),
                DMA((2,)),
                DMA((2,)),
                DMA((8,)),
                DMA((8,)),
                DMA((3, 2)),
                DMA((3, 2)),
                DMA((4,)),
                DMA((4,)),
                DMA((3, 2, 2)),
                DMA((3, 2, 2)),
                DMA((4, 2, 2)),
                DMA((4, 2, 2)),
                DMA((2, 2)),
                DMA((2, 2)),
                DMA((2, 2, 2)),
                DMA((2, 2, 2)),
                DMA((4,)),
                DMA((4,)),
            ],
            compiler_params=pltpu.CompilerParams(
                collective_id=0, has_side_effects=True, vmem_limit_bytes=VMEM_LIMIT
            ),
            name="block",
        )(tokens, out_grad, gate_weight, up_weight, down_weight)
    )
    return tuple(
        pl.pallas_call(
            store_kernel,
            out_shape=shapes,
            in_specs=[HBM] * 4,
            out_specs=(HBM,) * 4,
            scratch_shapes=[pltpu.VMEM(s.shape, s.dtype) for s in shapes] + [DMA((2, 4))],
            compiler_params=pltpu.CompilerParams(vmem_limit_bytes=VMEM_LIMIT),
            name="store",
        )(*found)
    )


def solution(mesh):
    return jax.shard_map(
        body,
        mesh=mesh,
        in_specs=(
            P("fsdp", "tp"),
            P("fsdp", "tp"),
            P("fsdp", "tp"),
            P("fsdp", "tp"),
            P("tp", "fsdp"),
        ),
        out_specs=(P("fsdp", "tp"), P("fsdp", "tp"), P("fsdp", "tp"), P("tp", "fsdp")),
        check_vma=False,
    )
```

```python
import functools
import math

import jax
import jax.numpy as jnp
from jax import lax
from jax.sharding import PartitionSpec as P
from jax.experimental import pallas as pl
from jax.experimental.pallas import tpu as pltpu

MESH = pl.DeviceIdType.MESH
F32 = jnp.float32
BF16 = jnp.bfloat16
VMEM_LIMIT = 60 * 1024 * 1024
XFIRST = 64
ROWS = ((0,), (0,))
COLS = ((1,), (1,))


def kernel(
    factor,
    tokens,
    grads,
    gate_weight,
    up_weight,
    down_weight,
    result,
    gate_out,
    up_out,
    down_out,
    gate_own,
    up_own,
    down_own,
    xg,
    wf,
    df,
    sa,
    zla,
    sb,
    zlb,
    acts,
    hidden,
    dg,
    tw,
    dpart,
    gpart,
    dtwo,
    gtwo,
    done,
    gone,
    dmid,
    gmid,
    dland,
    gland,
    gown,
    total,
    near,
    rounded,
    load,
    keep,
    z_send,
    z_recv,
    x_send,
    x_recv,
    p_send,
    p_recv,
    v_send,
    v_recv,
    zx_send,
    zx_recv,
    px_send,
    px_recv,
    y_send,
    y_recv,
    a_send,
    a_recv,
    b_send,
    b_recv,
    t_send,
    t_recv,
    u_send,
    u_recv,
    f_send,
    f_recv,
    dx_send,
    dx_recv,
    dp_send,
    dp_recv,
    two_send,
    two_recv,
    one_send,
    one_recv,
    r_send,
    r_recv,
):
    f, t = lax.axis_index("fsdp"), lax.axis_index("tp")
    h, y = lax.div(f, 4), lax.rem(f, 4)
    l, x, k = lax.div(t, 8), lax.rem(lax.div(t, 2), 4), lax.rem(t, 2)
    outer = h == l
    inner = h != l
    rows, shard = tokens.shape
    deep, width = gate_weight.shape
    part = rows // 2
    zpart = (rows - XFIRST) // 2
    xpart = XFIRST // 2
    odd = (h - l) * (h - l)
    home = h * (1 - odd) + 2 * odd
    wide = 2 * width

    def at(xx, yy, hh, ll, kk):
        return (hh * 4 + yy, ll * 8 + xx * 2 + kk)

    xs = (lax.rem(x + 3, 4), lax.rem(x + 1, 4), lax.rem(x + 2, 4))
    ys = (lax.rem(y + 3, 4), lax.rem(y + 1, 4), lax.rem(y + 2, 4))
    right, left = at(xs[1], y, h, l, k), at(xs[0], y, h, l, k)
    north, south = at(x, ys[1], h, l, k), at(x, ys[0], h, l, k)
    mate = at(x, y, h, l, 1 - k)
    flip = at(x, y, h, 1 - l, k)
    across = at(x, y, 1 - h, 1 - l, k)
    opposite = at(x, y, 1 - h, l, k)
    me = 2 * x + k

    def remote(src, dst, send, recv, device):
        return pltpu.make_async_remote_copy(
            src_ref=src,
            dst_ref=dst,
            send_sem=send,
            recv_sem=recv,
            device_id=device,
            device_id_type=MESH,
        )

    copies = [
        pltpu.make_async_copy(ref, spot, load.at[i])
        for i, (ref, spot) in enumerate(
            (
                (tokens, xg.at[k * 4 + x, 0, home]),
                (gate_weight, wf.at[y, 0]),
                (up_weight, wf.at[y, 1]),
                (grads, xg.at[k * 4 + x, 1, home]),
                (down_weight, df.at[y]),
            )
        )
    ]
    for copy in copies:
        copy.start()

    barrier = pltpu.get_barrier_semaphore()
    for j in range(1, 16):
        pl.semaphore_signal(
            barrier, inc=1, device_id=(f, lax.rem(t + j, 16)), device_id_type=MESH
        )
    for peer in (north, south, opposite, across):
        pl.semaphore_signal(barrier, inc=1, device_id=peer, device_id_type=MESH)
    pl.semaphore_wait(barrier, 19)

    for copy in copies:
        copy.wait()

    def w_spot(o, w, q):
        if w == 2:
            return df.at[o, pl.ds(q * (width // 2), width // 2)]
        return wf.at[o, w, pl.ds(q * (deep // 2), deep // 2)]

    def w_out(way, w, q):
        return remote(
            w_spot(y, w, q),
            w_spot(y, w, q),
            y_send.at[way, w, q],
            y_recv.at[way, w, q],
            (north, south)[way],
        )

    def w_on(w, q):
        here = w_spot(ys[q], w, q)
        return remote(here, here, y_send.at[2, w, q], y_recv.at[2, w, q], (north, south)[q])

    def w_in(d, w, q):
        here = w_spot(ys[d], w, q)
        return remote(here, here, y_send.at[2, w, q], y_recv.at[d, w, q], north)

    def w_start(w):
        for way, q in ((0, 0), (1, 1), (0, 1), (1, 0)):
            w_out(way, w, q).start()

    def w_forward(w):
        for q in range(2):
            w_in(q, w, q).wait_recv()
            w_on(w, q).start()

    def w_rest(w):
        for q in range(2):
            w_in(1 - q, w, q).wait_recv()
            w_in(2, w, q).wait_recv()

    slot = (h, 1 - h)

    def x_own(m, q):
        return xg.at[k * 4 + x, m, home, pl.ds(q * zpart, zpart)]

    def x_spot(p, o, j, m, q):
        return xg.at[p * 4 + o, m, slot[j], pl.ds(q * zpart, zpart)]

    def z_out(m, q, device, j):
        spot = xg.at[k * 4 + x, m, h, pl.ds(q * zpart, zpart)]
        return remote(x_own(m, q), spot, z_send.at[0, m, q], z_recv.at[j, m, q], device)

    def z_on(m, q):
        here = x_spot(k, x, 1, m, q)
        return remote(here, here, z_send.at[1, m, q], z_recv.at[1, m, q], flip)

    def z_in(j, m, q):
        here = x_spot(k, x, j, m, q)
        return remote(here, here, z_send.at[0, m, q], z_recv.at[j, m, q], flip)

    def x_out(way, src, j, m, q):
        return remote(
            src,
            x_spot(k, x, j, m, q),
            x_send.at[way, j, m, q],
            x_recv.at[way, j, m, q],
            (right, left)[way],
        )

    def x_on(j, m, q):
        here = x_spot(k, xs[q], j, m, q)
        return remote(
            here, here, x_send.at[2, j, m, q], x_recv.at[2, j, m, q], (right, left)[q]
        )

    def x_in(d, j, m, q):
        here = x_spot(k, xs[d], j, m, q)
        return remote(here, here, x_send.at[2, j, m, q], x_recv.at[d, j, m, q], right)

    places = (*xs, x)

    def p_out(d, src, j, m, q):
        return remote(
            src,
            x_spot(k, places[d], j, m, q),
            p_send.at[d, j, m, q],
            p_recv.at[d, j, m, q],
            mate,
        )

    def p_in(d, j, m, q):
        here = x_spot(1 - k, places[d], j, m, q)
        return remote(here, here, p_send.at[d, j, m, q], p_recv.at[d, j, m, q], mate)

    def spread(src, j, m, q):
        for way in (0, 1) if q == 0 else (1, 0):
            x_out(way, src, j, m, q).start()
        p_out(3, src, j, m, q).start()

    def passed(d, j, m, q):
        x_in(d, j, m, q).wait_recv()
        if d == q:
            x_on(j, m, q).start()
        p_out(d, x_spot(k, places[d], j, m, q), j, m, q).start()

    def z_forward(m, q):
        @pl.when(inner)
        def _():
            z_in(1, m, q).wait_recv()
            z_on(m, q).start()

    def z_spread(m, q, own_too):
        @pl.when(inner)
        def _():
            z_in(0, m, q).wait_recv()
            spread(x_spot(k, x, 0, m, q), 0, m, q)

        @pl.when(outer)
        def _():
            if own_too:
                spread(x_own(m, q), 0, m, q)
            z_in(1, m, q).wait_recv()

        spread(x_spot(k, x, 1, m, q), 1, m, q)

    def v_spot(o, m, q):
        return xg.at[k * 4 + o, m, home, pl.ds(2 * zpart + q * xpart, xpart)]

    def v_out(way, m, q):
        here = v_spot(x, m, q)
        return remote(
            here, here, v_send.at[way, m, q], v_recv.at[way, m, q], (right, left)[way]
        )

    def v_on(m, q):
        here = v_spot(xs[q], m, q)
        return remote(here, here, v_send.at[2, m, q], v_recv.at[2, m, q], (right, left)[q])

    def v_in(d, m, q):
        here = v_spot(xs[d], m, q)
        return remote(here, here, v_send.at[2, m, q], v_recv.at[d, m, q], right)

    def zx_spot(p, d, m, at_s):
        return xg.at[p * 4 + places[d], m, at_s, pl.ds(2 * zpart, XFIRST)]

    def zx_out(d, m, device, j):
        return remote(
            zx_spot(k, d, m, home),
            zx_spot(k, d, m, h),
            zx_send.at[0, d, m],
            zx_recv.at[j, d, m],
            device,
        )

    def zx_on(d, m):
        here = zx_spot(k, d, m, 1 - h)
        return remote(here, here, zx_send.at[1, d, m], zx_recv.at[1, d, m], flip)

    def zx_in(j, d, m):
        here = zx_spot(k, d, m, slot[j])
        return remote(here, here, zx_send.at[0, d, m], zx_recv.at[j, d, m], flip)

    def px_out(d, j, m):
        here = zx_spot(k, d, m, slot[j])
        return remote(here, here, px_send.at[d, j, m], px_recv.at[d, j, m], mate)

    def px_in(d, j, m):
        here = zx_spot(1 - k, d, m, slot[j])
        return remote(here, here, px_send.at[d, j, m], px_recv.at[d, j, m], mate)

    def v_start(m):
        for q in range(2):
            for way in (0, 1) if q == 0 else (1, 0):
                v_out(way, m, q).start()

    def v_near(m):
        for q in range(2):
            v_in(q, m, q).wait_recv()
            v_on(m, q).start()
        for q in range(2):
            v_in(1 - q, m, q).wait_recv()

    def v_far(m):
        for q in range(2):
            v_in(2, m, q).wait_recv()

    def zx_start(m, ds):
        for d in ds:

            @pl.when(outer)
            def _(d=d):
                zx_out(d, m, flip, 0).start()
                px_out(d, 0, m).start()

            @pl.when(inner)
            def _(d=d):
                zx_out(d, m, across, 1).start()

    def zx_take(m, ds):
        for d in ds:

            @pl.when(inner)
            def _(d=d):
                zx_in(1, d, m).wait_recv()
                zx_on(d, m).start()
                px_out(d, 1, m).start()
                zx_in(0, d, m).wait_recv()
                px_out(d, 0, m).start()

            @pl.when(outer)
            def _(d=d):
                zx_in(1, d, m).wait_recv()
                px_out(d, 1, m).start()

    def z_start(m):
        @pl.when(outer)
        def _():
            for q in range(2):
                z_out(m, q, flip, 0).start()

        @pl.when(inner)
        def _():
            for q in range(2):
                z_out(m, q, across, 1).start()

    v_start(0)
    z_start(0)

    @pl.when(outer)
    def _():
        for q in range(2):
            spread(x_own(0, q), 0, 0, q)

    zx_start(0, (3,))
    w_start(0)
    w_start(1)

    v_near(0)
    zx_start(0, (0, 1))
    z_forward(0, 0)
    z_spread(0, 0, False)
    v_far(0)
    zx_start(0, (2,))
    z_start(1)
    v_start(1)
    zx_start(1, (3,))
    z_forward(0, 1)
    z_spread(0, 1, False)
    w_forward(0)
    for j in range(2):
        passed(0, j, 0, 0)
        passed(1, j, 0, 0)
    zx_take(0, (3, 0, 1))
    v_near(1)
    zx_start(1, (0, 1))
    z_forward(1, 0)
    w_forward(1)
    w_start(2)
    for j in range(2):
        passed(1, j, 0, 1)
        passed(0, j, 0, 1)
    zx_take(0, (2,))
    v_far(1)
    zx_start(1, (2,))
    z_forward(1, 1)
    w_rest(0)
    w_rest(1)
    quarter = shard // 4

    def t_rows(u):
        return pl.ds(lax.rem(u, 2) * shard + y * quarter, quarter)

    def t_out(j):
        u = lax.rem(me + j, 8)
        return remote(
            wf.at[lax.div(u, 2), :, t_rows(u)],
            tw.at[me, :, pl.ds(y * quarter, quarter)],
            t_send.at[j],
            t_recv.at[j],
            (f, l * 8 + u),
        )

    def t_in(j):
        u = lax.rem(me + 8 - j, 8)
        spot = tw.at[u, :, pl.ds(y * quarter, quarter)]
        return remote(spot, spot, t_send.at[j], t_recv.at[j], (f, l * 8 + u))

    def u_spot(o, q):
        return tw.at[pl.ds(q * 4, 4), :, pl.ds(o * quarter, quarter)]

    def u_out(way, q):
        here = u_spot(y, q)
        return remote(here, here, u_send.at[way, q], u_recv.at[way, q], (north, south)[way])

    def u_on(q):
        here = u_spot(ys[q], q)
        return remote(here, here, u_send.at[2, q], u_recv.at[2, q], (north, south)[q])

    def u_in(d, q):
        here = u_spot(ys[d], q)
        return remote(here, here, u_send.at[2, q], u_recv.at[d, q], north)

    @pl.loop(1, 8)
    def _(j):
        t_out(j).start()

    tw[me, :, pl.ds(y * quarter, quarter)] = wf[x, :, t_rows(me)]
    for q in range(2):
        z_spread(1, q, True)
    tall = 2 * rows

    def block(m, o):
        return jnp.concatenate(
            [xg[p * 4 + o, m, :2].reshape(tall, shard) for p in range(2)], axis=1
        )

    def pair_in(d, m):
        for q in range(2):
            for j in range(2):
                p_in(d, j, m, q).wait_recv()
        for j in range(2):
            px_in(d, j, m).wait_recv()

    def gate_up(d):
        o = places[d]
        weights = jnp.concatenate([wf[o, 0], wf[o, 1]], axis=1)
        term = jnp.dot(block(0, o), weights, preferred_element_type=F32)
        sa[...] = term if d == 3 else sa[...] + term

    for d in (3, 0, 1):
        pair_in(d, 0)
        gate_up(d)
    for q in range(2):
        for j in range(2):
            passed(2, j, 0, q)
    pair_in(2, 0)
    gate_up(2)
    def swap(src, dst, send, recv):
        def copy(c):
            at_c = pl.ds(c * rows, rows)
            return remote(src.at[at_c], dst.at[at_c], send.at[c], recv.at[c], opposite)

        return copy

    a_swap = swap(sa, zla, a_send, a_recv)
    b_swap = swap(sb, zlb, b_send, b_recv)

    for j in range(2):
        passed(0, j, 1, 0)
        passed(1, j, 1, 0)
        if j == 0:
            for c in range(2):
                a_swap(c).start()
    zx_take(1, (3, 0, 1, 2))
    w_forward(2)
    for j in range(2):
        passed(1, j, 1, 1)
        passed(0, j, 1, 1)

    @pl.loop(1, 8)
    def _(j):
        t_in(j).wait_recv()

    for way, q in ((0, 0), (1, 1), (0, 1), (1, 0)):
        u_out(way, q).start()
    for c in range(2):
        a_swap(c).wait_recv()
    sums = sa[...] + zla[...]
    gate, up = sums[:, :width], sums[:, width:]
    squashed = jax.nn.sigmoid(gate)
    activated = gate * squashed
    slope = squashed * (1.0 + gate * (1.0 - squashed))
    acts[:, :width] = up * slope
    acts[:, width:] = activated
    hidden[...] = (activated * up).astype(BF16)

    def grad_in(d):
        o = places[d]
        term = lax.dot_general(
            block(1, o), df[o], (COLS, ((), ())), preferred_element_type=F32
        )
        sb[...] = term if d == 3 else sb[...] + term

    w_rest(2)
    for d in (3, 0, 1):
        pair_in(d, 1)
        grad_in(d)
    for q in range(2):
        for j in range(2):
            passed(2, j, 1, q)
    pair_in(2, 1)
    grad_in(2)
    def down_part(o):
        return lax.dot_general(
            hidden[...], block(1, o), (ROWS, ((), ())), preferred_element_type=F32
        )

    def gate_part(o):
        return lax.dot_general(
            block(0, o), dg[me], (ROWS, ((), ())), preferred_element_type=F32
        )

    twos, mids, parts, ones, lands = (
        (dtwo, gtwo),
        (dmid, gmid),
        (dpart, gpart),
        (done, gone),
        (dland, gland),
    )

    def halves(i, q):
        size = twos[i].shape[0] // 2
        return pl.ds(q * size, size)

    def two_out(i, q):
        return remote(
            twos[i].at[halves(i, q)],
            mids[i].at[q],
            two_send.at[i, q],
            two_recv.at[i, q],
            (north, south)[q],
        )

    def one_out(i, way, q):
        return remote(
            ones[i].at[way, halves(i, q)],
            lands[i].at[way, halves(i, q)],
            one_send.at[i, way, q],
            one_recv.at[i, way, q],
            (north, south)[way],
        )

    def one_parts(i, fn):
        for way in range(2):
            q = way
            term = fn(ys[1 - way])
            size = term.shape[0] // 2
            parts[i][way] = term[q * size : (q + 1) * size]
            ones[i][way, halves(i, 1 - q)] = term[(1 - q) * size : (2 - q) * size].astype(BF16)

    def one_merge(i):
        for way in range(2):
            two_out(i, way).wait_recv()
            ones[i][way, halves(i, way)] = (
                parts[i][way] + mids[i][way].astype(F32)
            ).astype(BF16)

    def finals(i):
        for way in range(2):
            for q in range(2):
                one_out(i, way, q).wait_recv()
        return lands[i][0].astype(F32) + lands[i][1].astype(F32)

    dtwo[...] = down_part(ys[2]).astype(BF16)
    for c in range(2):
        b_swap(c).start()
    one_parts(0, down_part)
    for q in range(2):
        two_out(0, q).start()
    for way in range(2):
        one_out(0, way, 1 - way).start()
    for q in range(2):
        u_in(q, q).wait_recv()
        u_on(q).start()
    down_own[...] = down_part(y)

    for c in range(2):
        b_swap(c).wait_recv()

    hidden_grad = sb[...] + zlb[...]
    dg[me, :, :width] = (hidden_grad * acts[:, :width]).astype(BF16)
    dg[me, :, width:] = (hidden_grad * acts[:, width:]).astype(BF16)
    gtwo[...] = gate_part(ys[2]).astype(BF16)

    turn = (1 - l, l)

    def d_spot(c, o, e, q):
        return dg.at[o * 2 + c, pl.ds(turn[e] * rows + q * part, part)]

    def dx_out(way, e, q):
        here = d_spot(k, x, e, q)
        return remote(
            here, here, dx_send.at[way, e, q], dx_recv.at[way, e, q], (right, left)[way]
        )

    def dx_on(e, q):
        here = d_spot(k, xs[q], e, q)
        return remote(here, here, dx_send.at[2, e, q], dx_recv.at[2, e, q], (right, left)[q])

    def dx_in(d, e, q):
        here = d_spot(k, xs[d], e, q)
        return remote(here, here, dx_send.at[2, e, q], dx_recv.at[d, e, q], right)

    def dp_out(d, e, q):
        here = d_spot(k, places[d], e, q)
        return remote(here, here, dp_send.at[d, e, q], dp_recv.at[d, e, q], mate)

    def dp_in(d, e, q):
        here = d_spot(1 - k, places[d], e, q)
        return remote(here, here, dp_send.at[d, e, q], dp_recv.at[d, e, q], mate)

    def d_start(e):
        for q in range(2):
            for way in (0, 1) if q == 0 else (1, 0):
                dx_out(way, e, q).start()
            dp_out(3, e, q).start()

    def d_passed(d, e, q):
        dx_in(d, e, q).wait_recv()
        if d == q:
            dx_on(e, q).start()
        dp_out(d, e, q).start()

    def d_near(e):
        for q in range(2):
            d_passed(q, e, q)
        for q in range(2):
            d_passed(1 - q, e, q)

    def gather(d, e):
        base = places[d] * 2
        at_s = pl.ds(turn[e] * rows, rows)
        left_side = jnp.concatenate([dg[base, at_s], dg[base + 1, at_s]], axis=1)
        right_side = jnp.concatenate(
            [tw[base, 0], tw[base, 1], tw[base + 1, 0], tw[base + 1, 1]], axis=1
        )
        term = lax.dot_general(
            left_side, right_side, (COLS, ((), ())), preferred_element_type=F32
        )
        total[e] = term if d == 3 else total[e] + term

    def gathers(e, ds):
        for d in ds:
            for q in range(2):
                dp_in(d, e, q).wait_recv()
            gather(d, e)

    piece = rows // 4

    def f_out(c):
        at_c = pl.ds(c * piece, piece)
        return remote(total.at[0, at_c], near.at[at_c], f_send.at[c], f_recv.at[c], flip)

    def r_out(c):
        at_c = pl.ds(c * piece, piece)
        return remote(rounded.at[at_c], result.at[at_c], r_send.at[c], r_recv.at[c], across)

    d_start(0)
    one_parts(1, gate_part)
    for q in range(2):
        two_out(1, q).start()
    for way in range(2):
        one_out(1, way, 1 - way).start()
    gown[...] = gate_part(y)
    d_near(0)
    d_start(1)
    one_merge(0)
    for q in range(2):
        u_in(1 - q, q).wait_recv()
        u_in(2, q).wait_recv()
    for way in range(2):
        one_out(0, way, way).start()
    gathers(0, (3, 0, 1))
    for q in range(2):
        d_passed(2, 0, q)
    gathers(0, (2,))
    d_near(1)
    for c in range(4):
        f_out(c).start()
    one_merge(1)
    gathers(1, (3,))
    for way in range(2):
        one_out(1, way, way).start()
    gathers(1, (0, 1))
    for q in range(2):
        d_passed(2, 1, q)
    gathers(1, (2,))
    down_own[...] = factor * (down_own[...] + finals(0))
    keeps = [
        pltpu.make_async_copy(src, dst, keep.at[i])
        for i, (src, dst) in enumerate(
            ((down_own, down_out), (gate_own, gate_out), (up_own, up_out), (rounded, result))
        )
    ]
    keeps[0].start()
    for c in range(4):
        f_out(c).wait_recv()
        at_c = pl.ds(c * piece, piece)
        rounded[at_c] = (total[1, at_c] + near[at_c]).astype(BF16)

        if c:

            @pl.when(inner)
            def _(c=c):
                r_out(c - 1).start()

    both = factor * (gown[...] + finals(1))
    gate_own[...] = both[:, :width]
    up_own[...] = both[:, width:]
    @pl.when(inner)
    def _():
        r_out(3).start()

    @pl.when(outer)
    def _():
        keeps[3].start()

    for copy in keeps[1:3]:
        copy.start()

    for m in range(2):
        for d in range(4):
            zx_in(0, d, m).wait_send()
            for j in range(2):
                px_out(d, j, m).wait_send()

            @pl.when(inner)
            def _(d=d, m=m):
                zx_on(d, m).wait_send()

        for q in range(2):
            for way in range(2):
                v_out(way, m, q).wait_send()
            v_on(m, q).wait_send()
            z_in(0, m, q).wait_send()

            @pl.when(inner)
            def _(m=m, q=q):
                z_on(m, q).wait_send()

            for j in range(2):
                for way in range(2):
                    x_out(way, x_own(m, q), j, m, q).wait_send()
                x_on(j, m, q).wait_send()
                for d in range(4):
                    p_out(d, x_own(m, q), j, m, q).wait_send()
    for w in range(3):
        for q in range(2):
            for way in range(2):
                w_out(way, w, q).wait_send()
            w_on(w, q).wait_send()
    for c in range(2):
        for copy in (a_swap(c), b_swap(c), f_out(c), f_out(2 + c)):
            copy.wait_send()
        for i in range(2):
            two_out(i, c).wait_send()
            for q in range(2):
                one_out(i, c, q).wait_send()
        for way in range(2):
            u_out(way, c).wait_send()
        u_on(c).wait_send()
        for e in range(2):
            for way in range(2):
                dx_out(way, e, c).wait_send()
            dx_on(e, c).wait_send()
            for d in range(4):
                dp_out(d, e, c).wait_send()

    @pl.loop(1, 8)
    def _(j):
        t_out(j).wait_send()

    @pl.when(inner)
    def _():
        for c in range(4):
            r_out(c).wait()

    @pl.when(outer)
    def _():
        keeps[3].wait()

    for copy in keeps[:3]:
        copy.wait()


def store_kernel(*refs):
    found, kept, held, sem = refs[:4], refs[4:8], refs[8:12], refs[12]
    loads = [pltpu.make_async_copy(found[i], held[i], sem.at[0, i]) for i in range(4)]
    stores = [pltpu.make_async_copy(held[i], kept[i], sem.at[1, i]) for i in range(4)]
    for copy in loads:
        copy.start()
    for i in range(4):
        loads[i].wait()
        stores[i].start()
    for copy in stores:
        copy.wait()


HBM = pl.BlockSpec(memory_space=pltpu.HBM)
DMA = pltpu.SemaphoreType.DMA


def body(tokens, out_grad, gate_weight, up_weight, down_weight):
    nf, nt = lax.axis_size("fsdp"), lax.axis_size("tp")
    rows, shard = tokens.shape
    deep, width = gate_weight.shape
    assert nf == 8 and nt == 16 and deep == 2 * shard
    factor = 1.0 / math.sqrt(rows * nf)
    tall = 2 * rows
    wide = 2 * width

    shapes = (
        jax.ShapeDtypeStruct((rows, shard), BF16),
        jax.ShapeDtypeStruct((deep, width), F32),
        jax.ShapeDtypeStruct((deep, width), F32),
        jax.ShapeDtypeStruct((width, deep), F32),
    )
    found = tuple(
        pl.pallas_call(
            functools.partial(kernel, factor),
            out_shape=shapes,
            in_specs=[HBM] * 5,
            out_specs=(HBM,) * 4,
            scratch_shapes=[
                pltpu.VMEM((deep, width), F32),
                pltpu.VMEM((deep, width), F32),
                pltpu.VMEM((width, deep), F32),
                pltpu.VMEM((8, 2, 3, rows, shard), BF16),
                pltpu.VMEM((4, 2, deep, width), BF16),
                pltpu.VMEM((4, width, deep), BF16),
                pltpu.VMEM((tall, wide), F32),
                pltpu.VMEM((tall, wide), F32),
                pltpu.VMEM((tall, width), F32),
                pltpu.VMEM((tall, width), F32),
                pltpu.VMEM((tall, wide), F32),
                pltpu.VMEM((tall, width), BF16),
                pltpu.VMEM((8, tall, wide), BF16),
                pltpu.VMEM((8, 2, shard, width), BF16),
                pltpu.VMEM((2, width // 2, deep), F32),
                pltpu.VMEM((2, deep // 2, wide), F32),
                pltpu.VMEM((width, deep), BF16),
                pltpu.VMEM((deep, wide), BF16),
                pltpu.VMEM((2, width, deep), BF16),
                pltpu.VMEM((2, deep, wide), BF16),
                pltpu.VMEM((2, width // 2, deep), BF16),
                pltpu.VMEM((2, deep // 2, wide), BF16),
                pltpu.VMEM((2, width, deep), BF16),
                pltpu.VMEM((2, deep, wide), BF16),
                pltpu.VMEM((deep, wide), F32),
                pltpu.VMEM((2, rows, shard), F32),
                pltpu.VMEM((rows, shard), F32),
                pltpu.VMEM((rows, shard), BF16),
                DMA((5,)),
                DMA((4,)),
                DMA((2, 2, 2)),
                DMA((2, 2, 2)),
                DMA((3, 2, 2, 2)),
                DMA((3, 2, 2, 2)),
                DMA((4, 2, 2, 2)),
                DMA((4, 2, 2, 2)),
                DMA((3, 2, 2)),
                DMA((3, 2, 2)),
                DMA((2, 4, 2)),
                DMA((2, 4, 2)),
                DMA((4, 2, 2)),
                DMA((4, 2, 2)),
                DMA((3, 3, 2)),
                DMA((3, 3, 2)),
                DMA((2,)),
                DMA((2,)),
                DMA((2,)),
                DMA((2,)),
                DMA((8,)),
                DMA((8,)),
                DMA((3, 2)),
                DMA((3, 2)),
                DMA((4,)),
                DMA((4,)),
                DMA((3, 2, 2)),
                DMA((3, 2, 2)),
                DMA((4, 2, 2)),
                DMA((4, 2, 2)),
                DMA((2, 2)),
                DMA((2, 2)),
                DMA((2, 2, 2)),
                DMA((2, 2, 2)),
                DMA((4,)),
                DMA((4,)),
            ],
            compiler_params=pltpu.CompilerParams(
                collective_id=0, has_side_effects=True, vmem_limit_bytes=VMEM_LIMIT
            ),
            name="block",
        )(tokens, out_grad, gate_weight, up_weight, down_weight)
    )
    return tuple(
        pl.pallas_call(
            store_kernel,
            out_shape=shapes,
            in_specs=[HBM] * 4,
            out_specs=(HBM,) * 4,
            scratch_shapes=[pltpu.VMEM(s.shape, s.dtype) for s in shapes] + [DMA((2, 4))],
            compiler_params=pltpu.CompilerParams(vmem_limit_bytes=VMEM_LIMIT),
            name="store",
        )(*found)
    )


def solution(mesh):
    return jax.shard_map(
        body,
        mesh=mesh,
        in_specs=(
            P("fsdp", "tp"),
            P("fsdp", "tp"),
            P("fsdp", "tp"),
            P("fsdp", "tp"),
            P("tp", "fsdp"),
        ),
        out_specs=(P("fsdp", "tp"), P("fsdp", "tp"), P("fsdp", "tp"), P("tp", "fsdp")),
        check_vma=False,
    )
```

```python
import functools
import math

import jax
import jax.numpy as jnp
from jax import lax
from jax.sharding import PartitionSpec as P
from jax.experimental import pallas as pl
from jax.experimental.pallas import tpu as pltpu

MESH = pl.DeviceIdType.MESH
F32 = jnp.float32
BF16 = jnp.bfloat16
VMEM_LIMIT = 60 * 1024 * 1024
XFIRST = 32
ROWS = ((0,), (0,))
COLS = ((1,), (1,))


def kernel(
    factor,
    tokens,
    grads,
    gate_weight,
    up_weight,
    down_weight,
    result,
    gate_out,
    up_out,
    down_out,
    gate_own,
    up_own,
    down_own,
    xg,
    wf,
    df,
    sa,
    zla,
    sb,
    zlb,
    acts,
    hidden,
    dg,
    tw,
    dpart,
    gpart,
    dtwo,
    gtwo,
    done,
    gone,
    dmid,
    gmid,
    dland,
    gland,
    gown,
    total,
    near,
    rounded,
    load,
    keep,
    z_send,
    z_recv,
    x_send,
    x_recv,
    p_send,
    p_recv,
    v_send,
    v_recv,
    zx_send,
    zx_recv,
    px_send,
    px_recv,
    y_send,
    y_recv,
    a_send,
    a_recv,
    b_send,
    b_recv,
    t_send,
    t_recv,
    u_send,
    u_recv,
    g_send,
    g_recv,
    f_send,
    f_recv,
    dx_send,
    dx_recv,
    dp_send,
    dp_recv,
    two_send,
    two_recv,
    one_send,
    one_recv,
    r_send,
    r_recv,
):
    f, t = lax.axis_index("fsdp"), lax.axis_index("tp")
    h, y = lax.div(f, 4), lax.rem(f, 4)
    l, x, k = lax.div(t, 8), lax.rem(lax.div(t, 2), 4), lax.rem(t, 2)
    outer = h == l
    inner = h != l
    rows, shard = tokens.shape
    deep, width = gate_weight.shape
    part = rows // 2
    zparts = ((rows - XFIRST) // 2, part)
    first = rows - XFIRST
    xpart = XFIRST // 2
    odd = (h - l) * (h - l)
    home = h * (1 - odd) + 2 * odd
    wide = 2 * width

    def at(xx, yy, hh, ll, kk):
        return (hh * 4 + yy, ll * 8 + xx * 2 + kk)

    xs = (lax.rem(x + 3, 4), lax.rem(x + 1, 4), lax.rem(x + 2, 4))
    ys = (lax.rem(y + 3, 4), lax.rem(y + 1, 4), lax.rem(y + 2, 4))
    right, left = at(xs[1], y, h, l, k), at(xs[0], y, h, l, k)
    north, south = at(x, ys[1], h, l, k), at(x, ys[0], h, l, k)
    mate = at(x, y, h, l, 1 - k)
    flip = at(x, y, h, 1 - l, k)
    across = at(x, y, 1 - h, 1 - l, k)
    opposite = at(x, y, 1 - h, l, k)
    me = 2 * x + k

    def remote(src, dst, send, recv, device):
        return pltpu.make_async_remote_copy(
            src_ref=src,
            dst_ref=dst,
            send_sem=send,
            recv_sem=recv,
            device_id=device,
            device_id_type=MESH,
        )

    copies = [
        pltpu.make_async_copy(ref, spot, load.at[i])
        for i, (ref, spot) in enumerate(
            (
                (tokens, xg.at[k * 4 + x, 0, home]),
                (gate_weight, wf.at[y, 0]),
                (up_weight, wf.at[y, 1]),
                (grads, xg.at[k * 4 + x, 1, home]),
                (down_weight, df.at[y]),
            )
        )
    ]
    for copy in copies:
        copy.start()

    barrier = pltpu.get_barrier_semaphore()
    for j in range(1, 16):
        pl.semaphore_signal(
            barrier, inc=1, device_id=(f, lax.rem(t + j, 16)), device_id_type=MESH
        )
    for peer in (north, south, opposite, across):
        pl.semaphore_signal(barrier, inc=1, device_id=peer, device_id_type=MESH)
    pl.semaphore_wait(barrier, 19)

    for copy in copies:
        copy.wait()

    def w_spot(o, w, q):
        if w == 2:
            return df.at[o, pl.ds(q * (width // 2), width // 2)]
        return wf.at[o, w, pl.ds(q * (deep // 2), deep // 2)]

    def w_out(way, w, q):
        return remote(
            w_spot(y, w, q),
            w_spot(y, w, q),
            y_send.at[way, w, q],
            y_recv.at[way, w, q],
            (north, south)[way],
        )

    def w_on(w, q):
        here = w_spot(ys[q], w, q)
        return remote(here, here, y_send.at[2, w, q], y_recv.at[2, w, q], (north, south)[q])

    def w_in(d, w, q):
        here = w_spot(ys[d], w, q)
        return remote(here, here, y_send.at[2, w, q], y_recv.at[d, w, q], north)

    def w_start(w):
        for way, q in ((0, 0), (1, 1), (0, 1), (1, 0)):
            w_out(way, w, q).start()

    def w_forward(w):
        for q in range(2):
            w_in(q, w, q).wait_recv()
            w_on(w, q).start()

    def w_rest(w):
        for q in range(2):
            w_in(1 - q, w, q).wait_recv()
            w_in(2, w, q).wait_recv()

    slot = (h, 1 - h)

    def x_own(m, q):
        return xg.at[k * 4 + x, m, home, pl.ds(q * zparts[m], zparts[m])]

    def x_spot(p, o, j, m, q):
        return xg.at[p * 4 + o, m, slot[j], pl.ds(q * zparts[m], zparts[m])]

    def z_out(m, q, device, j):
        spot = xg.at[k * 4 + x, m, h, pl.ds(q * zparts[m], zparts[m])]
        return remote(x_own(m, q), spot, z_send.at[0, m, q], z_recv.at[j, m, q], device)

    def z_on(m, q):
        here = x_spot(k, x, 1, m, q)
        return remote(here, here, z_send.at[1, m, q], z_recv.at[1, m, q], flip)

    def z_in(j, m, q):
        here = x_spot(k, x, j, m, q)
        return remote(here, here, z_send.at[0, m, q], z_recv.at[j, m, q], flip)

    def x_out(way, src, j, m, q):
        return remote(
            src,
            x_spot(k, x, j, m, q),
            x_send.at[way, j, m, q],
            x_recv.at[way, j, m, q],
            (right, left)[way],
        )

    def x_on(j, m, q):
        here = x_spot(k, xs[q], j, m, q)
        return remote(
            here, here, x_send.at[2, j, m, q], x_recv.at[2, j, m, q], (right, left)[q]
        )

    def x_in(d, j, m, q):
        here = x_spot(k, xs[d], j, m, q)
        return remote(here, here, x_send.at[2, j, m, q], x_recv.at[d, j, m, q], right)

    places = (*xs, x)

    def p_out(d, src, j, m, q):
        return remote(
            src,
            x_spot(k, places[d], j, m, q),
            p_send.at[d, j, m, q],
            p_recv.at[d, j, m, q],
            mate,
        )

    def p_in(d, j, m, q):
        here = x_spot(1 - k, places[d], j, m, q)
        return remote(here, here, p_send.at[d, j, m, q], p_recv.at[d, j, m, q], mate)

    def spread(src, j, m, q):
        for way in (0, 1) if q == 0 else (1, 0):
            x_out(way, src, j, m, q).start()
        p_out(3, src, j, m, q).start()

    def passed(d, j, m, q):
        x_in(d, j, m, q).wait_recv()
        if d == q:
            x_on(j, m, q).start()
        p_out(d, x_spot(k, places[d], j, m, q), j, m, q).start()

    def z_forward(m, q):
        @pl.when(inner)
        def _():
            z_in(1, m, q).wait_recv()
            z_on(m, q).start()

    def z_near(m, q):
        @pl.when(inner)
        def _():
            z_in(0, m, q).wait_recv()

        spread(x_spot(k, x, 0, m, q), 0, m, q)

    def z_far(m, q):
        @pl.when(outer)
        def _():
            z_in(1, m, q).wait_recv()

        spread(x_spot(k, x, 1, m, q), 1, m, q)

    def z_near_inner(m, q):
        @pl.when(inner)
        def _():
            z_in(0, m, q).wait_recv()
            spread(x_spot(k, x, 0, m, q), 0, m, q)

    quarter = shard // 4

    def t_rows(u):
        return pl.ds(lax.rem(u, 2) * shard + y * quarter, quarter)

    def t_out(j):
        u = lax.rem(me + j, 8)
        return remote(
            wf.at[lax.div(u, 2), 0, t_rows(u)],
            tw.at[me, 0, pl.ds(y * quarter, quarter)],
            t_send.at[j],
            t_recv.at[j],
            (f, l * 8 + u),
        )

    def t_in(j):
        u = lax.rem(me + 8 - j, 8)
        spot = tw.at[u, 0, pl.ds(y * quarter, quarter)]
        return remote(spot, spot, t_send.at[j], t_recv.at[j], (f, l * 8 + u))

    def g_rows(u):
        return pl.ds(lax.rem(u, 2) * shard, shard)

    def g_out(j):
        u = lax.rem(me + j, 8)
        return remote(
            wf.at[lax.div(u, 2), 1, g_rows(u)],
            tw.at[me, 1],
            g_send.at[j],
            g_recv.at[j],
            (f, l * 8 + u),
        )

    def g_in(j):
        u = lax.rem(me + 8 - j, 8)
        spot = tw.at[u, 1]
        return remote(spot, spot, g_send.at[j], g_recv.at[j], (f, l * 8 + u))

    def u_spot(o, q):
        return tw.at[pl.ds(q * 4, 4), 0, pl.ds(o * quarter, quarter)]

    def u_out(way, q):
        here = u_spot(y, q)
        return remote(here, here, u_send.at[way, q], u_recv.at[way, q], (north, south)[way])

    def u_on(q):
        here = u_spot(ys[q], q)
        return remote(here, here, u_send.at[2, q], u_recv.at[2, q], (north, south)[q])

    def u_in(d, q):
        here = u_spot(ys[d], q)
        return remote(here, here, u_send.at[2, q], u_recv.at[d, q], north)

    def v_spot(o, q):
        return xg.at[k * 4 + o, 0, home, pl.ds(first + q * xpart, xpart)]

    def v_out(way, q):
        here = v_spot(x, q)
        return remote(
            here, here, v_send.at[way, q], v_recv.at[way, q], (right, left)[way]
        )

    def v_on(q):
        here = v_spot(xs[q], q)
        return remote(here, here, v_send.at[2, q], v_recv.at[2, q], (right, left)[q])

    def v_in(d, q):
        here = v_spot(xs[d], q)
        return remote(here, here, v_send.at[2, q], v_recv.at[d, q], right)

    def zx_spot(p, d, at_s):
        return xg.at[p * 4 + places[d], 0, at_s, pl.ds(first, XFIRST)]

    def zx_out(d, device, j):
        return remote(
            zx_spot(k, d, home),
            zx_spot(k, d, h),
            zx_send.at[0, d],
            zx_recv.at[j, d],
            device,
        )

    def zx_on(d):
        here = zx_spot(k, d, 1 - h)
        return remote(here, here, zx_send.at[1, d], zx_recv.at[1, d], flip)

    def zx_in(j, d):
        here = zx_spot(k, d, slot[j])
        return remote(here, here, zx_send.at[0, d], zx_recv.at[j, d], flip)

    def px_out(d, j):
        here = zx_spot(k, d, slot[j])
        return remote(here, here, px_send.at[d, j], px_recv.at[d, j], mate)

    def px_in(d, j):
        here = zx_spot(1 - k, d, slot[j])
        return remote(here, here, px_send.at[d, j], px_recv.at[d, j], mate)

    def v_start():
        for q in range(2):
            for way in (0, 1) if q == 0 else (1, 0):
                v_out(way, q).start()

    def v_near():
        for q in range(2):
            v_in(q, q).wait_recv()
            v_on(q).start()
        for q in range(2):
            v_in(1 - q, q).wait_recv()

    def v_far():
        for q in range(2):
            v_in(2, q).wait_recv()

    def zx_start(ds):
        for d in ds:

            @pl.when(outer)
            def _(d=d):
                zx_out(d, flip, 0).start()
                px_out(d, 0).start()

            @pl.when(inner)
            def _(d=d):
                zx_out(d, across, 1).start()

    def zx_pass(ds):
        for d in ds:

            @pl.when(inner)
            def _(d=d):
                zx_in(1, d).wait_recv()
                zx_on(d).start()

    def zx_take(ds):
        for d in ds:

            @pl.when(inner)
            def _(d=d):
                zx_in(0, d).wait_recv()
                px_out(d, 0).start()

            @pl.when(outer)
            def _(d=d):
                zx_in(1, d).wait_recv()

            px_out(d, 1).start()

    def z_start(m):
        @pl.when(outer)
        def _():
            for q in range(2):
                z_out(m, q, flip, 0).start()

        @pl.when(inner)
        def _():
            for q in range(2):
                z_out(m, q, across, 1).start()

    v_start()
    z_start(0)

    @pl.when(outer)
    def _():
        for q in range(2):
            spread(x_own(0, q), 0, 0, q)

    zx_start((3,))
    w_start(0)
    w_start(1)

    v_near()
    zx_start((0, 1))
    z_forward(0, 0)
    z_near_inner(0, 0)
    z_far(0, 0)
    v_far()
    zx_start((2,))
    z_start(1)
    z_forward(0, 1)
    z_near_inner(0, 1)
    z_far(0, 1)
    w_forward(0)
    for j in range(2):
        passed(0, j, 0, 0)
        passed(1, j, 0, 0)
    w_forward(1)
    w_start(2)
    for j in range(2):
        passed(1, j, 0, 1)
        passed(0, j, 0, 1)
    z_forward(1, 0)
    zx_pass((3, 0, 1))
    z_forward(1, 1)
    zx_pass((2,))
    z_near(1, 0)
    z_near(1, 1)
    w_rest(0)
    w_rest(1)

    @pl.loop(1, 8)
    def _(j):
        t_out(j).start()

    z_far(1, 0)
    z_far(1, 1)
    w_forward(2)
    zx_take((3, 0, 1, 2))
    tall = 2 * rows

    def block(m, o):
        return jnp.concatenate(
            [xg[p * 4 + o, m, :2].reshape(tall, shard) for p in range(2)], axis=1
        )

    def pair_in(d, m):
        for q in range(2):
            for j in range(2):
                p_in(d, j, m, q).wait_recv()
        if m == 0:
            for j in range(2):
                px_in(d, j).wait_recv()

    def gate_up(d):
        o = places[d]
        weights = jnp.concatenate([wf[o, 0], wf[o, 1]], axis=1)
        term = jnp.dot(block(0, o), weights, preferred_element_type=F32)
        sa[...] = term if d == 3 else sa[...] + term

    for d in (3, 0, 1):
        pair_in(d, 0)
        gate_up(d)
    for q in range(2):
        for j in range(2):
            passed(2, j, 0, q)
    pair_in(2, 0)
    gate_up(2)
    turn = (1 - l, l)

    def swap(src, dst, send, recv):
        def copy(c):
            at_c = pl.ds(turn[c] * rows, rows)
            return remote(src.at[at_c], dst.at[at_c], send.at[c], recv.at[c], opposite)

        return copy

    a_swap = swap(sa, zla, a_send, a_recv)
    b_swap = swap(sb, zlb, b_send, b_recv)

    a_swap(0).start()
    tw[me, 0, pl.ds(y * quarter, quarter)] = wf[x, 0, t_rows(me)]
    tw[me, 1] = wf[x, 1, g_rows(me)]
    a_swap(1).start()
    @pl.loop(1, 8)
    def _(j):
        t_in(j).wait_recv()

    for way, q in ((0, 0), (1, 1), (0, 1), (1, 0)):
        u_out(way, q).start()
    for j in range(2):
        passed(0, j, 1, 0)
        passed(1, j, 1, 0)
    for j in range(2):
        passed(1, j, 1, 1)
        passed(0, j, 1, 1)

    for q in range(2):
        u_in(q, q).wait_recv()
        u_on(q).start()
    def grad_in(d):
        o = places[d]
        term = lax.dot_general(
            block(1, o), df[o], (COLS, ((), ())), preferred_element_type=F32
        )
        sb[...] = term if d == 3 else sb[...] + term

    @pl.loop(1, 8)
    def _(j):
        g_out(j).start()

    w_rest(2)
    for d in (3, 0, 1):
        pair_in(d, 1)
        grad_in(d)
    for q in range(2):
        for j in range(2):
            passed(2, j, 1, q)
    for c in range(2):
        a_swap(c).wait_recv()
    sums = sa[...] + zla[...]
    gate, up = sums[:, :width], sums[:, width:]
    squashed = jax.nn.sigmoid(gate)
    activated = gate * squashed
    slope = squashed * (1.0 + gate * (1.0 - squashed))
    acts[:, :width] = up * slope
    acts[:, width:] = activated
    hidden[...] = (activated * up).astype(BF16)

    pair_in(2, 1)
    for c in range(2):
        at_s = pl.ds(turn[c] * rows, rows)
        last = jnp.concatenate([xg[p * 4 + xs[2], 1, turn[c]] for p in range(2)], axis=1)
        sb[at_s] += lax.dot_general(
            last, df[xs[2]], (COLS, ((), ())), preferred_element_type=F32
        )
        if c:
            b_swap(0).start()
    def down_part(o):
        return lax.dot_general(
            hidden[...], block(1, o), (ROWS, ((), ())), preferred_element_type=F32
        )

    def gate_part(o):
        return lax.dot_general(
            block(0, o), dg[me], (ROWS, ((), ())), preferred_element_type=F32
        )

    twos, mids, parts, ones, lands = (
        (dtwo, gtwo),
        (dmid, gmid),
        (dpart, gpart),
        (done, gone),
        (dland, gland),
    )

    def halves(i, q):
        size = twos[i].shape[0] // 2
        return pl.ds(q * size, size)

    def two_out(i, q):
        return remote(
            twos[i].at[halves(i, q)],
            mids[i].at[q],
            two_send.at[i, q],
            two_recv.at[i, q],
            (north, south)[q],
        )

    def one_out(i, way, q):
        return remote(
            ones[i].at[way, halves(i, q)],
            lands[i].at[way, halves(i, q)],
            one_send.at[i, way, q],
            one_recv.at[i, way, q],
            (north, south)[way],
        )

    def one_parts(i, fn):
        for way in range(2):
            q = way
            term = fn(ys[1 - way])
            size = term.shape[0] // 2
            parts[i][way] = term[q * size : (q + 1) * size]
            ones[i][way, halves(i, 1 - q)] = term[(1 - q) * size : (2 - q) * size].astype(BF16)

    def one_merge(i):
        for way in range(2):
            two_out(i, way).wait_recv()
            ones[i][way, halves(i, way)] = (
                parts[i][way] + mids[i][way].astype(F32)
            ).astype(BF16)

    def finals(i):
        for way in range(2):
            for q in range(2):
                one_out(i, way, q).wait_recv()
        return lands[i][0].astype(F32) + lands[i][1].astype(F32)

    dtwo[...] = down_part(ys[2]).astype(BF16)
    b_swap(1).start()
    one_parts(0, down_part)
    for q in range(2):
        two_out(0, q).start()
    for way in range(2):
        one_out(0, way, 1 - way).start()

    def d_spot(c, o, e, q):
        return dg.at[o * 2 + c, pl.ds(turn[e] * rows + q * part, part)]

    def dx_out(way, e, q):
        here = d_spot(k, x, e, q)
        return remote(
            here, here, dx_send.at[way, e, q], dx_recv.at[way, e, q], (right, left)[way]
        )

    def dx_on(e, q):
        here = d_spot(k, xs[q], e, q)
        return remote(here, here, dx_send.at[2, e, q], dx_recv.at[2, e, q], (right, left)[q])

    def dx_in(d, e, q):
        here = d_spot(k, xs[d], e, q)
        return remote(here, here, dx_send.at[2, e, q], dx_recv.at[d, e, q], right)

    def dp_out(d, e, q):
        here = d_spot(k, places[d], e, q)
        return remote(here, here, dp_send.at[d, e, q], dp_recv.at[d, e, q], mate)

    def dp_in(d, e, q):
        here = d_spot(1 - k, places[d], e, q)
        return remote(here, here, dp_send.at[d, e, q], dp_recv.at[d, e, q], mate)

    def d_start(e):
        for q in range(2):
            for way in (0, 1) if q == 0 else (1, 0):
                dx_out(way, e, q).start()
            dp_out(3, e, q).start()

    def d_passed(d, e, q):
        dx_in(d, e, q).wait_recv()
        if d == q:
            dx_on(e, q).start()
        dp_out(d, e, q).start()

    def d_near(e):
        for q in range(2):
            d_passed(q, e, q)
        for q in range(2):
            d_passed(1 - q, e, q)

    def gather(d, e):
        base = places[d] * 2
        at_s = pl.ds(turn[e] * rows, rows)
        left_side = jnp.concatenate([dg[base, at_s], dg[base + 1, at_s]], axis=1)
        right_side = jnp.concatenate(
            [tw[base, 0], tw[base, 1], tw[base + 1, 0], tw[base + 1, 1]], axis=1
        )
        term = lax.dot_general(
            left_side, right_side, (COLS, ((), ())), preferred_element_type=F32
        )
        total[e] = term if d == 3 else total[e] + term

    def gathers(e, ds):
        for d in ds:
            for q in range(2):
                dp_in(d, e, q).wait_recv()
            gather(d, e)

    piece = rows // 4

    def f_out(c):
        at_c = pl.ds(c * piece, piece)
        return remote(total.at[0, at_c], near.at[at_c], f_send.at[c], f_recv.at[c], flip)

    def r_out(c):
        at_c = pl.ds(c * piece, piece)
        return remote(rounded.at[at_c], result.at[at_c], r_send.at[c], r_recv.at[c], across)

    def delta(e):
        b_swap(e).wait_recv()
        at_s = pl.ds(turn[e] * rows, rows)
        hidden_grad = sb[at_s] + zlb[at_s]
        dg[me, at_s, :width] = (hidden_grad * acts[at_s, :width]).astype(BF16)
        dg[me, at_s, width:] = (hidden_grad * acts[at_s, width:]).astype(BF16)

    delta(0)
    down_own[...] = down_part(y)
    d_start(0)
    delta(1)
    gtwo[...] = gate_part(ys[2]).astype(BF16)
    one_parts(1, gate_part)
    for q in range(2):
        two_out(1, q).start()
    for way in range(2):
        one_out(1, way, 1 - way).start()
    gown[...] = gate_part(y)
    d_near(0)
    d_start(1)
    one_merge(0)
    for q in range(2):
        u_in(1 - q, q).wait_recv()
        u_in(2, q).wait_recv()
    for way in range(2):
        one_out(0, way, way).start()
    @pl.loop(1, 8)
    def _(j):
        g_in(j).wait_recv()

    gathers(0, (3, 0, 1))
    for q in range(2):
        d_passed(2, 0, q)
    gathers(0, (2,))
    for c in range(2):
        f_out(c).start()
    d_near(1)
    for c in range(2, 4):
        f_out(c).start()
    one_merge(1)
    gathers(1, (3,))
    for way in range(2):
        one_out(1, way, way).start()
    gathers(1, (0, 1))
    for q in range(2):
        d_passed(2, 1, q)
    gathers(1, (2,))
    down_own[...] = factor * (down_own[...] + finals(0))
    keeps = [
        pltpu.make_async_copy(src, dst, keep.at[i])
        for i, (src, dst) in enumerate(
            ((down_own, down_out), (gate_own, gate_out), (up_own, up_out), (rounded, result))
        )
    ]
    keeps[0].start()
    for c in range(4):
        f_out(c).wait_recv()
        at_c = pl.ds(c * piece, piece)
        rounded[at_c] = (total[1, at_c] + near[at_c]).astype(BF16)

        if c:

            @pl.when(inner)
            def _(c=c):
                r_out(c - 1).start()

    both = factor * (gown[...] + finals(1))
    gate_own[...] = both[:, :width]
    up_own[...] = both[:, width:]
    @pl.when(inner)
    def _():
        r_out(3).start()

    @pl.when(outer)
    def _():
        keeps[3].start()

    for copy in keeps[1:3]:
        copy.start()

    for d in range(4):
        zx_in(0, d).wait_send()
        for j in range(2):
            px_out(d, j).wait_send()

        @pl.when(inner)
        def _(d=d):
            zx_on(d).wait_send()

    for q in range(2):
        for way in range(2):
            v_out(way, q).wait_send()
        v_on(q).wait_send()
    for m in range(2):
        for q in range(2):
            z_in(0, m, q).wait_send()

            @pl.when(inner)
            def _(m=m, q=q):
                z_on(m, q).wait_send()

            for j in range(2):
                for way in range(2):
                    x_out(way, x_own(m, q), j, m, q).wait_send()
                x_on(j, m, q).wait_send()
                for d in range(4):
                    p_out(d, x_own(m, q), j, m, q).wait_send()
    for w in range(3):
        for q in range(2):
            for way in range(2):
                w_out(way, w, q).wait_send()
            w_on(w, q).wait_send()
    for c in range(2):
        for copy in (a_swap(c), b_swap(c), f_out(c), f_out(2 + c)):
            copy.wait_send()
        for i in range(2):
            two_out(i, c).wait_send()
            for q in range(2):
                one_out(i, c, q).wait_send()
        for way in range(2):
            u_out(way, c).wait_send()
        u_on(c).wait_send()
        for e in range(2):
            for way in range(2):
                dx_out(way, e, c).wait_send()
            dx_on(e, c).wait_send()
            for d in range(4):
                dp_out(d, e, c).wait_send()

    @pl.loop(1, 8)
    def _(j):
        t_out(j).wait_send()
        g_out(j).wait_send()

    @pl.when(inner)
    def _():
        for c in range(4):
            r_out(c).wait()

    @pl.when(outer)
    def _():
        keeps[3].wait()

    for copy in keeps[:3]:
        copy.wait()


def store_kernel(*refs):
    found, kept, held, sem = refs[:4], refs[4:8], refs[8:12], refs[12]
    loads = [pltpu.make_async_copy(found[i], held[i], sem.at[0, i]) for i in range(4)]
    stores = [pltpu.make_async_copy(held[i], kept[i], sem.at[1, i]) for i in range(4)]
    for copy in loads:
        copy.start()
    for i in range(4):
        loads[i].wait()
        stores[i].start()
    for copy in stores:
        copy.wait()


HBM = pl.BlockSpec(memory_space=pltpu.HBM)
DMA = pltpu.SemaphoreType.DMA


def body(tokens, out_grad, gate_weight, up_weight, down_weight):
    nf, nt = lax.axis_size("fsdp"), lax.axis_size("tp")
    rows, shard = tokens.shape
    deep, width = gate_weight.shape
    assert nf == 8 and nt == 16 and deep == 2 * shard
    factor = 1.0 / math.sqrt(rows * nf)
    tall = 2 * rows
    wide = 2 * width

    shapes = (
        jax.ShapeDtypeStruct((rows, shard), BF16),
        jax.ShapeDtypeStruct((deep, width), F32),
        jax.ShapeDtypeStruct((deep, width), F32),
        jax.ShapeDtypeStruct((width, deep), F32),
    )
    found = tuple(
        pl.pallas_call(
            functools.partial(kernel, factor),
            out_shape=shapes,
            in_specs=[HBM] * 5,
            out_specs=(HBM,) * 4,
            scratch_shapes=[
                pltpu.VMEM((deep, width), F32),
                pltpu.VMEM((deep, width), F32),
                pltpu.VMEM((width, deep), F32),
                pltpu.VMEM((8, 2, 3, rows, shard), BF16),
                pltpu.VMEM((4, 2, deep, width), BF16),
                pltpu.VMEM((4, width, deep), BF16),
                pltpu.VMEM((tall, wide), F32),
                pltpu.VMEM((tall, wide), F32),
                pltpu.VMEM((tall, width), F32),
                pltpu.VMEM((tall, width), F32),
                pltpu.VMEM((tall, wide), F32),
                pltpu.VMEM((tall, width), BF16),
                pltpu.VMEM((8, tall, wide), BF16),
                pltpu.VMEM((8, 2, shard, width), BF16),
                pltpu.VMEM((2, width // 2, deep), F32),
                pltpu.VMEM((2, deep // 2, wide), F32),
                pltpu.VMEM((width, deep), BF16),
                pltpu.VMEM((deep, wide), BF16),
                pltpu.VMEM((2, width, deep), BF16),
                pltpu.VMEM((2, deep, wide), BF16),
                pltpu.VMEM((2, width // 2, deep), BF16),
                pltpu.VMEM((2, deep // 2, wide), BF16),
                pltpu.VMEM((2, width, deep), BF16),
                pltpu.VMEM((2, deep, wide), BF16),
                pltpu.VMEM((deep, wide), F32),
                pltpu.VMEM((2, rows, shard), F32),
                pltpu.VMEM((rows, shard), F32),
                pltpu.VMEM((rows, shard), BF16),
                DMA((5,)),
                DMA((4,)),
                DMA((2, 2, 2)),
                DMA((2, 2, 2)),
                DMA((3, 2, 2, 2)),
                DMA((3, 2, 2, 2)),
                DMA((4, 2, 2, 2)),
                DMA((4, 2, 2, 2)),
                DMA((3, 2)),
                DMA((3, 2)),
                DMA((2, 4)),
                DMA((2, 4)),
                DMA((4, 2)),
                DMA((4, 2)),
                DMA((3, 3, 2)),
                DMA((3, 3, 2)),
                DMA((2,)),
                DMA((2,)),
                DMA((2,)),
                DMA((2,)),
                DMA((8,)),
                DMA((8,)),
                DMA((3, 2)),
                DMA((3, 2)),
                DMA((8,)),
                DMA((8,)),
                DMA((4,)),
                DMA((4,)),
                DMA((3, 2, 2)),
                DMA((3, 2, 2)),
                DMA((4, 2, 2)),
                DMA((4, 2, 2)),
                DMA((2, 2)),
                DMA((2, 2)),
                DMA((2, 2, 2)),
                DMA((2, 2, 2)),
                DMA((4,)),
                DMA((4,)),
            ],
            compiler_params=pltpu.CompilerParams(
                collective_id=0, has_side_effects=True, vmem_limit_bytes=VMEM_LIMIT
            ),
            name="block",
        )(tokens, out_grad, gate_weight, up_weight, down_weight)
    )
    return tuple(
        pl.pallas_call(
            store_kernel,
            out_shape=shapes,
            in_specs=[HBM] * 4,
            out_specs=(HBM,) * 4,
            scratch_shapes=[pltpu.VMEM(s.shape, s.dtype) for s in shapes] + [DMA((2, 4))],
            compiler_params=pltpu.CompilerParams(vmem_limit_bytes=VMEM_LIMIT),
            name="store",
        )(*found)
    )


def solution(mesh):
    return jax.shard_map(
        body,
        mesh=mesh,
        in_specs=(
            P("fsdp", "tp"),
            P("fsdp", "tp"),
            P("fsdp", "tp"),
            P("fsdp", "tp"),
            P("tp", "fsdp"),
        ),
        out_specs=(P("fsdp", "tp"), P("fsdp", "tp"), P("fsdp", "tp"), P("tp", "fsdp")),
        check_vma=False,
    )
```

```python
import functools
import math

import jax
import jax.numpy as jnp
from jax import lax
from jax.sharding import PartitionSpec as P
from jax.experimental import pallas as pl
from jax.experimental.pallas import tpu as pltpu

MESH = pl.DeviceIdType.MESH
F32 = jnp.float32
BF16 = jnp.bfloat16
VMEM_LIMIT = 60 * 1024 * 1024
XFIRST = 32
DIRECT = 256
ROWS = ((0,), (0,))
COLS = ((1,), (1,))


def kernel(
    factor,
    tokens,
    grads,
    gate_weight,
    up_weight,
    down_weight,
    result,
    gate_out,
    up_out,
    down_out,
    gate_own,
    up_own,
    down_own,
    xg,
    wf,
    df,
    sa,
    zla,
    sb,
    zlb,
    acts,
    hidden,
    dg,
    tw,
    dpart,
    gpart,
    dtwo,
    gtwo,
    done,
    gone,
    dmid,
    gmid,
    dland,
    gland,
    gown,
    total,
    near,
    rounded,
    load,
    keep,
    z_send,
    z_recv,
    x_send,
    x_recv,
    p_send,
    p_recv,
    v_send,
    v_recv,
    zx_send,
    zx_recv,
    px_send,
    px_recv,
    y_send,
    y_recv,
    a_send,
    a_recv,
    b_send,
    b_recv,
    t_send,
    t_recv,
    u_send,
    u_recv,
    g_send,
    g_recv,
    f_send,
    f_recv,
    dx_send,
    dx_recv,
    dp_send,
    dp_recv,
    two_send,
    two_recv,
    one_send,
    one_recv,
    r_send,
    r_recv,
):
    f, t = lax.axis_index("fsdp"), lax.axis_index("tp")
    h, y = lax.div(f, 4), lax.rem(f, 4)
    l, x, k = lax.div(t, 8), lax.rem(lax.div(t, 2), 4), lax.rem(t, 2)
    outer = h == l
    inner = h != l
    rows, shard = tokens.shape
    deep, width = gate_weight.shape
    part = rows // 2
    zparts = ((rows - XFIRST) // 2, part)
    first = rows - XFIRST
    xpart = XFIRST // 2
    odd = (h - l) * (h - l)
    home = h * (1 - odd) + 2 * odd
    wide = 2 * width

    def at(xx, yy, hh, ll, kk):
        return (hh * 4 + yy, ll * 8 + xx * 2 + kk)

    xs = (lax.rem(x + 3, 4), lax.rem(x + 1, 4), lax.rem(x + 2, 4))
    ys = (lax.rem(y + 3, 4), lax.rem(y + 1, 4), lax.rem(y + 2, 4))
    right, left = at(xs[1], y, h, l, k), at(xs[0], y, h, l, k)
    north, south = at(x, ys[1], h, l, k), at(x, ys[0], h, l, k)
    mate = at(x, y, h, l, 1 - k)
    flip = at(x, y, h, 1 - l, k)
    across = at(x, y, 1 - h, 1 - l, k)
    opposite = at(x, y, 1 - h, l, k)
    me = 2 * x + k

    def remote(src, dst, send, recv, device):
        return pltpu.make_async_remote_copy(
            src_ref=src,
            dst_ref=dst,
            send_sem=send,
            recv_sem=recv,
            device_id=device,
            device_id_type=MESH,
        )

    copies = [
        pltpu.make_async_copy(ref, spot, load.at[i])
        for i, (ref, spot) in enumerate(
            (
                (tokens, xg.at[k * 4 + x, 0, home]),
                (gate_weight, wf.at[y, 0]),
                (up_weight, wf.at[y, 1]),
                (grads, xg.at[k * 4 + x, 1, home]),
                (down_weight, df.at[y]),
            )
        )
    ]
    for copy in copies:
        copy.start()

    barrier = pltpu.get_barrier_semaphore()
    for j in range(1, 16):
        pl.semaphore_signal(
            barrier, inc=1, device_id=(f, lax.rem(t + j, 16)), device_id_type=MESH
        )
    for peer in (north, south, opposite, across):
        pl.semaphore_signal(barrier, inc=1, device_id=peer, device_id_type=MESH)
    pl.semaphore_wait(barrier, 19)

    for copy in copies:
        copy.wait()

    def w_spot(o, w, q):
        if w == 2:
            return df.at[o, pl.ds(q * (width // 2), width // 2)]
        return wf.at[o, w, pl.ds(q * (deep // 2), deep // 2)]

    def w_out(way, w, q):
        return remote(
            w_spot(y, w, q),
            w_spot(y, w, q),
            y_send.at[way, w, q],
            y_recv.at[way, w, q],
            (north, south)[way],
        )

    def w_on(w, q):
        here = w_spot(ys[q], w, q)
        return remote(here, here, y_send.at[2, w, q], y_recv.at[2, w, q], (north, south)[q])

    def w_in(d, w, q):
        here = w_spot(ys[d], w, q)
        return remote(here, here, y_send.at[2, w, q], y_recv.at[d, w, q], north)

    def w_start(w):
        for way, q in ((0, 0), (1, 1), (0, 1), (1, 0)):
            w_out(way, w, q).start()

    def w_forward(w):
        for q in range(2):
            w_in(q, w, q).wait_recv()
            w_on(w, q).start()

    def w_rest(w):
        for q in range(2):
            w_in(1 - q, w, q).wait_recv()
            w_in(2, w, q).wait_recv()

    slot = (h, 1 - h)

    def x_own(m, q):
        return xg.at[k * 4 + x, m, home, pl.ds(q * zparts[m], zparts[m])]

    def x_spot(p, o, j, m, q):
        return xg.at[p * 4 + o, m, slot[j], pl.ds(q * zparts[m], zparts[m])]

    def z_out(m, q, device, j):
        spot = xg.at[k * 4 + x, m, h, pl.ds(q * zparts[m], zparts[m])]
        return remote(x_own(m, q), spot, z_send.at[0, m, q], z_recv.at[j, m, q], device)

    def z_on(m, q):
        here = x_spot(k, x, 1, m, q)
        return remote(here, here, z_send.at[1, m, q], z_recv.at[1, m, q], flip)

    def z_in(j, m, q):
        here = x_spot(k, x, j, m, q)
        return remote(here, here, z_send.at[0, m, q], z_recv.at[j, m, q], flip)

    def x_out(way, src, j, m, q):
        return remote(
            src,
            x_spot(k, x, j, m, q),
            x_send.at[way, j, m, q],
            x_recv.at[way, j, m, q],
            (right, left)[way],
        )

    def x_on(j, m, q):
        here = x_spot(k, xs[q], j, m, q)
        return remote(
            here, here, x_send.at[2, j, m, q], x_recv.at[2, j, m, q], (right, left)[q]
        )

    def x_in(d, j, m, q):
        here = x_spot(k, xs[d], j, m, q)
        return remote(here, here, x_send.at[2, j, m, q], x_recv.at[d, j, m, q], right)

    places = (*xs, x)

    def p_out(d, src, j, m, q):
        return remote(
            src,
            x_spot(k, places[d], j, m, q),
            p_send.at[d, j, m, q],
            p_recv.at[d, j, m, q],
            mate,
        )

    def p_in(d, j, m, q):
        here = x_spot(1 - k, places[d], j, m, q)
        return remote(here, here, p_send.at[d, j, m, q], p_recv.at[d, j, m, q], mate)

    def spread(src, j, m, q):
        for way in (0, 1) if q == 0 else (1, 0):
            x_out(way, src, j, m, q).start()
        p_out(3, src, j, m, q).start()

    def passed(d, j, m, q):
        x_in(d, j, m, q).wait_recv()
        if d == q:
            x_on(j, m, q).start()
        p_out(d, x_spot(k, places[d], j, m, q), j, m, q).start()

    def z_forward(m, q):
        @pl.when(inner)
        def _():
            z_in(1, m, q).wait_recv()
            z_on(m, q).start()

    def z_near(m, q):
        @pl.when(inner)
        def _():
            z_in(0, m, q).wait_recv()

        spread(x_spot(k, x, 0, m, q), 0, m, q)

    def z_far(m, q):
        @pl.when(outer)
        def _():
            z_in(1, m, q).wait_recv()

        spread(x_spot(k, x, 1, m, q), 1, m, q)

    def z_near_inner(m, q):
        @pl.when(inner)
        def _():
            z_in(0, m, q).wait_recv()
            spread(x_spot(k, x, 0, m, q), 0, m, q)

    fourths = (shard // 4, (shard - DIRECT) // 4)
    bases = (0, DIRECT)

    def t_copy(u, w, j):
        return remote(
            wf.at[
                lax.div(u, 2),
                w,
                pl.ds(lax.rem(u, 2) * shard + bases[w] + y * fourths[w], fourths[w]),
            ],
            tw.at[me, w, pl.ds(bases[w] + y * fourths[w], fourths[w])],
            t_send.at[w, j],
            t_recv.at[w, j],
            (f, l * 8 + u),
        )

    def t_out(w, j):
        return t_copy(lax.rem(me + j, 8), w, j)

    def t_in(w, j):
        u = lax.rem(me + 8 - j, 8)
        spot = tw.at[u, w, pl.ds(bases[w] + y * fourths[w], fourths[w])]
        return remote(spot, spot, t_send.at[w, j], t_recv.at[w, j], (f, l * 8 + u))

    def g_out(j):
        u = lax.rem(me + j, 8)
        return remote(
            wf.at[lax.div(u, 2), 1, pl.ds(lax.rem(u, 2) * shard, DIRECT)],
            tw.at[me, 1, pl.ds(0, DIRECT)],
            g_send.at[j],
            g_recv.at[j],
            (f, l * 8 + u),
        )

    def g_in(j):
        u = lax.rem(me + 8 - j, 8)
        spot = tw.at[u, 1, pl.ds(0, DIRECT)]
        return remote(spot, spot, g_send.at[j], g_recv.at[j], (f, l * 8 + u))

    def u_spot(o, w, q):
        return tw.at[pl.ds(q * 4, 4), w, pl.ds(bases[w] + o * fourths[w], fourths[w])]

    def u_out(way, w, q):
        here = u_spot(y, w, q)
        return remote(
            here, here, u_send.at[way, w, q], u_recv.at[way, w, q], (north, south)[way]
        )

    def u_on(w, q):
        here = u_spot(ys[q], w, q)
        return remote(here, here, u_send.at[2, w, q], u_recv.at[2, w, q], (north, south)[q])

    def u_in(d, w, q):
        here = u_spot(ys[d], w, q)
        return remote(here, here, u_send.at[2, w, q], u_recv.at[d, w, q], north)

    def v_spot(o, q):
        return xg.at[k * 4 + o, 0, home, pl.ds(first + q * xpart, xpart)]

    def v_out(way, q):
        here = v_spot(x, q)
        return remote(
            here, here, v_send.at[way, q], v_recv.at[way, q], (right, left)[way]
        )

    def v_on(q):
        here = v_spot(xs[q], q)
        return remote(here, here, v_send.at[2, q], v_recv.at[2, q], (right, left)[q])

    def v_in(d, q):
        here = v_spot(xs[d], q)
        return remote(here, here, v_send.at[2, q], v_recv.at[d, q], right)

    def zx_spot(p, d, at_s):
        return xg.at[p * 4 + places[d], 0, at_s, pl.ds(first, XFIRST)]

    def zx_out(d, device, j):
        return remote(
            zx_spot(k, d, home),
            zx_spot(k, d, h),
            zx_send.at[0, d],
            zx_recv.at[j, d],
            device,
        )

    def zx_on(d):
        here = zx_spot(k, d, 1 - h)
        return remote(here, here, zx_send.at[1, d], zx_recv.at[1, d], flip)

    def zx_in(j, d):
        here = zx_spot(k, d, slot[j])
        return remote(here, here, zx_send.at[0, d], zx_recv.at[j, d], flip)

    def px_out(d, j):
        here = zx_spot(k, d, slot[j])
        return remote(here, here, px_send.at[d, j], px_recv.at[d, j], mate)

    def px_in(d, j):
        here = zx_spot(1 - k, d, slot[j])
        return remote(here, here, px_send.at[d, j], px_recv.at[d, j], mate)

    def v_start():
        for q in range(2):
            for way in (0, 1) if q == 0 else (1, 0):
                v_out(way, q).start()

    def v_near():
        for q in range(2):
            v_in(q, q).wait_recv()
            v_on(q).start()
        for q in range(2):
            v_in(1 - q, q).wait_recv()

    def v_far():
        for q in range(2):
            v_in(2, q).wait_recv()

    def zx_start(ds):
        for d in ds:

            @pl.when(outer)
            def _(d=d):
                zx_out(d, flip, 0).start()
                px_out(d, 0).start()

            @pl.when(inner)
            def _(d=d):
                zx_out(d, across, 1).start()

    def zx_pass(ds):
        for d in ds:

            @pl.when(inner)
            def _(d=d):
                zx_in(1, d).wait_recv()
                zx_on(d).start()

    def zx_take(ds):
        for d in ds:

            @pl.when(inner)
            def _(d=d):
                zx_in(0, d).wait_recv()
                px_out(d, 0).start()

            @pl.when(outer)
            def _(d=d):
                zx_in(1, d).wait_recv()

            px_out(d, 1).start()

    def z_start(m):
        @pl.when(outer)
        def _():
            for q in range(2):
                z_out(m, q, flip, 0).start()

        @pl.when(inner)
        def _():
            for q in range(2):
                z_out(m, q, across, 1).start()

    v_start()
    z_start(0)

    @pl.when(outer)
    def _():
        for q in range(2):
            spread(x_own(0, q), 0, 0, q)

    zx_start((3,))
    w_start(0)
    w_start(1)

    v_near()
    zx_start((0, 1))
    z_forward(0, 0)
    z_near_inner(0, 0)
    z_far(0, 0)
    v_far()
    zx_start((2,))
    z_start(1)
    z_forward(0, 1)
    z_near_inner(0, 1)
    z_far(0, 1)
    w_forward(0)
    for j in range(2):
        passed(0, j, 0, 0)
        passed(1, j, 0, 0)
    w_forward(1)
    w_start(2)
    for j in range(2):
        passed(1, j, 0, 1)
        passed(0, j, 0, 1)
    z_forward(1, 0)
    zx_pass((3, 0, 1))
    z_forward(1, 1)
    zx_pass((2,))
    z_near(1, 0)
    z_near(1, 1)
    w_rest(0)
    w_rest(1)

    @pl.loop(1, 8)
    def _(j):
        for w in range(2):
            t_out(w, j).start()

    z_far(1, 0)
    z_far(1, 1)
    w_forward(2)
    zx_take((3, 0, 1, 2))
    tall = 2 * rows

    def block(m, o):
        return jnp.concatenate(
            [xg[p * 4 + o, m, :2].reshape(tall, shard) for p in range(2)], axis=1
        )

    def pair_in(d, m):
        for q in range(2):
            for j in range(2):
                p_in(d, j, m, q).wait_recv()
        if m == 0:
            for j in range(2):
                px_in(d, j).wait_recv()

    def gate_up(d):
        o = places[d]
        weights = jnp.concatenate([wf[o, 0], wf[o, 1]], axis=1)
        term = jnp.dot(block(0, o), weights, preferred_element_type=F32)
        sa[...] = term if d == 3 else sa[...] + term

    for d in (3, 0, 1):
        pair_in(d, 0)
        gate_up(d)
    for q in range(2):
        for j in range(2):
            passed(2, j, 0, q)
    pair_in(2, 0)
    gate_up(2)
    turn = (1 - l, l)

    def swap(src, dst, send, recv):
        def copy(c):
            at_c = pl.ds(turn[c] * rows, rows)
            return remote(src.at[at_c], dst.at[at_c], send.at[c], recv.at[c], opposite)

        return copy

    a_swap = swap(sa, zla, a_send, a_recv)
    b_swap = swap(sb, zlb, b_send, b_recv)

    a_swap(0).start()
    for w in range(2):
        mine_w = pl.ds(bases[w] + y * fourths[w], fourths[w])
        tw[me, w, mine_w] = wf[x, w, pl.ds(k * shard + bases[w] + y * fourths[w], fourths[w])]
    tw[me, 1, :DIRECT] = wf[x, 1, pl.ds(k * shard, DIRECT)]
    a_swap(1).start()
    @pl.loop(1, 8)
    def _(j):
        for w in range(2):
            t_in(w, j).wait_recv()

    for w in range(2):
        for way, q in ((0, 0), (1, 1), (0, 1), (1, 0)):
            u_out(way, w, q).start()
    for j in range(2):
        passed(0, j, 1, 0)
        passed(1, j, 1, 0)
    for j in range(2):
        passed(1, j, 1, 1)
        passed(0, j, 1, 1)

    def grad_in(d):
        o = places[d]
        term = lax.dot_general(
            block(1, o), df[o], (COLS, ((), ())), preferred_element_type=F32
        )
        sb[...] = term if d == 3 else sb[...] + term

    w_rest(2)
    for d in (3, 0, 1):
        pair_in(d, 1)
        grad_in(d)
    for q in range(2):
        for j in range(2):
            passed(2, j, 1, q)
    @pl.loop(1, 8)
    def _(j):
        g_out(j).start()

    for w in range(2):
        for q in range(2):
            u_in(q, w, q).wait_recv()
            u_on(w, q).start()
    for c in range(2):
        a_swap(c).wait_recv()
    sums = sa[...] + zla[...]
    gate, up = sums[:, :width], sums[:, width:]
    squashed = jax.nn.sigmoid(gate)
    activated = gate * squashed
    slope = squashed * (1.0 + gate * (1.0 - squashed))
    acts[:, :width] = up * slope
    acts[:, width:] = activated
    hidden[...] = (activated * up).astype(BF16)

    pair_in(2, 1)
    for c in range(2):
        at_s = pl.ds(turn[c] * rows, rows)
        last = jnp.concatenate([xg[p * 4 + xs[2], 1, turn[c]] for p in range(2)], axis=1)
        sb[at_s] += lax.dot_general(
            last, df[xs[2]], (COLS, ((), ())), preferred_element_type=F32
        )
        if c:
            b_swap(0).start()
    def down_part(o):
        return lax.dot_general(
            hidden[...], block(1, o), (ROWS, ((), ())), preferred_element_type=F32
        )

    def gate_part(o):
        return lax.dot_general(
            block(0, o), dg[me], (ROWS, ((), ())), preferred_element_type=F32
        )

    twos, mids, parts, ones, lands = (
        (dtwo, gtwo),
        (dmid, gmid),
        (dpart, gpart),
        (done, gone),
        (dland, gland),
    )

    def halves(i, q):
        size = twos[i].shape[0] // 2
        return pl.ds(q * size, size)

    def two_out(i, q):
        return remote(
            twos[i].at[halves(i, q)],
            mids[i].at[q],
            two_send.at[i, q],
            two_recv.at[i, q],
            (north, south)[q],
        )

    def one_out(i, way, q):
        return remote(
            ones[i].at[way, halves(i, q)],
            lands[i].at[way, halves(i, q)],
            one_send.at[i, way, q],
            one_recv.at[i, way, q],
            (north, south)[way],
        )

    def one_parts(i, fn):
        for way in range(2):
            q = way
            term = fn(ys[1 - way])
            size = term.shape[0] // 2
            parts[i][way] = term[q * size : (q + 1) * size]
            ones[i][way, halves(i, 1 - q)] = term[(1 - q) * size : (2 - q) * size].astype(BF16)

    def one_merge(i):
        for way in range(2):
            two_out(i, way).wait_recv()
            ones[i][way, halves(i, way)] = (
                parts[i][way] + mids[i][way].astype(F32)
            ).astype(BF16)

    def finals(i):
        for way in range(2):
            for q in range(2):
                one_out(i, way, q).wait_recv()
        return lands[i][0].astype(F32) + lands[i][1].astype(F32)

    dtwo[...] = down_part(ys[2]).astype(BF16)
    b_swap(1).start()
    one_parts(0, down_part)
    for q in range(2):
        two_out(0, q).start()
    for way in range(2):
        one_out(0, way, 1 - way).start()

    def d_spot(c, o, e, q):
        return dg.at[o * 2 + c, pl.ds(turn[e] * rows + q * part, part)]

    def dx_out(way, e, q):
        here = d_spot(k, x, e, q)
        return remote(
            here, here, dx_send.at[way, e, q], dx_recv.at[way, e, q], (right, left)[way]
        )

    def dx_on(e, q):
        here = d_spot(k, xs[q], e, q)
        return remote(here, here, dx_send.at[2, e, q], dx_recv.at[2, e, q], (right, left)[q])

    def dx_in(d, e, q):
        here = d_spot(k, xs[d], e, q)
        return remote(here, here, dx_send.at[2, e, q], dx_recv.at[d, e, q], right)

    def dp_out(d, e, q):
        here = d_spot(k, places[d], e, q)
        return remote(here, here, dp_send.at[d, e, q], dp_recv.at[d, e, q], mate)

    def dp_in(d, e, q):
        here = d_spot(1 - k, places[d], e, q)
        return remote(here, here, dp_send.at[d, e, q], dp_recv.at[d, e, q], mate)

    def d_start(e):
        for q in range(2):
            for way in (0, 1) if q == 0 else (1, 0):
                dx_out(way, e, q).start()
            dp_out(3, e, q).start()

    def d_passed(d, e, q):
        dx_in(d, e, q).wait_recv()
        if d == q:
            dx_on(e, q).start()
        dp_out(d, e, q).start()

    def d_near(e):
        for q in range(2):
            d_passed(q, e, q)
        for q in range(2):
            d_passed(1 - q, e, q)

    def gather(d, e):
        base = places[d] * 2
        at_s = pl.ds(turn[e] * rows, rows)
        left_side = jnp.concatenate([dg[base, at_s], dg[base + 1, at_s]], axis=1)
        right_side = jnp.concatenate(
            [tw[base, 0], tw[base, 1], tw[base + 1, 0], tw[base + 1, 1]], axis=1
        )
        term = lax.dot_general(
            left_side, right_side, (COLS, ((), ())), preferred_element_type=F32
        )
        total[e] = term if d == 3 else total[e] + term

    def gathers(e, ds):
        for d in ds:
            for q in range(2):
                dp_in(d, e, q).wait_recv()
            gather(d, e)

    piece = rows // 4

    def f_out(c):
        at_c = pl.ds(c * piece, piece)
        return remote(total.at[0, at_c], near.at[at_c], f_send.at[c], f_recv.at[c], flip)

    def r_out(c):
        at_c = pl.ds(c * piece, piece)
        return remote(rounded.at[at_c], result.at[at_c], r_send.at[c], r_recv.at[c], across)

    def delta(e):
        b_swap(e).wait_recv()
        at_s = pl.ds(turn[e] * rows, rows)
        hidden_grad = sb[at_s] + zlb[at_s]
        dg[me, at_s, :width] = (hidden_grad * acts[at_s, :width]).astype(BF16)
        dg[me, at_s, width:] = (hidden_grad * acts[at_s, width:]).astype(BF16)

    delta(0)
    down_own[...] = down_part(y)
    d_start(0)
    delta(1)
    one_merge(0)
    gtwo[...] = gate_part(ys[2]).astype(BF16)
    for way in range(2):
        one_out(0, way, way).start()
    d_near(0)
    d_start(1)
    for q in range(2):
        two_out(1, q).start()
    one_parts(1, gate_part)
    for way in range(2):
        one_out(1, way, 1 - way).start()
    gown[...] = gate_part(y)
    for q in range(2):
        for w in range(2):
            u_in(1 - q, w, q).wait_recv()
            u_in(2, w, q).wait_recv()
    @pl.loop(1, 8)
    def _(j):
        g_in(j).wait_recv()

    gathers(0, (3, 0, 1))
    for q in range(2):
        d_passed(2, 0, q)
    gathers(0, (2,))
    for c in range(2):
        f_out(c).start()
    d_near(1)
    for c in range(2, 4):
        f_out(c).start()
    one_merge(1)
    gathers(1, (3,))
    for way in range(2):
        one_out(1, way, way).start()
    gathers(1, (0, 1))
    for q in range(2):
        d_passed(2, 1, q)
    gathers(1, (2,))
    keeps = [
        pltpu.make_async_copy(src, dst, keep.at[i])
        for i, (src, dst) in enumerate(
            ((down_own, down_out), (gate_own, gate_out), (up_own, up_out), (rounded, result))
        )
    ]
    for c in range(4):
        f_out(c).wait_recv()
        at_c = pl.ds(c * piece, piece)
        rounded[at_c] = (total[1, at_c] + near[at_c]).astype(BF16)

        if c:

            @pl.when(inner)
            def _(c=c):
                r_out(c - 1).start()

    down_own[...] = factor * (down_own[...] + finals(0))
    @pl.when(inner)
    def _():
        r_out(3).start()

    @pl.when(outer)
    def _():
        keeps[3].start()

    both = factor * (gown[...] + finals(1))
    gate_own[...] = both[:, :width]
    up_own[...] = both[:, width:]
    for copy in keeps[:3]:
        copy.start()

    for d in range(4):
        zx_in(0, d).wait_send()
        for j in range(2):
            px_out(d, j).wait_send()

        @pl.when(inner)
        def _(d=d):
            zx_on(d).wait_send()

    for q in range(2):
        for way in range(2):
            v_out(way, q).wait_send()
        v_on(q).wait_send()
    for m in range(2):
        for q in range(2):
            z_in(0, m, q).wait_send()

            @pl.when(inner)
            def _(m=m, q=q):
                z_on(m, q).wait_send()

            for j in range(2):
                for way in range(2):
                    x_out(way, x_own(m, q), j, m, q).wait_send()
                x_on(j, m, q).wait_send()
                for d in range(4):
                    p_out(d, x_own(m, q), j, m, q).wait_send()
    for w in range(3):
        for q in range(2):
            for way in range(2):
                w_out(way, w, q).wait_send()
            w_on(w, q).wait_send()
    for c in range(2):
        for copy in (a_swap(c), b_swap(c), f_out(c), f_out(2 + c)):
            copy.wait_send()
        for i in range(2):
            two_out(i, c).wait_send()
            for q in range(2):
                one_out(i, c, q).wait_send()
        for w in range(2):
            for way in range(2):
                u_out(way, w, c).wait_send()
            u_on(w, c).wait_send()
        for e in range(2):
            for way in range(2):
                dx_out(way, e, c).wait_send()
            dx_on(e, c).wait_send()
            for d in range(4):
                dp_out(d, e, c).wait_send()

    @pl.loop(1, 8)
    def _(j):
        for w in range(2):
            t_out(w, j).wait_send()
        g_out(j).wait_send()

    @pl.when(inner)
    def _():
        for c in range(4):
            r_out(c).wait()

    @pl.when(outer)
    def _():
        keeps[3].wait()

    for copy in keeps[:3]:
        copy.wait()


def store_kernel(*refs):
    found, kept, held, sem = refs[:4], refs[4:8], refs[8:12], refs[12]
    loads = [pltpu.make_async_copy(found[i], held[i], sem.at[0, i]) for i in range(4)]
    stores = [pltpu.make_async_copy(held[i], kept[i], sem.at[1, i]) for i in range(4)]
    for copy in loads:
        copy.start()
    for i in range(4):
        loads[i].wait()
        stores[i].start()
    for copy in stores:
        copy.wait()


HBM = pl.BlockSpec(memory_space=pltpu.HBM)
DMA = pltpu.SemaphoreType.DMA


def body(tokens, out_grad, gate_weight, up_weight, down_weight):
    nf, nt = lax.axis_size("fsdp"), lax.axis_size("tp")
    rows, shard = tokens.shape
    deep, width = gate_weight.shape
    assert nf == 8 and nt == 16 and deep == 2 * shard
    factor = 1.0 / math.sqrt(rows * nf)
    tall = 2 * rows
    wide = 2 * width

    shapes = (
        jax.ShapeDtypeStruct((rows, shard), BF16),
        jax.ShapeDtypeStruct((deep, width), F32),
        jax.ShapeDtypeStruct((deep, width), F32),
        jax.ShapeDtypeStruct((width, deep), F32),
    )
    found = tuple(
        pl.pallas_call(
            functools.partial(kernel, factor),
            out_shape=shapes,
            in_specs=[HBM] * 5,
            out_specs=(HBM,) * 4,
            scratch_shapes=[
                pltpu.VMEM((deep, width), F32),
                pltpu.VMEM((deep, width), F32),
                pltpu.VMEM((width, deep), F32),
                pltpu.VMEM((8, 2, 3, rows, shard), BF16),
                pltpu.VMEM((4, 2, deep, width), BF16),
                pltpu.VMEM((4, width, deep), BF16),
                pltpu.VMEM((tall, wide), F32),
                pltpu.VMEM((tall, wide), F32),
                pltpu.VMEM((tall, width), F32),
                pltpu.VMEM((tall, width), F32),
                pltpu.VMEM((tall, wide), F32),
                pltpu.VMEM((tall, width), BF16),
                pltpu.VMEM((8, tall, wide), BF16),
                pltpu.VMEM((8, 2, shard, width), BF16),
                pltpu.VMEM((2, width // 2, deep), F32),
                pltpu.VMEM((2, deep // 2, wide), F32),
                pltpu.VMEM((width, deep), BF16),
                pltpu.VMEM((deep, wide), BF16),
                pltpu.VMEM((2, width, deep), BF16),
                pltpu.VMEM((2, deep, wide), BF16),
                pltpu.VMEM((2, width // 2, deep), BF16),
                pltpu.VMEM((2, deep // 2, wide), BF16),
                pltpu.VMEM((2, width, deep), BF16),
                pltpu.VMEM((2, deep, wide), BF16),
                pltpu.VMEM((deep, wide), F32),
                pltpu.VMEM((2, rows, shard), F32),
                pltpu.VMEM((rows, shard), F32),
                pltpu.VMEM((rows, shard), BF16),
                DMA((5,)),
                DMA((4,)),
                DMA((2, 2, 2)),
                DMA((2, 2, 2)),
                DMA((3, 2, 2, 2)),
                DMA((3, 2, 2, 2)),
                DMA((4, 2, 2, 2)),
                DMA((4, 2, 2, 2)),
                DMA((3, 2)),
                DMA((3, 2)),
                DMA((2, 4)),
                DMA((2, 4)),
                DMA((4, 2)),
                DMA((4, 2)),
                DMA((3, 3, 2)),
                DMA((3, 3, 2)),
                DMA((2,)),
                DMA((2,)),
                DMA((2,)),
                DMA((2,)),
                DMA((2, 8)),
                DMA((2, 8)),
                DMA((3, 2, 2)),
                DMA((3, 2, 2)),
                DMA((8,)),
                DMA((8,)),
                DMA((4,)),
                DMA((4,)),
                DMA((3, 2, 2)),
                DMA((3, 2, 2)),
                DMA((4, 2, 2)),
                DMA((4, 2, 2)),
                DMA((2, 2)),
                DMA((2, 2)),
                DMA((2, 2, 2)),
                DMA((2, 2, 2)),
                DMA((4,)),
                DMA((4,)),
            ],
            compiler_params=pltpu.CompilerParams(
                collective_id=0, has_side_effects=True, vmem_limit_bytes=VMEM_LIMIT
            ),
            name="block",
        )(tokens, out_grad, gate_weight, up_weight, down_weight)
    )
    return tuple(
        pl.pallas_call(
            store_kernel,
            out_shape=shapes,
            in_specs=[HBM] * 4,
            out_specs=(HBM,) * 4,
            scratch_shapes=[pltpu.VMEM(s.shape, s.dtype) for s in shapes] + [DMA((2, 4))],
            compiler_params=pltpu.CompilerParams(vmem_limit_bytes=VMEM_LIMIT),
            name="store",
        )(*found)
    )


def solution(mesh):
    return jax.shard_map(
        body,
        mesh=mesh,
        in_specs=(
            P("fsdp", "tp"),
            P("fsdp", "tp"),
            P("fsdp", "tp"),
            P("fsdp", "tp"),
            P("tp", "fsdp"),
        ),
        out_specs=(P("fsdp", "tp"), P("fsdp", "tp"), P("fsdp", "tp"), P("tp", "fsdp")),
        check_vma=False,
    )
```

```python
import functools
import math

import jax
import jax.numpy as jnp
from jax import lax
from jax.sharding import PartitionSpec as P
from jax.experimental import pallas as pl
from jax.experimental.pallas import tpu as pltpu

MESH = pl.DeviceIdType.MESH
F32 = jnp.float32
BF16 = jnp.bfloat16
VMEM_LIMIT = 60 * 1024 * 1024
XFIRST = 32
DIRECT = 384
ROWS = ((0,), (0,))
COLS = ((1,), (1,))


def kernel(
    factor,
    tokens,
    grads,
    gate_weight,
    up_weight,
    down_weight,
    result,
    gate_out,
    up_out,
    down_out,
    gate_own,
    up_own,
    down_own,
    xg,
    wf,
    df,
    sa,
    zla,
    sb,
    zlb,
    acts,
    hidden,
    dg,
    tw,
    dpart,
    gpart,
    dtwo,
    gtwo,
    done,
    gone,
    dmid,
    gmid,
    dland,
    gland,
    gown,
    total,
    near,
    rounded,
    load,
    keep,
    z_send,
    z_recv,
    x_send,
    x_recv,
    p_send,
    p_recv,
    v_send,
    v_recv,
    zx_send,
    zx_recv,
    y_send,
    y_recv,
    a_send,
    a_recv,
    b_send,
    b_recv,
    t_send,
    t_recv,
    u_send,
    u_recv,
    g_send,
    g_recv,
    f_send,
    f_recv,
    dx_send,
    dx_recv,
    dp_send,
    dp_recv,
    two_send,
    two_recv,
    one_send,
    one_recv,
    r_send,
    r_recv,
):
    f, t = lax.axis_index("fsdp"), lax.axis_index("tp")
    h, y = lax.div(f, 4), lax.rem(f, 4)
    l, x, k = lax.div(t, 8), lax.rem(lax.div(t, 2), 4), lax.rem(t, 2)
    outer = h == l
    inner = h != l
    rows, shard = tokens.shape
    deep, width = gate_weight.shape
    part = rows // 2
    zparts = ((rows - XFIRST) // 2, part)
    first = rows - XFIRST
    xpart = XFIRST // 2
    odd = (h - l) * (h - l)
    home = h * (1 - odd) + 2 * odd
    wide = 2 * width

    def at(xx, yy, hh, ll, kk):
        return (hh * 4 + yy, ll * 8 + xx * 2 + kk)

    xs = (lax.rem(x + 3, 4), lax.rem(x + 1, 4), lax.rem(x + 2, 4))
    ys = (lax.rem(y + 3, 4), lax.rem(y + 1, 4), lax.rem(y + 2, 4))
    right, left = at(xs[1], y, h, l, k), at(xs[0], y, h, l, k)
    north, south = at(x, ys[1], h, l, k), at(x, ys[0], h, l, k)
    mate = at(x, y, h, l, 1 - k)
    flip = at(x, y, h, 1 - l, k)
    across = at(x, y, 1 - h, 1 - l, k)
    opposite = at(x, y, 1 - h, l, k)
    me = 2 * x + k

    def remote(src, dst, send, recv, device):
        return pltpu.make_async_remote_copy(
            src_ref=src,
            dst_ref=dst,
            send_sem=send,
            recv_sem=recv,
            device_id=device,
            device_id_type=MESH,
        )

    copies = [
        pltpu.make_async_copy(ref, spot, load)
        for ref, spot in (
            (tokens, xg.at[k * 4 + x, 0, home]),
            (gate_weight, wf.at[y, 0]),
            (up_weight, wf.at[y, 1]),
            (grads, xg.at[k * 4 + x, 1, home]),
            (down_weight, df.at[y]),
        )
    ]
    for copy in copies:
        copy.start()

    barrier = pltpu.get_barrier_semaphore()
    for j in range(1, 16):
        pl.semaphore_signal(
            barrier, inc=1, device_id=(f, lax.rem(t + j, 16)), device_id_type=MESH
        )
    for peer in (north, south, opposite, across):
        pl.semaphore_signal(barrier, inc=1, device_id=peer, device_id_type=MESH)
    pl.semaphore_wait(barrier, 19)

    all_in = xg.at[pl.ds(0, 5), 0, 0]
    pltpu.make_async_copy(all_in, all_in, load).wait()

    def w_spot(o, w, q):
        if w == 2:
            return df.at[o, pl.ds(q * (width // 2), width // 2)]
        return wf.at[o, w, pl.ds(q * (deep // 2), deep // 2)]

    def w_out(way, w, q):
        return remote(
            w_spot(y, w, q),
            w_spot(y, w, q),
            y_send,
            y_recv.at[w, q if way == q else 2],
            (north, south)[way],
        )

    def w_on(w, q):
        here = w_spot(ys[q], w, q)
        return remote(here, here, y_send, y_recv.at[w, 2], (north, south)[q])

    def w_wait(w, e, here):
        remote(here, here, y_send, y_recv.at[w, e], north).wait_recv()

    def w_start(w):
        for way, q in ((0, 0), (1, 1), (0, 1), (1, 0)):
            w_out(way, w, q).start()

    def w_forward(w):
        for q in range(2):
            w_wait(w, q, w_spot(ys[q], w, q))
            w_on(w, q).start()

    def w_rest(w):
        w_wait(w, 2, df.at[pl.ds(0, 2)] if w == 2 else wf.at[pl.ds(0, 2), w])

    slot = (h, 1 - h)

    def x_own(m, q):
        return xg.at[k * 4 + x, m, home, pl.ds(q * zparts[m], zparts[m])]

    def x_spot(p, o, j, m, q):
        return xg.at[p * 4 + o, m, slot[j], pl.ds(q * zparts[m], zparts[m])]

    def z_out(m, q, device, j):
        spot = xg.at[k * 4 + x, m, h, pl.ds(q * zparts[m], zparts[m])]
        return remote(x_own(m, q), spot, z_send.at[0], z_recv.at[j, m, q], device)

    def z_on(m, q):
        here = x_spot(k, x, 1, m, q)
        return remote(here, here, z_send.at[1], z_recv.at[1, m, q], flip)

    def z_in(j, m, q):
        here = x_spot(k, x, j, m, q)
        return remote(here, here, z_send.at[0], z_recv.at[j, m, q], flip)

    def x_out(way, src, j, m, q):
        return remote(
            src,
            x_spot(k, x, j, m, q),
            x_send,
            x_recv.at[m, q, 2 * way + j],
            (right, left)[way],
        )

    def x_on(j, m, q):
        here = x_spot(k, xs[q], j, m, q)
        return remote(
            here, here, x_send, x_recv.at[m, q, 4], (right, left)[q]
        )

    def x_wait(m, q, e, here):
        remote(here, here, x_send, x_recv.at[m, q, e], right).wait_recv()

    places = (*xs, x)

    def p_out(d, src, j, m, q):
        return remote(
            src,
            x_spot(k, places[d], j, m, q),
            p_send,
            p_recv.at[d, m],
            mate,
        )

    def spread(src, j, m, q):
        for way in (0, 1) if q == 0 else (1, 0):
            x_out(way, src, j, m, q).start()
        p_out(3, src, j, m, q).start()

    def passed(d, j, m, q):
        x_wait(m, q, 2 * d + j, x_spot(k, xs[d], j, m, q))
        if d == q:
            x_on(j, m, q).start()
        p_out(d, x_spot(k, places[d], j, m, q), j, m, q).start()

    def x_rest(m):
        for q in range(2):
            here = xg.at[k * 4 + xs[2], m, pl.ds(0, 2), pl.ds(q * zparts[m], zparts[m])]
            x_wait(m, q, 4, here)
            for j in range(2):
                p_out(2, x_spot(k, xs[2], j, m, q), j, m, q).start()

    def z_forward(m, q):
        @pl.when(inner)
        def _():
            z_in(1, m, q).wait_recv()
            z_on(m, q).start()

    def z_near(m, q):
        @pl.when(inner)
        def _():
            z_in(0, m, q).wait_recv()

        spread(x_spot(k, x, 0, m, q), 0, m, q)

    def z_far(m, q):
        @pl.when(outer)
        def _():
            z_in(1, m, q).wait_recv()

        spread(x_spot(k, x, 1, m, q), 1, m, q)

    def z_near_inner(m, q):
        @pl.when(inner)
        def _():
            z_in(0, m, q).wait_recv()
            spread(x_spot(k, x, 0, m, q), 0, m, q)

    fourths = (shard // 4, (shard - DIRECT) // 4)
    bases = (0, DIRECT)

    def t_copy(u, w):
        return remote(
            wf.at[
                lax.div(u, 2),
                w,
                pl.ds(lax.rem(u, 2) * shard + bases[w] + y * fourths[w], fourths[w]),
            ],
            tw.at[me, w, pl.ds(bases[w] + y * fourths[w], fourths[w])],
            t_send,
            t_recv,
            (f, l * 8 + u),
        )

    def t_out(w, j):
        return t_copy(lax.rem(me + j, 8), w)

    def t_all():
        here = tw.at[pl.ds(0, 7), 0, pl.ds(0, fourths[0] + fourths[1])]
        return remote(here, here, t_send, t_recv, mate)

    def g_out(j):
        u = lax.rem(me + j, 8)
        return remote(
            wf.at[lax.div(u, 2), 1, pl.ds(lax.rem(u, 2) * shard, DIRECT)],
            tw.at[me, 1, pl.ds(0, DIRECT)],
            g_send,
            g_recv,
            (f, l * 8 + u),
        )

    def g_all():
        here = tw.at[pl.ds(0, 7), 1, pl.ds(0, DIRECT)]
        return remote(here, here, g_send, g_recv, mate)

    def u_spot(o, w, q):
        return tw.at[pl.ds(q * 4, 4), w, pl.ds(bases[w] + o * fourths[w], fourths[w])]

    def u_out(way, w, q):
        here = u_spot(y, w, q)
        return remote(
            here, here, u_send, u_recv.at[q if way == q else 2], (north, south)[way]
        )

    def u_on(w, q):
        here = u_spot(ys[q], w, q)
        return remote(here, here, u_send, u_recv.at[2], (north, south)[q])

    def u_wait(e, here):
        remote(here, here, u_send, u_recv.at[e], north).wait_recv()

    def v_spot(o, q):
        return xg.at[k * 4 + o, 0, home, pl.ds(first + q * xpart, xpart)]

    def v_out(way, q):
        here = v_spot(x, q)
        return remote(
            here, here, v_send, v_recv.at[q if way == q else 2], (right, left)[way]
        )

    def v_on(q):
        here = v_spot(xs[q], q)
        return remote(here, here, v_send, v_recv.at[3], (right, left)[q])

    def v_wait(e, here):
        remote(here, here, v_send, v_recv.at[e], right).wait_recv()

    def zx_spot(p, d, at_s):
        return xg.at[p * 4 + places[d], 0, at_s, pl.ds(first, XFIRST)]

    def zx_out(d, device, j):
        return remote(
            zx_spot(k, d, home),
            zx_spot(k, d, h),
            zx_send.at[0],
            zx_recv.at[j + (j * d == 2)],
            device,
        )

    def zx_on(d):
        here = zx_spot(k, d, 1 - h)
        return remote(here, here, zx_send.at[1], zx_recv.at[1 + (d == 2)], flip)

    def zx_wait(e, count):
        here = xg.at[pl.ds(0, count), 0, 0, pl.ds(first, XFIRST)]
        remote(here, here, zx_send.at[0], zx_recv.at[e], flip).wait_recv()

    def px_out(d, j):
        here = zx_spot(k, d, slot[j])
        return remote(here, here, p_send, p_recv.at[d, 0], mate)

    def v_start():
        for q in range(2):
            for way in (0, 1) if q == 0 else (1, 0):
                v_out(way, q).start()

    def v_near():
        for q in range(2):
            v_wait(q, v_spot(xs[q], q))
            v_on(q).start()
        v_wait(2, zx_spot(k, 0, home))

    def v_far():
        v_wait(3, zx_spot(k, 2, home))

    def zx_start(ds):
        for d in ds:

            @pl.when(outer)
            def _(d=d):
                zx_out(d, flip, 0).start()
                px_out(d, 0).start()

            @pl.when(inner)
            def _(d=d):
                zx_out(d, across, 1).start()

    def zx_pass(e, ds):
        @pl.when(inner)
        def _():
            zx_wait(e, len(ds))
            for d in ds:
                zx_on(d).start()

    def zx_take():
        @pl.when(inner)
        def _():
            zx_wait(0, 4)
            for d in range(4):
                px_out(d, 0).start()

        @pl.when(outer)
        def _():
            zx_wait(1, 3)
            zx_wait(2, 1)

        for d in range(4):
            px_out(d, 1).start()

    def z_start(m):
        @pl.when(outer)
        def _():
            for q in range(2):
                z_out(m, q, flip, 0).start()

        @pl.when(inner)
        def _():
            for q in range(2):
                z_out(m, q, across, 1).start()

    v_start()
    z_start(0)

    @pl.when(outer)
    def _():
        for q in range(2):
            spread(x_own(0, q), 0, 0, q)

    zx_start((3,))
    w_start(0)
    w_start(1)

    v_near()
    zx_start((0, 1))
    z_forward(0, 0)
    z_near_inner(0, 0)
    z_far(0, 0)
    v_far()
    zx_start((2,))
    z_start(1)
    z_forward(0, 1)
    z_near_inner(0, 1)
    z_far(0, 1)
    w_forward(0)
    for j in range(2):
        passed(0, j, 0, 0)
        passed(1, j, 0, 0)
    w_forward(1)
    w_start(2)
    for j in range(2):
        passed(1, j, 0, 1)
        passed(0, j, 0, 1)
    z_forward(1, 0)
    zx_pass(1, (3, 0, 1))
    z_forward(1, 1)
    zx_pass(2, (2,))
    z_near(1, 0)
    z_near(1, 1)
    w_rest(0)
    w_rest(1)

    @pl.loop(1, 8)
    def _(j):
        for w in range(2):
            t_out(w, j).start()

    z_far(1, 0)
    z_far(1, 1)
    w_forward(2)
    zx_take()
    tall = 2 * rows

    def block(m, o):
        return jnp.concatenate(
            [xg[p * 4 + o, m, :2].reshape(tall, shard) for p in range(2)], axis=1
        )

    def pair_in(d, m):
        here = xg.at[(1 - k) * 4 + places[d], m, pl.ds(0, 2)]
        remote(here, here, p_send, p_recv.at[d, m], mate).wait_recv()

    def gate_up(d):
        o = places[d]
        weights = jnp.concatenate([wf[o, 0], wf[o, 1]], axis=1)
        term = jnp.dot(block(0, o), weights, preferred_element_type=F32)
        sa[...] = term if d == 3 else sa[...] + term

    for d in (3, 0, 1):
        pair_in(d, 0)
        gate_up(d)
    x_rest(0)
    pair_in(2, 0)
    gate_up(2)
    turn = (1 - l, l)

    def swap(src, dst, send, recvs):
        def copy(c):
            at_c = pl.ds(turn[c] * rows, rows)
            return remote(src.at[at_c], dst.at[at_c], send, recvs[c], opposite)

        return copy

    a_swap = swap(sa, zla, a_send, (a_recv, a_recv))
    b_swap = swap(sb, zlb, b_send, (b_recv.at[0], b_recv.at[1]))
    a_all = remote(sa, zla, a_send, a_recv, opposite)
    b_all = remote(sb, zlb, b_send, b_recv.at[0], opposite)

    a_swap(0).start()
    for w in range(2):
        mine_w = pl.ds(bases[w] + y * fourths[w], fourths[w])
        tw[me, w, mine_w] = wf[x, w, pl.ds(k * shard + bases[w] + y * fourths[w], fourths[w])]
    tw[me, 1, :DIRECT] = wf[x, 1, pl.ds(k * shard, DIRECT)]
    a_swap(1).start()
    t_all().wait_recv()

    for w in range(2):
        for way, q in ((0, 0), (1, 1), (0, 1), (1, 0)):
            u_out(way, w, q).start()
    for j in range(2):
        passed(0, j, 1, 0)
        passed(1, j, 1, 0)
    for j in range(2):
        passed(1, j, 1, 1)
        passed(0, j, 1, 1)

    def grad_in(d):
        o = places[d]
        term = lax.dot_general(
            block(1, o), df[o], (COLS, ((), ())), preferred_element_type=F32
        )
        sb[...] = term if d == 3 else sb[...] + term

    w_rest(2)
    for d in (3, 0, 1):
        pair_in(d, 1)
        grad_in(d)
    x_rest(1)
    @pl.loop(1, 8)
    def _(j):
        g_out(j).start()

    for q in range(2):
        u_wait(q, tw.at[pl.ds(q * 4, 4), 0, pl.ds(0, fourths[0] + fourths[1])])
        for w in range(2):
            u_on(w, q).start()
    a_all.wait_recv()
    sums = sa[...] + zla[...]
    gate, up = sums[:, :width], sums[:, width:]
    squashed = jax.nn.sigmoid(gate)
    activated = gate * squashed
    slope = squashed * (1.0 + gate * (1.0 - squashed))
    acts[:, :width] = up * slope
    acts[:, width:] = activated
    hidden[...] = (activated * up).astype(BF16)

    pair_in(2, 1)
    for c in range(2):
        at_s = pl.ds(turn[c] * rows, rows)
        last = jnp.concatenate([xg[p * 4 + xs[2], 1, turn[c]] for p in range(2)], axis=1)
        sb[at_s] += lax.dot_general(
            last, df[xs[2]], (COLS, ((), ())), preferred_element_type=F32
        )
        if c:
            b_swap(0).start()
    def down_part(o):
        return lax.dot_general(
            hidden[...], block(1, o), (ROWS, ((), ())), preferred_element_type=F32
        )

    def gate_part(o):
        return lax.dot_general(
            block(0, o), dg[me], (ROWS, ((), ())), preferred_element_type=F32
        )

    twos, mids, parts, ones, lands = (
        (dtwo, gtwo),
        (dmid, gmid),
        (dpart, gpart),
        (done, gone),
        (dland, gland),
    )

    def halves(i, q):
        size = twos[i].shape[0] // 2
        return pl.ds(q * size, size)

    def two_out(i, q):
        return remote(
            twos[i].at[halves(i, q)],
            mids[i].at[q],
            two_send.at[i],
            two_recv.at[i, q],
            (north, south)[q],
        )

    def one_out(i, way, q):
        return remote(
            ones[i].at[way, halves(i, q)],
            lands[i].at[way, halves(i, q)],
            one_send.at[i],
            one_recv.at[i],
            (north, south)[way],
        )

    def one_parts(i, fn):
        for way in range(2):
            q = way
            term = fn(ys[1 - way])
            size = term.shape[0] // 2
            parts[i][way] = term[q * size : (q + 1) * size]
            ones[i][way, halves(i, 1 - q)] = term[(1 - q) * size : (2 - q) * size].astype(BF16)

    def one_merge(i):
        for way in range(2):
            two_out(i, way).wait_recv()
            ones[i][way, halves(i, way)] = (
                parts[i][way] + mids[i][way].astype(F32)
            ).astype(BF16)

    def finals(i):
        remote(ones[i], lands[i], one_send.at[i], one_recv.at[i], north).wait_recv()
        return lands[i][0].astype(F32) + lands[i][1].astype(F32)

    dtwo[...] = down_part(ys[2]).astype(BF16)
    b_swap(1).start()
    one_parts(0, down_part)
    for q in range(2):
        two_out(0, q).start()
    for way in range(2):
        one_out(0, way, 1 - way).start()

    def d_spot(c, o, e, q):
        return dg.at[o * 2 + c, pl.ds(turn[e] * rows + q * part, part)]

    def dx_out(way, e, q):
        here = d_spot(k, x, e, q)
        return remote(
            here, here, dx_send, dx_recv.at[way, e, q], (right, left)[way]
        )

    def dx_on(e, q):
        here = d_spot(k, xs[q], e, q)
        return remote(here, here, dx_send, dx_recv.at[2, e, 0], (right, left)[q])

    def dx_in(d, e, q):
        here = d_spot(k, xs[d], e, q)
        return remote(here, here, dx_send, dx_recv.at[d, e, q], right)

    def dp_out(d, e, q):
        here = d_spot(k, places[d], e, q)
        return remote(here, here, dp_send, dp_recv.at[d, e], mate)

    def d_half(c, d, e):
        return dg.at[places[d] * 2 + c, pl.ds(turn[e] * rows, rows)]

    def d_far(e):
        here = d_half(k, 2, e)
        remote(here, here, dx_send, dx_recv.at[2, e, 0], right).wait_recv()
        for q in range(2):
            dp_out(2, e, q).start()

    def d_start(e):
        for q in range(2):
            for way in (0, 1) if q == 0 else (1, 0):
                dx_out(way, e, q).start()
            dp_out(3, e, q).start()

    def d_passed(d, e, q):
        dx_in(d, e, q).wait_recv()
        if d == q:
            dx_on(e, q).start()
        dp_out(d, e, q).start()

    def d_near(e):
        for q in range(2):
            d_passed(q, e, q)
        for q in range(2):
            d_passed(1 - q, e, q)

    def gather(d, e):
        base = places[d] * 2
        at_s = pl.ds(turn[e] * rows, rows)
        left_side = jnp.concatenate([dg[base, at_s], dg[base + 1, at_s]], axis=1)
        right_side = jnp.concatenate(
            [tw[base, 0], tw[base, 1], tw[base + 1, 0], tw[base + 1, 1]], axis=1
        )
        term = lax.dot_general(
            left_side, right_side, (COLS, ((), ())), preferred_element_type=F32
        )
        total[e] = term if d == 3 else total[e] + term

    def gathers(e, ds):
        for d in ds:
            here = d_half(1 - k, d, e)
            remote(here, here, dp_send, dp_recv.at[d, e], mate).wait_recv()
            gather(d, e)

    piece = rows // 4

    def f_out(c):
        at_c = pl.ds(c * piece, piece)
        return remote(total.at[0, at_c], near.at[at_c], f_send, f_recv.at[c], flip)

    def r_out(c):
        at_c = pl.ds(c * piece, piece)
        return remote(rounded.at[at_c], result.at[at_c], r_send, r_recv, across)

    def delta(e):
        b_swap(e).wait_recv()
        at_s = pl.ds(turn[e] * rows, rows)
        hidden_grad = sb[at_s] + zlb[at_s]
        dg[me, at_s, :width] = (hidden_grad * acts[at_s, :width]).astype(BF16)
        dg[me, at_s, width:] = (hidden_grad * acts[at_s, width:]).astype(BF16)

    delta(0)
    down_own[...] = down_part(y)
    d_start(0)
    delta(1)
    one_merge(0)
    gtwo[...] = gate_part(ys[2]).astype(BF16)
    for way in range(2):
        one_out(0, way, way).start()
    d_near(0)
    d_start(1)
    for q in range(2):
        two_out(1, q).start()
    one_parts(1, gate_part)
    for way in range(2):
        one_out(1, way, 1 - way).start()
    gown[...] = gate_part(y)
    u_wait(2, tw.at[:, :, pl.ds(0, fourths[0] + fourths[1])])
    g_all().wait_recv()

    gathers(0, (3, 0, 1))
    d_far(0)
    gathers(0, (2,))
    for c in range(2):
        f_out(c).start()
    d_near(1)
    for c in range(2, 4):
        f_out(c).start()
    one_merge(1)
    gathers(1, (3,))
    for way in range(2):
        one_out(1, way, way).start()
    gathers(1, (0, 1))
    d_far(1)
    gathers(1, (2,))
    keeps = [
        pltpu.make_async_copy(src, dst, keep.at[i])
        for i, (src, dst) in enumerate(
            ((down_own, down_out), (gate_own, gate_out), (up_own, up_out), (rounded, result))
        )
    ]
    for c in range(4):
        f_out(c).wait_recv()
        at_c = pl.ds(c * piece, piece)
        rounded[at_c] = (total[1, at_c] + near[at_c]).astype(BF16)

        if c:

            @pl.when(inner)
            def _(c=c):
                r_out(c - 1).start()

    down_own[...] = factor * (down_own[...] + finals(0))
    @pl.when(inner)
    def _():
        r_out(3).start()

    @pl.when(outer)
    def _():
        keeps[3].start()

    both = factor * (gown[...] + finals(1))
    gate_own[...] = both[:, :width]
    up_own[...] = both[:, width:]
    for copy in keeps[:3]:
        copy.start()

    sent = [
        (xg.at[0, :, 0, pl.ds(0, 240)], z_send.at[0]),
        (xg.at[pl.ds(0, 4), 0, 0, pl.ds(0, XFIRST)], zx_send.at[0]),
        (xg.at[pl.ds(0, 3), 0, 0, pl.ds(0, XFIRST)], v_send),
        (xg.at[pl.ds(0, 4), 0, :, pl.ds(0, 240)], x_send),
        (xg.at[:, :, 0], p_send),
        (xg.at[pl.ds(0, 3), 0], y_send),
        (tw.at[:, :, pl.ds(0, 3 * (fourths[0] + fourths[1]) // 2)], u_send),
        (dg.at[pl.ds(0, 3)], dx_send),
        (dg.at[pl.ds(0, 4)], dp_send),
        (total.at[0], f_send),
        (dtwo, two_send.at[0]),
        (gtwo, two_send.at[1]),
        (done, one_send.at[0]),
        (gone, one_send.at[1]),
    ]
    for here, sem in sent:
        remote(here, here, sem, load, mate).wait_send()
    for copy in (a_all, b_all, t_all(), g_all()):
        copy.wait_send()

    @pl.when(inner)
    def _():
        for here, sem in (
            (xg.at[0, :, 0, pl.ds(0, 240)], z_send.at[1]),
            (xg.at[pl.ds(0, 4), 0, 0, pl.ds(0, XFIRST)], zx_send.at[1]),
        ):
            remote(here, here, sem, load, mate).wait_send()
        remote(rounded, result, r_send, r_recv, across).wait()

    @pl.when(outer)
    def _():
        keeps[3].wait()

    for copy in keeps[:3]:
        copy.wait()


def store_kernel(*refs):
    found, kept, held, sem = refs[:4], refs[4:8], refs[8:12], refs[12]
    loads = [pltpu.make_async_copy(found[i], held[i], sem.at[0, i]) for i in range(4)]
    stores = [pltpu.make_async_copy(held[i], kept[i], sem.at[1, i]) for i in range(4)]
    for copy in loads:
        copy.start()
    for i in range(4):
        loads[i].wait()
        stores[i].start()
    for copy in stores:
        copy.wait()


HBM = pl.BlockSpec(memory_space=pltpu.HBM)
DMA = pltpu.SemaphoreType.DMA


def body(tokens, out_grad, gate_weight, up_weight, down_weight):
    nf, nt = lax.axis_size("fsdp"), lax.axis_size("tp")
    rows, shard = tokens.shape
    deep, width = gate_weight.shape
    assert nf == 8 and nt == 16 and deep == 2 * shard
    factor = 1.0 / math.sqrt(rows * nf)
    tall = 2 * rows
    wide = 2 * width

    shapes = (
        jax.ShapeDtypeStruct((rows, shard), BF16),
        jax.ShapeDtypeStruct((deep, width), F32),
        jax.ShapeDtypeStruct((deep, width), F32),
        jax.ShapeDtypeStruct((width, deep), F32),
    )
    found = tuple(
        pl.pallas_call(
            functools.partial(kernel, factor),
            out_shape=shapes,
            in_specs=[HBM] * 5,
            out_specs=(HBM,) * 4,
            scratch_shapes=[
                pltpu.VMEM((deep, width), F32),
                pltpu.VMEM((deep, width), F32),
                pltpu.VMEM((width, deep), F32),
                pltpu.VMEM((8, 2, 3, rows, shard), BF16),
                pltpu.VMEM((4, 2, deep, width), BF16),
                pltpu.VMEM((4, width, deep), BF16),
                pltpu.VMEM((tall, wide), F32),
                pltpu.VMEM((tall, wide), F32),
                pltpu.VMEM((tall, width), F32),
                pltpu.VMEM((tall, width), F32),
                pltpu.VMEM((tall, wide), F32),
                pltpu.VMEM((tall, width), BF16),
                pltpu.VMEM((8, tall, wide), BF16),
                pltpu.VMEM((8, 2, shard, width), BF16),
                pltpu.VMEM((2, width // 2, deep), F32),
                pltpu.VMEM((2, deep // 2, wide), F32),
                pltpu.VMEM((width, deep), BF16),
                pltpu.VMEM((deep, wide), BF16),
                pltpu.VMEM((2, width, deep), BF16),
                pltpu.VMEM((2, deep, wide), BF16),
                pltpu.VMEM((2, width // 2, deep), BF16),
                pltpu.VMEM((2, deep // 2, wide), BF16),
                pltpu.VMEM((2, width, deep), BF16),
                pltpu.VMEM((2, deep, wide), BF16),
                pltpu.VMEM((deep, wide), F32),
                pltpu.VMEM((2, rows, shard), F32),
                pltpu.VMEM((rows, shard), F32),
                pltpu.VMEM((rows, shard), BF16),
                DMA(()),
                DMA((4,)),
                DMA((2,)),
                DMA((2, 2, 2)),
                DMA(()),
                DMA((2, 2, 5)),
                DMA(()),
                DMA((4, 2)),
                DMA(()),
                DMA((4,)),
                DMA((2,)),
                DMA((3,)),
                DMA(()),
                DMA((3, 3)),
                DMA(()),
                DMA(()),
                DMA(()),
                DMA((2,)),
                DMA(()),
                DMA(()),
                DMA(()),
                DMA((3,)),
                DMA(()),
                DMA(()),
                DMA(()),
                DMA((4,)),
                DMA(()),
                DMA((3, 2, 2)),
                DMA(()),
                DMA((4, 2)),
                DMA((2,)),
                DMA((2, 2)),
                DMA((2,)),
                DMA((2,)),
                DMA(()),
                DMA(()),
            ],
            compiler_params=pltpu.CompilerParams(
                collective_id=0, has_side_effects=True, vmem_limit_bytes=VMEM_LIMIT
            ),
            name="block",
        )(tokens, out_grad, gate_weight, up_weight, down_weight)
    )
    return tuple(
        pl.pallas_call(
            store_kernel,
            out_shape=shapes,
            in_specs=[HBM] * 4,
            out_specs=(HBM,) * 4,
            scratch_shapes=[pltpu.VMEM(s.shape, s.dtype) for s in shapes] + [DMA((2, 4))],
            compiler_params=pltpu.CompilerParams(vmem_limit_bytes=VMEM_LIMIT),
            name="store",
        )(*found)
    )


def solution(mesh):
    return jax.shard_map(
        body,
        mesh=mesh,
        in_specs=(
            P("fsdp", "tp"),
            P("fsdp", "tp"),
            P("fsdp", "tp"),
            P("fsdp", "tp"),
            P("tp", "fsdp"),
        ),
        out_specs=(P("fsdp", "tp"), P("fsdp", "tp"), P("fsdp", "tp"), P("tp", "fsdp")),
        check_vma=False,
    )
```

```python
import functools
import math

import jax
import jax.numpy as jnp
from jax import lax
from jax.sharding import PartitionSpec as P
from jax.experimental import pallas as pl
from jax.experimental.pallas import tpu as pltpu

MESH = pl.DeviceIdType.MESH
F32 = jnp.float32
BF16 = jnp.bfloat16
VMEM_LIMIT = 60 * 1024 * 1024
XFIRST = 32
PIECES = 8
DIRECT = 384
ROWS = ((0,), (0,))
COLS = ((1,), (1,))


def kernel(
    factor,
    tokens,
    grads,
    gate_weight,
    up_weight,
    down_weight,
    result,
    gate_out,
    up_out,
    down_out,
    gate_own,
    up_own,
    down_own,
    xg,
    wf,
    df,
    sa,
    zla,
    sb,
    zlb,
    acts,
    hidden,
    dg,
    tw,
    dpart,
    gpart,
    dtwo,
    gtwo,
    done,
    gone,
    dmid,
    gmid,
    dland,
    gland,
    gown,
    total,
    near,
    rounded,
    load,
    keep,
    z_send,
    z_recv,
    x_send,
    x_recv,
    p_send,
    p_recv,
    v_send,
    v_recv,
    zx_send,
    zx_recv,
    y_send,
    y_recv,
    a_send,
    a_recv,
    b_send,
    b_recv,
    t_send,
    t_recv,
    u_send,
    u_recv,
    g_send,
    g_recv,
    f_send,
    f_recv,
    dx_send,
    dx_recv,
    dp_send,
    dp_recv,
    two_send,
    two_recv,
    one_send,
    one_recv,
    r_send,
    r_recv,
):
    f, t = lax.axis_index("fsdp"), lax.axis_index("tp")
    h, y = lax.div(f, 4), lax.rem(f, 4)
    l, x, k = lax.div(t, 8), lax.rem(lax.div(t, 2), 4), lax.rem(t, 2)
    outer = h == l
    inner = h != l
    rows, shard = tokens.shape
    deep, width = gate_weight.shape
    part = rows // 2
    zparts = ((rows - XFIRST) // 2, part)
    first = rows - XFIRST
    xpart = XFIRST // 2
    odd = (h - l) * (h - l)
    home = h * (1 - odd) + 2 * odd
    wide = 2 * width

    def at(xx, yy, hh, ll, kk):
        return (hh * 4 + yy, ll * 8 + xx * 2 + kk)

    xs = (lax.rem(x + 3, 4), lax.rem(x + 1, 4), lax.rem(x + 2, 4))
    ys = (lax.rem(y + 3, 4), lax.rem(y + 1, 4), lax.rem(y + 2, 4))
    right, left = at(xs[1], y, h, l, k), at(xs[0], y, h, l, k)
    north, south = at(x, ys[1], h, l, k), at(x, ys[0], h, l, k)
    mate = at(x, y, h, l, 1 - k)
    flip = at(x, y, h, 1 - l, k)
    across = at(x, y, 1 - h, 1 - l, k)
    opposite = at(x, y, 1 - h, l, k)
    me = 2 * x + k

    def remote(src, dst, send, recv, device):
        return pltpu.make_async_remote_copy(
            src_ref=src,
            dst_ref=dst,
            send_sem=send,
            recv_sem=recv,
            device_id=device,
            device_id_type=MESH,
        )

    copies = [
        pltpu.make_async_copy(ref, spot, load)
        for ref, spot in (
            (tokens, xg.at[k * 4 + x, 0, home]),
            (gate_weight, wf.at[y, 0]),
            (up_weight, wf.at[y, 1]),
            (grads, xg.at[k * 4 + x, 1, home]),
            (down_weight, df.at[y]),
        )
    ]
    for copy in copies:
        copy.start()

    barrier = pltpu.get_barrier_semaphore()
    for j in range(1, 16):
        pl.semaphore_signal(
            barrier, inc=1, device_id=(f, lax.rem(t + j, 16)), device_id_type=MESH
        )
    for peer in (north, south, opposite, across):
        pl.semaphore_signal(barrier, inc=1, device_id=peer, device_id_type=MESH)
    pl.semaphore_wait(barrier, 19)

    all_in = xg.at[pl.ds(0, 5), 0, 0]
    pltpu.make_async_copy(all_in, all_in, load).wait()

    def w_spot(o, w, q):
        if w == 2:
            return df.at[o, pl.ds(q * (width // 2), width // 2)]
        return wf.at[o, w, pl.ds(q * (deep // 2), deep // 2)]

    def w_out(way, w, q):
        return remote(
            w_spot(y, w, q),
            w_spot(y, w, q),
            y_send,
            y_recv.at[w, q if way == q else 2],
            (north, south)[way],
        )

    def w_on(w, q):
        here = w_spot(ys[q], w, q)
        return remote(here, here, y_send, y_recv.at[w, 2], (north, south)[q])

    def w_wait(w, e, here):
        remote(here, here, y_send, y_recv.at[w, e], north).wait_recv()

    def w_start(w):
        for way, q in ((0, 0), (1, 1), (0, 1), (1, 0)):
            w_out(way, w, q).start()

    def w_forward(w):
        for q in range(2):
            w_wait(w, q, w_spot(ys[q], w, q))
            w_on(w, q).start()

    def w_rest(w):
        w_wait(w, 2, df.at[pl.ds(0, 2)] if w == 2 else wf.at[pl.ds(0, 2), w])

    slot = (h, 1 - h)

    def x_own(m, q):
        return xg.at[k * 4 + x, m, home, pl.ds(q * zparts[m], zparts[m])]

    def x_spot(p, o, j, m, q):
        return xg.at[p * 4 + o, m, slot[j], pl.ds(q * zparts[m], zparts[m])]

    def z_out(m, q, device, j):
        spot = xg.at[k * 4 + x, m, h, pl.ds(q * zparts[m], zparts[m])]
        return remote(x_own(m, q), spot, z_send.at[0], z_recv.at[j, m, q], device)

    def z_on(m, q):
        here = x_spot(k, x, 1, m, q)
        return remote(here, here, z_send.at[1], z_recv.at[1, m, q], flip)

    def z_in(j, m, q):
        here = x_spot(k, x, j, m, q)
        return remote(here, here, z_send.at[0], z_recv.at[j, m, q], flip)

    def x_out(way, src, j, m, q):
        return remote(
            src,
            x_spot(k, x, j, m, q),
            x_send,
            x_recv.at[m, q, 2 * way + j],
            (right, left)[way],
        )

    def x_on(j, m, q):
        here = x_spot(k, xs[q], j, m, q)
        return remote(
            here, here, x_send, x_recv.at[m, q, 4], (right, left)[q]
        )

    def x_wait(m, q, e, here):
        remote(here, here, x_send, x_recv.at[m, q, e], right).wait_recv()

    places = (*xs, x)

    def p_out(d, src, j, m, q):
        return remote(
            src,
            x_spot(k, places[d], j, m, q),
            p_send,
            p_recv.at[d, m],
            mate,
        )

    def spread(src, j, m, q):
        for way in (0, 1) if q == 0 else (1, 0):
            x_out(way, src, j, m, q).start()
        p_out(3, src, j, m, q).start()

    def passed(d, j, m, q):
        x_wait(m, q, 2 * d + j, x_spot(k, xs[d], j, m, q))
        if d == q:
            x_on(j, m, q).start()
        p_out(d, x_spot(k, places[d], j, m, q), j, m, q).start()

    def x_rest(m):
        for q in range(2):
            here = xg.at[k * 4 + xs[2], m, pl.ds(0, 2), pl.ds(q * zparts[m], zparts[m])]
            x_wait(m, q, 4, here)
            for j in range(2):
                p_out(2, x_spot(k, xs[2], j, m, q), j, m, q).start()

    def z_forward(m, q):
        @pl.when(inner)
        def _():
            z_in(1, m, q).wait_recv()
            z_on(m, q).start()

    def z_near(m, q):
        @pl.when(inner)
        def _():
            z_in(0, m, q).wait_recv()

        spread(x_spot(k, x, 0, m, q), 0, m, q)

    def z_far(m, q):
        @pl.when(outer)
        def _():
            z_in(1, m, q).wait_recv()

        spread(x_spot(k, x, 1, m, q), 1, m, q)

    def z_near_inner(m, q):
        @pl.when(inner)
        def _():
            z_in(0, m, q).wait_recv()
            spread(x_spot(k, x, 0, m, q), 0, m, q)

    fourths = (shard // 4, (shard - DIRECT) // 4)
    bases = (0, DIRECT)

    def t_copy(u, w):
        return remote(
            wf.at[
                lax.div(u, 2),
                w,
                pl.ds(lax.rem(u, 2) * shard + bases[w] + y * fourths[w], fourths[w]),
            ],
            tw.at[me, w, pl.ds(bases[w] + y * fourths[w], fourths[w])],
            t_send,
            t_recv,
            (f, l * 8 + u),
        )

    def t_out(w, j):
        return t_copy(lax.rem(me + j, 8), w)

    def t_all():
        here = tw.at[pl.ds(0, 7), 0, pl.ds(0, fourths[0] + fourths[1])]
        return remote(here, here, t_send, t_recv, mate)

    def g_out(j):
        u = lax.rem(me + j, 8)
        return remote(
            wf.at[lax.div(u, 2), 1, pl.ds(lax.rem(u, 2) * shard, DIRECT)],
            tw.at[me, 1, pl.ds(0, DIRECT)],
            g_send,
            g_recv,
            (f, l * 8 + u),
        )

    def g_all():
        here = tw.at[pl.ds(0, 7), 1, pl.ds(0, DIRECT)]
        return remote(here, here, g_send, g_recv, mate)

    def u_spot(o, w, q):
        return tw.at[pl.ds(q * 4, 4), w, pl.ds(bases[w] + o * fourths[w], fourths[w])]

    def u_out(way, w, q):
        here = u_spot(y, w, q)
        return remote(
            here, here, u_send, u_recv.at[q if way == q else 2], (north, south)[way]
        )

    def u_on(w, q):
        here = u_spot(ys[q], w, q)
        return remote(here, here, u_send, u_recv.at[2], (north, south)[q])

    def u_wait(e, here):
        remote(here, here, u_send, u_recv.at[e], north).wait_recv()

    def v_spot(o, q):
        return xg.at[k * 4 + o, 0, home, pl.ds(first + q * xpart, xpart)]

    def v_out(way, q):
        here = v_spot(x, q)
        return remote(
            here, here, v_send, v_recv.at[q if way == q else 2], (right, left)[way]
        )

    def v_on(q):
        here = v_spot(xs[q], q)
        return remote(here, here, v_send, v_recv.at[3], (right, left)[q])

    def v_wait(e, here):
        remote(here, here, v_send, v_recv.at[e], right).wait_recv()

    def zx_spot(p, d, at_s):
        return xg.at[p * 4 + places[d], 0, at_s, pl.ds(first, XFIRST)]

    def zx_out(d, device, j):
        return remote(
            zx_spot(k, d, home),
            zx_spot(k, d, h),
            zx_send.at[0],
            zx_recv.at[j + (j * d == 2)],
            device,
        )

    def zx_on(d):
        here = zx_spot(k, d, 1 - h)
        return remote(here, here, zx_send.at[1], zx_recv.at[1 + (d == 2)], flip)

    def zx_wait(e, count):
        here = xg.at[pl.ds(0, count), 0, 0, pl.ds(first, XFIRST)]
        remote(here, here, zx_send.at[0], zx_recv.at[e], flip).wait_recv()

    def px_out(d, j):
        here = zx_spot(k, d, slot[j])
        return remote(here, here, p_send, p_recv.at[d, 0], mate)

    def v_start():
        for q in range(2):
            for way in (0, 1) if q == 0 else (1, 0):
                v_out(way, q).start()

    def v_near():
        for q in range(2):
            v_wait(q, v_spot(xs[q], q))
            v_on(q).start()
        v_wait(2, zx_spot(k, 0, home))

    def v_far():
        v_wait(3, zx_spot(k, 2, home))

    def zx_start(ds):
        for d in ds:

            @pl.when(outer)
            def _(d=d):
                zx_out(d, flip, 0).start()
                px_out(d, 0).start()

            @pl.when(inner)
            def _(d=d):
                zx_out(d, across, 1).start()

    def zx_pass(e, ds):
        @pl.when(inner)
        def _():
            zx_wait(e, len(ds))
            for d in ds:
                zx_on(d).start()

    def zx_take():
        @pl.when(inner)
        def _():
            zx_wait(0, 4)
            for d in range(4):
                px_out(d, 0).start()

        @pl.when(outer)
        def _():
            zx_wait(1, 3)
            zx_wait(2, 1)

        for d in range(4):
            px_out(d, 1).start()

    def z_start(m):
        @pl.when(outer)
        def _():
            for q in range(2):
                z_out(m, q, flip, 0).start()

        @pl.when(inner)
        def _():
            for q in range(2):
                z_out(m, q, across, 1).start()

    v_start()
    z_start(0)

    @pl.when(outer)
    def _():
        for q in range(2):
            spread(x_own(0, q), 0, 0, q)

    zx_start((3,))
    w_start(0)
    w_start(1)

    v_near()
    zx_start((0, 1))
    z_forward(0, 0)
    z_near_inner(0, 0)
    z_far(0, 0)
    v_far()
    zx_start((2,))
    z_start(1)
    z_forward(0, 1)
    z_near_inner(0, 1)
    z_far(0, 1)
    w_forward(0)
    for j in range(2):
        passed(0, j, 0, 0)
        passed(1, j, 0, 0)
    w_forward(1)
    w_start(2)
    for j in range(2):
        passed(1, j, 0, 1)
        passed(0, j, 0, 1)
    z_forward(1, 0)
    zx_pass(1, (3, 0, 1))
    z_forward(1, 1)
    zx_pass(2, (2,))
    z_near(1, 0)
    z_near(1, 1)
    w_rest(0)
    w_rest(1)

    @pl.loop(1, 8)
    def _(j):
        for w in range(2):
            t_out(w, j).start()

    z_far(1, 0)
    z_far(1, 1)
    w_forward(2)
    zx_take()
    tall = 2 * rows

    def block(m, o):
        return jnp.concatenate(
            [xg[p * 4 + o, m, :2].reshape(tall, shard) for p in range(2)], axis=1
        )

    def pair_in(d, m):
        here = xg.at[(1 - k) * 4 + places[d], m, pl.ds(0, 2)]
        remote(here, here, p_send, p_recv.at[d, m], mate).wait_recv()

    def gate_up(d):
        o = places[d]
        weights = jnp.concatenate([wf[o, 0], wf[o, 1]], axis=1)
        term = jnp.dot(block(0, o), weights, preferred_element_type=F32)
        sa[...] = term if d == 3 else sa[...] + term

    for d in (3, 0, 1):
        pair_in(d, 0)
        gate_up(d)
    x_rest(0)
    pair_in(2, 0)
    gate_up(2)
    turn = (1 - l, l)

    def swap(src, dst, send, recvs):
        def copy(c):
            at_c = pl.ds(turn[c] * rows, rows)
            return remote(src.at[at_c], dst.at[at_c], send, recvs[c], opposite)

        return copy

    a_swap = swap(sa, zla, a_send, (a_recv, a_recv))
    b_swap = swap(sb, zlb, b_send, (b_recv.at[0], b_recv.at[1]))
    a_all = remote(sa, zla, a_send, a_recv, opposite)
    b_all = remote(sb, zlb, b_send, b_recv.at[0], opposite)

    a_swap(0).start()
    for w in range(2):
        mine_w = pl.ds(bases[w] + y * fourths[w], fourths[w])
        tw[me, w, mine_w] = wf[x, w, pl.ds(k * shard + bases[w] + y * fourths[w], fourths[w])]
    tw[me, 1, :DIRECT] = wf[x, 1, pl.ds(k * shard, DIRECT)]
    a_swap(1).start()
    t_all().wait_recv()

    for w in range(2):
        for way, q in ((0, 0), (1, 1), (0, 1), (1, 0)):
            u_out(way, w, q).start()
    for j in range(2):
        passed(0, j, 1, 0)
        passed(1, j, 1, 0)
    for j in range(2):
        passed(1, j, 1, 1)
        passed(0, j, 1, 1)

    def grad_in(d):
        o = places[d]
        term = lax.dot_general(
            block(1, o), df[o], (COLS, ((), ())), preferred_element_type=F32
        )
        sb[...] = term if d == 3 else sb[...] + term

    w_rest(2)
    for d in (3, 0, 1):
        pair_in(d, 1)
        grad_in(d)
    x_rest(1)
    @pl.loop(1, 8)
    def _(j):
        g_out(j).start()

    for q in range(2):
        u_wait(q, tw.at[pl.ds(q * 4, 4), 0, pl.ds(0, fourths[0] + fourths[1])])
        for w in range(2):
            u_on(w, q).start()
    a_all.wait_recv()
    sums = sa[...] + zla[...]
    gate, up = sums[:, :width], sums[:, width:]
    squashed = jax.nn.sigmoid(gate)
    activated = gate * squashed
    slope = squashed * (1.0 + gate * (1.0 - squashed))
    acts[:, :width] = up * slope
    acts[:, width:] = activated
    hidden[...] = (activated * up).astype(BF16)

    pair_in(2, 1)
    for c in range(2):
        at_s = pl.ds(turn[c] * rows, rows)
        last = jnp.concatenate([xg[p * 4 + xs[2], 1, turn[c]] for p in range(2)], axis=1)
        sb[at_s] += lax.dot_general(
            last, df[xs[2]], (COLS, ((), ())), preferred_element_type=F32
        )
        if c:
            b_swap(0).start()
    def down_part(o):
        return lax.dot_general(
            hidden[...], block(1, o), (ROWS, ((), ())), preferred_element_type=F32
        )

    def down_mine(q):
        at_q = pl.ds(q * (width // 2), width // 2)
        down_own[at_q] = lax.dot_general(
            hidden[:, q * (width // 2) : (q + 1) * (width // 2)],
            block(1, y),
            (ROWS, ((), ())),
            preferred_element_type=F32,
        )

    def gate_part(o):
        return lax.dot_general(
            block(0, o), dg[me], (ROWS, ((), ())), preferred_element_type=F32
        )

    twos, mids, parts, ones, lands = (
        (dtwo, gtwo),
        (dmid, gmid),
        (dpart, gpart),
        (done, gone),
        (dland, gland),
    )

    def halves(i, q):
        size = twos[i].shape[0] // 2
        return pl.ds(q * size, size)

    def two_out(i, q):
        return remote(
            twos[i].at[halves(i, q)],
            mids[i].at[q],
            two_send.at[i],
            two_recv.at[i, q],
            (north, south)[q],
        )

    def one_out(i, way, q):
        return remote(
            ones[i].at[way, halves(i, q)],
            lands[i].at[way, halves(i, q)],
            one_send.at[i],
            one_recv.at[i],
            (north, south)[way],
        )

    def one_part(i, fn, way):
        q = way
        term = fn(ys[1 - way])
        size = term.shape[0] // 2
        parts[i][way] = term[q * size : (q + 1) * size]
        ones[i][way, halves(i, 1 - q)] = term[(1 - q) * size : (2 - q) * size].astype(BF16)

    def one_merge(i):
        for way in range(2):
            two_out(i, way).wait_recv()
            ones[i][way, halves(i, way)] = (
                parts[i][way] + mids[i][way].astype(F32)
            ).astype(BF16)

    def finals(i):
        remote(ones[i], lands[i], one_send.at[i], one_recv.at[i], north).wait_recv()
        return lands[i][0].astype(F32) + lands[i][1].astype(F32)

    dtwo[...] = down_part(ys[2]).astype(BF16)
    b_swap(1).start()
    one_part(0, down_part, 0)
    for q in range(2):
        two_out(0, q).start()
    one_part(0, down_part, 1)
    for way in range(2):
        one_out(0, way, 1 - way).start()

    def d_spot(c, o, e, q):
        return dg.at[o * 2 + c, pl.ds(turn[e] * rows + q * part, part)]

    def dx_out(way, e, q):
        here = d_spot(k, x, e, q)
        return remote(
            here, here, dx_send, dx_recv.at[way, e, q], (right, left)[way]
        )

    def dx_on(e, q):
        here = d_spot(k, xs[q], e, q)
        return remote(here, here, dx_send, dx_recv.at[2, e, 0], (right, left)[q])

    def dx_in(d, e, q):
        here = d_spot(k, xs[d], e, q)
        return remote(here, here, dx_send, dx_recv.at[d, e, q], right)

    def dp_out(d, e, q):
        here = d_spot(k, places[d], e, q)
        return remote(here, here, dp_send, dp_recv.at[d, e], mate)

    def d_half(c, d, e):
        return dg.at[places[d] * 2 + c, pl.ds(turn[e] * rows, rows)]

    def d_far(e):
        here = d_half(k, 2, e)
        remote(here, here, dx_send, dx_recv.at[2, e, 0], right).wait_recv()
        for q in range(2):
            dp_out(2, e, q).start()

    def d_start(e):
        for q in range(2):
            for way in (0, 1) if q == 0 else (1, 0):
                dx_out(way, e, q).start()
            dp_out(3, e, q).start()

    def d_passed(d, e, q):
        dx_in(d, e, q).wait_recv()
        if d == q:
            dx_on(e, q).start()
        dp_out(d, e, q).start()

    def d_near(e):
        for q in range(2):
            d_passed(q, e, q)
        for q in range(2):
            d_passed(1 - q, e, q)

    def gather(d, e):
        base = places[d] * 2
        at_s = pl.ds(turn[e] * rows, rows)
        left_side = jnp.concatenate([dg[base, at_s], dg[base + 1, at_s]], axis=1)
        right_side = jnp.concatenate(
            [tw[base, 0], tw[base, 1], tw[base + 1, 0], tw[base + 1, 1]], axis=1
        )
        term = lax.dot_general(
            left_side, right_side, (COLS, ((), ())), preferred_element_type=F32
        )
        total[e] = term if d == 3 else total[e] + term

    def gathers(e, ds):
        for d in ds:
            here = d_half(1 - k, d, e)
            remote(here, here, dp_send, dp_recv.at[d, e], mate).wait_recv()
            gather(d, e)

    piece = rows // PIECES

    def f_out(c):
        at_c = pl.ds(c * piece, piece)
        return remote(total.at[0, at_c], near.at[at_c], f_send, f_recv.at[c], flip)

    def r_out(c):
        at_c = pl.ds(c * piece, piece)
        return remote(rounded.at[at_c], result.at[at_c], r_send, r_recv, across)

    def delta(e):
        b_swap(e).wait_recv()
        at_s = pl.ds(turn[e] * rows, rows)
        hidden_grad = sb[at_s] + zlb[at_s]
        dg[me, at_s, :width] = (hidden_grad * acts[at_s, :width]).astype(BF16)
        dg[me, at_s, width:] = (hidden_grad * acts[at_s, width:]).astype(BF16)

    delta(0)
    down_mine(0)
    d_start(0)
    one_merge(0)
    down_mine(1)
    for way in range(2):
        one_out(0, way, way).start()
    delta(1)
    gtwo[...] = gate_part(ys[2]).astype(BF16)
    one_part(1, gate_part, 0)
    for q in range(2):
        two_out(1, q).start()
    one_part(1, gate_part, 1)
    one_out(1, 0, 1).start()
    d_near(0)
    one_out(1, 1, 0).start()
    d_start(1)
    gown[...] = gate_part(y)
    u_wait(2, tw.at[:, :, pl.ds(0, fourths[0] + fourths[1])])
    g_all().wait_recv()

    gathers(0, (3, 0, 1))
    d_far(0)
    gathers(0, (2,))
    for c in range(PIECES // 2):
        f_out(c).start()
    d_near(1)
    for c in range(PIECES // 2, PIECES):
        f_out(c).start()
    one_merge(1)
    gathers(1, (3,))
    for way in range(2):
        one_out(1, way, way).start()
    gathers(1, (0, 1))
    d_far(1)
    gathers(1, (2,))
    keeps = [
        pltpu.make_async_copy(src, dst, keep.at[i])
        for i, (src, dst) in enumerate(
            ((down_own, down_out), (gate_own, gate_out), (up_own, up_out), (rounded, result))
        )
    ]
    for c in range(PIECES):
        f_out(c).wait_recv()
        at_c = pl.ds(c * piece, piece)
        rounded[at_c] = (total[1, at_c] + near[at_c]).astype(BF16)

        if c:

            @pl.when(inner)
            def _(c=c):
                r_out(c - 1).start()

    down_own[...] = factor * (down_own[...] + finals(0))
    @pl.when(inner)
    def _():
        r_out(PIECES - 1).start()

    @pl.when(outer)
    def _():
        keeps[3].start()

    both = factor * (gown[...] + finals(1))
    gate_own[...] = both[:, :width]
    up_own[...] = both[:, width:]
    for copy in keeps[:3]:
        copy.start()

    sent = [
        (xg.at[0, :, 0, pl.ds(0, 240)], z_send.at[0]),
        (xg.at[pl.ds(0, 4), 0, 0, pl.ds(0, XFIRST)], zx_send.at[0]),
        (xg.at[pl.ds(0, 3), 0, 0, pl.ds(0, XFIRST)], v_send),
        (xg.at[pl.ds(0, 4), 0, :, pl.ds(0, 240)], x_send),
        (xg.at[:, :, 0], p_send),
        (xg.at[pl.ds(0, 3), 0], y_send),
        (tw.at[:, :, pl.ds(0, 3 * (fourths[0] + fourths[1]) // 2)], u_send),
        (dg.at[pl.ds(0, 3)], dx_send),
        (dg.at[pl.ds(0, 4)], dp_send),
        (total.at[0], f_send),
        (dtwo, two_send.at[0]),
        (gtwo, two_send.at[1]),
        (done, one_send.at[0]),
        (gone, one_send.at[1]),
    ]
    for here, sem in sent:
        remote(here, here, sem, load, mate).wait_send()
    for copy in (a_all, b_all, t_all(), g_all()):
        copy.wait_send()

    @pl.when(inner)
    def _():
        for here, sem in (
            (xg.at[0, :, 0, pl.ds(0, 240)], z_send.at[1]),
            (xg.at[pl.ds(0, 4), 0, 0, pl.ds(0, XFIRST)], zx_send.at[1]),
        ):
            remote(here, here, sem, load, mate).wait_send()
        remote(rounded, result, r_send, r_recv, across).wait()

    @pl.when(outer)
    def _():
        keeps[3].wait()

    for copy in keeps[:3]:
        copy.wait()


def store_kernel(*refs):
    found, kept, held, sem = refs[:4], refs[4:8], refs[8:12], refs[12]
    loads = [pltpu.make_async_copy(found[i], held[i], sem.at[0, i]) for i in range(4)]
    stores = [pltpu.make_async_copy(held[i], kept[i], sem.at[1, i]) for i in range(4)]
    for copy in loads:
        copy.start()
    for i in range(4):
        loads[i].wait()
        stores[i].start()
    for copy in stores:
        copy.wait()


HBM = pl.BlockSpec(memory_space=pltpu.HBM)
DMA = pltpu.SemaphoreType.DMA


def body(tokens, out_grad, gate_weight, up_weight, down_weight):
    nf, nt = lax.axis_size("fsdp"), lax.axis_size("tp")
    rows, shard = tokens.shape
    deep, width = gate_weight.shape
    assert nf == 8 and nt == 16 and deep == 2 * shard
    factor = 1.0 / math.sqrt(rows * nf)
    tall = 2 * rows
    wide = 2 * width

    shapes = (
        jax.ShapeDtypeStruct((rows, shard), BF16),
        jax.ShapeDtypeStruct((deep, width), F32),
        jax.ShapeDtypeStruct((deep, width), F32),
        jax.ShapeDtypeStruct((width, deep), F32),
    )
    found = tuple(
        pl.pallas_call(
            functools.partial(kernel, factor),
            out_shape=shapes,
            in_specs=[HBM] * 5,
            out_specs=(HBM,) * 4,
            scratch_shapes=[
                pltpu.VMEM((deep, width), F32),
                pltpu.VMEM((deep, width), F32),
                pltpu.VMEM((width, deep), F32),
                pltpu.VMEM((8, 2, 3, rows, shard), BF16),
                pltpu.VMEM((4, 2, deep, width), BF16),
                pltpu.VMEM((4, width, deep), BF16),
                pltpu.VMEM((tall, wide), F32),
                pltpu.VMEM((tall, wide), F32),
                pltpu.VMEM((tall, width), F32),
                pltpu.VMEM((tall, width), F32),
                pltpu.VMEM((tall, wide), F32),
                pltpu.VMEM((tall, width), BF16),
                pltpu.VMEM((8, tall, wide), BF16),
                pltpu.VMEM((8, 2, shard, width), BF16),
                pltpu.VMEM((2, width // 2, deep), F32),
                pltpu.VMEM((2, deep // 2, wide), F32),
                pltpu.VMEM((width, deep), BF16),
                pltpu.VMEM((deep, wide), BF16),
                pltpu.VMEM((2, width, deep), BF16),
                pltpu.VMEM((2, deep, wide), BF16),
                pltpu.VMEM((2, width // 2, deep), BF16),
                pltpu.VMEM((2, deep // 2, wide), BF16),
                pltpu.VMEM((2, width, deep), BF16),
                pltpu.VMEM((2, deep, wide), BF16),
                pltpu.VMEM((deep, wide), F32),
                pltpu.VMEM((2, rows, shard), F32),
                pltpu.VMEM((rows, shard), F32),
                pltpu.VMEM((rows, shard), BF16),
                DMA(()),
                DMA((4,)),
                DMA((2,)),
                DMA((2, 2, 2)),
                DMA(()),
                DMA((2, 2, 5)),
                DMA(()),
                DMA((4, 2)),
                DMA(()),
                DMA((4,)),
                DMA((2,)),
                DMA((3,)),
                DMA(()),
                DMA((3, 3)),
                DMA(()),
                DMA(()),
                DMA(()),
                DMA((2,)),
                DMA(()),
                DMA(()),
                DMA(()),
                DMA((3,)),
                DMA(()),
                DMA(()),
                DMA(()),
                DMA((PIECES,)),
                DMA(()),
                DMA((3, 2, 2)),
                DMA(()),
                DMA((4, 2)),
                DMA((2,)),
                DMA((2, 2)),
                DMA((2,)),
                DMA((2,)),
                DMA(()),
                DMA(()),
            ],
            compiler_params=pltpu.CompilerParams(
                collective_id=0, has_side_effects=True, vmem_limit_bytes=VMEM_LIMIT
            ),
            name="block",
        )(tokens, out_grad, gate_weight, up_weight, down_weight)
    )
    return tuple(
        pl.pallas_call(
            store_kernel,
            out_shape=shapes,
            in_specs=[HBM] * 4,
            out_specs=(HBM,) * 4,
            scratch_shapes=[pltpu.VMEM(s.shape, s.dtype) for s in shapes] + [DMA((2, 4))],
            compiler_params=pltpu.CompilerParams(vmem_limit_bytes=VMEM_LIMIT),
            name="store",
        )(*found)
    )


def solution(mesh):
    return jax.shard_map(
        body,
        mesh=mesh,
        in_specs=(
            P("fsdp", "tp"),
            P("fsdp", "tp"),
            P("fsdp", "tp"),
            P("fsdp", "tp"),
            P("tp", "fsdp"),
        ),
        out_specs=(P("fsdp", "tp"), P("fsdp", "tp"), P("fsdp", "tp"), P("tp", "fsdp")),
        check_vma=False,
    )
```

```python
import functools
import math

import jax
import jax.numpy as jnp
from jax import lax
from jax.sharding import PartitionSpec as P
from jax.experimental import pallas as pl
from jax.experimental.pallas import tpu as pltpu

MESH = pl.DeviceIdType.MESH
F32 = jnp.float32
BF16 = jnp.bfloat16
VMEM_LIMIT = 60 * 1024 * 1024
XFIRST = 32
PIECES = 8
DIRECT = 384
ROWS = ((0,), (0,))
COLS = ((1,), (1,))


def kernel(
    factor,
    tokens,
    grads,
    gate_weight,
    up_weight,
    down_weight,
    result,
    gate_out,
    up_out,
    down_out,
    gate_own,
    up_own,
    down_own,
    xg,
    wf,
    df,
    sa,
    zla,
    sb,
    zlb,
    acts,
    hidden,
    dg,
    tw,
    dpart,
    gpart,
    dtwo,
    gtwo,
    done,
    gone,
    dmid,
    gmid,
    dland,
    gland,
    gown,
    total,
    near,
    slim,
    slim_near,
    rounded,
    load,
    keep,
    z_send,
    z_recv,
    x_send,
    x_recv,
    p_send,
    p_recv,
    v_send,
    v_recv,
    zx_send,
    zx_recv,
    y_send,
    y_recv,
    a_send,
    a_recv,
    b_send,
    b_recv,
    t_send,
    t_recv,
    u_send,
    u_recv,
    g_send,
    g_recv,
    f_send,
    f_recv,
    dx_send,
    dx_recv,
    dp_send,
    dp_recv,
    two_send,
    two_recv,
    one_send,
    one_recv,
    r_send,
    r_recv,
):
    f, t = lax.axis_index("fsdp"), lax.axis_index("tp")
    h, y = lax.div(f, 4), lax.rem(f, 4)
    l, x, k = lax.div(t, 8), lax.rem(lax.div(t, 2), 4), lax.rem(t, 2)
    outer = h == l
    inner = h != l
    rows, shard = tokens.shape
    deep, width = gate_weight.shape
    part = rows // 2
    zparts = ((rows - XFIRST) // 2, part)
    first = rows - XFIRST
    xpart = XFIRST // 2
    odd = (h - l) * (h - l)
    home = h * (1 - odd) + 2 * odd
    wide = 2 * width

    def at(xx, yy, hh, ll, kk):
        return (hh * 4 + yy, ll * 8 + xx * 2 + kk)

    xs = (lax.rem(x + 3, 4), lax.rem(x + 1, 4), lax.rem(x + 2, 4))
    ys = (lax.rem(y + 3, 4), lax.rem(y + 1, 4), lax.rem(y + 2, 4))
    right, left = at(xs[1], y, h, l, k), at(xs[0], y, h, l, k)
    north, south = at(x, ys[1], h, l, k), at(x, ys[0], h, l, k)
    mate = at(x, y, h, l, 1 - k)
    flip = at(x, y, h, 1 - l, k)
    across = at(x, y, 1 - h, 1 - l, k)
    opposite = at(x, y, 1 - h, l, k)
    me = 2 * x + k

    def remote(src, dst, send, recv, device):
        return pltpu.make_async_remote_copy(
            src_ref=src,
            dst_ref=dst,
            send_sem=send,
            recv_sem=recv,
            device_id=device,
            device_id_type=MESH,
        )

    copies = [
        pltpu.make_async_copy(ref, spot, load)
        for ref, spot in (
            (tokens, xg.at[k * 4 + x, 0, home]),
            (gate_weight, wf.at[y, 0]),
            (up_weight, wf.at[y, 1]),
            (grads, xg.at[k * 4 + x, 1, home]),
            (down_weight, df.at[y]),
        )
    ]
    for copy in copies:
        copy.start()

    barrier = pltpu.get_barrier_semaphore()
    for j in range(1, 16):
        pl.semaphore_signal(
            barrier, inc=1, device_id=(f, lax.rem(t + j, 16)), device_id_type=MESH
        )
    for peer in (north, south, opposite, across):
        pl.semaphore_signal(barrier, inc=1, device_id=peer, device_id_type=MESH)
    pl.semaphore_wait(barrier, 19)

    all_in = xg.at[pl.ds(0, 5), 0, 0]
    pltpu.make_async_copy(all_in, all_in, load).wait()

    def w_spot(o, w, q):
        if w == 2:
            return df.at[o, pl.ds(q * (width // 2), width // 2)]
        return wf.at[o, w, pl.ds(q * (deep // 2), deep // 2)]

    def w_out(way, w, q):
        return remote(
            w_spot(y, w, q),
            w_spot(y, w, q),
            y_send,
            y_recv.at[w, q if way == q else 2],
            (north, south)[way],
        )

    def w_on(w, q):
        here = w_spot(ys[q], w, q)
        return remote(here, here, y_send, y_recv.at[w, 2], (north, south)[q])

    def w_wait(w, e, here):
        remote(here, here, y_send, y_recv.at[w, e], north).wait_recv()

    def w_start(w):
        for way, q in ((0, 0), (1, 1), (0, 1), (1, 0)):
            w_out(way, w, q).start()

    def w_forward(w):
        for q in range(2):
            w_wait(w, q, w_spot(ys[q], w, q))
            w_on(w, q).start()

    def w_rest(w):
        w_wait(w, 2, df.at[pl.ds(0, 2)] if w == 2 else wf.at[pl.ds(0, 2), w])

    slot = (h, 1 - h)

    def x_own(m, q):
        return xg.at[k * 4 + x, m, home, pl.ds(q * zparts[m], zparts[m])]

    def x_spot(p, o, j, m, q):
        return xg.at[p * 4 + o, m, slot[j], pl.ds(q * zparts[m], zparts[m])]

    def z_out(m, q, device, j):
        spot = xg.at[k * 4 + x, m, h, pl.ds(q * zparts[m], zparts[m])]
        return remote(x_own(m, q), spot, z_send.at[0], z_recv.at[j, m, q], device)

    def z_on(m, q):
        here = x_spot(k, x, 1, m, q)
        return remote(here, here, z_send.at[1], z_recv.at[1, m, q], flip)

    def z_in(j, m, q):
        here = x_spot(k, x, j, m, q)
        return remote(here, here, z_send.at[0], z_recv.at[j, m, q], flip)

    def x_out(way, src, j, m, q):
        return remote(
            src,
            x_spot(k, x, j, m, q),
            x_send,
            x_recv.at[m, q, 2 * way + j],
            (right, left)[way],
        )

    def x_on(j, m, q):
        here = x_spot(k, xs[q], j, m, q)
        return remote(
            here, here, x_send, x_recv.at[m, q, 4], (right, left)[q]
        )

    def x_wait(m, q, e, here):
        remote(here, here, x_send, x_recv.at[m, q, e], right).wait_recv()

    places = (*xs, x)

    def p_out(d, src, j, m, q):
        return remote(
            src,
            x_spot(k, places[d], j, m, q),
            p_send,
            p_recv.at[d, m],
            mate,
        )

    def spread(src, j, m, q):
        for way in (0, 1) if q == 0 else (1, 0):
            x_out(way, src, j, m, q).start()
        p_out(3, src, j, m, q).start()

    def passed(d, j, m, q):
        x_wait(m, q, 2 * d + j, x_spot(k, xs[d], j, m, q))
        if d == q:
            x_on(j, m, q).start()
        p_out(d, x_spot(k, places[d], j, m, q), j, m, q).start()

    def x_rest(m):
        for q in range(2):
            here = xg.at[k * 4 + xs[2], m, pl.ds(0, 2), pl.ds(q * zparts[m], zparts[m])]
            x_wait(m, q, 4, here)
            for j in range(2):
                p_out(2, x_spot(k, xs[2], j, m, q), j, m, q).start()

    def z_forward(m, q):
        @pl.when(inner)
        def _():
            z_in(1, m, q).wait_recv()
            z_on(m, q).start()

    def z_near(m, q):
        @pl.when(inner)
        def _():
            z_in(0, m, q).wait_recv()

        spread(x_spot(k, x, 0, m, q), 0, m, q)

    def z_far(m, q):
        @pl.when(outer)
        def _():
            z_in(1, m, q).wait_recv()

        spread(x_spot(k, x, 1, m, q), 1, m, q)

    def z_near_inner(m, q):
        @pl.when(inner)
        def _():
            z_in(0, m, q).wait_recv()
            spread(x_spot(k, x, 0, m, q), 0, m, q)

    fourths = (shard // 4, (shard - DIRECT) // 4)
    bases = (0, DIRECT)

    def t_copy(u, w):
        return remote(
            wf.at[
                lax.div(u, 2),
                w,
                pl.ds(lax.rem(u, 2) * shard + bases[w] + y * fourths[w], fourths[w]),
            ],
            tw.at[me, w, pl.ds(bases[w] + y * fourths[w], fourths[w])],
            t_send,
            t_recv,
            (f, l * 8 + u),
        )

    def t_out(w, j):
        return t_copy(lax.rem(me + j, 8), w)

    def t_all():
        here = tw.at[pl.ds(0, 7), 0, pl.ds(0, fourths[0] + fourths[1])]
        return remote(here, here, t_send, t_recv, mate)

    def g_out(j):
        u = lax.rem(me + j, 8)
        return remote(
            wf.at[lax.div(u, 2), 1, pl.ds(lax.rem(u, 2) * shard, DIRECT)],
            tw.at[me, 1, pl.ds(0, DIRECT)],
            g_send,
            g_recv,
            (f, l * 8 + u),
        )

    def g_all():
        here = tw.at[pl.ds(0, 7), 1, pl.ds(0, DIRECT)]
        return remote(here, here, g_send, g_recv, mate)

    def u_spot(o, w, q):
        return tw.at[pl.ds(q * 4, 4), w, pl.ds(bases[w] + o * fourths[w], fourths[w])]

    def u_out(way, w, q):
        here = u_spot(y, w, q)
        return remote(
            here, here, u_send, u_recv.at[q if way == q else 2], (north, south)[way]
        )

    def u_on(w, q):
        here = u_spot(ys[q], w, q)
        return remote(here, here, u_send, u_recv.at[2], (north, south)[q])

    def u_wait(e, here):
        remote(here, here, u_send, u_recv.at[e], north).wait_recv()

    def v_spot(o, q):
        return xg.at[k * 4 + o, 0, home, pl.ds(first + q * xpart, xpart)]

    def v_out(way, q):
        here = v_spot(x, q)
        return remote(
            here, here, v_send, v_recv.at[q if way == q else 2], (right, left)[way]
        )

    def v_on(q):
        here = v_spot(xs[q], q)
        return remote(here, here, v_send, v_recv.at[3], (right, left)[q])

    def v_wait(e, here):
        remote(here, here, v_send, v_recv.at[e], right).wait_recv()

    def zx_spot(p, d, at_s):
        return xg.at[p * 4 + places[d], 0, at_s, pl.ds(first, XFIRST)]

    def zx_out(d, device, j):
        return remote(
            zx_spot(k, d, home),
            zx_spot(k, d, h),
            zx_send.at[0],
            zx_recv.at[j + (j * d == 2)],
            device,
        )

    def zx_on(d):
        here = zx_spot(k, d, 1 - h)
        return remote(here, here, zx_send.at[1], zx_recv.at[1 + (d == 2)], flip)

    def zx_wait(e, count):
        here = xg.at[pl.ds(0, count), 0, 0, pl.ds(first, XFIRST)]
        remote(here, here, zx_send.at[0], zx_recv.at[e], flip).wait_recv()

    def px_out(d, j):
        here = zx_spot(k, d, slot[j])
        return remote(here, here, p_send, p_recv.at[d, 0], mate)

    def v_start():
        for q in range(2):
            for way in (0, 1) if q == 0 else (1, 0):
                v_out(way, q).start()

    def v_near():
        for q in range(2):
            v_wait(q, v_spot(xs[q], q))
            v_on(q).start()
        v_wait(2, zx_spot(k, 0, home))

    def v_far():
        v_wait(3, zx_spot(k, 2, home))

    def zx_start(ds):
        for d in ds:

            @pl.when(outer)
            def _(d=d):
                zx_out(d, flip, 0).start()
                px_out(d, 0).start()

            @pl.when(inner)
            def _(d=d):
                zx_out(d, across, 1).start()

    def zx_pass(e, ds):
        @pl.when(inner)
        def _():
            zx_wait(e, len(ds))
            for d in ds:
                zx_on(d).start()

    def zx_take():
        @pl.when(inner)
        def _():
            zx_wait(0, 4)
            for d in range(4):
                px_out(d, 0).start()

        @pl.when(outer)
        def _():
            zx_wait(1, 3)
            zx_wait(2, 1)

        for d in range(4):
            px_out(d, 1).start()

    def z_start(m):
        @pl.when(outer)
        def _():
            for q in range(2):
                z_out(m, q, flip, 0).start()

        @pl.when(inner)
        def _():
            for q in range(2):
                z_out(m, q, across, 1).start()

    v_start()
    z_start(0)

    @pl.when(outer)
    def _():
        for q in range(2):
            spread(x_own(0, q), 0, 0, q)

    zx_start((3,))
    w_start(0)
    w_start(1)

    v_near()
    zx_start((0, 1))
    z_forward(0, 0)
    z_near_inner(0, 0)
    z_far(0, 0)
    v_far()
    zx_start((2,))
    z_start(1)
    z_forward(0, 1)
    z_near_inner(0, 1)
    z_far(0, 1)
    w_forward(0)
    for j in range(2):
        passed(0, j, 0, 0)
        passed(1, j, 0, 0)
    w_forward(1)
    w_start(2)
    for j in range(2):
        passed(1, j, 0, 1)
        passed(0, j, 0, 1)
    z_forward(1, 0)
    zx_pass(1, (3, 0, 1))
    z_forward(1, 1)
    zx_pass(2, (2,))
    z_near(1, 0)
    z_near(1, 1)
    w_rest(0)
    w_rest(1)

    @pl.loop(1, 8)
    def _(j):
        for w in range(2):
            t_out(w, j).start()

    z_far(1, 0)
    z_far(1, 1)
    w_forward(2)
    zx_take()
    tall = 2 * rows

    def block(m, o):
        return jnp.concatenate(
            [xg[p * 4 + o, m, :2].reshape(tall, shard) for p in range(2)], axis=1
        )

    def pair_in(d, m):
        here = xg.at[(1 - k) * 4 + places[d], m, pl.ds(0, 2)]
        remote(here, here, p_send, p_recv.at[d, m], mate).wait_recv()

    def gate_up(d):
        o = places[d]
        weights = jnp.concatenate([wf[o, 0], wf[o, 1]], axis=1)
        term = jnp.dot(block(0, o), weights, preferred_element_type=F32)
        sa[...] = term if d == 3 else sa[...] + term

    for d in (3, 0, 1):
        pair_in(d, 0)
        gate_up(d)
    x_rest(0)
    pair_in(2, 0)
    gate_up(2)
    turn = (1 - l, l)

    def swap(src, dst, send, recvs):
        def copy(c):
            at_c = pl.ds(turn[c] * rows, rows)
            return remote(src.at[at_c], dst.at[at_c], send, recvs[c], opposite)

        return copy

    a_swap = swap(sa, zla, a_send, (a_recv, a_recv))
    b_swap = swap(sb, zlb, b_send, (b_recv.at[0], b_recv.at[1]))
    a_all = remote(sa, zla, a_send, a_recv, opposite)
    b_all = remote(sb, zlb, b_send, b_recv.at[0], opposite)

    a_swap(0).start()
    for w in range(2):
        mine_w = pl.ds(bases[w] + y * fourths[w], fourths[w])
        tw[me, w, mine_w] = wf[x, w, pl.ds(k * shard + bases[w] + y * fourths[w], fourths[w])]
    tw[me, 1, :DIRECT] = wf[x, 1, pl.ds(k * shard, DIRECT)]
    a_swap(1).start()
    t_all().wait_recv()

    for w in range(2):
        for way, q in ((0, 0), (1, 1), (0, 1), (1, 0)):
            u_out(way, w, q).start()
    for j in range(2):
        passed(0, j, 1, 0)
        passed(1, j, 1, 0)
    for j in range(2):
        passed(1, j, 1, 1)
        passed(0, j, 1, 1)

    def grad_in(d):
        o = places[d]
        term = lax.dot_general(
            block(1, o), df[o], (COLS, ((), ())), preferred_element_type=F32
        )
        sb[...] = term if d == 3 else sb[...] + term

    w_rest(2)
    for d in (3, 0, 1):
        pair_in(d, 1)
        grad_in(d)
    x_rest(1)
    @pl.loop(1, 8)
    def _(j):
        g_out(j).start()

    for q in range(2):
        u_wait(q, tw.at[pl.ds(q * 4, 4), 0, pl.ds(0, fourths[0] + fourths[1])])
        for w in range(2):
            u_on(w, q).start()
    a_all.wait_recv()
    sums = sa[...] + zla[...]
    gate, up = sums[:, :width], sums[:, width:]
    squashed = jax.nn.sigmoid(gate)
    activated = gate * squashed
    slope = squashed * (1.0 + gate * (1.0 - squashed))
    acts[:, :width] = up * slope
    acts[:, width:] = activated
    hidden[...] = (activated * up).astype(BF16)

    pair_in(2, 1)
    def down_part(o):
        return lax.dot_general(
            hidden[...], block(1, o), (ROWS, ((), ())), preferred_element_type=F32
        )

    def down_mine(q):
        at_q = pl.ds(q * (width // 2), width // 2)
        down_own[at_q] = lax.dot_general(
            hidden[:, q * (width // 2) : (q + 1) * (width // 2)],
            block(1, y),
            (ROWS, ((), ())),
            preferred_element_type=F32,
        )

    def gate_part(o):
        return lax.dot_general(
            block(0, o), dg[me], (ROWS, ((), ())), preferred_element_type=F32
        )

    twos, mids, parts, ones, lands = (
        (dtwo, gtwo),
        (dmid, gmid),
        (dpart, gpart),
        (done, gone),
        (dland, gland),
    )

    def halves(i, q):
        size = twos[i].shape[0] // 2
        return pl.ds(q * size, size)

    def two_out(i, q):
        return remote(
            twos[i].at[halves(i, q)],
            mids[i].at[q],
            two_send.at[i],
            two_recv.at[i, q],
            (north, south)[q],
        )

    def one_out(i, way, q):
        return remote(
            ones[i].at[way, halves(i, q)],
            lands[i].at[way, halves(i, q)],
            one_send.at[i],
            one_recv.at[i],
            (north, south)[way],
        )

    def one_part(i, fn, way):
        q = way
        term = fn(ys[1 - way])
        size = term.shape[0] // 2
        parts[i][way] = term[q * size : (q + 1) * size]
        ones[i][way, halves(i, 1 - q)] = term[(1 - q) * size : (2 - q) * size].astype(BF16)

    def one_merge(i):
        for way in range(2):
            two_out(i, way).wait_recv()
            ones[i][way, halves(i, way)] = (
                parts[i][way] + mids[i][way].astype(F32)
            ).astype(BF16)

    def finals(i):
        remote(ones[i], lands[i], one_send.at[i], one_recv.at[i], north).wait_recv()
        return lands[i][0].astype(F32) + lands[i][1].astype(F32)

    def grad_last(c):
        at_s = pl.ds(turn[c] * rows, rows)
        last = jnp.concatenate([xg[p * 4 + xs[2], 1, turn[c]] for p in range(2)], axis=1)
        sb[at_s] += lax.dot_general(
            last, df[xs[2]], (COLS, ((), ())), preferred_element_type=F32
        )

    dtwo[...] = down_part(ys[2]).astype(BF16)
    grad_last(0)
    for q in range(2):
        two_out(0, q).start()
    grad_last(1)
    b_swap(0).start()
    one_part(0, down_part, 0)
    b_swap(1).start()
    one_part(0, down_part, 1)
    for way in range(2):
        one_out(0, way, 1 - way).start()
    one_merge(0)
    def d_spot(c, o, e, q):
        return dg.at[o * 2 + c, pl.ds(turn[e] * rows + q * part, part)]

    def dx_out(way, e, q):
        here = d_spot(k, x, e, q)
        return remote(
            here, here, dx_send, dx_recv.at[way, e, q], (right, left)[way]
        )

    def dx_on(e, q):
        here = d_spot(k, xs[q], e, q)
        return remote(here, here, dx_send, dx_recv.at[2, e, 0], (right, left)[q])

    def dx_in(d, e, q):
        here = d_spot(k, xs[d], e, q)
        return remote(here, here, dx_send, dx_recv.at[d, e, q], right)

    def dp_out(d, e, q):
        here = d_spot(k, places[d], e, q)
        return remote(here, here, dp_send, dp_recv.at[d, e], mate)

    def d_half(c, d, e):
        return dg.at[places[d] * 2 + c, pl.ds(turn[e] * rows, rows)]

    def d_far(e):
        here = d_half(k, 2, e)
        remote(here, here, dx_send, dx_recv.at[2, e, 0], right).wait_recv()
        for q in range(2):
            dp_out(2, e, q).start()

    def d_start(e):
        for q in range(2):
            for way in (0, 1) if q == 0 else (1, 0):
                dx_out(way, e, q).start()
            dp_out(3, e, q).start()

    def d_passed(d, e, q):
        dx_in(d, e, q).wait_recv()
        if d == q:
            dx_on(e, q).start()
        dp_out(d, e, q).start()

    def d_near(e):
        for q in range(2):
            d_passed(q, e, q)
        for q in range(2):
            d_passed(1 - q, e, q)

    def gather(d, e):
        base = places[d] * 2
        at_s = pl.ds(turn[e] * rows, rows)
        left_side = jnp.concatenate([dg[base, at_s], dg[base + 1, at_s]], axis=1)
        right_side = jnp.concatenate(
            [tw[base, 0], tw[base, 1], tw[base + 1, 0], tw[base + 1, 1]], axis=1
        )
        term = lax.dot_general(
            left_side, right_side, (COLS, ((), ())), preferred_element_type=F32
        )
        total[e] = term if d == 3 else total[e] + term

    def gathers(e, ds):
        for d in ds:
            here = d_half(1 - k, d, e)
            remote(here, here, dp_send, dp_recv.at[d, e], mate).wait_recv()
            gather(d, e)

    piece = rows // PIECES

    def f_out(c):
        at_c = pl.ds(c * piece, piece)
        return (
            remote(total.at[0, at_c, pl.ds(0, wide)], near.at[at_c], f_send, f_recv.at[c], flip),
            remote(slim.at[at_c], slim_near.at[at_c], f_send, f_recv.at[c], flip),
        )

    def f_start(cs):
        for c in cs:
            for copy in f_out(c):
                copy.start()

    def f_wait(c):
        here = near.at[pl.ds(0, 3 * piece // 2)]
        remote(here, here, f_send, f_recv.at[c], flip).wait_recv()

    def r_out(c):
        at_c = pl.ds(c * piece, piece)
        return remote(rounded.at[at_c], result.at[at_c], r_send, r_recv, across)

    def delta(e):
        b_swap(e).wait_recv()
        at_s = pl.ds(turn[e] * rows, rows)
        hidden_grad = sb[at_s] + zlb[at_s]
        dg[me, at_s, :width] = (hidden_grad * acts[at_s, :width]).astype(BF16)
        dg[me, at_s, width:] = (hidden_grad * acts[at_s, width:]).astype(BF16)

    delta(0)
    for way in range(2):
        one_out(0, way, way).start()
    down_mine(0)
    d_start(0)
    down_mine(1)
    delta(1)
    gtwo[...] = gate_part(ys[2]).astype(BF16)
    one_part(1, gate_part, 0)
    for q in range(2):
        two_out(1, q).start()
    one_part(1, gate_part, 1)
    one_out(1, 0, 1).start()
    d_near(0)
    one_out(1, 1, 0).start()
    d_start(1)
    gown[...] = gate_part(y)
    u_wait(2, tw.at[:, :, pl.ds(0, fourths[0] + fourths[1])])
    g_all().wait_recv()

    gathers(0, (3, 0, 1))
    d_far(0)
    gathers(0, (2,))
    slim[...] = total[0, :, wide:].astype(BF16)
    f_start(range(PIECES // 2))
    d_near(1)
    f_start(range(PIECES // 2, PIECES))
    one_merge(1)
    gathers(1, (3,))
    for way in range(2):
        one_out(1, way, way).start()
    gathers(1, (0, 1))
    d_far(1)
    gathers(1, (2,))
    keeps = [
        pltpu.make_async_copy(src, dst, keep.at[i])
        for i, (src, dst) in enumerate(
            ((down_own, down_out), (gate_own, gate_out), (up_own, up_out), (rounded, result))
        )
    ]
    for c in range(PIECES):
        f_wait(c)
        at_c = pl.ds(c * piece, piece)
        rounded[at_c, :wide] = (total[1, at_c, :wide] + near[at_c]).astype(BF16)
        rounded[at_c, wide:] = (total[1, at_c, wide:] + slim_near[at_c].astype(F32)).astype(BF16)

        if c:

            @pl.when(inner)
            def _(c=c):
                r_out(c - 1).start()

    down_own[...] = factor * (down_own[...] + finals(0))
    @pl.when(inner)
    def _():
        r_out(PIECES - 1).start()

    @pl.when(outer)
    def _():
        keeps[3].start()

    both = factor * (gown[...] + finals(1))
    gate_own[...] = both[:, :width]
    up_own[...] = both[:, width:]
    for copy in keeps[:3]:
        copy.start()

    sent = [
        (xg.at[0, :, 0, pl.ds(0, 240)], z_send.at[0]),
        (xg.at[pl.ds(0, 4), 0, 0, pl.ds(0, XFIRST)], zx_send.at[0]),
        (xg.at[pl.ds(0, 3), 0, 0, pl.ds(0, XFIRST)], v_send),
        (xg.at[pl.ds(0, 4), 0, :, pl.ds(0, 240)], x_send),
        (xg.at[:, :, 0], p_send),
        (xg.at[pl.ds(0, 3), 0], y_send),
        (tw.at[:, :, pl.ds(0, 3 * (fourths[0] + fourths[1]) // 2)], u_send),
        (dg.at[pl.ds(0, 3)], dx_send),
        (dg.at[pl.ds(0, 4)], dp_send),
        (total.at[0, pl.ds(0, 3 * rows // 4)], f_send),
        (dtwo, two_send.at[0]),
        (gtwo, two_send.at[1]),
        (done, one_send.at[0]),
        (gone, one_send.at[1]),
    ]
    for here, sem in sent:
        remote(here, here, sem, load, mate).wait_send()
    for copy in (a_all, b_all, t_all(), g_all()):
        copy.wait_send()

    @pl.when(inner)
    def _():
        for here, sem in (
            (xg.at[0, :, 0, pl.ds(0, 240)], z_send.at[1]),
            (xg.at[pl.ds(0, 4), 0, 0, pl.ds(0, XFIRST)], zx_send.at[1]),
        ):
            remote(here, here, sem, load, mate).wait_send()
        remote(rounded, result, r_send, r_recv, across).wait()

    @pl.when(outer)
    def _():
        keeps[3].wait()

    for copy in keeps[:3]:
        copy.wait()


def store_kernel(*refs):
    found, kept, held, sem = refs[:4], refs[4:8], refs[8:12], refs[12]
    loads = [pltpu.make_async_copy(found[i], held[i], sem.at[0, i]) for i in range(4)]
    stores = [pltpu.make_async_copy(held[i], kept[i], sem.at[1, i]) for i in range(4)]
    for copy in loads:
        copy.start()
    for i in range(4):
        loads[i].wait()
        stores[i].start()
    for copy in stores:
        copy.wait()


HBM = pl.BlockSpec(memory_space=pltpu.HBM)
DMA = pltpu.SemaphoreType.DMA


def body(tokens, out_grad, gate_weight, up_weight, down_weight):
    nf, nt = lax.axis_size("fsdp"), lax.axis_size("tp")
    rows, shard = tokens.shape
    deep, width = gate_weight.shape
    assert nf == 8 and nt == 16 and deep == 2 * shard
    factor = 1.0 / math.sqrt(rows * nf)
    tall = 2 * rows
    wide = 2 * width

    shapes = (
        jax.ShapeDtypeStruct((rows, shard), BF16),
        jax.ShapeDtypeStruct((deep, width), F32),
        jax.ShapeDtypeStruct((deep, width), F32),
        jax.ShapeDtypeStruct((width, deep), F32),
    )
    found = tuple(
        pl.pallas_call(
            functools.partial(kernel, factor),
            out_shape=shapes,
            in_specs=[HBM] * 5,
            out_specs=(HBM,) * 4,
            scratch_shapes=[
                pltpu.VMEM((deep, width), F32),
                pltpu.VMEM((deep, width), F32),
                pltpu.VMEM((width, deep), F32),
                pltpu.VMEM((8, 2, 3, rows, shard), BF16),
                pltpu.VMEM((4, 2, deep, width), BF16),
                pltpu.VMEM((4, width, deep), BF16),
                pltpu.VMEM((tall, wide), F32),
                pltpu.VMEM((tall, wide), F32),
                pltpu.VMEM((tall, width), F32),
                pltpu.VMEM((tall, width), F32),
                pltpu.VMEM((tall, wide), F32),
                pltpu.VMEM((tall, width), BF16),
                pltpu.VMEM((8, tall, wide), BF16),
                pltpu.VMEM((8, 2, shard, width), BF16),
                pltpu.VMEM((2, width // 2, deep), F32),
                pltpu.VMEM((2, deep // 2, wide), F32),
                pltpu.VMEM((width, deep), BF16),
                pltpu.VMEM((deep, wide), BF16),
                pltpu.VMEM((2, width, deep), BF16),
                pltpu.VMEM((2, deep, wide), BF16),
                pltpu.VMEM((2, width // 2, deep), BF16),
                pltpu.VMEM((2, deep // 2, wide), BF16),
                pltpu.VMEM((2, width, deep), BF16),
                pltpu.VMEM((2, deep, wide), BF16),
                pltpu.VMEM((deep, wide), F32),
                pltpu.VMEM((2, rows, shard), F32),
                pltpu.VMEM((rows, wide), F32),
                pltpu.VMEM((rows, wide), BF16),
                pltpu.VMEM((rows, wide), BF16),
                pltpu.VMEM((rows, shard), BF16),
                DMA(()),
                DMA((4,)),
                DMA((2,)),
                DMA((2, 2, 2)),
                DMA(()),
                DMA((2, 2, 5)),
                DMA(()),
                DMA((4, 2)),
                DMA(()),
                DMA((4,)),
                DMA((2,)),
                DMA((3,)),
                DMA(()),
                DMA((3, 3)),
                DMA(()),
                DMA(()),
                DMA(()),
                DMA((2,)),
                DMA(()),
                DMA(()),
                DMA(()),
                DMA((3,)),
                DMA(()),
                DMA(()),
                DMA(()),
                DMA((PIECES,)),
                DMA(()),
                DMA((3, 2, 2)),
                DMA(()),
                DMA((4, 2)),
                DMA((2,)),
                DMA((2, 2)),
                DMA((2,)),
                DMA((2,)),
                DMA(()),
                DMA(()),
            ],
            compiler_params=pltpu.CompilerParams(
                collective_id=0, has_side_effects=True, vmem_limit_bytes=VMEM_LIMIT
            ),
            name="block",
        )(tokens, out_grad, gate_weight, up_weight, down_weight)
    )
    return tuple(
        pl.pallas_call(
            store_kernel,
            out_shape=shapes,
            in_specs=[HBM] * 4,
            out_specs=(HBM,) * 4,
            scratch_shapes=[pltpu.VMEM(s.shape, s.dtype) for s in shapes] + [DMA((2, 4))],
            compiler_params=pltpu.CompilerParams(vmem_limit_bytes=VMEM_LIMIT),
            name="store",
        )(*found)
    )


def solution(mesh):
    return jax.shard_map(
        body,
        mesh=mesh,
        in_specs=(
            P("fsdp", "tp"),
            P("fsdp", "tp"),
            P("fsdp", "tp"),
            P("fsdp", "tp"),
            P("tp", "fsdp"),
        ),
        out_specs=(P("fsdp", "tp"), P("fsdp", "tp"), P("fsdp", "tp"), P("tp", "fsdp")),
        check_vma=False,
    )
```

```python
import functools
import math

import jax
import jax.numpy as jnp
from jax import lax
from jax.sharding import PartitionSpec as P
from jax.experimental import pallas as pl
from jax.experimental.pallas import tpu as pltpu

MESH = pl.DeviceIdType.MESH
F32 = jnp.float32
BF16 = jnp.bfloat16
VMEM_LIMIT = 60 * 1024 * 1024
XFIRST = 32
PIECES = 8
DIRECT = 384
ROWS = ((0,), (0,))
COLS = ((1,), (1,))


def kernel(
    factor,
    tokens,
    grads,
    gate_weight,
    up_weight,
    down_weight,
    result,
    gate_out,
    up_out,
    down_out,
    gate_own,
    up_own,
    down_own,
    xg,
    wf,
    df,
    sa,
    zla,
    sb,
    zlb,
    acts,
    hidden,
    dg,
    tw,
    dpart,
    gpart,
    dtwo,
    gtwo,
    done,
    gone,
    dmid,
    gmid,
    dland,
    gland,
    gown,
    total,
    near,
    slim,
    slim_near,
    rounded,
    load,
    keep,
    z_send,
    z_recv,
    x_send,
    x_recv,
    p_send,
    p_recv,
    v_send,
    v_recv,
    zx_send,
    zx_recv,
    y_send,
    y_recv,
    a_send,
    a_recv,
    b_send,
    b_recv,
    t_send,
    t_recv,
    u_send,
    u_recv,
    g_send,
    g_recv,
    f_send,
    f_recv,
    dx_send,
    dx_recv,
    dp_send,
    dp_recv,
    two_send,
    two_recv,
    one_send,
    one_recv,
    r_send,
    r_recv,
):
    f, t = lax.axis_index("fsdp"), lax.axis_index("tp")
    h, y = lax.div(f, 4), lax.rem(f, 4)
    l, x, k = lax.div(t, 8), lax.rem(lax.div(t, 2), 4), lax.rem(t, 2)
    outer = h == l
    inner = h != l
    rows, shard = tokens.shape
    deep, width = gate_weight.shape
    part = rows // 2
    zparts = ((rows - XFIRST) // 2, part)
    first = rows - XFIRST
    xpart = XFIRST // 2
    odd = (h - l) * (h - l)
    home = h * (1 - odd) + 2 * odd
    wide = 2 * width

    def at(xx, yy, hh, ll, kk):
        return (hh * 4 + yy, ll * 8 + xx * 2 + kk)

    xs = (lax.rem(x + 3, 4), lax.rem(x + 1, 4), lax.rem(x + 2, 4))
    ys = (lax.rem(y + 3, 4), lax.rem(y + 1, 4), lax.rem(y + 2, 4))
    right, left = at(xs[1], y, h, l, k), at(xs[0], y, h, l, k)
    north, south = at(x, ys[1], h, l, k), at(x, ys[0], h, l, k)
    mate = at(x, y, h, l, 1 - k)
    flip = at(x, y, h, 1 - l, k)
    across = at(x, y, 1 - h, 1 - l, k)
    opposite = at(x, y, 1 - h, l, k)
    me = 2 * x + k

    def remote(src, dst, send, recv, device):
        return pltpu.make_async_remote_copy(
            src_ref=src,
            dst_ref=dst,
            send_sem=send,
            recv_sem=recv,
            device_id=device,
            device_id_type=MESH,
        )

    copies = [
        pltpu.make_async_copy(ref, spot, load)
        for ref, spot in (
            (tokens, xg.at[k * 4 + x, 0, home]),
            (gate_weight, wf.at[y, 0]),
            (up_weight, wf.at[y, 1]),
            (grads, xg.at[k * 4 + x, 1, home]),
            (down_weight, df.at[y]),
        )
    ]
    for copy in copies:
        copy.start()

    barrier = pltpu.get_barrier_semaphore()
    for j in range(1, 16):
        pl.semaphore_signal(
            barrier, inc=1, device_id=(f, lax.rem(t + j, 16)), device_id_type=MESH
        )
    for peer in (north, south, opposite, across):
        pl.semaphore_signal(barrier, inc=1, device_id=peer, device_id_type=MESH)
    pl.semaphore_wait(barrier, 19)

    all_in = xg.at[pl.ds(0, 5), 0, 0]
    pltpu.make_async_copy(all_in, all_in, load).wait()

    def w_spot(o, w, q):
        if w == 2:
            return df.at[o, pl.ds(q * (width // 2), width // 2)]
        return wf.at[o, w, pl.ds(q * (deep // 2), deep // 2)]

    def w_out(way, w, q):
        return remote(
            w_spot(y, w, q),
            w_spot(y, w, q),
            y_send,
            y_recv.at[w, q if way == q else 2],
            (north, south)[way],
        )

    def w_on(w, q):
        here = w_spot(ys[q], w, q)
        return remote(here, here, y_send, y_recv.at[w, 2], (north, south)[q])

    def w_wait(w, e, here):
        remote(here, here, y_send, y_recv.at[w, e], north).wait_recv()

    def w_start(w):
        for way, q in ((0, 0), (1, 1), (0, 1), (1, 0)):
            w_out(way, w, q).start()

    def w_forward(w):
        for q in range(2):
            w_wait(w, q, w_spot(ys[q], w, q))
            w_on(w, q).start()

    def w_rest(w):
        w_wait(w, 2, df.at[pl.ds(0, 2)] if w == 2 else wf.at[pl.ds(0, 2), w])

    slot = (h, 1 - h)

    def x_own(m, q):
        return xg.at[k * 4 + x, m, home, pl.ds(q * zparts[m], zparts[m])]

    def x_spot(p, o, j, m, q):
        return xg.at[p * 4 + o, m, slot[j], pl.ds(q * zparts[m], zparts[m])]

    def z_out(m, q, device, j):
        spot = xg.at[k * 4 + x, m, h, pl.ds(q * zparts[m], zparts[m])]
        return remote(x_own(m, q), spot, z_send.at[0], z_recv.at[j, m, q], device)

    def z_on(m, q):
        here = x_spot(k, x, 1, m, q)
        return remote(here, here, z_send.at[1], z_recv.at[1, m, q], flip)

    def z_in(j, m, q):
        here = x_spot(k, x, j, m, q)
        return remote(here, here, z_send.at[0], z_recv.at[j, m, q], flip)

    def x_out(way, src, j, m, q):
        return remote(
            src,
            x_spot(k, x, j, m, q),
            x_send,
            x_recv.at[m, q, 2 * way + j],
            (right, left)[way],
        )

    def x_on(j, m, q):
        here = x_spot(k, xs[q], j, m, q)
        return remote(
            here, here, x_send, x_recv.at[m, q, 4], (right, left)[q]
        )

    def x_wait(m, q, e, here):
        remote(here, here, x_send, x_recv.at[m, q, e], right).wait_recv()

    places = (*xs, x)

    def p_out(d, src, j, m, q):
        return remote(
            src,
            x_spot(k, places[d], j, m, q),
            p_send,
            p_recv.at[d, m],
            mate,
        )

    def spread(src, j, m, q):
        for way in (0, 1) if q == 0 else (1, 0):
            x_out(way, src, j, m, q).start()
        p_out(3, src, j, m, q).start()

    def passed(d, j, m, q):
        x_wait(m, q, 2 * d + j, x_spot(k, xs[d], j, m, q))
        if d == q:
            x_on(j, m, q).start()
        p_out(d, x_spot(k, places[d], j, m, q), j, m, q).start()

    def x_rest(m):
        for q in range(2):
            here = xg.at[k * 4 + xs[2], m, pl.ds(0, 2), pl.ds(q * zparts[m], zparts[m])]
            x_wait(m, q, 4, here)
            for j in range(2):
                p_out(2, x_spot(k, xs[2], j, m, q), j, m, q).start()

    def z_forward(m, q):
        @pl.when(inner)
        def _():
            z_in(1, m, q).wait_recv()
            z_on(m, q).start()

    def z_near(m, q):
        @pl.when(inner)
        def _():
            z_in(0, m, q).wait_recv()

        spread(x_spot(k, x, 0, m, q), 0, m, q)

    def z_far(m, q):
        @pl.when(outer)
        def _():
            z_in(1, m, q).wait_recv()

        spread(x_spot(k, x, 1, m, q), 1, m, q)

    def z_near_inner(m, q):
        @pl.when(inner)
        def _():
            z_in(0, m, q).wait_recv()
            spread(x_spot(k, x, 0, m, q), 0, m, q)

    fourths = (shard // 4, (shard - DIRECT) // 4)
    bases = (0, DIRECT)

    def t_copy(u, w):
        return remote(
            wf.at[
                lax.div(u, 2),
                w,
                pl.ds(lax.rem(u, 2) * shard + bases[w] + y * fourths[w], fourths[w]),
            ],
            tw.at[me, w, pl.ds(bases[w] + y * fourths[w], fourths[w])],
            t_send,
            t_recv,
            (f, l * 8 + u),
        )

    def t_out(w, j):
        return t_copy(lax.rem(me + j, 8), w)

    def t_all():
        here = tw.at[pl.ds(0, 7), 0, pl.ds(0, fourths[0] + fourths[1])]
        return remote(here, here, t_send, t_recv, mate)

    def g_out(j):
        u = lax.rem(me + j, 8)
        return remote(
            wf.at[lax.div(u, 2), 1, pl.ds(lax.rem(u, 2) * shard, DIRECT)],
            tw.at[me, 1, pl.ds(0, DIRECT)],
            g_send,
            g_recv,
            (f, l * 8 + u),
        )

    def g_all():
        here = tw.at[pl.ds(0, 7), 1, pl.ds(0, DIRECT)]
        return remote(here, here, g_send, g_recv, mate)

    def u_spot(o, w, q):
        return tw.at[pl.ds(q * 4, 4), w, pl.ds(bases[w] + o * fourths[w], fourths[w])]

    def u_out(way, w, q):
        here = u_spot(y, w, q)
        return remote(
            here, here, u_send, u_recv.at[q if way == q else 2], (north, south)[way]
        )

    def u_on(w, q):
        here = u_spot(ys[q], w, q)
        return remote(here, here, u_send, u_recv.at[2], (north, south)[q])

    def u_wait(e, here):
        remote(here, here, u_send, u_recv.at[e], north).wait_recv()

    def v_spot(o, q):
        return xg.at[k * 4 + o, 0, home, pl.ds(first + q * xpart, xpart)]

    def v_out(way, q):
        here = v_spot(x, q)
        return remote(
            here, here, v_send, v_recv.at[q if way == q else 2], (right, left)[way]
        )

    def v_on(q):
        here = v_spot(xs[q], q)
        return remote(here, here, v_send, v_recv.at[3], (right, left)[q])

    def v_wait(e, here):
        remote(here, here, v_send, v_recv.at[e], right).wait_recv()

    def zx_spot(p, d, at_s):
        return xg.at[p * 4 + places[d], 0, at_s, pl.ds(first, XFIRST)]

    def zx_out(d, device, j):
        return remote(
            zx_spot(k, d, home),
            zx_spot(k, d, h),
            zx_send.at[0],
            zx_recv.at[j + (j * d == 2)],
            device,
        )

    def zx_on(d):
        here = zx_spot(k, d, 1 - h)
        return remote(here, here, zx_send.at[1], zx_recv.at[1 + (d == 2)], flip)

    def zx_wait(e, count):
        here = xg.at[pl.ds(0, count), 0, 0, pl.ds(first, XFIRST)]
        remote(here, here, zx_send.at[0], zx_recv.at[e], flip).wait_recv()

    def px_out(d, j):
        here = zx_spot(k, d, slot[j])
        return remote(here, here, p_send, p_recv.at[d, 0], mate)

    def v_start():
        for q in range(2):
            for way in (0, 1) if q == 0 else (1, 0):
                v_out(way, q).start()

    def v_near():
        for q in range(2):
            v_wait(q, v_spot(xs[q], q))
            v_on(q).start()
        v_wait(2, zx_spot(k, 0, home))

    def v_far():
        v_wait(3, zx_spot(k, 2, home))

    def zx_start(ds):
        for d in ds:

            @pl.when(outer)
            def _(d=d):
                zx_out(d, flip, 0).start()
                px_out(d, 0).start()

            @pl.when(inner)
            def _(d=d):
                zx_out(d, across, 1).start()

    def zx_pass(e, ds):
        @pl.when(inner)
        def _():
            zx_wait(e, len(ds))
            for d in ds:
                zx_on(d).start()

    def zx_take():
        @pl.when(inner)
        def _():
            zx_wait(0, 4)
            for d in range(4):
                px_out(d, 0).start()

        @pl.when(outer)
        def _():
            zx_wait(1, 3)
            zx_wait(2, 1)

        for d in range(4):
            px_out(d, 1).start()

    def z_start(m):
        @pl.when(outer)
        def _():
            for q in range(2):
                z_out(m, q, flip, 0).start()

        @pl.when(inner)
        def _():
            for q in range(2):
                z_out(m, q, across, 1).start()

    v_start()
    z_start(0)

    @pl.when(outer)
    def _():
        for q in range(2):
            spread(x_own(0, q), 0, 0, q)

    zx_start((3,))
    w_start(0)
    w_start(1)

    v_near()
    zx_start((0, 1))
    z_forward(0, 0)
    z_near_inner(0, 0)
    z_far(0, 0)
    v_far()
    zx_start((2,))
    z_start(1)
    z_forward(0, 1)
    z_near_inner(0, 1)
    z_far(0, 1)
    w_forward(0)
    for j in range(2):
        passed(0, j, 0, 0)
        passed(1, j, 0, 0)
    w_forward(1)
    w_start(2)
    for j in range(2):
        passed(1, j, 0, 1)
        passed(0, j, 0, 1)
    z_forward(1, 0)
    zx_pass(1, (3, 0, 1))
    z_forward(1, 1)
    zx_pass(2, (2,))
    w_rest(0)
    w_rest(1)

    @pl.loop(1, 8)
    def _(j):
        for w in range(2):
            t_out(w, j).start()

    z_near(1, 0)
    z_near(1, 1)
    z_far(1, 0)
    z_far(1, 1)
    w_forward(2)
    zx_take()
    tall = 2 * rows

    def block(m, o):
        return jnp.concatenate(
            [xg[p * 4 + o, m, :2].reshape(tall, shard) for p in range(2)], axis=1
        )

    def pair_in(d, m):
        here = xg.at[(1 - k) * 4 + places[d], m, pl.ds(0, 2)]
        remote(here, here, p_send, p_recv.at[d, m], mate).wait_recv()

    def gate_up(d):
        o = places[d]
        weights = jnp.concatenate([wf[o, 0], wf[o, 1]], axis=1)
        term = jnp.dot(block(0, o), weights, preferred_element_type=F32)
        sa[...] = term if d == 3 else sa[...] + term

    for d in (3, 0, 1):
        pair_in(d, 0)
        gate_up(d)
    x_rest(0)
    pair_in(2, 0)
    gate_up(2)
    turn = (1 - l, l)

    def swap(src, dst, send, recvs):
        def copy(c):
            at_c = pl.ds(turn[c] * rows, rows)
            return remote(src.at[at_c], dst.at[at_c], send, recvs[c], opposite)

        return copy

    a_swap = swap(sa, zla, a_send, (a_recv, a_recv))
    b_swap = swap(sb, zlb, b_send, (b_recv.at[0], b_recv.at[1]))
    a_all = remote(sa, zla, a_send, a_recv, opposite)
    b_all = remote(sb, zlb, b_send, b_recv.at[0], opposite)

    a_swap(0).start()
    for w in range(2):
        mine_w = pl.ds(bases[w] + y * fourths[w], fourths[w])
        tw[me, w, mine_w] = wf[x, w, pl.ds(k * shard + bases[w] + y * fourths[w], fourths[w])]
    tw[me, 1, :DIRECT] = wf[x, 1, pl.ds(k * shard, DIRECT)]
    a_swap(1).start()
    t_all().wait_recv()

    for w in range(2):
        for way, q in ((0, 0), (1, 1), (0, 1), (1, 0)):
            u_out(way, w, q).start()
    for j in range(2):
        passed(0, j, 1, 0)
        passed(1, j, 1, 0)
    for j in range(2):
        passed(1, j, 1, 1)
        passed(0, j, 1, 1)

    def grad_in(d):
        o = places[d]
        term = lax.dot_general(
            block(1, o), df[o], (COLS, ((), ())), preferred_element_type=F32
        )
        sb[...] = term if d == 3 else sb[...] + term

    w_rest(2)
    for d in (3, 0, 1):
        pair_in(d, 1)
        grad_in(d)
    def down_half(o, p):
        return lax.dot_general(
            hidden[...],
            xg[p * 4 + o, 1, :2].reshape(tall, shard),
            (ROWS, ((), ())),
            preferred_element_type=F32,
        )

    def gate_part(o):
        return lax.dot_general(
            block(0, o), dg[me], (ROWS, ((), ())), preferred_element_type=F32
        )

    twos, mids, parts, ones, lands = (
        (dtwo, gtwo),
        (dmid, gmid),
        (dpart, gpart),
        (done, gone),
        (dland, gland),
    )

    def halves(i, q):
        return q if i == 0 else pl.ds(q * shard, shard)

    def beside(way):
        return lax.rem(y + 1 + 2 * way, 4)

    def two_out(i, q):
        return remote(
            twos[i].at[halves(i, q)],
            mids[i].at[q],
            two_send.at[i],
            two_recv.at[i, q],
            at(x, beside(q), h, l, k),
        )

    def one_out(i, way, q):
        return remote(
            ones[i].at[way, halves(i, q)],
            lands[i].at[way, halves(i, q)],
            one_send.at[i],
            one_recv.at[i],
            at(x, beside(way), h, l, k),
        )

    def one_part(way):
        term = gate_part(beside(way))
        gpart[way] = term[way * shard : (way + 1) * shard]
        gone[way, halves(1, 1 - way)] = term[(1 - way) * shard : (2 - way) * shard].astype(BF16)

    def one_merge(i):
        for way in range(2):
            two_out(i, way).wait_recv()
            ones[i][way, halves(i, way)] = (
                parts[i][way] + mids[i][way].astype(F32)
            ).astype(BF16)

    def finals(i):
        remote(ones[i], lands[i], one_send.at[i], one_recv.at[i], north).wait_recv()
        return lands[i][0].astype(F32) + lands[i][1].astype(F32)

    def grad_last(c):
        at_s = pl.ds(turn[c] * rows, rows)
        last = jnp.concatenate([xg[p * 4 + xs[2], 1, turn[c]] for p in range(2)], axis=1)
        sb[at_s] += lax.dot_general(
            last, df[xs[2]], (COLS, ((), ())), preferred_element_type=F32
        )

    for q in range(2):
        u_wait(q, tw.at[pl.ds(q * 4, 4), 0, pl.ds(0, fourths[0] + fourths[1])])
        for w in range(2):
            u_on(w, q).start()
    x_rest(1)
    @pl.loop(1, 8)
    def _(j):
        g_out(j).start()

    a_all.wait_recv()
    sums = sa[...] + zla[...]
    gate, up = sums[:, :width], sums[:, width:]
    squashed = jax.nn.sigmoid(gate)
    activated = gate * squashed
    slope = squashed * (1.0 + gate * (1.0 - squashed))
    acts[:, :width] = up * slope
    acts[:, width:] = activated
    hidden[...] = (activated * up).astype(BF16)

    dtwo[k] = down_half(ys[2], k).astype(BF16)
    done[1 - k, k] = down_half(beside(1 - k), k).astype(BF16)
    two_out(0, k).start()
    pair_in(2, 1)
    grad_last(0)
    grad_last(1)
    b_swap(0).start()
    dtwo[1 - k] = down_half(ys[2], 1 - k).astype(BF16)
    b_swap(1).start()
    done[k, 1 - k] = down_half(beside(k), 1 - k).astype(BF16)
    two_out(0, 1 - k).start()
    one_out(0, 1 - k, k).start()
    dpart[k] = down_half(beside(k), k)
    one_out(0, k, 1 - k).start()
    dpart[1 - k] = down_half(beside(1 - k), 1 - k)
    one_merge(0)
    def d_spot(c, o, e, q):
        return dg.at[o * 2 + c, pl.ds(turn[e] * rows + q * part, part)]

    def dx_out(way, e, q):
        here = d_spot(k, x, e, q)
        return remote(
            here, here, dx_send, dx_recv.at[way, e, q], (right, left)[way]
        )

    def dx_on(e, q):
        here = d_spot(k, xs[q], e, q)
        return remote(here, here, dx_send, dx_recv.at[2, e, 0], (right, left)[q])

    def dx_in(d, e, q):
        here = d_spot(k, xs[d], e, q)
        return remote(here, here, dx_send, dx_recv.at[d, e, q], right)

    def dp_out(d, e, q):
        here = d_spot(k, places[d], e, q)
        return remote(here, here, dp_send, dp_recv.at[d, e], mate)

    def d_half(c, d, e):
        return dg.at[places[d] * 2 + c, pl.ds(turn[e] * rows, rows)]

    def d_far(e):
        here = d_half(k, 2, e)
        remote(here, here, dx_send, dx_recv.at[2, e, 0], right).wait_recv()
        for q in range(2):
            dp_out(2, e, q).start()

    def d_start(e):
        for q in range(2):
            for way in (0, 1) if q == 0 else (1, 0):
                dx_out(way, e, q).start()
            dp_out(3, e, q).start()

    def d_passed(d, e, q):
        dx_in(d, e, q).wait_recv()
        if d == q:
            dx_on(e, q).start()
        dp_out(d, e, q).start()

    def d_near(e):
        for q in range(2):
            d_passed(q, e, q)
        for q in range(2):
            d_passed(1 - q, e, q)

    def gather(d, e):
        base = places[d] * 2
        at_s = pl.ds(turn[e] * rows, rows)
        left_side = jnp.concatenate([dg[base, at_s], dg[base + 1, at_s]], axis=1)
        right_side = jnp.concatenate(
            [tw[base, 0], tw[base, 1], tw[base + 1, 0], tw[base + 1, 1]], axis=1
        )
        term = lax.dot_general(
            left_side, right_side, (COLS, ((), ())), preferred_element_type=F32
        )
        total[e] = term if d == 3 else total[e] + term

    def gathers(e, ds):
        for d in ds:
            here = d_half(1 - k, d, e)
            remote(here, here, dp_send, dp_recv.at[d, e], mate).wait_recv()
            gather(d, e)

    piece = rows // PIECES

    def f_out(c):
        at_c = pl.ds(c * piece, piece)
        return (
            remote(total.at[0, at_c, pl.ds(0, wide)], near.at[at_c], f_send, f_recv.at[c], flip),
            remote(slim.at[at_c], slim_near.at[at_c], f_send, f_recv.at[c], flip),
        )

    def f_start(cs):
        for c in cs:
            for copy in f_out(c):
                copy.start()

    def f_wait(c):
        here = near.at[pl.ds(0, 3 * piece // 2)]
        remote(here, here, f_send, f_recv.at[c], flip).wait_recv()

    def r_out(c):
        at_c = pl.ds(c * piece, piece)
        return remote(rounded.at[at_c], result.at[at_c], r_send, r_recv, across)

    def delta(e):
        b_swap(e).wait_recv()
        at_s = pl.ds(turn[e] * rows, rows)
        hidden_grad = sb[at_s] + zlb[at_s]
        dg[me, at_s, :width] = (hidden_grad * acts[at_s, :width]).astype(BF16)
        dg[me, at_s, width:] = (hidden_grad * acts[at_s, width:]).astype(BF16)

    delta(0)
    for way in range(2):
        one_out(0, way, way).start()
    down_own[:, :shard] = down_half(y, 0)
    d_start(0)
    down_own[:, shard:] = down_half(y, 1)
    delta(1)
    gtwo[...] = gate_part(ys[2]).astype(BF16)
    one_part(0)
    for q in range(2):
        two_out(1, q).start()
    one_part(1)
    one_out(1, 0, 1).start()
    d_near(0)
    one_out(1, 1, 0).start()
    d_start(1)
    gown[...] = gate_part(y)
    u_wait(2, tw.at[:, :, pl.ds(0, fourths[0] + fourths[1])])
    g_all().wait_recv()

    gathers(0, (3, 0, 1))
    d_far(0)
    gathers(0, (2,))
    slim[...] = total[0, :, wide:].astype(BF16)
    f_start(range(PIECES // 2))
    d_near(1)
    f_start(range(PIECES // 2, PIECES))
    one_merge(1)
    gathers(1, (3,))
    for way in range(2):
        one_out(1, way, way).start()
    gathers(1, (0, 1))
    d_far(1)
    gathers(1, (2,))
    keeps = [
        pltpu.make_async_copy(src, dst, keep.at[i])
        for i, (src, dst) in enumerate(
            ((down_own, down_out), (gate_own, gate_out), (up_own, up_out), (rounded, result))
        )
    ]
    for c in range(PIECES):
        f_wait(c)
        at_c = pl.ds(c * piece, piece)
        rounded[at_c, :wide] = (total[1, at_c, :wide] + near[at_c]).astype(BF16)
        rounded[at_c, wide:] = (total[1, at_c, wide:] + slim_near[at_c].astype(F32)).astype(BF16)

        if c:

            @pl.when(inner)
            def _(c=c):
                r_out(c - 1).start()

    both = finals(0)
    for p in range(2):
        at_p = slice(p * shard, (p + 1) * shard)
        down_own[:, at_p] = factor * (down_own[:, at_p] + both[p])
    @pl.when(inner)
    def _():
        r_out(PIECES - 1).start()

    @pl.when(outer)
    def _():
        keeps[3].start()

    both = factor * (gown[...] + finals(1))
    gate_own[...] = both[:, :width]
    up_own[...] = both[:, width:]
    for copy in keeps[:3]:
        copy.start()

    sent = [
        (xg.at[0, :, 0, pl.ds(0, 240)], z_send.at[0]),
        (xg.at[pl.ds(0, 4), 0, 0, pl.ds(0, XFIRST)], zx_send.at[0]),
        (xg.at[pl.ds(0, 3), 0, 0, pl.ds(0, XFIRST)], v_send),
        (xg.at[pl.ds(0, 4), 0, :, pl.ds(0, 240)], x_send),
        (xg.at[:, :, 0], p_send),
        (xg.at[pl.ds(0, 3), 0], y_send),
        (tw.at[:, :, pl.ds(0, 3 * (fourths[0] + fourths[1]) // 2)], u_send),
        (dg.at[pl.ds(0, 3)], dx_send),
        (dg.at[pl.ds(0, 4)], dp_send),
        (total.at[0, pl.ds(0, 3 * rows // 4)], f_send),
        (dtwo, two_send.at[0]),
        (gtwo, two_send.at[1]),
        (done, one_send.at[0]),
        (gone, one_send.at[1]),
    ]
    for here, sem in sent:
        remote(here, here, sem, load, mate).wait_send()
    for copy in (a_all, b_all, t_all(), g_all()):
        copy.wait_send()

    @pl.when(inner)
    def _():
        for here, sem in (
            (xg.at[0, :, 0, pl.ds(0, 240)], z_send.at[1]),
            (xg.at[pl.ds(0, 4), 0, 0, pl.ds(0, XFIRST)], zx_send.at[1]),
        ):
            remote(here, here, sem, load, mate).wait_send()
        remote(rounded, result, r_send, r_recv, across).wait()

    @pl.when(outer)
    def _():
        keeps[3].wait()

    for copy in keeps[:3]:
        copy.wait()


def store_kernel(*refs):
    found, kept, held, sem = refs[:4], refs[4:8], refs[8:12], refs[12]
    loads = [pltpu.make_async_copy(found[i], held[i], sem.at[0, i]) for i in range(4)]
    stores = [pltpu.make_async_copy(held[i], kept[i], sem.at[1, i]) for i in range(4)]
    for copy in loads:
        copy.start()
    for i in range(4):
        loads[i].wait()
        stores[i].start()
    for copy in stores:
        copy.wait()


HBM = pl.BlockSpec(memory_space=pltpu.HBM)
DMA = pltpu.SemaphoreType.DMA


def body(tokens, out_grad, gate_weight, up_weight, down_weight):
    nf, nt = lax.axis_size("fsdp"), lax.axis_size("tp")
    rows, shard = tokens.shape
    deep, width = gate_weight.shape
    assert nf == 8 and nt == 16 and deep == 2 * shard
    factor = 1.0 / math.sqrt(rows * nf)
    tall = 2 * rows
    wide = 2 * width

    shapes = (
        jax.ShapeDtypeStruct((rows, shard), BF16),
        jax.ShapeDtypeStruct((deep, width), F32),
        jax.ShapeDtypeStruct((deep, width), F32),
        jax.ShapeDtypeStruct((width, deep), F32),
    )
    found = tuple(
        pl.pallas_call(
            functools.partial(kernel, factor),
            out_shape=shapes,
            in_specs=[HBM] * 5,
            out_specs=(HBM,) * 4,
            scratch_shapes=[
                pltpu.VMEM((deep, width), F32),
                pltpu.VMEM((deep, width), F32),
                pltpu.VMEM((width, deep), F32),
                pltpu.VMEM((8, 2, 3, rows, shard), BF16),
                pltpu.VMEM((4, 2, deep, width), BF16),
                pltpu.VMEM((4, width, deep), BF16),
                pltpu.VMEM((tall, wide), F32),
                pltpu.VMEM((tall, wide), F32),
                pltpu.VMEM((tall, width), F32),
                pltpu.VMEM((tall, width), F32),
                pltpu.VMEM((tall, wide), F32),
                pltpu.VMEM((tall, width), BF16),
                pltpu.VMEM((8, tall, wide), BF16),
                pltpu.VMEM((8, 2, shard, width), BF16),
                pltpu.VMEM((2, width, shard), F32),
                pltpu.VMEM((2, deep // 2, wide), F32),
                pltpu.VMEM((2, width, shard), BF16),
                pltpu.VMEM((deep, wide), BF16),
                pltpu.VMEM((2, 2, width, shard), BF16),
                pltpu.VMEM((2, deep, wide), BF16),
                pltpu.VMEM((2, width, shard), BF16),
                pltpu.VMEM((2, deep // 2, wide), BF16),
                pltpu.VMEM((2, 2, width, shard), BF16),
                pltpu.VMEM((2, deep, wide), BF16),
                pltpu.VMEM((deep, wide), F32),
                pltpu.VMEM((2, rows, shard), F32),
                pltpu.VMEM((rows, wide), F32),
                pltpu.VMEM((rows, wide), BF16),
                pltpu.VMEM((rows, wide), BF16),
                pltpu.VMEM((rows, shard), BF16),
                DMA(()),
                DMA((4,)),
                DMA((2,)),
                DMA((2, 2, 2)),
                DMA(()),
                DMA((2, 2, 5)),
                DMA(()),
                DMA((4, 2)),
                DMA(()),
                DMA((4,)),
                DMA((2,)),
                DMA((3,)),
                DMA(()),
                DMA((3, 3)),
                DMA(()),
                DMA(()),
                DMA(()),
                DMA((2,)),
                DMA(()),
                DMA(()),
                DMA(()),
                DMA((3,)),
                DMA(()),
                DMA(()),
                DMA(()),
                DMA((PIECES,)),
                DMA(()),
                DMA((3, 2, 2)),
                DMA(()),
                DMA((4, 2)),
                DMA((2,)),
                DMA((2, 2)),
                DMA((2,)),
                DMA((2,)),
                DMA(()),
                DMA(()),
            ],
            compiler_params=pltpu.CompilerParams(
                collective_id=0, has_side_effects=True, vmem_limit_bytes=VMEM_LIMIT
            ),
            name="block",
        )(tokens, out_grad, gate_weight, up_weight, down_weight)
    )
    return tuple(
        pl.pallas_call(
            store_kernel,
            out_shape=shapes,
            in_specs=[HBM] * 4,
            out_specs=(HBM,) * 4,
            scratch_shapes=[pltpu.VMEM(s.shape, s.dtype) for s in shapes] + [DMA((2, 4))],
            compiler_params=pltpu.CompilerParams(vmem_limit_bytes=VMEM_LIMIT),
            name="store",
        )(*found)
    )


def solution(mesh):
    return jax.shard_map(
        body,
        mesh=mesh,
        in_specs=(
            P("fsdp", "tp"),
            P("fsdp", "tp"),
            P("fsdp", "tp"),
            P("fsdp", "tp"),
            P("tp", "fsdp"),
        ),
        out_specs=(P("fsdp", "tp"), P("fsdp", "tp"), P("fsdp", "tp"), P("tp", "fsdp")),
        check_vma=False,
    )
```

```python
import functools
import math

import jax
import jax.numpy as jnp
from jax import lax
from jax.sharding import PartitionSpec as P
from jax.experimental import pallas as pl
from jax.experimental.pallas import tpu as pltpu

MESH = pl.DeviceIdType.MESH
F32 = jnp.float32
BF16 = jnp.bfloat16
VMEM_LIMIT = 60 * 1024 * 1024
XFIRST = 32
PIECES = 8
DIRECT = 384
ROWS = ((0,), (0,))
COLS = ((1,), (1,))


def kernel(
    factor,
    tokens,
    grads,
    gate_weight,
    up_weight,
    down_weight,
    result,
    gate_out,
    up_out,
    down_out,
    gate_own,
    up_own,
    down_own,
    xg,
    wf,
    df,
    sa,
    zla,
    sb,
    zlb,
    acts,
    hidden,
    dg,
    tw,
    dpart,
    gpart,
    dtwo,
    gtwo,
    done,
    gone,
    dmid,
    gmid,
    dland,
    gland,
    gown,
    total,
    near,
    slim,
    slim_near,
    rounded,
    load,
    keep,
    z_send,
    z_recv,
    x_send,
    x_recv,
    p_send,
    p_recv,
    v_send,
    v_recv,
    zx_send,
    zx_recv,
    y_send,
    y_recv,
    a_send,
    a_recv,
    b_send,
    b_recv,
    t_send,
    t_recv,
    u_send,
    u_recv,
    g_send,
    g_recv,
    f_send,
    f_recv,
    dx_send,
    dx_recv,
    dp_send,
    dp_recv,
    two_send,
    two_recv,
    one_send,
    one_recv,
    r_send,
    r_recv,
):
    f, t = lax.axis_index("fsdp"), lax.axis_index("tp")
    h, y = lax.div(f, 4), lax.rem(f, 4)
    l, x, k = lax.div(t, 8), lax.rem(lax.div(t, 2), 4), lax.rem(t, 2)
    outer = h == l
    inner = h != l
    rows, shard = tokens.shape
    deep, width = gate_weight.shape
    part = rows // 2
    zparts = ((rows - XFIRST) // 2, part)
    first = rows - XFIRST
    xpart = XFIRST // 2
    odd = (h - l) * (h - l)
    home = h * (1 - odd) + 2 * odd
    wide = 2 * width

    def at(xx, yy, hh, ll, kk):
        return (hh * 4 + yy, ll * 8 + xx * 2 + kk)

    xs = (lax.rem(x + 3, 4), lax.rem(x + 1, 4), lax.rem(x + 2, 4))
    ys = (lax.rem(y + 3, 4), lax.rem(y + 1, 4), lax.rem(y + 2, 4))
    right, left = at(xs[1], y, h, l, k), at(xs[0], y, h, l, k)
    north, south = at(x, ys[1], h, l, k), at(x, ys[0], h, l, k)
    mate = at(x, y, h, l, 1 - k)
    flip = at(x, y, h, 1 - l, k)
    across = at(x, y, 1 - h, 1 - l, k)
    opposite = at(x, y, 1 - h, l, k)
    me = 2 * x + k

    def remote(src, dst, send, recv, device):
        return pltpu.make_async_remote_copy(
            src_ref=src,
            dst_ref=dst,
            send_sem=send,
            recv_sem=recv,
            device_id=device,
            device_id_type=MESH,
        )

    copies = [
        pltpu.make_async_copy(ref, spot, load)
        for ref, spot in (
            (tokens, xg.at[k * 4 + x, 0, home]),
            (gate_weight, wf.at[y, 0]),
            (up_weight, wf.at[y, 1]),
            (grads, xg.at[k * 4 + x, 1, home]),
            (down_weight, df.at[y]),
        )
    ]
    for copy in copies:
        copy.start()

    barrier = pltpu.get_barrier_semaphore()
    for j in range(1, 16):
        pl.semaphore_signal(
            barrier, inc=1, device_id=(f, lax.rem(t + j, 16)), device_id_type=MESH
        )
    for peer in (north, south, opposite, across):
        pl.semaphore_signal(barrier, inc=1, device_id=peer, device_id_type=MESH)
    pl.semaphore_wait(barrier, 19)

    all_in = xg.at[pl.ds(0, 5), 0, 0]
    pltpu.make_async_copy(all_in, all_in, load).wait()

    def w_spot(o, w, q):
        if w == 2:
            return df.at[o, pl.ds(q * (width // 2), width // 2)]
        return wf.at[o, w, pl.ds(q * (deep // 2), deep // 2)]

    def w_out(way, w, q):
        return remote(
            w_spot(y, w, q),
            w_spot(y, w, q),
            y_send,
            y_recv.at[w, q if way == q else 2],
            (north, south)[way],
        )

    def w_on(w, q):
        here = w_spot(ys[q], w, q)
        return remote(here, here, y_send, y_recv.at[w, 2], (north, south)[q])

    def w_wait(w, e, here):
        remote(here, here, y_send, y_recv.at[w, e], north).wait_recv()

    def w_start(w):
        for way, q in ((0, 0), (1, 1), (0, 1), (1, 0)):
            w_out(way, w, q).start()

    def w_forward(w):
        for q in range(2):
            w_wait(w, q, w_spot(ys[q], w, q))
            w_on(w, q).start()

    def w_rest(w):
        w_wait(w, 2, df.at[pl.ds(0, 2)] if w == 2 else wf.at[pl.ds(0, 2), w])

    slot = (h, 1 - h)

    def x_own(m, q):
        return xg.at[k * 4 + x, m, home, pl.ds(q * zparts[m], zparts[m])]

    def x_spot(p, o, j, m, q):
        return xg.at[p * 4 + o, m, slot[j], pl.ds(q * zparts[m], zparts[m])]

    def z_out(m, q, device, j):
        spot = xg.at[k * 4 + x, m, h, pl.ds(q * zparts[m], zparts[m])]
        return remote(x_own(m, q), spot, z_send.at[0], z_recv.at[j, m, q], device)

    def z_on(m, q):
        here = x_spot(k, x, 1, m, q)
        return remote(here, here, z_send.at[1], z_recv.at[1, m, q], flip)

    def z_in(j, m, q):
        here = x_spot(k, x, j, m, q)
        return remote(here, here, z_send.at[0], z_recv.at[j, m, q], flip)

    def x_out(way, src, j, m, q):
        return remote(
            src,
            x_spot(k, x, j, m, q),
            x_send,
            x_recv.at[m, q, 2 * way + j],
            (right, left)[way],
        )

    def x_on(j, m, q):
        here = x_spot(k, xs[q], j, m, q)
        return remote(
            here, here, x_send, x_recv.at[m, q, 4], (right, left)[q]
        )

    def x_wait(m, q, e, here):
        remote(here, here, x_send, x_recv.at[m, q, e], right).wait_recv()

    places = (*xs, x)

    def p_out(d, src, j, m, q):
        return remote(
            src,
            x_spot(k, places[d], j, m, q),
            p_send,
            p_recv.at[d, m],
            mate,
        )

    def spread(src, j, m, q):
        for way in (0, 1) if q == 0 else (1, 0):
            x_out(way, src, j, m, q).start()
        p_out(3, src, j, m, q).start()

    def passed(d, j, m, q):
        x_wait(m, q, 2 * d + j, x_spot(k, xs[d], j, m, q))
        if d == q:
            x_on(j, m, q).start()
        p_out(d, x_spot(k, places[d], j, m, q), j, m, q).start()

    def x_rest(m):
        for q in range(2):
            here = xg.at[k * 4 + xs[2], m, pl.ds(0, 2), pl.ds(q * zparts[m], zparts[m])]
            x_wait(m, q, 4, here)
            for j in range(2):
                p_out(2, x_spot(k, xs[2], j, m, q), j, m, q).start()

    def z_forward(m, q):
        @pl.when(inner)
        def _():
            z_in(1, m, q).wait_recv()
            z_on(m, q).start()

    def z_near(m, q):
        @pl.when(inner)
        def _():
            z_in(0, m, q).wait_recv()

        spread(x_spot(k, x, 0, m, q), 0, m, q)

    def z_far(m, q):
        @pl.when(outer)
        def _():
            z_in(1, m, q).wait_recv()

        spread(x_spot(k, x, 1, m, q), 1, m, q)

    def z_near_inner(m, q):
        @pl.when(inner)
        def _():
            z_in(0, m, q).wait_recv()
            spread(x_spot(k, x, 0, m, q), 0, m, q)

    fourths = (shard // 4, (shard - DIRECT) // 4)
    bases = (0, DIRECT)

    def t_copy(u, w):
        return remote(
            wf.at[
                lax.div(u, 2),
                w,
                pl.ds(lax.rem(u, 2) * shard + bases[w] + y * fourths[w], fourths[w]),
            ],
            tw.at[me, w, pl.ds(bases[w] + y * fourths[w], fourths[w])],
            t_send,
            t_recv,
            (f, l * 8 + u),
        )

    def t_out(w, j):
        return t_copy(lax.rem(me + j, 8), w)

    def t_all():
        here = tw.at[pl.ds(0, 7), 0, pl.ds(0, fourths[0] + fourths[1])]
        return remote(here, here, t_send, t_recv, mate)

    def g_out(j):
        u = lax.rem(me + j, 8)
        return remote(
            wf.at[lax.div(u, 2), 1, pl.ds(lax.rem(u, 2) * shard, DIRECT)],
            tw.at[me, 1, pl.ds(0, DIRECT)],
            g_send,
            g_recv,
            (f, l * 8 + u),
        )

    def g_all():
        here = tw.at[pl.ds(0, 7), 1, pl.ds(0, DIRECT)]
        return remote(here, here, g_send, g_recv, mate)

    def u_spot(o, w, q):
        return tw.at[pl.ds(q * 4, 4), w, pl.ds(bases[w] + o * fourths[w], fourths[w])]

    def u_out(way, w, q):
        here = u_spot(y, w, q)
        return remote(
            here, here, u_send, u_recv.at[q if way == q else 2], (north, south)[way]
        )

    def u_on(w, q):
        here = u_spot(ys[q], w, q)
        return remote(here, here, u_send, u_recv.at[2], (north, south)[q])

    def u_wait(e, here):
        remote(here, here, u_send, u_recv.at[e], north).wait_recv()

    def v_spot(o, q):
        return xg.at[k * 4 + o, 0, home, pl.ds(first + q * xpart, xpart)]

    def v_out(way, q):
        here = v_spot(x, q)
        return remote(
            here, here, v_send, v_recv.at[q if way == q else 2], (right, left)[way]
        )

    def v_on(q):
        here = v_spot(xs[q], q)
        return remote(here, here, v_send, v_recv.at[3], (right, left)[q])

    def v_wait(e, here):
        remote(here, here, v_send, v_recv.at[e], right).wait_recv()

    def zx_spot(p, d, at_s):
        return xg.at[p * 4 + places[d], 0, at_s, pl.ds(first, XFIRST)]

    def zx_out(d, device, j):
        return remote(
            zx_spot(k, d, home),
            zx_spot(k, d, h),
            zx_send.at[0],
            zx_recv.at[j + (j * d == 2)],
            device,
        )

    def zx_on(d):
        here = zx_spot(k, d, 1 - h)
        return remote(here, here, zx_send.at[1], zx_recv.at[1 + (d == 2)], flip)

    def zx_wait(e, count):
        here = xg.at[pl.ds(0, count), 0, 0, pl.ds(first, XFIRST)]
        remote(here, here, zx_send.at[0], zx_recv.at[e], flip).wait_recv()

    def px_out(d, j):
        here = zx_spot(k, d, slot[j])
        return remote(here, here, p_send, p_recv.at[d, 0], mate)

    def v_start():
        for q in range(2):
            for way in (0, 1) if q == 0 else (1, 0):
                v_out(way, q).start()

    def v_near():
        for q in range(2):
            v_wait(q, v_spot(xs[q], q))
            v_on(q).start()
        v_wait(2, zx_spot(k, 0, home))

    def v_far():
        v_wait(3, zx_spot(k, 2, home))

    def zx_start(ds):
        for d in ds:

            @pl.when(outer)
            def _(d=d):
                zx_out(d, flip, 0).start()
                px_out(d, 0).start()

            @pl.when(inner)
            def _(d=d):
                zx_out(d, across, 1).start()

    def zx_pass(e, ds):
        @pl.when(inner)
        def _():
            zx_wait(e, len(ds))
            for d in ds:
                zx_on(d).start()

    def zx_take():
        @pl.when(inner)
        def _():
            zx_wait(0, 4)
            for d in range(4):
                px_out(d, 0).start()

        @pl.when(outer)
        def _():
            zx_wait(1, 3)
            zx_wait(2, 1)

        for d in range(4):
            px_out(d, 1).start()

    def z_start(m):
        @pl.when(outer)
        def _():
            for q in range(2):
                z_out(m, q, flip, 0).start()

        @pl.when(inner)
        def _():
            for q in range(2):
                z_out(m, q, across, 1).start()

    v_start()
    z_start(0)

    @pl.when(outer)
    def _():
        for q in range(2):
            spread(x_own(0, q), 0, 0, q)

    zx_start((3,))
    w_start(0)
    w_start(1)

    v_near()
    zx_start((0, 1))
    z_forward(0, 0)
    z_near_inner(0, 0)
    z_far(0, 0)
    v_far()
    zx_start((2,))
    z_start(1)
    z_forward(0, 1)
    z_near_inner(0, 1)
    z_far(0, 1)
    w_forward(0)
    for j in range(2):
        passed(0, j, 0, 0)
        passed(1, j, 0, 0)
    w_forward(1)
    w_start(2)
    for j in range(2):
        passed(1, j, 0, 1)
        passed(0, j, 0, 1)
    z_forward(1, 0)
    zx_pass(1, (3, 0, 1))
    z_forward(1, 1)
    zx_pass(2, (2,))
    w_rest(0)
    w_rest(1)

    @pl.loop(1, 8)
    def _(j):
        for w in range(2):
            t_out(w, j).start()

    z_near(1, 0)
    z_near(1, 1)
    z_far(1, 0)
    z_far(1, 1)
    w_forward(2)
    zx_take()
    tall = 2 * rows

    def block(m, o):
        return jnp.concatenate(
            [xg[p * 4 + o, m, :2].reshape(tall, shard) for p in range(2)], axis=1
        )

    def pair_in(d, m):
        here = xg.at[(1 - k) * 4 + places[d], m, pl.ds(0, 2)]
        remote(here, here, p_send, p_recv.at[d, m], mate).wait_recv()

    def gate_up(d):
        o = places[d]
        weights = jnp.concatenate([wf[o, 0], wf[o, 1]], axis=1)
        term = jnp.dot(block(0, o), weights, preferred_element_type=F32)
        sa[...] = term if d == 3 else sa[...] + term

    for d in (3, 0, 1):
        pair_in(d, 0)
        gate_up(d)
    x_rest(0)
    pair_in(2, 0)
    gate_up(2)
    turn = (1 - l, l)

    def swap(src, dst, send, recvs):
        def copy(c):
            at_c = pl.ds(turn[c] * rows, rows)
            return remote(src.at[at_c], dst.at[at_c], send, recvs[c], opposite)

        return copy

    a_swap = swap(sa, zla, a_send, (a_recv, a_recv))
    b_swap = swap(sb, zlb, b_send, (b_recv.at[0], b_recv.at[1]))
    a_all = remote(sa, zla, a_send, a_recv, opposite)
    b_all = remote(sb, zlb, b_send, b_recv.at[0], opposite)

    a_swap(0).start()
    for w in range(2):
        mine_w = pl.ds(bases[w] + y * fourths[w], fourths[w])
        tw[me, w, mine_w] = wf[x, w, pl.ds(k * shard + bases[w] + y * fourths[w], fourths[w])]
    tw[me, 1, :DIRECT] = wf[x, 1, pl.ds(k * shard, DIRECT)]
    a_swap(1).start()
    t_all().wait_recv()

    for w in range(2):
        for way, q in ((0, 0), (1, 1), (0, 1), (1, 0)):
            u_out(way, w, q).start()
    for j in range(2):
        passed(0, j, 1, 0)
        passed(1, j, 1, 0)
    for j in range(2):
        passed(1, j, 1, 1)
        passed(0, j, 1, 1)

    def grad_in(d):
        o = places[d]
        term = lax.dot_general(
            block(1, o), df[o], (COLS, ((), ())), preferred_element_type=F32
        )
        sb[...] = term if d == 3 else sb[...] + term

    w_rest(2)
    for d in (3, 0, 1):
        pair_in(d, 1)
        grad_in(d)
    def down_half(o, p):
        return lax.dot_general(
            hidden[...],
            xg[p * 4 + o, 1, :2].reshape(tall, shard),
            (ROWS, ((), ())),
            preferred_element_type=F32,
        )

    def gate_part(o):
        return lax.dot_general(
            block(0, o), dg[me], (ROWS, ((), ())), preferred_element_type=F32
        )

    twos, mids, parts, ones, lands = (
        (dtwo, gtwo),
        (dmid, gmid),
        (dpart, gpart),
        (done, gone),
        (dland, gland),
    )

    def halves(i, q):
        return q if i == 0 else pl.ds(q * shard, shard)

    def beside(way):
        return lax.rem(y + 1 + 2 * way, 4)

    def two_out(i, q):
        return remote(
            twos[i].at[halves(i, q)],
            mids[i].at[q],
            two_send.at[i],
            two_recv.at[i, q],
            at(x, beside(q), h, l, k),
        )

    def one_out(i, way, q):
        return remote(
            ones[i].at[way, halves(i, q)],
            lands[i].at[way, halves(i, q)],
            one_send.at[i],
            one_recv.at[i],
            at(x, beside(way), h, l, k),
        )

    def gate_half(o, p):
        return lax.dot_general(
            xg[p * 4 + o, 0, :2].reshape(tall, shard),
            dg[me],
            (ROWS, ((), ())),
            preferred_element_type=F32,
        )

    def gate_rows(o, p, e):
        return lax.dot_general(
            xg[p * 4 + o, 0, turn[e]],
            dg[me, pl.ds(turn[e] * rows, rows)],
            (ROWS, ((), ())),
            preferred_element_type=F32,
        )

    def one_merge(i):
        for way in range(2):
            two_out(i, way).wait_recv()
            ones[i][way, halves(i, way)] = (
                parts[i][way] + mids[i][way].astype(F32)
            ).astype(BF16)

    def finals(i):
        remote(ones[i], lands[i], one_send.at[i], one_recv.at[i], north).wait_recv()
        return lands[i][0].astype(F32) + lands[i][1].astype(F32)

    def grad_last(c):
        at_s = pl.ds(turn[c] * rows, rows)
        last = jnp.concatenate([xg[p * 4 + xs[2], 1, turn[c]] for p in range(2)], axis=1)
        sb[at_s] += lax.dot_general(
            last, df[xs[2]], (COLS, ((), ())), preferred_element_type=F32
        )

    for q in range(2):
        u_wait(q, tw.at[pl.ds(q * 4, 4), 0, pl.ds(0, fourths[0] + fourths[1])])
        for w in range(2):
            u_on(w, q).start()
    x_rest(1)
    @pl.loop(1, 8)
    def _(j):
        g_out(j).start()

    a_all.wait_recv()
    sums = sa[...] + zla[...]
    gate, up = sums[:, :width], sums[:, width:]
    squashed = jax.nn.sigmoid(gate)
    activated = gate * squashed
    slope = squashed * (1.0 + gate * (1.0 - squashed))
    acts[:, :width] = up * slope
    acts[:, width:] = activated
    hidden[...] = (activated * up).astype(BF16)

    dtwo[k] = down_half(ys[2], k).astype(BF16)
    done[1 - k, k] = down_half(beside(1 - k), k).astype(BF16)
    two_out(0, k).start()
    pair_in(2, 1)
    grad_last(0)
    grad_last(1)
    b_swap(0).start()
    dtwo[1 - k] = down_half(ys[2], 1 - k).astype(BF16)
    b_swap(1).start()
    done[k, 1 - k] = down_half(beside(k), 1 - k).astype(BF16)
    two_out(0, 1 - k).start()
    one_out(0, 1 - k, k).start()
    dpart[k] = down_half(beside(k), k)
    one_out(0, k, 1 - k).start()
    dpart[1 - k] = down_half(beside(1 - k), 1 - k)
    one_merge(0)
    def d_spot(c, o, e, q):
        return dg.at[o * 2 + c, pl.ds(turn[e] * rows + q * part, part)]

    def dx_out(way, e, q):
        here = d_spot(k, x, e, q)
        return remote(
            here, here, dx_send, dx_recv.at[way, e, q], (right, left)[way]
        )

    def dx_on(e, q):
        here = d_spot(k, xs[q], e, q)
        return remote(here, here, dx_send, dx_recv.at[2, e, 0], (right, left)[q])

    def dx_in(d, e, q):
        here = d_spot(k, xs[d], e, q)
        return remote(here, here, dx_send, dx_recv.at[d, e, q], right)

    def dp_out(d, e, q):
        here = d_spot(k, places[d], e, q)
        return remote(here, here, dp_send, dp_recv.at[d, e], mate)

    def d_half(c, d, e):
        return dg.at[places[d] * 2 + c, pl.ds(turn[e] * rows, rows)]

    def d_far(e):
        here = d_half(k, 2, e)
        remote(here, here, dx_send, dx_recv.at[2, e, 0], right).wait_recv()
        for q in range(2):
            dp_out(2, e, q).start()

    def d_start(e):
        for q in range(2):
            for way in (0, 1) if q == 0 else (1, 0):
                dx_out(way, e, q).start()
            dp_out(3, e, q).start()

    def d_passed(d, e, q):
        dx_in(d, e, q).wait_recv()
        if d == q:
            dx_on(e, q).start()
        dp_out(d, e, q).start()

    def d_near(e):
        for q in range(2):
            d_passed(q, e, q)
        for q in range(2):
            d_passed(1 - q, e, q)

    def gather(d, e):
        base = places[d] * 2
        at_s = pl.ds(turn[e] * rows, rows)
        left_side = jnp.concatenate([dg[base, at_s], dg[base + 1, at_s]], axis=1)
        right_side = jnp.concatenate(
            [tw[base, 0], tw[base, 1], tw[base + 1, 0], tw[base + 1, 1]], axis=1
        )
        term = lax.dot_general(
            left_side, right_side, (COLS, ((), ())), preferred_element_type=F32
        )
        total[e] = term if d == 3 else total[e] + term

    def gathers(e, ds):
        for d in ds:
            here = d_half(1 - k, d, e)
            remote(here, here, dp_send, dp_recv.at[d, e], mate).wait_recv()
            gather(d, e)

    piece = rows // PIECES

    def f_out(c):
        at_c = pl.ds(c * piece, piece)
        return (
            remote(total.at[0, at_c, pl.ds(0, wide)], near.at[at_c], f_send, f_recv.at[c], flip),
            remote(slim.at[at_c], slim_near.at[at_c], f_send, f_recv.at[c], flip),
        )

    def f_start(cs):
        for c in cs:
            for copy in f_out(c):
                copy.start()

    def f_wait(c):
        here = near.at[pl.ds(0, 3 * piece // 2)]
        remote(here, here, f_send, f_recv.at[c], flip).wait_recv()

    def r_out(c):
        at_c = pl.ds(c * piece, piece)
        return remote(rounded.at[at_c], result.at[at_c], r_send, r_recv, across)

    def delta(e):
        b_swap(e).wait_recv()
        at_s = pl.ds(turn[e] * rows, rows)
        hidden_grad = sb[at_s] + zlb[at_s]
        dg[me, at_s, :width] = (hidden_grad * acts[at_s, :width]).astype(BF16)
        dg[me, at_s, width:] = (hidden_grad * acts[at_s, width:]).astype(BF16)

    delta(0)
    for way in range(2):
        one_out(0, way, way).start()
    down_own[:, :shard] = down_half(y, 0)
    d_start(0)
    down_own[:, shard:] = down_half(y, 1)
    gown[...] = jnp.concatenate([gate_rows(ys[2], p, 0) for p in range(2)], axis=0)
    delta(1)
    for p in range(2):
        gtwo[halves(1, p)] = (gown[halves(1, p)] + gate_rows(ys[2], p, 1)).astype(BF16)
    two_out(1, 0).start()
    gone[0, halves(1, 1)] = gate_half(beside(0), 1).astype(BF16)
    two_out(1, 1).start()
    gone[1, halves(1, 0)] = gate_half(beside(1), 0).astype(BF16)
    one_out(1, 0, 1).start()
    gpart[0] = gate_half(beside(0), 0)
    one_out(1, 1, 0).start()
    gpart[1] = gate_half(beside(1), 1)
    d_near(0)
    d_start(1)
    gown[...] = gate_part(y)
    u_wait(2, tw.at[:, :, pl.ds(0, fourths[0] + fourths[1])])
    g_all().wait_recv()

    gathers(0, (3, 0, 1))
    d_far(0)
    gathers(0, (2,))
    slim[...] = total[0, :, wide:].astype(BF16)
    f_start(range(PIECES // 2))
    d_near(1)
    f_start(range(PIECES // 2, PIECES))
    one_merge(1)
    gathers(1, (3,))
    for way in range(2):
        one_out(1, way, way).start()
    gathers(1, (0, 1))
    d_far(1)
    gathers(1, (2,))
    keeps = [
        pltpu.make_async_copy(src, dst, keep.at[i])
        for i, (src, dst) in enumerate(
            ((down_own, down_out), (gate_own, gate_out), (up_own, up_out), (rounded, result))
        )
    ]
    for c in range(PIECES):
        f_wait(c)
        at_c = pl.ds(c * piece, piece)
        rounded[at_c, :wide] = (total[1, at_c, :wide] + near[at_c]).astype(BF16)
        rounded[at_c, wide:] = (total[1, at_c, wide:] + slim_near[at_c].astype(F32)).astype(BF16)

        if c:

            @pl.when(inner)
            def _(c=c):
                r_out(c - 1).start()

    both = finals(0)
    for p in range(2):
        at_p = slice(p * shard, (p + 1) * shard)
        down_own[:, at_p] = factor * (down_own[:, at_p] + both[p])
    @pl.when(inner)
    def _():
        r_out(PIECES - 1).start()

    @pl.when(outer)
    def _():
        keeps[3].start()

    both = factor * (gown[...] + finals(1))
    gate_own[...] = both[:, :width]
    up_own[...] = both[:, width:]
    for copy in keeps[:3]:
        copy.start()

    sent = [
        (xg.at[0, :, 0, pl.ds(0, 240)], z_send.at[0]),
        (xg.at[pl.ds(0, 4), 0, 0, pl.ds(0, XFIRST)], zx_send.at[0]),
        (xg.at[pl.ds(0, 3), 0, 0, pl.ds(0, XFIRST)], v_send),
        (xg.at[pl.ds(0, 4), 0, :, pl.ds(0, 240)], x_send),
        (xg.at[:, :, 0], p_send),
        (xg.at[pl.ds(0, 3), 0], y_send),
        (tw.at[:, :, pl.ds(0, 3 * (fourths[0] + fourths[1]) // 2)], u_send),
        (dg.at[pl.ds(0, 3)], dx_send),
        (dg.at[pl.ds(0, 4)], dp_send),
        (total.at[0, pl.ds(0, 3 * rows // 4)], f_send),
        (dtwo, two_send.at[0]),
        (gtwo, two_send.at[1]),
        (done, one_send.at[0]),
        (gone, one_send.at[1]),
    ]
    for here, sem in sent:
        remote(here, here, sem, load, mate).wait_send()
    for copy in (a_all, b_all, t_all(), g_all()):
        copy.wait_send()

    @pl.when(inner)
    def _():
        for here, sem in (
            (xg.at[0, :, 0, pl.ds(0, 240)], z_send.at[1]),
            (xg.at[pl.ds(0, 4), 0, 0, pl.ds(0, XFIRST)], zx_send.at[1]),
        ):
            remote(here, here, sem, load, mate).wait_send()
        remote(rounded, result, r_send, r_recv, across).wait()

    @pl.when(outer)
    def _():
        keeps[3].wait()

    for copy in keeps[:3]:
        copy.wait()


def store_kernel(*refs):
    found, kept, held, sem = refs[:4], refs[4:8], refs[8:12], refs[12]
    loads = [pltpu.make_async_copy(found[i], held[i], sem.at[0, i]) for i in range(4)]
    stores = [pltpu.make_async_copy(held[i], kept[i], sem.at[1, i]) for i in range(4)]
    for copy in loads:
        copy.start()
    for i in range(4):
        loads[i].wait()
        stores[i].start()
    for copy in stores:
        copy.wait()


HBM = pl.BlockSpec(memory_space=pltpu.HBM)
DMA = pltpu.SemaphoreType.DMA


def body(tokens, out_grad, gate_weight, up_weight, down_weight):
    nf, nt = lax.axis_size("fsdp"), lax.axis_size("tp")
    rows, shard = tokens.shape
    deep, width = gate_weight.shape
    assert nf == 8 and nt == 16 and deep == 2 * shard
    factor = 1.0 / math.sqrt(rows * nf)
    tall = 2 * rows
    wide = 2 * width

    shapes = (
        jax.ShapeDtypeStruct((rows, shard), BF16),
        jax.ShapeDtypeStruct((deep, width), F32),
        jax.ShapeDtypeStruct((deep, width), F32),
        jax.ShapeDtypeStruct((width, deep), F32),
    )
    found = tuple(
        pl.pallas_call(
            functools.partial(kernel, factor),
            out_shape=shapes,
            in_specs=[HBM] * 5,
            out_specs=(HBM,) * 4,
            scratch_shapes=[
                pltpu.VMEM((deep, width), F32),
                pltpu.VMEM((deep, width), F32),
                pltpu.VMEM((width, deep), F32),
                pltpu.VMEM((8, 2, 3, rows, shard), BF16),
                pltpu.VMEM((4, 2, deep, width), BF16),
                pltpu.VMEM((4, width, deep), BF16),
                pltpu.VMEM((tall, wide), F32),
                pltpu.VMEM((tall, wide), F32),
                pltpu.VMEM((tall, width), F32),
                pltpu.VMEM((tall, width), F32),
                pltpu.VMEM((tall, wide), F32),
                pltpu.VMEM((tall, width), BF16),
                pltpu.VMEM((8, tall, wide), BF16),
                pltpu.VMEM((8, 2, shard, width), BF16),
                pltpu.VMEM((2, width, shard), F32),
                pltpu.VMEM((2, deep // 2, wide), F32),
                pltpu.VMEM((2, width, shard), BF16),
                pltpu.VMEM((deep, wide), BF16),
                pltpu.VMEM((2, 2, width, shard), BF16),
                pltpu.VMEM((2, deep, wide), BF16),
                pltpu.VMEM((2, width, shard), BF16),
                pltpu.VMEM((2, deep // 2, wide), BF16),
                pltpu.VMEM((2, 2, width, shard), BF16),
                pltpu.VMEM((2, deep, wide), BF16),
                pltpu.VMEM((deep, wide), F32),
                pltpu.VMEM((2, rows, shard), F32),
                pltpu.VMEM((rows, wide), F32),
                pltpu.VMEM((rows, wide), BF16),
                pltpu.VMEM((rows, wide), BF16),
                pltpu.VMEM((rows, shard), BF16),
                DMA(()),
                DMA((4,)),
                DMA((2,)),
                DMA((2, 2, 2)),
                DMA(()),
                DMA((2, 2, 5)),
                DMA(()),
                DMA((4, 2)),
                DMA(()),
                DMA((4,)),
                DMA((2,)),
                DMA((3,)),
                DMA(()),
                DMA((3, 3)),
                DMA(()),
                DMA(()),
                DMA(()),
                DMA((2,)),
                DMA(()),
                DMA(()),
                DMA(()),
                DMA((3,)),
                DMA(()),
                DMA(()),
                DMA(()),
                DMA((PIECES,)),
                DMA(()),
                DMA((3, 2, 2)),
                DMA(()),
                DMA((4, 2)),
                DMA((2,)),
                DMA((2, 2)),
                DMA((2,)),
                DMA((2,)),
                DMA(()),
                DMA(()),
            ],
            compiler_params=pltpu.CompilerParams(
                collective_id=0, has_side_effects=True, vmem_limit_bytes=VMEM_LIMIT
            ),
            name="block",
        )(tokens, out_grad, gate_weight, up_weight, down_weight)
    )
    return tuple(
        pl.pallas_call(
            store_kernel,
            out_shape=shapes,
            in_specs=[HBM] * 4,
            out_specs=(HBM,) * 4,
            scratch_shapes=[pltpu.VMEM(s.shape, s.dtype) for s in shapes] + [DMA((2, 4))],
            compiler_params=pltpu.CompilerParams(vmem_limit_bytes=VMEM_LIMIT),
            name="store",
        )(*found)
    )


def solution(mesh):
    return jax.shard_map(
        body,
        mesh=mesh,
        in_specs=(
            P("fsdp", "tp"),
            P("fsdp", "tp"),
            P("fsdp", "tp"),
            P("fsdp", "tp"),
            P("tp", "fsdp"),
        ),
        out_specs=(P("fsdp", "tp"), P("fsdp", "tp"), P("fsdp", "tp"), P("tp", "fsdp")),
        check_vma=False,
    )
```

```python
import functools
import math

import jax
import jax.numpy as jnp
from jax import lax
from jax.sharding import PartitionSpec as P
from jax.experimental import pallas as pl
from jax.experimental.pallas import tpu as pltpu

MESH = pl.DeviceIdType.MESH
F32 = jnp.float32
BF16 = jnp.bfloat16
VMEM_LIMIT = 60 * 1024 * 1024
XFIRST = 32
PIECES = 8
DIRECT = 384
ROWS = ((0,), (0,))
COLS = ((1,), (1,))


def kernel(
    factor,
    tokens,
    grads,
    gate_weight,
    up_weight,
    down_weight,
    result,
    gate_out,
    up_out,
    down_out,
    gate_own,
    up_own,
    down_own,
    xg,
    wf,
    df,
    sa,
    zla,
    sb,
    zlb,
    acts,
    hidden,
    dg,
    tw,
    dpart,
    gpart,
    dtwo,
    gtwo,
    done,
    gone,
    dmid,
    gmid,
    dland,
    gland,
    gown,
    total,
    near,
    slim,
    slim_near,
    rounded,
    load,
    keep,
    z_send,
    z_recv,
    x_send,
    x_recv,
    p_send,
    p_recv,
    v_send,
    v_recv,
    zx_send,
    zx_recv,
    y_send,
    y_recv,
    a_send,
    a_recv,
    b_send,
    b_recv,
    t_send,
    t_recv,
    u_send,
    u_recv,
    g_send,
    g_recv,
    f_send,
    f_recv,
    dx_send,
    dx_recv,
    dp_send,
    dp_recv,
    two_send,
    two_recv,
    one_send,
    one_recv,
    r_send,
    r_recv,
):
    f, t = lax.axis_index("fsdp"), lax.axis_index("tp")
    h, y = lax.div(f, 4), lax.rem(f, 4)
    l, x, k = lax.div(t, 8), lax.rem(lax.div(t, 2), 4), lax.rem(t, 2)
    outer = h == l
    inner = h != l
    rows, shard = tokens.shape
    deep, width = gate_weight.shape
    part = rows // 2
    zparts = ((rows - XFIRST) // 2, part)
    first = rows - XFIRST
    xpart = XFIRST // 2
    odd = (h - l) * (h - l)
    home = h * (1 - odd) + 2 * odd
    wide = 2 * width

    def at(xx, yy, hh, ll, kk):
        return (hh * 4 + yy, ll * 8 + xx * 2 + kk)

    xs = (lax.rem(x + 3, 4), lax.rem(x + 1, 4), lax.rem(x + 2, 4))
    ys = (lax.rem(y + 3, 4), lax.rem(y + 1, 4), lax.rem(y + 2, 4))
    right, left = at(xs[1], y, h, l, k), at(xs[0], y, h, l, k)
    north, south = at(x, ys[1], h, l, k), at(x, ys[0], h, l, k)
    mate = at(x, y, h, l, 1 - k)
    flip = at(x, y, h, 1 - l, k)
    across = at(x, y, 1 - h, 1 - l, k)
    opposite = at(x, y, 1 - h, l, k)
    me = 2 * x + k

    def remote(src, dst, send, recv, device):
        return pltpu.make_async_remote_copy(
            src_ref=src,
            dst_ref=dst,
            send_sem=send,
            recv_sem=recv,
            device_id=device,
            device_id_type=MESH,
        )

    copies = [
        pltpu.make_async_copy(ref, spot, load)
        for ref, spot in (
            (tokens, xg.at[k * 4 + x, 0, home]),
            (gate_weight, wf.at[y, 0]),
            (up_weight, wf.at[y, 1]),
            (grads, xg.at[k * 4 + x, 1, home]),
            (down_weight, df.at[y]),
        )
    ]
    for copy in copies:
        copy.start()

    barrier = pltpu.get_barrier_semaphore()
    for j in range(1, 16):
        pl.semaphore_signal(
            barrier, inc=1, device_id=(f, lax.rem(t + j, 16)), device_id_type=MESH
        )
    for peer in (north, south, opposite, across):
        pl.semaphore_signal(barrier, inc=1, device_id=peer, device_id_type=MESH)
    pl.semaphore_wait(barrier, 19)

    all_in = xg.at[pl.ds(0, 5), 0, 0]
    pltpu.make_async_copy(all_in, all_in, load).wait()

    def w_spot(o, w, q):
        if w == 2:
            return df.at[o, pl.ds(q * (width // 2), width // 2)]
        return wf.at[o, w, pl.ds(q * (deep // 2), deep // 2)]

    def w_out(way, w, q):
        return remote(
            w_spot(y, w, q),
            w_spot(y, w, q),
            y_send,
            y_recv.at[w, q if way == q else 2],
            (north, south)[way],
        )

    def w_on(w, q):
        here = w_spot(ys[q], w, q)
        return remote(here, here, y_send, y_recv.at[w, 2], (north, south)[q])

    def w_wait(w, e, here):
        remote(here, here, y_send, y_recv.at[w, e], north).wait_recv()

    def w_start(w):
        for way, q in ((0, 0), (1, 1), (0, 1), (1, 0)):
            w_out(way, w, q).start()

    def w_forward(w):
        for q in range(2):
            w_wait(w, q, w_spot(ys[q], w, q))
            w_on(w, q).start()

    def w_rest(w):
        w_wait(w, 2, df.at[pl.ds(0, 2)] if w == 2 else wf.at[pl.ds(0, 2), w])

    slot = (h, 1 - h)

    def x_own(m, q):
        return xg.at[k * 4 + x, m, home, pl.ds(q * zparts[m], zparts[m])]

    def x_spot(p, o, j, m, q):
        return xg.at[p * 4 + o, m, slot[j], pl.ds(q * zparts[m], zparts[m])]

    def z_out(m, q, device, j):
        spot = xg.at[k * 4 + x, m, h, pl.ds(q * zparts[m], zparts[m])]
        return remote(x_own(m, q), spot, z_send.at[0], z_recv.at[j, m, q], device)

    def z_on(m, q):
        here = x_spot(k, x, 1, m, q)
        return remote(here, here, z_send.at[1], z_recv.at[1, m, q], flip)

    def z_in(j, m, q):
        here = x_spot(k, x, j, m, q)
        return remote(here, here, z_send.at[0], z_recv.at[j, m, q], flip)

    def x_out(way, src, j, m, q):
        return remote(
            src,
            x_spot(k, x, j, m, q),
            x_send,
            x_recv.at[m, q, 2 * way + j],
            (right, left)[way],
        )

    def x_on(j, m, q):
        here = x_spot(k, xs[q], j, m, q)
        return remote(
            here, here, x_send, x_recv.at[m, q, 4], (right, left)[q]
        )

    def x_wait(m, q, e, here):
        remote(here, here, x_send, x_recv.at[m, q, e], right).wait_recv()

    places = (*xs, x)

    def p_out(d, src, j, m, q):
        return remote(
            src,
            x_spot(k, places[d], j, m, q),
            p_send,
            p_recv.at[d, m],
            mate,
        )

    def spread(src, j, m, q):
        for way in (0, 1) if q == 0 else (1, 0):
            x_out(way, src, j, m, q).start()
        p_out(3, src, j, m, q).start()

    def passed(d, j, m, q):
        x_wait(m, q, 2 * d + j, x_spot(k, xs[d], j, m, q))
        if d == q:
            x_on(j, m, q).start()
        p_out(d, x_spot(k, places[d], j, m, q), j, m, q).start()

    def x_rest(m):
        for q in range(2):
            here = xg.at[k * 4 + xs[2], m, pl.ds(0, 2), pl.ds(q * zparts[m], zparts[m])]
            x_wait(m, q, 4, here)
            for j in range(2):
                p_out(2, x_spot(k, xs[2], j, m, q), j, m, q).start()

    def z_forward(m, q):
        @pl.when(inner)
        def _():
            z_in(1, m, q).wait_recv()
            z_on(m, q).start()

    def z_near(m, q):
        @pl.when(inner)
        def _():
            z_in(0, m, q).wait_recv()

        spread(x_spot(k, x, 0, m, q), 0, m, q)

    def z_far(m, q):
        @pl.when(outer)
        def _():
            z_in(1, m, q).wait_recv()

        spread(x_spot(k, x, 1, m, q), 1, m, q)

    def z_near_inner(m, q):
        @pl.when(inner)
        def _():
            z_in(0, m, q).wait_recv()
            spread(x_spot(k, x, 0, m, q), 0, m, q)

    fourths = (shard // 4, (shard - DIRECT) // 4)
    bases = (0, DIRECT)

    def t_copy(u, w):
        return remote(
            wf.at[
                lax.div(u, 2),
                w,
                pl.ds(lax.rem(u, 2) * shard + bases[w] + y * fourths[w], fourths[w]),
            ],
            tw.at[me, w, pl.ds(bases[w] + y * fourths[w], fourths[w])],
            t_send,
            t_recv,
            (f, l * 8 + u),
        )

    def t_out(w, j):
        return t_copy(lax.rem(me + j, 8), w)

    def t_all():
        here = tw.at[pl.ds(0, 7), 0, pl.ds(0, fourths[0] + fourths[1])]
        return remote(here, here, t_send, t_recv, mate)

    def g_out(j):
        u = lax.rem(me + j, 8)
        return remote(
            wf.at[lax.div(u, 2), 1, pl.ds(lax.rem(u, 2) * shard, DIRECT)],
            tw.at[me, 1, pl.ds(0, DIRECT)],
            g_send,
            g_recv,
            (f, l * 8 + u),
        )

    def g_all():
        here = tw.at[pl.ds(0, 7), 1, pl.ds(0, DIRECT)]
        return remote(here, here, g_send, g_recv, mate)

    def u_spot(o, w, q):
        return tw.at[pl.ds(q * 4, 4), w, pl.ds(bases[w] + o * fourths[w], fourths[w])]

    def u_out(way, w, q):
        here = u_spot(y, w, q)
        return remote(
            here, here, u_send, u_recv.at[q if way == q else 2], (north, south)[way]
        )

    def u_on(w, q):
        here = u_spot(ys[q], w, q)
        return remote(here, here, u_send, u_recv.at[2], (north, south)[q])

    def u_wait(e, here):
        remote(here, here, u_send, u_recv.at[e], north).wait_recv()

    def v_spot(o, q):
        return xg.at[k * 4 + o, 0, home, pl.ds(first + q * xpart, xpart)]

    def v_out(way, q):
        here = v_spot(x, q)
        return remote(
            here, here, v_send, v_recv.at[q if way == q else 2], (right, left)[way]
        )

    def v_on(q):
        here = v_spot(xs[q], q)
        return remote(here, here, v_send, v_recv.at[3], (right, left)[q])

    def v_wait(e, here):
        remote(here, here, v_send, v_recv.at[e], right).wait_recv()

    def zx_spot(p, d, at_s):
        return xg.at[p * 4 + places[d], 0, at_s, pl.ds(first, XFIRST)]

    def zx_out(d, device, j):
        return remote(
            zx_spot(k, d, home),
            zx_spot(k, d, h),
            zx_send.at[0],
            zx_recv.at[j + (j * d == 2)],
            device,
        )

    def zx_on(d):
        here = zx_spot(k, d, 1 - h)
        return remote(here, here, zx_send.at[1], zx_recv.at[1 + (d == 2)], flip)

    def zx_wait(e, count):
        here = xg.at[pl.ds(0, count), 0, 0, pl.ds(first, XFIRST)]
        remote(here, here, zx_send.at[0], zx_recv.at[e], flip).wait_recv()

    def px_out(d, j):
        here = zx_spot(k, d, slot[j])
        return remote(here, here, p_send, p_recv.at[d, 0], mate)

    def v_start():
        for q in range(2):
            for way in (0, 1) if q == 0 else (1, 0):
                v_out(way, q).start()

    def v_near():
        for q in range(2):
            v_wait(q, v_spot(xs[q], q))
            v_on(q).start()
        v_wait(2, zx_spot(k, 0, home))

    def v_far():
        v_wait(3, zx_spot(k, 2, home))

    def zx_start(ds):
        for d in ds:

            @pl.when(outer)
            def _(d=d):
                zx_out(d, flip, 0).start()
                px_out(d, 0).start()

            @pl.when(inner)
            def _(d=d):
                zx_out(d, across, 1).start()

    def zx_pass(e, ds):
        @pl.when(inner)
        def _():
            zx_wait(e, len(ds))
            for d in ds:
                zx_on(d).start()

    def zx_take():
        @pl.when(inner)
        def _():
            zx_wait(0, 4)
            for d in range(4):
                px_out(d, 0).start()

        @pl.when(outer)
        def _():
            zx_wait(1, 3)
            zx_wait(2, 1)

        for d in range(4):
            px_out(d, 1).start()

    def z_start(m):
        @pl.when(outer)
        def _():
            for q in range(2):
                z_out(m, q, flip, 0).start()

        @pl.when(inner)
        def _():
            for q in range(2):
                z_out(m, q, across, 1).start()

    v_start()
    z_start(0)

    @pl.when(outer)
    def _():
        for q in range(2):
            spread(x_own(0, q), 0, 0, q)

    zx_start((3,))
    w_start(0)
    w_start(1)

    v_near()
    zx_start((0, 1))
    z_forward(0, 0)
    z_near_inner(0, 0)
    z_far(0, 0)
    v_far()
    zx_start((2,))
    z_start(1)
    z_forward(0, 1)
    z_near_inner(0, 1)
    z_far(0, 1)
    w_forward(0)
    for j in range(2):
        passed(0, j, 0, 0)
        passed(1, j, 0, 0)
    w_forward(1)
    w_start(2)
    for j in range(2):
        passed(1, j, 0, 1)
        passed(0, j, 0, 1)
    z_forward(1, 0)
    zx_pass(1, (3, 0, 1))
    z_forward(1, 1)
    zx_pass(2, (2,))
    w_rest(0)
    w_rest(1)

    @pl.loop(1, 8)
    def _(j):
        for w in range(2):
            t_out(w, j).start()

    z_near(1, 0)
    z_near(1, 1)
    z_far(1, 0)
    z_far(1, 1)
    w_forward(2)
    zx_take()
    tall = 2 * rows

    def block(m, o):
        return jnp.concatenate(
            [xg[p * 4 + o, m, :2].reshape(tall, shard) for p in range(2)], axis=1
        )

    def pair_in(d, m):
        here = xg.at[(1 - k) * 4 + places[d], m, pl.ds(0, 2)]
        remote(here, here, p_send, p_recv.at[d, m], mate).wait_recv()

    def gate_up(d):
        o = places[d]
        weights = jnp.concatenate([wf[o, 0], wf[o, 1]], axis=1)
        term = jnp.dot(block(0, o), weights, preferred_element_type=F32)
        sa[...] = term if d == 3 else sa[...] + term

    for d in (3, 0, 1):
        pair_in(d, 0)
        gate_up(d)
    x_rest(0)
    pair_in(2, 0)
    gate_up(2)
    turn = (1 - l, l)

    def swap(src, dst, send, recvs):
        def copy(c):
            at_c = pl.ds(turn[c] * rows, rows)
            return remote(src.at[at_c], dst.at[at_c], send, recvs[c], opposite)

        return copy

    a_swap = swap(sa, zla, a_send, (a_recv, a_recv))
    b_swap = swap(sb, zlb, b_send, (b_recv.at[0], b_recv.at[1]))
    a_all = remote(sa, zla, a_send, a_recv, opposite)
    b_all = remote(sb, zlb, b_send, b_recv.at[0], opposite)

    a_swap(0).start()
    for w in range(2):
        mine_w = pl.ds(bases[w] + y * fourths[w], fourths[w])
        tw[me, w, mine_w] = wf[x, w, pl.ds(k * shard + bases[w] + y * fourths[w], fourths[w])]
    tw[me, 1, :DIRECT] = wf[x, 1, pl.ds(k * shard, DIRECT)]
    a_swap(1).start()
    t_all().wait_recv()

    for w in range(2):
        for way, q in ((0, 0), (1, 1), (0, 1), (1, 0)):
            u_out(way, w, q).start()
    for j in range(2):
        passed(0, j, 1, 0)
        passed(1, j, 1, 0)
    for j in range(2):
        passed(1, j, 1, 1)
        passed(0, j, 1, 1)

    def grad_in(d):
        o = places[d]
        term = lax.dot_general(
            block(1, o), df[o], (COLS, ((), ())), preferred_element_type=F32
        )
        sb[...] = term if d == 3 else sb[...] + term

    w_rest(2)
    for d in (3, 0, 1):
        pair_in(d, 1)
        grad_in(d)
    def down_half(o, p):
        return lax.dot_general(
            hidden[...],
            xg[p * 4 + o, 1, :2].reshape(tall, shard),
            (ROWS, ((), ())),
            preferred_element_type=F32,
        )

    def gate_part(o):
        return lax.dot_general(
            block(0, o), dg[me], (ROWS, ((), ())), preferred_element_type=F32
        )

    twos, mids, parts, ones, lands = (
        (dtwo, gtwo),
        (dmid, gmid),
        (dpart, gpart),
        (done, gone),
        (dland, gland),
    )

    def halves(i, q):
        return q if i == 0 else pl.ds(q * shard, shard)

    def beside(way):
        return lax.rem(y + 1 + 2 * way, 4)

    def two_out(i, q):
        return remote(
            twos[i].at[halves(i, q)],
            mids[i].at[q],
            two_send.at[i],
            two_recv.at[i],
            at(x, beside(q), h, l, k),
        )

    def one_out(i, way, q):
        return remote(
            ones[i].at[way, halves(i, q)],
            lands[i].at[way, halves(i, q)],
            one_send.at[i],
            one_recv.at[i],
            at(x, beside(way), h, l, k),
        )

    def gate_half(o, p):
        return lax.dot_general(
            xg[p * 4 + o, 0, :2].reshape(tall, shard),
            dg[me],
            (ROWS, ((), ())),
            preferred_element_type=F32,
        )

    def gate_rows(o, p, e):
        return lax.dot_general(
            xg[p * 4 + o, 0, turn[e]],
            dg[me, pl.ds(turn[e] * rows, rows)],
            (ROWS, ((), ())),
            preferred_element_type=F32,
        )

    def one_merge(i):
        remote(mids[i], mids[i], two_send.at[i], two_recv.at[i], north).wait_recv()
        for way in range(2):
            ones[i][way, halves(i, way)] = (
                parts[i][way] + mids[i][way].astype(F32)
            ).astype(BF16)

    def finals(i):
        remote(ones[i], lands[i], one_send.at[i], one_recv.at[i], north).wait_recv()
        return lands[i][0].astype(F32) + lands[i][1].astype(F32)

    def grad_last(c):
        at_s = pl.ds(turn[c] * rows, rows)
        last = jnp.concatenate([xg[p * 4 + xs[2], 1, turn[c]] for p in range(2)], axis=1)
        sb[at_s] += lax.dot_general(
            last, df[xs[2]], (COLS, ((), ())), preferred_element_type=F32
        )

    for q in range(2):
        u_wait(q, tw.at[pl.ds(q * 4, 4), 0, pl.ds(0, fourths[0] + fourths[1])])
        for w in range(2):
            u_on(w, q).start()
    x_rest(1)
    @pl.loop(1, 8)
    def _(j):
        g_out(j).start()

    a_all.wait_recv()
    sums = sa[...] + zla[...]
    gate, up = sums[:, :width], sums[:, width:]
    squashed = jax.nn.sigmoid(gate)
    activated = gate * squashed
    slope = squashed * (1.0 + gate * (1.0 - squashed))
    acts[:, :width] = up * slope
    acts[:, width:] = activated
    hidden[...] = (activated * up).astype(BF16)

    dtwo[k] = down_half(ys[2], k).astype(BF16)
    done[1 - k, k] = down_half(beside(1 - k), k).astype(BF16)
    two_out(0, k).start()
    pair_in(2, 1)
    grad_last(0)
    grad_last(1)
    b_swap(0).start()
    dtwo[1 - k] = down_half(ys[2], 1 - k).astype(BF16)
    b_swap(1).start()
    done[k, 1 - k] = down_half(beside(k), 1 - k).astype(BF16)
    two_out(0, 1 - k).start()
    one_out(0, 1 - k, k).start()
    dpart[k] = down_half(beside(k), k)
    one_out(0, k, 1 - k).start()
    dpart[1 - k] = down_half(beside(1 - k), 1 - k)
    one_merge(0)
    def d_spot(c, o, e, q):
        return dg.at[o * 2 + c, pl.ds(turn[e] * rows + q * part, part)]

    def dx_out(way, e, q):
        here = d_spot(k, x, e, q)
        return remote(
            here, here, dx_send, dx_recv.at[way, e, q], (right, left)[way]
        )

    def dx_on(e, q):
        here = d_spot(k, xs[q], e, q)
        return remote(here, here, dx_send, dx_recv.at[2, e, 0], (right, left)[q])

    def dx_in(d, e, q):
        here = d_spot(k, xs[d], e, q)
        return remote(here, here, dx_send, dx_recv.at[d, e, q], right)

    def dp_out(d, e, q):
        here = d_spot(k, places[d], e, q)
        return remote(here, here, dp_send, dp_recv.at[d, e], mate)

    def d_half(c, d, e):
        return dg.at[places[d] * 2 + c, pl.ds(turn[e] * rows, rows)]

    def d_far(e):
        here = d_half(k, 2, e)
        remote(here, here, dx_send, dx_recv.at[2, e, 0], right).wait_recv()
        for q in range(2):
            dp_out(2, e, q).start()

    def d_start(e):
        for q in range(2):
            for way in (0, 1) if q == 0 else (1, 0):
                dx_out(way, e, q).start()
            dp_out(3, e, q).start()

    def d_passed(d, e, q):
        dx_in(d, e, q).wait_recv()
        if d == q:
            dx_on(e, q).start()
        dp_out(d, e, q).start()

    def d_near(e):
        for q in range(2):
            d_passed(q, e, q)
        for q in range(2):
            d_passed(1 - q, e, q)

    def gather(d, e):
        base = places[d] * 2
        at_s = pl.ds(turn[e] * rows, rows)
        left_side = jnp.concatenate([dg[base, at_s], dg[base + 1, at_s]], axis=1)
        right_side = jnp.concatenate(
            [tw[base, 0], tw[base, 1], tw[base + 1, 0], tw[base + 1, 1]], axis=1
        )
        term = lax.dot_general(
            left_side, right_side, (COLS, ((), ())), preferred_element_type=F32
        )
        total[e] = term if d == 3 else total[e] + term

    def gathers(e, ds):
        for d in ds:
            here = d_half(1 - k, d, e)
            remote(here, here, dp_send, dp_recv.at[d, e], mate).wait_recv()
            gather(d, e)

    piece = rows // PIECES

    def f_out(c):
        at_c = pl.ds(c * piece, piece)
        return (
            remote(total.at[0, at_c, pl.ds(0, wide)], near.at[at_c], f_send, f_recv.at[c], flip),
            remote(slim.at[at_c], slim_near.at[at_c], f_send, f_recv.at[c], flip),
        )

    def f_start(cs):
        for c in cs:
            for copy in f_out(c):
                copy.start()

    def f_wait(c):
        here = near.at[pl.ds(0, 3 * piece // 2)]
        remote(here, here, f_send, f_recv.at[c], flip).wait_recv()

    def r_out(c):
        at_c = pl.ds(c * piece, piece)
        return remote(rounded.at[at_c], result.at[at_c], r_send, r_recv, across)

    def delta(e):
        b_swap(e).wait_recv()
        at_s = pl.ds(turn[e] * rows, rows)
        hidden_grad = sb[at_s] + zlb[at_s]
        dg[me, at_s, :width] = (hidden_grad * acts[at_s, :width]).astype(BF16)
        dg[me, at_s, width:] = (hidden_grad * acts[at_s, width:]).astype(BF16)

    delta(0)
    for way in range(2):
        one_out(0, way, way).start()
    down_own[:, :shard] = down_half(y, 0)
    d_start(0)
    down_own[:, shard:] = down_half(y, 1)
    gown[...] = jnp.concatenate([gate_rows(ys[2], p, 0) for p in range(2)], axis=0)
    delta(1)
    for p in range(2):
        gtwo[halves(1, p)] = (gown[halves(1, p)] + gate_rows(ys[2], p, 1)).astype(BF16)
    two_out(1, 0).start()
    gone[0, halves(1, 1)] = gate_half(beside(0), 1).astype(BF16)
    two_out(1, 1).start()
    gone[1, halves(1, 0)] = gate_half(beside(1), 0).astype(BF16)
    one_out(1, 0, 1).start()
    gpart[0] = gate_half(beside(0), 0)
    one_out(1, 1, 0).start()
    gpart[1] = gate_half(beside(1), 1)
    d_near(0)
    d_start(1)
    gown[...] = gate_part(y)
    u_wait(2, tw.at[:, :, pl.ds(0, fourths[0] + fourths[1])])
    g_all().wait_recv()

    gathers(0, (3, 0, 1))
    d_far(0)
    gathers(0, (2,))
    slim[...] = total[0, :, wide:].astype(BF16)
    f_start(range(PIECES // 2))
    d_near(1)
    f_start(range(PIECES // 2, PIECES))
    one_merge(1)
    gathers(1, (3,))
    for way in range(2):
        one_out(1, way, way).start()
    gathers(1, (0, 1))
    d_far(1)
    gathers(1, (2,))
    keeps = [
        pltpu.make_async_copy(src, dst, keep.at[i])
        for i, (src, dst) in enumerate(
            ((down_own, down_out), (gate_own, gate_out), (up_own, up_out), (rounded, result))
        )
    ]
    for c in range(PIECES):
        f_wait(c)
        at_c = pl.ds(c * piece, piece)
        rounded[at_c, :wide] = (total[1, at_c, :wide] + near[at_c]).astype(BF16)
        rounded[at_c, wide:] = (total[1, at_c, wide:] + slim_near[at_c].astype(F32)).astype(BF16)

        if c:

            @pl.when(inner)
            def _(c=c):
                r_out(c - 1).start()

    both = finals(0)
    for p in range(2):
        at_p = slice(p * shard, (p + 1) * shard)
        down_own[:, at_p] = factor * (down_own[:, at_p] + both[p])
    @pl.when(inner)
    def _():
        r_out(PIECES - 1).start()

    @pl.when(outer)
    def _():
        keeps[3].start()

    keeps[0].start()
    last = finals(1)
    gate_own[...] = factor * (gown[:, :width] + last[:, :width])
    up_own[...] = factor * (gown[:, width:] + last[:, width:])
    for copy in keeps[1:3]:
        copy.start()

    sent = [
        (xg.at[0, :, 0, pl.ds(0, 240)], z_send.at[0]),
        (xg.at[pl.ds(0, 4), 0, 0, pl.ds(0, XFIRST)], zx_send.at[0]),
        (xg.at[pl.ds(0, 3), 0, 0, pl.ds(0, XFIRST)], v_send),
        (xg.at[pl.ds(0, 4), 0, :, pl.ds(0, 240)], x_send),
        (xg.at[:, :, 0], p_send),
        (xg.at[pl.ds(0, 3), 0], y_send),
        (tw.at[:, :, pl.ds(0, 3 * (fourths[0] + fourths[1]) // 2)], u_send),
        (dg.at[pl.ds(0, 3)], dx_send),
        (dg.at[pl.ds(0, 4)], dp_send),
        (total.at[0, pl.ds(0, 3 * rows // 4)], f_send),
        (dtwo, two_send.at[0]),
        (gtwo, two_send.at[1]),
        (done, one_send.at[0]),
        (gone, one_send.at[1]),
    ]
    for here, sem in sent:
        remote(here, here, sem, load, mate).wait_send()
    for copy in (a_all, b_all, t_all(), g_all()):
        copy.wait_send()

    @pl.when(inner)
    def _():
        for here, sem in (
            (xg.at[0, :, 0, pl.ds(0, 240)], z_send.at[1]),
            (xg.at[pl.ds(0, 4), 0, 0, pl.ds(0, XFIRST)], zx_send.at[1]),
        ):
            remote(here, here, sem, load, mate).wait_send()
        remote(rounded, result, r_send, r_recv, across).wait()

    @pl.when(outer)
    def _():
        keeps[3].wait()

    for copy in keeps[:3]:
        copy.wait()


def store_kernel(*refs):
    found, kept, held, sem = refs[:4], refs[4:8], refs[8:12], refs[12]
    loads = [pltpu.make_async_copy(found[i], held[i], sem.at[0, i]) for i in range(4)]
    stores = [pltpu.make_async_copy(held[i], kept[i], sem.at[1, i]) for i in range(4)]
    for copy in loads:
        copy.start()
    for i in range(4):
        loads[i].wait()
        stores[i].start()
    for copy in stores:
        copy.wait()


HBM = pl.BlockSpec(memory_space=pltpu.HBM)
DMA = pltpu.SemaphoreType.DMA


def body(tokens, out_grad, gate_weight, up_weight, down_weight):
    nf, nt = lax.axis_size("fsdp"), lax.axis_size("tp")
    rows, shard = tokens.shape
    deep, width = gate_weight.shape
    assert nf == 8 and nt == 16 and deep == 2 * shard
    factor = 1.0 / math.sqrt(rows * nf)
    tall = 2 * rows
    wide = 2 * width

    shapes = (
        jax.ShapeDtypeStruct((rows, shard), BF16),
        jax.ShapeDtypeStruct((deep, width), F32),
        jax.ShapeDtypeStruct((deep, width), F32),
        jax.ShapeDtypeStruct((width, deep), F32),
    )
    found = tuple(
        pl.pallas_call(
            functools.partial(kernel, factor),
            out_shape=shapes,
            in_specs=[HBM] * 5,
            out_specs=(HBM,) * 4,
            scratch_shapes=[
                pltpu.VMEM((deep, width), F32),
                pltpu.VMEM((deep, width), F32),
                pltpu.VMEM((width, deep), F32),
                pltpu.VMEM((8, 2, 3, rows, shard), BF16),
                pltpu.VMEM((4, 2, deep, width), BF16),
                pltpu.VMEM((4, width, deep), BF16),
                pltpu.VMEM((tall, wide), F32),
                pltpu.VMEM((tall, wide), F32),
                pltpu.VMEM((tall, width), F32),
                pltpu.VMEM((tall, width), F32),
                pltpu.VMEM((tall, wide), F32),
                pltpu.VMEM((tall, width), BF16),
                pltpu.VMEM((8, tall, wide), BF16),
                pltpu.VMEM((8, 2, shard, width), BF16),
                pltpu.VMEM((2, width, shard), F32),
                pltpu.VMEM((2, deep // 2, wide), F32),
                pltpu.VMEM((2, width, shard), BF16),
                pltpu.VMEM((deep, wide), BF16),
                pltpu.VMEM((2, 2, width, shard), BF16),
                pltpu.VMEM((2, deep, wide), BF16),
                pltpu.VMEM((2, width, shard), BF16),
                pltpu.VMEM((2, deep // 2, wide), BF16),
                pltpu.VMEM((2, 2, width, shard), BF16),
                pltpu.VMEM((2, deep, wide), BF16),
                pltpu.VMEM((deep, wide), F32),
                pltpu.VMEM((2, rows, shard), F32),
                pltpu.VMEM((rows, wide), F32),
                pltpu.VMEM((rows, wide), BF16),
                pltpu.VMEM((rows, wide), BF16),
                pltpu.VMEM((rows, shard), BF16),
                DMA(()),
                DMA((4,)),
                DMA((2,)),
                DMA((2, 2, 2)),
                DMA(()),
                DMA((2, 2, 5)),
                DMA(()),
                DMA((4, 2)),
                DMA(()),
                DMA((4,)),
                DMA((2,)),
                DMA((3,)),
                DMA(()),
                DMA((3, 3)),
                DMA(()),
                DMA(()),
                DMA(()),
                DMA((2,)),
                DMA(()),
                DMA(()),
                DMA(()),
                DMA((3,)),
                DMA(()),
                DMA(()),
                DMA(()),
                DMA((PIECES,)),
                DMA(()),
                DMA((3, 2, 2)),
                DMA(()),
                DMA((4, 2)),
                DMA((2,)),
                DMA((2,)),
                DMA((2,)),
                DMA((2,)),
                DMA(()),
                DMA(()),
            ],
            compiler_params=pltpu.CompilerParams(
                collective_id=0, has_side_effects=True, vmem_limit_bytes=VMEM_LIMIT
            ),
            name="block",
        )(tokens, out_grad, gate_weight, up_weight, down_weight)
    )
    return tuple(
        pl.pallas_call(
            store_kernel,
            out_shape=shapes,
            in_specs=[HBM] * 4,
            out_specs=(HBM,) * 4,
            scratch_shapes=[pltpu.VMEM(s.shape, s.dtype) for s in shapes] + [DMA((2, 4))],
            compiler_params=pltpu.CompilerParams(vmem_limit_bytes=VMEM_LIMIT),
            name="store",
        )(*found)
    )


def solution(mesh):
    return jax.shard_map(
        body,
        mesh=mesh,
        in_specs=(
            P("fsdp", "tp"),
            P("fsdp", "tp"),
            P("fsdp", "tp"),
            P("fsdp", "tp"),
            P("tp", "fsdp"),
        ),
        out_specs=(P("fsdp", "tp"), P("fsdp", "tp"), P("fsdp", "tp"), P("tp", "fsdp")),
        check_vma=False,
    )
```

```python
import functools
import math

import jax
import jax.numpy as jnp
from jax import lax
from jax.sharding import PartitionSpec as P
from jax.experimental import pallas as pl
from jax.experimental.pallas import tpu as pltpu

MESH = pl.DeviceIdType.MESH
F32 = jnp.float32
BF16 = jnp.bfloat16
VMEM_LIMIT = 60 * 1024 * 1024
XFIRST = 32
PIECES = 8
DIRECT = 384
ROWS = ((0,), (0,))
COLS = ((1,), (1,))


def kernel(
    factor,
    tokens,
    grads,
    gate_weight,
    up_weight,
    down_weight,
    result,
    gate_out,
    up_out,
    down_out,
    gate_own,
    up_own,
    down_own,
    xg,
    wf,
    df,
    sa,
    zla,
    sb,
    zlb,
    acts,
    hidden,
    dg,
    tw,
    dpart,
    gpart,
    dtwo,
    gtwo,
    done,
    gone,
    dmid,
    gmid,
    dland,
    gland,
    gown,
    total,
    near,
    slim,
    slim_near,
    rounded,
    load,
    keep,
    z_send,
    z_recv,
    x_send,
    x_recv,
    p_send,
    p_recv,
    v_send,
    v_recv,
    zx_send,
    zx_recv,
    y_send,
    y_recv,
    a_send,
    a_recv,
    b_send,
    b_recv,
    t_send,
    t_recv,
    u_send,
    u_recv,
    g_send,
    g_recv,
    f_send,
    f_recv,
    dx_send,
    dx_recv,
    dp_send,
    dp_recv,
    two_send,
    two_recv,
    one_send,
    one_recv,
    r_send,
    r_recv,
):
    f, t = lax.axis_index("fsdp"), lax.axis_index("tp")
    h, y = lax.div(f, 4), lax.rem(f, 4)
    l, x, k = lax.div(t, 8), lax.rem(lax.div(t, 2), 4), lax.rem(t, 2)
    outer = h == l
    inner = h != l
    rows, shard = tokens.shape
    deep, width = gate_weight.shape
    part = rows // 2
    zparts = ((rows - XFIRST) // 2, part)
    first = rows - XFIRST
    xpart = XFIRST // 2
    odd = (h - l) * (h - l)
    home = h * (1 - odd) + 2 * odd
    wide = 2 * width

    def at(xx, yy, hh, ll, kk):
        return (hh * 4 + yy, ll * 8 + xx * 2 + kk)

    xs = (lax.rem(x + 3, 4), lax.rem(x + 1, 4), lax.rem(x + 2, 4))
    ys = (lax.rem(y + 3, 4), lax.rem(y + 1, 4), lax.rem(y + 2, 4))
    right, left = at(xs[1], y, h, l, k), at(xs[0], y, h, l, k)
    north, south = at(x, ys[1], h, l, k), at(x, ys[0], h, l, k)
    mate = at(x, y, h, l, 1 - k)
    flip = at(x, y, h, 1 - l, k)
    across = at(x, y, 1 - h, 1 - l, k)
    opposite = at(x, y, 1 - h, l, k)
    me = 2 * x + k

    def remote(src, dst, send, recv, device):
        return pltpu.make_async_remote_copy(
            src_ref=src,
            dst_ref=dst,
            send_sem=send,
            recv_sem=recv,
            device_id=device,
            device_id_type=MESH,
        )

    copies = [
        pltpu.make_async_copy(ref, spot, load)
        for ref, spot in (
            (tokens, xg.at[k * 4 + x, 0, home]),
            (gate_weight, wf.at[y, 0]),
            (up_weight, wf.at[y, 1]),
            (grads, xg.at[k * 4 + x, 1, home]),
            (down_weight, df.at[y]),
        )
    ]
    for copy in copies:
        copy.start()

    barrier = pltpu.get_barrier_semaphore()
    for j in range(1, 16):
        pl.semaphore_signal(
            barrier, inc=1, device_id=(f, lax.rem(t + j, 16)), device_id_type=MESH
        )
    for peer in (north, south, opposite, across):
        pl.semaphore_signal(barrier, inc=1, device_id=peer, device_id_type=MESH)
    pl.semaphore_wait(barrier, 19)

    all_in = xg.at[pl.ds(0, 5), 0, 0]
    pltpu.make_async_copy(all_in, all_in, load).wait()

    def w_spot(o, w, q):
        if w == 2:
            return df.at[o, pl.ds(q * (width // 2), width // 2)]
        return wf.at[o, w, pl.ds(q * (deep // 2), deep // 2)]

    def w_out(way, w, q):
        return remote(
            w_spot(y, w, q),
            w_spot(y, w, q),
            y_send,
            y_recv.at[w, q if way == q else 2],
            (north, south)[way],
        )

    def w_on(w, q):
        here = w_spot(ys[q], w, q)
        return remote(here, here, y_send, y_recv.at[w, 2], (north, south)[q])

    def w_wait(w, e, here):
        remote(here, here, y_send, y_recv.at[w, e], north).wait_recv()

    def w_start(w):
        for way, q in ((0, 0), (1, 1), (0, 1), (1, 0)):
            w_out(way, w, q).start()

    def w_forward(w):
        for q in range(2):
            w_wait(w, q, w_spot(ys[q], w, q))
            w_on(w, q).start()

    def w_rest(w):
        w_wait(w, 2, df.at[pl.ds(0, 2)] if w == 2 else wf.at[pl.ds(0, 2), w])

    slot = (h, 1 - h)

    def x_own(m, q):
        return xg.at[k * 4 + x, m, home, pl.ds(q * zparts[m], zparts[m])]

    def x_spot(p, o, j, m, q):
        return xg.at[p * 4 + o, m, slot[j], pl.ds(q * zparts[m], zparts[m])]

    def z_out(m, q, device, j):
        spot = xg.at[k * 4 + x, m, h, pl.ds(q * zparts[m], zparts[m])]
        return remote(x_own(m, q), spot, z_send.at[0], z_recv.at[j, m, q], device)

    def z_on(m, q):
        here = x_spot(k, x, 1, m, q)
        return remote(here, here, z_send.at[1], z_recv.at[1, m, q], flip)

    def z_in(j, m, q):
        here = x_spot(k, x, j, m, q)
        return remote(here, here, z_send.at[0], z_recv.at[j, m, q], flip)

    def x_out(way, src, j, m, q):
        return remote(
            src,
            x_spot(k, x, j, m, q),
            x_send,
            x_recv.at[m, q, 2 * way + j],
            (right, left)[way],
        )

    def x_on(j, m, q):
        here = x_spot(k, xs[q], j, m, q)
        return remote(
            here, here, x_send, x_recv.at[m, q, 4], (right, left)[q]
        )

    def x_wait(m, q, e, here):
        remote(here, here, x_send, x_recv.at[m, q, e], right).wait_recv()

    places = (*xs, x)

    def p_out(d, src, j, m, q):
        return remote(
            src,
            x_spot(k, places[d], j, m, q),
            p_send,
            p_recv.at[d, m],
            mate,
        )

    def spread(src, j, m, q):
        for way in (0, 1) if q == 0 else (1, 0):
            x_out(way, src, j, m, q).start()
        p_out(3, src, j, m, q).start()

    def passed(d, j, m, q):
        x_wait(m, q, 2 * d + j, x_spot(k, xs[d], j, m, q))
        if d == q:
            x_on(j, m, q).start()
        p_out(d, x_spot(k, places[d], j, m, q), j, m, q).start()

    def x_rest(m):
        for q in range(2):
            here = xg.at[k * 4 + xs[2], m, pl.ds(0, 2), pl.ds(q * zparts[m], zparts[m])]
            x_wait(m, q, 4, here)
            for j in range(2):
                p_out(2, x_spot(k, xs[2], j, m, q), j, m, q).start()

    def z_forward(m, q):
        @pl.when(inner)
        def _():
            z_in(1, m, q).wait_recv()
            z_on(m, q).start()

    def z_near(m, q):
        @pl.when(inner)
        def _():
            z_in(0, m, q).wait_recv()

        spread(x_spot(k, x, 0, m, q), 0, m, q)

    def z_far(m, q):
        @pl.when(outer)
        def _():
            z_in(1, m, q).wait_recv()

        spread(x_spot(k, x, 1, m, q), 1, m, q)

    def z_near_inner(m, q):
        @pl.when(inner)
        def _():
            z_in(0, m, q).wait_recv()
            spread(x_spot(k, x, 0, m, q), 0, m, q)

    fourths = (shard // 4, (shard - DIRECT) // 4)
    bases = (0, DIRECT)

    def t_copy(u, w):
        return remote(
            wf.at[
                lax.div(u, 2),
                w,
                pl.ds(lax.rem(u, 2) * shard + bases[w] + y * fourths[w], fourths[w]),
            ],
            tw.at[me, w, pl.ds(bases[w] + y * fourths[w], fourths[w])],
            t_send,
            t_recv,
            (f, l * 8 + u),
        )

    def t_out(w, j):
        return t_copy(lax.rem(me + j, 8), w)

    def t_all():
        here = tw.at[pl.ds(0, 7), 0, pl.ds(0, fourths[0] + fourths[1])]
        return remote(here, here, t_send, t_recv, mate)

    def g_out(j):
        u = lax.rem(me + j, 8)
        return remote(
            wf.at[lax.div(u, 2), 1, pl.ds(lax.rem(u, 2) * shard, DIRECT)],
            tw.at[me, 1, pl.ds(0, DIRECT)],
            g_send,
            g_recv,
            (f, l * 8 + u),
        )

    def g_all():
        here = tw.at[pl.ds(0, 7), 1, pl.ds(0, DIRECT)]
        return remote(here, here, g_send, g_recv, mate)

    def u_spot(o, w, q):
        return tw.at[pl.ds(q * 4, 4), w, pl.ds(bases[w] + o * fourths[w], fourths[w])]

    def u_out(way, w, q):
        here = u_spot(y, w, q)
        return remote(
            here, here, u_send, u_recv.at[q if way == q else 2], (north, south)[way]
        )

    def u_on(w, q):
        here = u_spot(ys[q], w, q)
        return remote(here, here, u_send, u_recv.at[2], (north, south)[q])

    def u_wait(e, here):
        remote(here, here, u_send, u_recv.at[e], north).wait_recv()

    def v_spot(o, q):
        return xg.at[k * 4 + o, 0, home, pl.ds(first + q * xpart, xpart)]

    def v_out(way, q):
        here = v_spot(x, q)
        return remote(
            here, here, v_send, v_recv.at[q if way == q else 2], (right, left)[way]
        )

    def v_on(q):
        here = v_spot(xs[q], q)
        return remote(here, here, v_send, v_recv.at[3], (right, left)[q])

    def v_wait(e, here):
        remote(here, here, v_send, v_recv.at[e], right).wait_recv()

    def zx_spot(p, d, at_s):
        return xg.at[p * 4 + places[d], 0, at_s, pl.ds(first, XFIRST)]

    def zx_out(d, device, j):
        return remote(
            zx_spot(k, d, home),
            zx_spot(k, d, h),
            zx_send.at[0],
            zx_recv.at[j + (j * d == 2)],
            device,
        )

    def zx_on(d):
        here = zx_spot(k, d, 1 - h)
        return remote(here, here, zx_send.at[1], zx_recv.at[1 + (d == 2)], flip)

    def zx_wait(e, count):
        here = xg.at[pl.ds(0, count), 0, 0, pl.ds(first, XFIRST)]
        remote(here, here, zx_send.at[0], zx_recv.at[e], flip).wait_recv()

    def px_out(d, j):
        here = zx_spot(k, d, slot[j])
        return remote(here, here, p_send, p_recv.at[d, 0], mate)

    def v_start():
        for q in range(2):
            for way in (0, 1) if q == 0 else (1, 0):
                v_out(way, q).start()

    def v_near():
        for q in range(2):
            v_wait(q, v_spot(xs[q], q))
            v_on(q).start()
        v_wait(2, zx_spot(k, 0, home))

    def v_far():
        v_wait(3, zx_spot(k, 2, home))

    def zx_start(ds):
        for d in ds:

            @pl.when(outer)
            def _(d=d):
                zx_out(d, flip, 0).start()
                px_out(d, 0).start()

            @pl.when(inner)
            def _(d=d):
                zx_out(d, across, 1).start()

    def zx_pass(e, ds):
        @pl.when(inner)
        def _():
            zx_wait(e, len(ds))
            for d in ds:
                zx_on(d).start()

    def zx_take():
        @pl.when(inner)
        def _():
            zx_wait(0, 4)
            for d in range(4):
                px_out(d, 0).start()

        @pl.when(outer)
        def _():
            zx_wait(1, 3)
            zx_wait(2, 1)

        for d in range(4):
            px_out(d, 1).start()

    def z_start(m):
        @pl.when(outer)
        def _():
            for q in range(2):
                z_out(m, q, flip, 0).start()

        @pl.when(inner)
        def _():
            for q in range(2):
                z_out(m, q, across, 1).start()

    v_start()
    z_start(0)

    @pl.when(outer)
    def _():
        for q in range(2):
            spread(x_own(0, q), 0, 0, q)

    zx_start((3,))
    w_start(0)
    w_start(1)

    v_near()
    zx_start((0, 1))
    z_forward(0, 0)
    z_near_inner(0, 0)
    z_far(0, 0)
    v_far()
    zx_start((2,))
    z_start(1)
    z_forward(0, 1)
    z_near_inner(0, 1)
    z_far(0, 1)
    w_forward(0)
    for j in range(2):
        passed(0, j, 0, 0)
        passed(1, j, 0, 0)
    w_forward(1)
    w_start(2)
    for j in range(2):
        passed(1, j, 0, 1)
        passed(0, j, 0, 1)
    z_forward(1, 0)
    zx_pass(1, (3, 0, 1))
    z_forward(1, 1)
    zx_pass(2, (2,))
    w_rest(0)
    w_rest(1)

    @pl.loop(1, 8)
    def _(j):
        for w in range(2):
            t_out(w, j).start()

    z_near(1, 0)
    z_near(1, 1)
    z_far(1, 0)
    z_far(1, 1)
    w_forward(2)
    zx_take()
    tall = 2 * rows

    def block(m, o):
        return jnp.concatenate(
            [xg[p * 4 + o, m, :2].reshape(tall, shard) for p in range(2)], axis=1
        )

    def pair_in(d, m):
        here = xg.at[(1 - k) * 4 + places[d], m, pl.ds(0, 2)]
        remote(here, here, p_send, p_recv.at[d, m], mate).wait_recv()

    def gate_up(d):
        o = places[d]
        weights = jnp.concatenate([wf[o, 0], wf[o, 1]], axis=1)
        term = jnp.dot(block(0, o), weights, preferred_element_type=F32)
        sa[...] = term if d == 3 else sa[...] + term

    for d in (3, 0, 1):
        pair_in(d, 0)
        gate_up(d)
    x_rest(0)
    pair_in(2, 0)
    gate_up(2)
    turn = (1 - l, l)

    def swap(src, dst, send, recvs):
        def copy(c):
            at_c = pl.ds(turn[c] * rows, rows)
            return remote(src.at[at_c], dst.at[at_c], send, recvs[c], opposite)

        return copy

    a_swap = swap(sa, zla, a_send, (a_recv, a_recv))
    b_swap = swap(sb, zlb, b_send, (b_recv.at[0], b_recv.at[1]))
    a_all = remote(sa, zla, a_send, a_recv, opposite)
    b_all = remote(sb, zlb, b_send, b_recv.at[0], opposite)

    a_swap(0).start()
    for w in range(2):
        mine_w = pl.ds(bases[w] + y * fourths[w], fourths[w])
        tw[me, w, mine_w] = wf[x, w, pl.ds(k * shard + bases[w] + y * fourths[w], fourths[w])]
    tw[me, 1, :DIRECT] = wf[x, 1, pl.ds(k * shard, DIRECT)]
    a_swap(1).start()
    t_all().wait_recv()

    for w in range(2):
        for way, q in ((0, 0), (1, 1), (0, 1), (1, 0)):
            u_out(way, w, q).start()
    for j in range(2):
        passed(0, j, 1, 0)
        passed(1, j, 1, 0)
    for j in range(2):
        passed(1, j, 1, 1)
        passed(0, j, 1, 1)

    def grad_in(d):
        o = places[d]
        term = lax.dot_general(
            block(1, o), df[o], (COLS, ((), ())), preferred_element_type=F32
        )
        sb[...] = term if d == 3 else sb[...] + term

    w_rest(2)
    for d in (3, 0, 1):
        pair_in(d, 1)
        grad_in(d)
    def down_half(o, p):
        return lax.dot_general(
            hidden[...],
            xg[p * 4 + o, 1, :2].reshape(tall, shard),
            (ROWS, ((), ())),
            preferred_element_type=F32,
        )

    def gate_part(o):
        return lax.dot_general(
            block(0, o), dg[me], (ROWS, ((), ())), preferred_element_type=F32
        )

    twos, mids, parts, ones, lands = (
        (dtwo, gtwo),
        (dmid, gmid),
        (dpart, gpart),
        (done, gone),
        (dland, gland),
    )

    def halves(i, q):
        return q if i == 0 else pl.ds(q * shard, shard)

    def beside(way):
        return lax.rem(y + 1 + 2 * way, 4)

    def two_out(i, q):
        return remote(
            twos[i].at[halves(i, q)],
            mids[i].at[q],
            two_send.at[i],
            two_recv.at[i],
            at(x, beside(q), h, l, k),
        )

    def one_out(i, way, q):
        return remote(
            ones[i].at[way, halves(i, q)],
            lands[i].at[way, halves(i, q)],
            one_send.at[i],
            one_recv.at[i],
            at(x, beside(way), h, l, k),
        )

    def gate_half(o, p):
        return lax.dot_general(
            xg[p * 4 + o, 0, :2].reshape(tall, shard),
            dg[me],
            (ROWS, ((), ())),
            preferred_element_type=F32,
        )

    def gate_rows(o, p, e):
        return lax.dot_general(
            xg[p * 4 + o, 0, turn[e]],
            dg[me, pl.ds(turn[e] * rows, rows)],
            (ROWS, ((), ())),
            preferred_element_type=F32,
        )

    def one_merge(i):
        remote(mids[i], mids[i], two_send.at[i], two_recv.at[i], north).wait_recv()
        for way in range(2):
            ones[i][way, halves(i, way)] = (
                parts[i][way] + mids[i][way].astype(F32)
            ).astype(BF16)

    def finals(i):
        remote(ones[i], lands[i], one_send.at[i], one_recv.at[i], north).wait_recv()
        return lands[i][0].astype(F32) + lands[i][1].astype(F32)

    def grad_last(c):
        at_s = pl.ds(turn[c] * rows, rows)
        last = jnp.concatenate([xg[p * 4 + xs[2], 1, turn[c]] for p in range(2)], axis=1)
        sb[at_s] += lax.dot_general(
            last, df[xs[2]], (COLS, ((), ())), preferred_element_type=F32
        )

    for q in range(2):
        u_wait(q, tw.at[pl.ds(q * 4, 4), 0, pl.ds(0, fourths[0] + fourths[1])])
        for w in range(2):
            u_on(w, q).start()
    x_rest(1)
    @pl.loop(1, 8)
    def _(j):
        g_out(j).start()

    a_all.wait_recv()
    sums = sa[...] + zla[...]
    gate, up = sums[:, :width], sums[:, width:]
    squashed = jax.nn.sigmoid(gate)
    activated = gate * squashed
    slope = squashed * (1.0 + gate * (1.0 - squashed))
    acts[:, :width] = up * slope
    acts[:, width:] = activated
    hidden[...] = (activated * up).astype(BF16)

    dtwo[k] = down_half(ys[2], k).astype(BF16)
    done[1 - k, k] = down_half(beside(1 - k), k).astype(BF16)
    two_out(0, k).start()
    pair_in(2, 1)
    grad_last(0)
    dtwo[1 - k] = down_half(ys[2], 1 - k).astype(BF16)
    b_swap(0).start()
    grad_last(1)
    two_out(0, 1 - k).start()
    one_out(0, 1 - k, k).start()
    done[k, 1 - k] = down_half(beside(k), 1 - k).astype(BF16)
    b_swap(1).start()
    dpart[k] = down_half(beside(k), k)
    one_out(0, k, 1 - k).start()
    dpart[1 - k] = down_half(beside(1 - k), 1 - k)
    one_merge(0)
    def d_spot(c, o, e, q):
        return dg.at[o * 2 + c, pl.ds(turn[e] * rows + q * part, part)]

    def dx_out(way, e, q):
        here = d_spot(k, x, e, q)
        return remote(
            here, here, dx_send, dx_recv.at[way, e, q], (right, left)[way]
        )

    def dx_on(e, q):
        here = d_spot(k, xs[q], e, q)
        return remote(here, here, dx_send, dx_recv.at[2, e, 0], (right, left)[q])

    def dx_in(d, e, q):
        here = d_spot(k, xs[d], e, q)
        return remote(here, here, dx_send, dx_recv.at[d, e, q], right)

    def dp_out(d, e, q):
        here = d_spot(k, places[d], e, q)
        return remote(here, here, dp_send, dp_recv.at[d, e], mate)

    def d_half(c, d, e):
        return dg.at[places[d] * 2 + c, pl.ds(turn[e] * rows, rows)]

    def d_far(e):
        here = d_half(k, 2, e)
        remote(here, here, dx_send, dx_recv.at[2, e, 0], right).wait_recv()
        for q in range(2):
            dp_out(2, e, q).start()

    def d_start(e):
        for q in range(2):
            for way in (0, 1) if q == 0 else (1, 0):
                dx_out(way, e, q).start()
            dp_out(3, e, q).start()

    def d_passed(d, e, q):
        dx_in(d, e, q).wait_recv()
        if d == q:
            dx_on(e, q).start()
        dp_out(d, e, q).start()

    def d_near(e):
        for q in range(2):
            d_passed(q, e, q)
        for q in range(2):
            d_passed(1 - q, e, q)

    def gather(d, e):
        base = places[d] * 2
        at_s = pl.ds(turn[e] * rows, rows)
        left_side = jnp.concatenate([dg[base, at_s], dg[base + 1, at_s]], axis=1)
        right_side = jnp.concatenate(
            [tw[base, 0], tw[base, 1], tw[base + 1, 0], tw[base + 1, 1]], axis=1
        )
        term = lax.dot_general(
            left_side, right_side, (COLS, ((), ())), preferred_element_type=F32
        )
        total[e] = term if d == 3 else total[e] + term

    def gathers(e, ds):
        for d in ds:
            here = d_half(1 - k, d, e)
            remote(here, here, dp_send, dp_recv.at[d, e], mate).wait_recv()
            gather(d, e)

    piece = rows // PIECES

    def f_out(c):
        at_c = pl.ds(c * piece, piece)
        return (
            remote(total.at[0, at_c, pl.ds(0, wide)], near.at[at_c], f_send, f_recv.at[c], flip),
            remote(slim.at[at_c], slim_near.at[at_c], f_send, f_recv.at[c], flip),
        )

    def f_start(cs):
        for c in cs:
            for copy in f_out(c):
                copy.start()

    def f_wait(c):
        here = near.at[pl.ds(0, 3 * piece // 2)]
        remote(here, here, f_send, f_recv.at[c], flip).wait_recv()

    def r_out(c):
        at_c = pl.ds(c * piece, piece)
        return remote(rounded.at[at_c], result.at[at_c], r_send, r_recv, across)

    def delta(e):
        b_swap(e).wait_recv()
        at_s = pl.ds(turn[e] * rows, rows)
        hidden_grad = sb[at_s] + zlb[at_s]
        dg[me, at_s, :width] = (hidden_grad * acts[at_s, :width]).astype(BF16)
        dg[me, at_s, width:] = (hidden_grad * acts[at_s, width:]).astype(BF16)

    delta(0)
    for way in range(2):
        one_out(0, way, way).start()
    down_own[:, :shard] = down_half(y, 0)
    d_start(0)
    down_own[:, shard:] = down_half(y, 1)
    gown[...] = jnp.concatenate([gate_rows(ys[2], p, 0) for p in range(2)], axis=0)
    delta(1)
    for p in range(2):
        gtwo[halves(1, p)] = (gown[halves(1, p)] + gate_rows(ys[2], p, 1)).astype(BF16)
    two_out(1, 0).start()
    gone[0, halves(1, 1)] = gate_half(beside(0), 1).astype(BF16)
    two_out(1, 1).start()
    gone[1, halves(1, 0)] = gate_half(beside(1), 0).astype(BF16)
    one_out(1, 0, 1).start()
    gpart[0] = gate_half(beside(0), 0)
    one_out(1, 1, 0).start()
    gpart[1] = gate_half(beside(1), 1)
    d_near(0)
    d_start(1)
    gown[...] = gate_part(y)
    u_wait(2, tw.at[:, :, pl.ds(0, fourths[0] + fourths[1])])
    g_all().wait_recv()

    gathers(0, (3, 0, 1))
    d_far(0)
    gathers(0, (2,))
    slim[...] = total[0, :, wide:].astype(BF16)
    f_start(range(PIECES // 2))
    d_near(1)
    f_start(range(PIECES // 2, PIECES))
    one_merge(1)
    gathers(1, (3,))
    for way in range(2):
        one_out(1, way, way).start()
    gathers(1, (0, 1))
    d_far(1)
    gathers(1, (2,))
    keeps = [
        pltpu.make_async_copy(src, dst, keep.at[i])
        for i, (src, dst) in enumerate(
            ((down_own, down_out), (gate_own, gate_out), (up_own, up_out), (rounded, result))
        )
    ]
    for c in range(PIECES):
        f_wait(c)
        at_c = pl.ds(c * piece, piece)
        rounded[at_c, :wide] = (total[1, at_c, :wide] + near[at_c]).astype(BF16)
        rounded[at_c, wide:] = (total[1, at_c, wide:] + slim_near[at_c].astype(F32)).astype(BF16)

        if c:

            @pl.when(inner)
            def _(c=c):
                r_out(c - 1).start()

    both = finals(0)
    for p in range(2):
        at_p = slice(p * shard, (p + 1) * shard)
        down_own[:, at_p] = factor * (down_own[:, at_p] + both[p])
    @pl.when(inner)
    def _():
        r_out(PIECES - 1).start()

    @pl.when(outer)
    def _():
        keeps[3].start()

    keeps[0].start()
    last = finals(1)
    gate_own[...] = factor * (gown[:, :width] + last[:, :width])
    up_own[...] = factor * (gown[:, width:] + last[:, width:])
    for copy in keeps[1:3]:
        copy.start()

    sent = [
        (xg.at[0, :, 0, pl.ds(0, 240)], z_send.at[0]),
        (xg.at[pl.ds(0, 4), 0, 0, pl.ds(0, XFIRST)], zx_send.at[0]),
        (xg.at[pl.ds(0, 3), 0, 0, pl.ds(0, XFIRST)], v_send),
        (xg.at[pl.ds(0, 4), 0, :, pl.ds(0, 240)], x_send),
        (xg.at[:, :, 0], p_send),
        (xg.at[pl.ds(0, 3), 0], y_send),
        (tw.at[:, :, pl.ds(0, 3 * (fourths[0] + fourths[1]) // 2)], u_send),
        (dg.at[pl.ds(0, 3)], dx_send),
        (dg.at[pl.ds(0, 4)], dp_send),
        (total.at[0, pl.ds(0, 3 * rows // 4)], f_send),
        (dtwo, two_send.at[0]),
        (gtwo, two_send.at[1]),
        (done, one_send.at[0]),
        (gone, one_send.at[1]),
    ]
    for here, sem in sent:
        remote(here, here, sem, load, mate).wait_send()
    for copy in (a_all, b_all, t_all(), g_all()):
        copy.wait_send()

    @pl.when(inner)
    def _():
        for here, sem in (
            (xg.at[0, :, 0, pl.ds(0, 240)], z_send.at[1]),
            (xg.at[pl.ds(0, 4), 0, 0, pl.ds(0, XFIRST)], zx_send.at[1]),
        ):
            remote(here, here, sem, load, mate).wait_send()
        remote(rounded, result, r_send, r_recv, across).wait()

    @pl.when(outer)
    def _():
        keeps[3].wait()

    for copy in keeps[:3]:
        copy.wait()


def store_kernel(*refs):
    found, kept, held, sem = refs[:4], refs[4:8], refs[8:12], refs[12]
    loads = [pltpu.make_async_copy(found[i], held[i], sem.at[0, i]) for i in range(4)]
    stores = [pltpu.make_async_copy(held[i], kept[i], sem.at[1, i]) for i in range(4)]
    for copy in loads:
        copy.start()
    for i in range(4):
        loads[i].wait()
        stores[i].start()
    for copy in stores:
        copy.wait()


HBM = pl.BlockSpec(memory_space=pltpu.HBM)
DMA = pltpu.SemaphoreType.DMA


def body(tokens, out_grad, gate_weight, up_weight, down_weight):
    nf, nt = lax.axis_size("fsdp"), lax.axis_size("tp")
    rows, shard = tokens.shape
    deep, width = gate_weight.shape
    assert nf == 8 and nt == 16 and deep == 2 * shard
    factor = 1.0 / math.sqrt(rows * nf)
    tall = 2 * rows
    wide = 2 * width

    shapes = (
        jax.ShapeDtypeStruct((rows, shard), BF16),
        jax.ShapeDtypeStruct((deep, width), F32),
        jax.ShapeDtypeStruct((deep, width), F32),
        jax.ShapeDtypeStruct((width, deep), F32),
    )
    found = tuple(
        pl.pallas_call(
            functools.partial(kernel, factor),
            out_shape=shapes,
            in_specs=[HBM] * 5,
            out_specs=(HBM,) * 4,
            scratch_shapes=[
                pltpu.VMEM((deep, width), F32),
                pltpu.VMEM((deep, width), F32),
                pltpu.VMEM((width, deep), F32),
                pltpu.VMEM((8, 2, 3, rows, shard), BF16),
                pltpu.VMEM((4, 2, deep, width), BF16),
                pltpu.VMEM((4, width, deep), BF16),
                pltpu.VMEM((tall, wide), F32),
                pltpu.VMEM((tall, wide), F32),
                pltpu.VMEM((tall, width), F32),
                pltpu.VMEM((tall, width), F32),
                pltpu.VMEM((tall, wide), F32),
                pltpu.VMEM((tall, width), BF16),
                pltpu.VMEM((8, tall, wide), BF16),
                pltpu.VMEM((8, 2, shard, width), BF16),
                pltpu.VMEM((2, width, shard), F32),
                pltpu.VMEM((2, deep // 2, wide), F32),
                pltpu.VMEM((2, width, shard), BF16),
                pltpu.VMEM((deep, wide), BF16),
                pltpu.VMEM((2, 2, width, shard), BF16),
                pltpu.VMEM((2, deep, wide), BF16),
                pltpu.VMEM((2, width, shard), BF16),
                pltpu.VMEM((2, deep // 2, wide), BF16),
                pltpu.VMEM((2, 2, width, shard), BF16),
                pltpu.VMEM((2, deep, wide), BF16),
                pltpu.VMEM((deep, wide), F32),
                pltpu.VMEM((2, rows, shard), F32),
                pltpu.VMEM((rows, wide), F32),
                pltpu.VMEM((rows, wide), BF16),
                pltpu.VMEM((rows, wide), BF16),
                pltpu.VMEM((rows, shard), BF16),
                DMA(()),
                DMA((4,)),
                DMA((2,)),
                DMA((2, 2, 2)),
                DMA(()),
                DMA((2, 2, 5)),
                DMA(()),
                DMA((4, 2)),
                DMA(()),
                DMA((4,)),
                DMA((2,)),
                DMA((3,)),
                DMA(()),
                DMA((3, 3)),
                DMA(()),
                DMA(()),
                DMA(()),
                DMA((2,)),
                DMA(()),
                DMA(()),
                DMA(()),
                DMA((3,)),
                DMA(()),
                DMA(()),
                DMA(()),
                DMA((PIECES,)),
                DMA(()),
                DMA((3, 2, 2)),
                DMA(()),
                DMA((4, 2)),
                DMA((2,)),
                DMA((2,)),
                DMA((2,)),
                DMA((2,)),
                DMA(()),
                DMA(()),
            ],
            compiler_params=pltpu.CompilerParams(
                collective_id=0, has_side_effects=True, vmem_limit_bytes=VMEM_LIMIT
            ),
            name="block",
        )(tokens, out_grad, gate_weight, up_weight, down_weight)
    )
    return tuple(
        pl.pallas_call(
            store_kernel,
            out_shape=shapes,
            in_specs=[HBM] * 4,
            out_specs=(HBM,) * 4,
            scratch_shapes=[pltpu.VMEM(s.shape, s.dtype) for s in shapes] + [DMA((2, 4))],
            compiler_params=pltpu.CompilerParams(vmem_limit_bytes=VMEM_LIMIT),
            name="store",
        )(*found)
    )


def solution(mesh):
    return jax.shard_map(
        body,
        mesh=mesh,
        in_specs=(
            P("fsdp", "tp"),
            P("fsdp", "tp"),
            P("fsdp", "tp"),
            P("fsdp", "tp"),
            P("tp", "fsdp"),
        ),
        out_specs=(P("fsdp", "tp"), P("fsdp", "tp"), P("fsdp", "tp"), P("tp", "fsdp")),
        check_vma=False,
    )
```

```python
import functools
import math

import jax
import jax.numpy as jnp
from jax import lax
from jax.sharding import PartitionSpec as P
from jax.experimental import pallas as pl
from jax.experimental.pallas import tpu as pltpu

MESH = pl.DeviceIdType.MESH
F32 = jnp.float32
BF16 = jnp.bfloat16
VMEM_LIMIT = 60 * 1024 * 1024
XFIRST = 32
PIECES = 8
DIRECT = 384
ROWS = ((0,), (0,))
COLS = ((1,), (1,))


def kernel(
    factor,
    tokens,
    grads,
    gate_weight,
    up_weight,
    down_weight,
    result,
    gate_out,
    up_out,
    down_out,
    gate_own,
    up_own,
    down_own,
    xg,
    wf,
    df,
    sa,
    zla,
    sb,
    zlb,
    acts,
    hidden,
    dg,
    tw,
    dpart,
    gpart,
    dtwo,
    gtwo,
    done,
    gone,
    dmid,
    gmid,
    dland,
    gland,
    gown,
    total,
    near,
    slim,
    slim_near,
    rounded,
    load,
    keep,
    z_send,
    z_recv,
    x_send,
    x_recv,
    p_send,
    p_recv,
    v_send,
    v_recv,
    zx_send,
    zx_recv,
    y_send,
    y_recv,
    a_send,
    a_recv,
    b_send,
    b_recv,
    t_send,
    t_recv,
    u_send,
    u_recv,
    g_send,
    g_recv,
    f_send,
    f_recv,
    dx_send,
    dx_recv,
    dp_send,
    dp_recv,
    two_send,
    two_recv,
    one_send,
    one_recv,
    r_send,
    r_recv,
):
    f, t = lax.axis_index("fsdp"), lax.axis_index("tp")
    h, y = lax.div(f, 4), lax.rem(f, 4)
    l, x, k = lax.div(t, 8), lax.rem(lax.div(t, 2), 4), lax.rem(t, 2)
    outer = h == l
    inner = h != l
    rows, shard = tokens.shape
    deep, width = gate_weight.shape
    part = rows // 2
    zparts = ((rows - XFIRST) // 2, part)
    first = rows - XFIRST
    xpart = XFIRST // 2
    odd = (h - l) * (h - l)
    home = h * (1 - odd) + 2 * odd
    wide = 2 * width

    def at(xx, yy, hh, ll, kk):
        return (hh * 4 + yy, ll * 8 + xx * 2 + kk)

    xs = (lax.rem(x + 3, 4), lax.rem(x + 1, 4), lax.rem(x + 2, 4))
    ys = (lax.rem(y + 3, 4), lax.rem(y + 1, 4), lax.rem(y + 2, 4))
    right, left = at(xs[1], y, h, l, k), at(xs[0], y, h, l, k)
    north, south = at(x, ys[1], h, l, k), at(x, ys[0], h, l, k)
    mate = at(x, y, h, l, 1 - k)
    flip = at(x, y, h, 1 - l, k)
    across = at(x, y, 1 - h, 1 - l, k)
    opposite = at(x, y, 1 - h, l, k)
    me = 2 * x + k

    def remote(src, dst, send, recv, device):
        return pltpu.make_async_remote_copy(
            src_ref=src,
            dst_ref=dst,
            send_sem=send,
            recv_sem=recv,
            device_id=device,
            device_id_type=MESH,
        )

    copies = [
        pltpu.make_async_copy(ref, spot, load)
        for ref, spot in (
            (tokens, xg.at[k * 4 + x, 0, home]),
            (gate_weight, wf.at[y, 0]),
            (up_weight, wf.at[y, 1]),
            (grads, xg.at[k * 4 + x, 1, home]),
            (down_weight, df.at[y]),
        )
    ]
    for copy in copies:
        copy.start()

    barrier = pltpu.get_barrier_semaphore()
    for j in range(1, 16):
        pl.semaphore_signal(
            barrier, inc=1, device_id=(f, lax.rem(t + j, 16)), device_id_type=MESH
        )
    for peer in (north, south, opposite, across):
        pl.semaphore_signal(barrier, inc=1, device_id=peer, device_id_type=MESH)
    pl.semaphore_wait(barrier, 19)

    all_in = xg.at[pl.ds(0, 5), 0, 0]
    pltpu.make_async_copy(all_in, all_in, load).wait()

    def w_spot(o, w, q):
        if w == 2:
            return df.at[o, pl.ds(q * (width // 2), width // 2)]
        return wf.at[o, w, pl.ds(q * (deep // 2), deep // 2)]

    def w_out(way, w, q):
        return remote(
            w_spot(y, w, q),
            w_spot(y, w, q),
            y_send,
            y_recv.at[w, q if way == q else 2],
            (north, south)[way],
        )

    def w_on(w, q):
        here = w_spot(ys[q], w, q)
        return remote(here, here, y_send, y_recv.at[w, 2], (north, south)[q])

    def w_wait(w, e, here):
        remote(here, here, y_send, y_recv.at[w, e], north).wait_recv()

    def w_start(w):
        for way, q in ((0, 0), (1, 1), (0, 1), (1, 0)):
            w_out(way, w, q).start()

    def w_forward(w):
        for q in range(2):
            w_wait(w, q, w_spot(ys[q], w, q))
            w_on(w, q).start()

    def w_rest(w):
        w_wait(w, 2, df.at[pl.ds(0, 2)] if w == 2 else wf.at[pl.ds(0, 2), w])

    slot = (h, 1 - h)

    def x_own(m, q):
        return xg.at[k * 4 + x, m, home, pl.ds(q * zparts[m], zparts[m])]

    def x_spot(p, o, j, m, q):
        return xg.at[p * 4 + o, m, slot[j], pl.ds(q * zparts[m], zparts[m])]

    def z_out(m, q, device, j):
        spot = xg.at[k * 4 + x, m, h, pl.ds(q * zparts[m], zparts[m])]
        return remote(x_own(m, q), spot, z_send.at[0], z_recv.at[j, m, q], device)

    def z_on(m, q):
        here = x_spot(k, x, 1, m, q)
        return remote(here, here, z_send.at[1], z_recv.at[1, m, q], flip)

    def z_in(j, m, q):
        here = x_spot(k, x, j, m, q)
        return remote(here, here, z_send.at[0], z_recv.at[j, m, q], flip)

    def x_out(way, src, j, m, q):
        return remote(
            src,
            x_spot(k, x, j, m, q),
            x_send,
            x_recv.at[m, q, 2 * way + j],
            (right, left)[way],
        )

    def x_on(j, m, q):
        here = x_spot(k, xs[q], j, m, q)
        return remote(
            here, here, x_send, x_recv.at[m, q, 4], (right, left)[q]
        )

    def x_wait(m, q, e, here):
        remote(here, here, x_send, x_recv.at[m, q, e], right).wait_recv()

    places = (*xs, x)

    def p_out(d, src, j, m, q):
        return remote(
            src,
            x_spot(k, places[d], j, m, q),
            p_send,
            p_recv.at[d, m],
            mate,
        )

    def spread(src, j, m, q):
        for way in (0, 1) if q == 0 else (1, 0):
            x_out(way, src, j, m, q).start()
        p_out(3, src, j, m, q).start()

    def passed(d, j, m, q):
        x_wait(m, q, 2 * d + j, x_spot(k, xs[d], j, m, q))
        if d == q:
            x_on(j, m, q).start()
        p_out(d, x_spot(k, places[d], j, m, q), j, m, q).start()

    def x_rest(m):
        for q in range(2):
            here = xg.at[k * 4 + xs[2], m, pl.ds(0, 2), pl.ds(q * zparts[m], zparts[m])]
            x_wait(m, q, 4, here)
            for j in range(2):
                p_out(2, x_spot(k, xs[2], j, m, q), j, m, q).start()

    def z_forward(m, q):
        @pl.when(inner)
        def _():
            z_in(1, m, q).wait_recv()
            z_on(m, q).start()

    def z_near(m, q):
        @pl.when(inner)
        def _():
            z_in(0, m, q).wait_recv()

        spread(x_spot(k, x, 0, m, q), 0, m, q)

    def z_far(m, q):
        @pl.when(outer)
        def _():
            z_in(1, m, q).wait_recv()

        spread(x_spot(k, x, 1, m, q), 1, m, q)

    def z_near_inner(m, q):
        @pl.when(inner)
        def _():
            z_in(0, m, q).wait_recv()
            spread(x_spot(k, x, 0, m, q), 0, m, q)

    fourths = (shard // 4, (shard - DIRECT) // 4)
    bases = (0, DIRECT)

    def t_copy(u, w):
        return remote(
            wf.at[
                lax.div(u, 2),
                w,
                pl.ds(lax.rem(u, 2) * shard + bases[w] + y * fourths[w], fourths[w]),
            ],
            tw.at[me, w, pl.ds(bases[w] + y * fourths[w], fourths[w])],
            t_send,
            t_recv,
            (f, l * 8 + u),
        )

    def t_out(w, j):
        return t_copy(lax.rem(me + j, 8), w)

    def t_all():
        here = tw.at[pl.ds(0, 7), 0, pl.ds(0, fourths[0] + fourths[1])]
        return remote(here, here, t_send, t_recv, mate)

    def g_out(j):
        u = lax.rem(me + j, 8)
        return remote(
            wf.at[lax.div(u, 2), 1, pl.ds(lax.rem(u, 2) * shard, DIRECT)],
            tw.at[me, 1, pl.ds(0, DIRECT)],
            g_send,
            g_recv,
            (f, l * 8 + u),
        )

    def g_all():
        here = tw.at[pl.ds(0, 7), 1, pl.ds(0, DIRECT)]
        return remote(here, here, g_send, g_recv, mate)

    def u_spot(o, w, q):
        return tw.at[pl.ds(q * 4, 4), w, pl.ds(bases[w] + o * fourths[w], fourths[w])]

    def u_out(way, w, q):
        here = u_spot(y, w, q)
        return remote(
            here, here, u_send, u_recv.at[q if way == q else 2], (north, south)[way]
        )

    def u_on(w, q):
        here = u_spot(ys[q], w, q)
        return remote(here, here, u_send, u_recv.at[2], (north, south)[q])

    def u_wait(e, here):
        remote(here, here, u_send, u_recv.at[e], north).wait_recv()

    def v_spot(o, q):
        return xg.at[k * 4 + o, 0, home, pl.ds(first + q * xpart, xpart)]

    def v_out(way, q):
        here = v_spot(x, q)
        return remote(
            here, here, v_send, v_recv.at[q if way == q else 2], (right, left)[way]
        )

    def v_on(q):
        here = v_spot(xs[q], q)
        return remote(here, here, v_send, v_recv.at[3], (right, left)[q])

    def v_wait(e, here):
        remote(here, here, v_send, v_recv.at[e], right).wait_recv()

    def zx_spot(p, d, at_s):
        return xg.at[p * 4 + places[d], 0, at_s, pl.ds(first, XFIRST)]

    def zx_out(d, device, j):
        return remote(
            zx_spot(k, d, home),
            zx_spot(k, d, h),
            zx_send.at[0],
            zx_recv.at[j + (j * d == 2)],
            device,
        )

    def zx_on(d):
        here = zx_spot(k, d, 1 - h)
        return remote(here, here, zx_send.at[1], zx_recv.at[1 + (d == 2)], flip)

    def zx_wait(e, count):
        here = xg.at[pl.ds(0, count), 0, 0, pl.ds(first, XFIRST)]
        remote(here, here, zx_send.at[0], zx_recv.at[e], flip).wait_recv()

    def px_out(d, j):
        here = zx_spot(k, d, slot[j])
        return remote(here, here, p_send, p_recv.at[d, 0], mate)

    def v_start():
        for q in range(2):
            for way in (0, 1) if q == 0 else (1, 0):
                v_out(way, q).start()

    def v_near():
        for q in range(2):
            v_wait(q, v_spot(xs[q], q))
            v_on(q).start()
        v_wait(2, zx_spot(k, 0, home))

    def v_far():
        v_wait(3, zx_spot(k, 2, home))

    def zx_start(ds):
        for d in ds:

            @pl.when(outer)
            def _(d=d):
                zx_out(d, flip, 0).start()
                px_out(d, 0).start()

            @pl.when(inner)
            def _(d=d):
                zx_out(d, across, 1).start()

    def zx_pass(e, ds):
        @pl.when(inner)
        def _():
            zx_wait(e, len(ds))
            for d in ds:
                zx_on(d).start()

    def zx_take():
        @pl.when(inner)
        def _():
            zx_wait(0, 4)
            for d in range(4):
                px_out(d, 0).start()

        @pl.when(outer)
        def _():
            zx_wait(1, 3)
            zx_wait(2, 1)

        for d in range(4):
            px_out(d, 1).start()

    def z_start(m):
        @pl.when(outer)
        def _():
            for q in range(2):
                z_out(m, q, flip, 0).start()

        @pl.when(inner)
        def _():
            for q in range(2):
                z_out(m, q, across, 1).start()

    v_start()
    z_start(0)

    @pl.when(outer)
    def _():
        for q in range(2):
            spread(x_own(0, q), 0, 0, q)

    zx_start((3,))
    w_start(0)
    w_start(1)

    v_near()
    zx_start((0, 1))
    z_forward(0, 0)
    z_near_inner(0, 0)
    z_far(0, 0)
    v_far()
    zx_start((2,))
    z_start(1)
    z_forward(0, 1)
    z_near_inner(0, 1)
    z_far(0, 1)
    w_forward(0)
    for j in range(2):
        passed(0, j, 0, 0)
        passed(1, j, 0, 0)
    w_forward(1)
    w_start(2)
    for j in range(2):
        passed(1, j, 0, 1)
        passed(0, j, 0, 1)
    z_forward(1, 0)
    zx_pass(1, (3, 0, 1))
    z_forward(1, 1)
    zx_pass(2, (2,))
    w_rest(0)
    w_rest(1)

    @pl.loop(1, 8)
    def _(j):
        for w in range(2):
            t_out(w, j).start()

    z_near(1, 0)
    z_near(1, 1)
    z_far(1, 0)
    z_far(1, 1)
    w_forward(2)
    zx_take()
    tall = 2 * rows

    def block(m, o):
        return jnp.concatenate(
            [xg[p * 4 + o, m, :2].reshape(tall, shard) for p in range(2)], axis=1
        )

    def pair_in(d, m):
        here = xg.at[(1 - k) * 4 + places[d], m, pl.ds(0, 2)]
        remote(here, here, p_send, p_recv.at[d, m], mate).wait_recv()

    def gate_up(d):
        o = places[d]
        weights = jnp.concatenate([wf[o, 0], wf[o, 1]], axis=1)
        term = jnp.dot(block(0, o), weights, preferred_element_type=F32)
        sa[...] = term if d == 3 else sa[...] + term

    for d in (3, 0):
        pair_in(d, 0)
        gate_up(d)
    x_rest(0)
    pair_in(1, 0)
    gate_up(1)
    pair_in(2, 0)
    gate_up(2)
    turn = (1 - l, l)

    def swap(src, dst, send, recvs):
        def copy(c):
            at_c = pl.ds(turn[c] * rows, rows)
            return remote(src.at[at_c], dst.at[at_c], send, recvs[c], opposite)

        return copy

    a_swap = swap(sa, zla, a_send, (a_recv, a_recv))
    b_swap = swap(sb, zlb, b_send, (b_recv.at[0], b_recv.at[1]))
    a_all = remote(sa, zla, a_send, a_recv, opposite)
    b_all = remote(sb, zlb, b_send, b_recv.at[0], opposite)

    a_swap(0).start()
    for w in range(2):
        mine_w = pl.ds(bases[w] + y * fourths[w], fourths[w])
        tw[me, w, mine_w] = wf[x, w, pl.ds(k * shard + bases[w] + y * fourths[w], fourths[w])]
    tw[me, 1, :DIRECT] = wf[x, 1, pl.ds(k * shard, DIRECT)]
    a_swap(1).start()
    t_all().wait_recv()

    for w in range(2):
        for way, q in ((0, 0), (1, 1), (0, 1), (1, 0)):
            u_out(way, w, q).start()
    for j in range(2):
        passed(0, j, 1, 0)
        passed(1, j, 1, 0)
    for j in range(2):
        passed(1, j, 1, 1)
        passed(0, j, 1, 1)

    def grad_in(d):
        o = places[d]
        term = lax.dot_general(
            block(1, o), df[o], (COLS, ((), ())), preferred_element_type=F32
        )
        sb[...] = term if d == 3 else sb[...] + term

    w_rest(2)
    for d in (3, 0, 1):
        pair_in(d, 1)
        grad_in(d)
    def down_half(o, p):
        return lax.dot_general(
            hidden[...],
            xg[p * 4 + o, 1, :2].reshape(tall, shard),
            (ROWS, ((), ())),
            preferred_element_type=F32,
        )

    def gate_part(o):
        return lax.dot_general(
            block(0, o), dg[me], (ROWS, ((), ())), preferred_element_type=F32
        )

    twos, mids, parts, ones, lands = (
        (dtwo, gtwo),
        (dmid, gmid),
        (dpart, gpart),
        (done, gone),
        (dland, gland),
    )

    def halves(i, q):
        return q if i == 0 else pl.ds(q * shard, shard)

    def beside(way):
        return lax.rem(y + 1 + 2 * way, 4)

    def two_out(i, q):
        return remote(
            twos[i].at[halves(i, q)],
            mids[i].at[q],
            two_send.at[i],
            two_recv.at[i],
            at(x, beside(q), h, l, k),
        )

    def one_out(i, way, q):
        return remote(
            ones[i].at[way, halves(i, q)],
            lands[i].at[way, halves(i, q)],
            one_send.at[i],
            one_recv.at[i],
            at(x, beside(way), h, l, k),
        )

    def gate_half(o, p):
        return lax.dot_general(
            xg[p * 4 + o, 0, :2].reshape(tall, shard),
            dg[me],
            (ROWS, ((), ())),
            preferred_element_type=F32,
        )

    def gate_rows(o, p, e):
        return lax.dot_general(
            xg[p * 4 + o, 0, turn[e]],
            dg[me, pl.ds(turn[e] * rows, rows)],
            (ROWS, ((), ())),
            preferred_element_type=F32,
        )

    def one_merge(i):
        remote(mids[i], mids[i], two_send.at[i], two_recv.at[i], north).wait_recv()
        for way in range(2):
            ones[i][way, halves(i, way)] = (
                parts[i][way] + mids[i][way].astype(F32)
            ).astype(BF16)

    def finals(i):
        remote(ones[i], lands[i], one_send.at[i], one_recv.at[i], north).wait_recv()
        return lands[i][0].astype(F32) + lands[i][1].astype(F32)

    def grad_last(c):
        at_s = pl.ds(turn[c] * rows, rows)
        last = jnp.concatenate([xg[p * 4 + xs[2], 1, turn[c]] for p in range(2)], axis=1)
        sb[at_s] += lax.dot_general(
            last, df[xs[2]], (COLS, ((), ())), preferred_element_type=F32
        )

    for q in range(2):
        u_wait(q, tw.at[pl.ds(q * 4, 4), 0, pl.ds(0, fourths[0] + fourths[1])])
        for w in range(2):
            u_on(w, q).start()
    x_rest(1)
    @pl.loop(1, 8)
    def _(j):
        g_out(j).start()

    a_all.wait_recv()
    sums = sa[...] + zla[...]
    gate, up = sums[:, :width], sums[:, width:]
    squashed = jax.nn.sigmoid(gate)
    activated = gate * squashed
    slope = squashed * (1.0 + gate * (1.0 - squashed))
    acts[:, :width] = up * slope
    acts[:, width:] = activated
    hidden[...] = (activated * up).astype(BF16)

    dtwo[k] = down_half(ys[2], k).astype(BF16)
    done[1 - k, k] = down_half(beside(1 - k), k).astype(BF16)
    two_out(0, k).start()
    pair_in(2, 1)
    grad_last(0)
    dtwo[1 - k] = down_half(ys[2], 1 - k).astype(BF16)
    b_swap(0).start()
    grad_last(1)
    two_out(0, 1 - k).start()
    one_out(0, 1 - k, k).start()
    done[k, 1 - k] = down_half(beside(k), 1 - k).astype(BF16)
    b_swap(1).start()
    dpart[k] = down_half(beside(k), k)
    one_out(0, k, 1 - k).start()
    dpart[1 - k] = down_half(beside(1 - k), 1 - k)
    one_merge(0)
    def d_spot(c, o, e, q):
        return dg.at[o * 2 + c, pl.ds(turn[e] * rows + q * part, part)]

    def dx_out(way, e, q):
        here = d_spot(k, x, e, q)
        return remote(
            here, here, dx_send, dx_recv.at[way, e, q], (right, left)[way]
        )

    def dx_on(e, q):
        here = d_spot(k, xs[q], e, q)
        return remote(here, here, dx_send, dx_recv.at[2, e, 0], (right, left)[q])

    def dx_in(d, e, q):
        here = d_spot(k, xs[d], e, q)
        return remote(here, here, dx_send, dx_recv.at[d, e, q], right)

    def dp_out(d, e, q):
        here = d_spot(k, places[d], e, q)
        return remote(here, here, dp_send, dp_recv.at[d, e], mate)

    def d_half(c, d, e):
        return dg.at[places[d] * 2 + c, pl.ds(turn[e] * rows, rows)]

    def d_far(e):
        here = d_half(k, 2, e)
        remote(here, here, dx_send, dx_recv.at[2, e, 0], right).wait_recv()
        for q in range(2):
            dp_out(2, e, q).start()

    def d_start(e):
        for q in range(2):
            for way in (0, 1) if q == 0 else (1, 0):
                dx_out(way, e, q).start()
            dp_out(3, e, q).start()

    def d_passed(d, e, q):
        dx_in(d, e, q).wait_recv()
        if d == q:
            dx_on(e, q).start()
        dp_out(d, e, q).start()

    def d_near(e):
        for q in range(2):
            d_passed(q, e, q)
        for q in range(2):
            d_passed(1 - q, e, q)

    def gather(d, e):
        base = places[d] * 2
        at_s = pl.ds(turn[e] * rows, rows)
        left_side = jnp.concatenate([dg[base, at_s], dg[base + 1, at_s]], axis=1)
        right_side = jnp.concatenate(
            [tw[base, 0], tw[base, 1], tw[base + 1, 0], tw[base + 1, 1]], axis=1
        )
        term = lax.dot_general(
            left_side, right_side, (COLS, ((), ())), preferred_element_type=F32
        )
        total[e] = term if d == 3 else total[e] + term

    def gathers(e, ds):
        for d in ds:
            here = d_half(1 - k, d, e)
            remote(here, here, dp_send, dp_recv.at[d, e], mate).wait_recv()
            gather(d, e)

    piece = rows // PIECES

    def f_out(c):
        at_c = pl.ds(c * piece, piece)
        return (
            remote(total.at[0, at_c, pl.ds(0, wide)], near.at[at_c], f_send, f_recv.at[c], flip),
            remote(slim.at[at_c], slim_near.at[at_c], f_send, f_recv.at[c], flip),
        )

    def f_start(cs):
        for c in cs:
            for copy in f_out(c):
                copy.start()

    def f_wait(c):
        here = near.at[pl.ds(0, 3 * piece // 2)]
        remote(here, here, f_send, f_recv.at[c], flip).wait_recv()

    def r_out(c):
        at_c = pl.ds(c * piece, piece)
        return remote(rounded.at[at_c], result.at[at_c], r_send, r_recv, across)

    def delta(e):
        b_swap(e).wait_recv()
        at_s = pl.ds(turn[e] * rows, rows)
        hidden_grad = sb[at_s] + zlb[at_s]
        dg[me, at_s, :width] = (hidden_grad * acts[at_s, :width]).astype(BF16)
        dg[me, at_s, width:] = (hidden_grad * acts[at_s, width:]).astype(BF16)

    delta(0)
    for way in range(2):
        one_out(0, way, way).start()
    down_own[:, :shard] = down_half(y, 0)
    d_start(0)
    down_own[:, shard:] = down_half(y, 1)
    gown[...] = jnp.concatenate([gate_rows(ys[2], p, 0) for p in range(2)], axis=0)
    delta(1)
    for p in range(2):
        gtwo[halves(1, p)] = (gown[halves(1, p)] + gate_rows(ys[2], p, 1)).astype(BF16)
    two_out(1, 0).start()
    gone[0, halves(1, 1)] = gate_half(beside(0), 1).astype(BF16)
    two_out(1, 1).start()
    gone[1, halves(1, 0)] = gate_half(beside(1), 0).astype(BF16)
    one_out(1, 0, 1).start()
    gpart[0] = gate_half(beside(0), 0)
    one_out(1, 1, 0).start()
    gpart[1] = gate_half(beside(1), 1)
    d_near(0)
    d_start(1)
    gown[...] = gate_part(y)
    u_wait(2, tw.at[:, :, pl.ds(0, fourths[0] + fourths[1])])
    g_all().wait_recv()

    gathers(0, (3, 0, 1))
    d_far(0)
    gathers(0, (2,))
    slim[...] = total[0, :, wide:].astype(BF16)
    f_start(range(PIECES // 2))
    d_near(1)
    f_start(range(PIECES // 2, PIECES))
    one_merge(1)
    gathers(1, (3,))
    for way in range(2):
        one_out(1, way, way).start()
    gathers(1, (0, 1))
    d_far(1)
    gathers(1, (2,))
    keeps = [
        pltpu.make_async_copy(src, dst, keep.at[i])
        for i, (src, dst) in enumerate(
            ((down_own, down_out), (gate_own, gate_out), (up_own, up_out), (rounded, result))
        )
    ]
    for c in range(PIECES):
        f_wait(c)
        at_c = pl.ds(c * piece, piece)
        rounded[at_c, :wide] = (total[1, at_c, :wide] + near[at_c]).astype(BF16)
        rounded[at_c, wide:] = (total[1, at_c, wide:] + slim_near[at_c].astype(F32)).astype(BF16)

        if c:

            @pl.when(inner)
            def _(c=c):
                r_out(c - 1).start()

    both = finals(0)
    for p in range(2):
        at_p = slice(p * shard, (p + 1) * shard)
        down_own[:, at_p] = factor * (down_own[:, at_p] + both[p])
    @pl.when(inner)
    def _():
        r_out(PIECES - 1).start()

    @pl.when(outer)
    def _():
        keeps[3].start()

    keeps[0].start()
    last = finals(1)
    gate_own[...] = factor * (gown[:, :width] + last[:, :width])
    up_own[...] = factor * (gown[:, width:] + last[:, width:])
    for copy in keeps[1:3]:
        copy.start()

    sent = [
        (xg.at[0, :, 0, pl.ds(0, 240)], z_send.at[0]),
        (xg.at[pl.ds(0, 4), 0, 0, pl.ds(0, XFIRST)], zx_send.at[0]),
        (xg.at[pl.ds(0, 3), 0, 0, pl.ds(0, XFIRST)], v_send),
        (xg.at[pl.ds(0, 4), 0, :, pl.ds(0, 240)], x_send),
        (xg.at[:, :, 0], p_send),
        (xg.at[pl.ds(0, 3), 0], y_send),
        (tw.at[:, :, pl.ds(0, 3 * (fourths[0] + fourths[1]) // 2)], u_send),
        (dg.at[pl.ds(0, 3)], dx_send),
        (dg.at[pl.ds(0, 4)], dp_send),
        (total.at[0, pl.ds(0, 3 * rows // 4)], f_send),
        (dtwo, two_send.at[0]),
        (gtwo, two_send.at[1]),
        (done, one_send.at[0]),
        (gone, one_send.at[1]),
    ]
    for here, sem in sent:
        remote(here, here, sem, load, mate).wait_send()
    for copy in (a_all, b_all, t_all(), g_all()):
        copy.wait_send()

    @pl.when(inner)
    def _():
        for here, sem in (
            (xg.at[0, :, 0, pl.ds(0, 240)], z_send.at[1]),
            (xg.at[pl.ds(0, 4), 0, 0, pl.ds(0, XFIRST)], zx_send.at[1]),
        ):
            remote(here, here, sem, load, mate).wait_send()
        remote(rounded, result, r_send, r_recv, across).wait()

    @pl.when(outer)
    def _():
        keeps[3].wait()

    for copy in keeps[:3]:
        copy.wait()


def store_kernel(*refs):
    found, kept, held, sem = refs[:4], refs[4:8], refs[8:12], refs[12]
    loads = [pltpu.make_async_copy(found[i], held[i], sem.at[0, i]) for i in range(4)]
    stores = [pltpu.make_async_copy(held[i], kept[i], sem.at[1, i]) for i in range(4)]
    for copy in loads:
        copy.start()
    for i in range(4):
        loads[i].wait()
        stores[i].start()
    for copy in stores:
        copy.wait()


HBM = pl.BlockSpec(memory_space=pltpu.HBM)
DMA = pltpu.SemaphoreType.DMA


def body(tokens, out_grad, gate_weight, up_weight, down_weight):
    nf, nt = lax.axis_size("fsdp"), lax.axis_size("tp")
    rows, shard = tokens.shape
    deep, width = gate_weight.shape
    assert nf == 8 and nt == 16 and deep == 2 * shard
    factor = 1.0 / math.sqrt(rows * nf)
    tall = 2 * rows
    wide = 2 * width

    shapes = (
        jax.ShapeDtypeStruct((rows, shard), BF16),
        jax.ShapeDtypeStruct((deep, width), F32),
        jax.ShapeDtypeStruct((deep, width), F32),
        jax.ShapeDtypeStruct((width, deep), F32),
    )
    found = tuple(
        pl.pallas_call(
            functools.partial(kernel, factor),
            out_shape=shapes,
            in_specs=[HBM] * 5,
            out_specs=(HBM,) * 4,
            scratch_shapes=[
                pltpu.VMEM((deep, width), F32),
                pltpu.VMEM((deep, width), F32),
                pltpu.VMEM((width, deep), F32),
                pltpu.VMEM((8, 2, 3, rows, shard), BF16),
                pltpu.VMEM((4, 2, deep, width), BF16),
                pltpu.VMEM((4, width, deep), BF16),
                pltpu.VMEM((tall, wide), F32),
                pltpu.VMEM((tall, wide), F32),
                pltpu.VMEM((tall, width), F32),
                pltpu.VMEM((tall, width), F32),
                pltpu.VMEM((tall, wide), F32),
                pltpu.VMEM((tall, width), BF16),
                pltpu.VMEM((8, tall, wide), BF16),
                pltpu.VMEM((8, 2, shard, width), BF16),
                pltpu.VMEM((2, width, shard), F32),
                pltpu.VMEM((2, deep // 2, wide), F32),
                pltpu.VMEM((2, width, shard), BF16),
                pltpu.VMEM((deep, wide), BF16),
                pltpu.VMEM((2, 2, width, shard), BF16),
                pltpu.VMEM((2, deep, wide), BF16),
                pltpu.VMEM((2, width, shard), BF16),
                pltpu.VMEM((2, deep // 2, wide), BF16),
                pltpu.VMEM((2, 2, width, shard), BF16),
                pltpu.VMEM((2, deep, wide), BF16),
                pltpu.VMEM((deep, wide), F32),
                pltpu.VMEM((2, rows, shard), F32),
                pltpu.VMEM((rows, wide), F32),
                pltpu.VMEM((rows, wide), BF16),
                pltpu.VMEM((rows, wide), BF16),
                pltpu.VMEM((rows, shard), BF16),
                DMA(()),
                DMA((4,)),
                DMA((2,)),
                DMA((2, 2, 2)),
                DMA(()),
                DMA((2, 2, 5)),
                DMA(()),
                DMA((4, 2)),
                DMA(()),
                DMA((4,)),
                DMA((2,)),
                DMA((3,)),
                DMA(()),
                DMA((3, 3)),
                DMA(()),
                DMA(()),
                DMA(()),
                DMA((2,)),
                DMA(()),
                DMA(()),
                DMA(()),
                DMA((3,)),
                DMA(()),
                DMA(()),
                DMA(()),
                DMA((PIECES,)),
                DMA(()),
                DMA((3, 2, 2)),
                DMA(()),
                DMA((4, 2)),
                DMA((2,)),
                DMA((2,)),
                DMA((2,)),
                DMA((2,)),
                DMA(()),
                DMA(()),
            ],
            compiler_params=pltpu.CompilerParams(
                collective_id=0, has_side_effects=True, vmem_limit_bytes=VMEM_LIMIT
            ),
            name="block",
        )(tokens, out_grad, gate_weight, up_weight, down_weight)
    )
    return tuple(
        pl.pallas_call(
            store_kernel,
            out_shape=shapes,
            in_specs=[HBM] * 4,
            out_specs=(HBM,) * 4,
            scratch_shapes=[pltpu.VMEM(s.shape, s.dtype) for s in shapes] + [DMA((2, 4))],
            compiler_params=pltpu.CompilerParams(vmem_limit_bytes=VMEM_LIMIT),
            name="store",
        )(*found)
    )


def solution(mesh):
    return jax.shard_map(
        body,
        mesh=mesh,
        in_specs=(
            P("fsdp", "tp"),
            P("fsdp", "tp"),
            P("fsdp", "tp"),
            P("fsdp", "tp"),
            P("tp", "fsdp"),
        ),
        out_specs=(P("fsdp", "tp"), P("fsdp", "tp"), P("fsdp", "tp"), P("tp", "fsdp")),
        check_vma=False,
    )
```
